32 devices in a mesh: dp: 8 (over y, x, core), tensor: 4 (over z).
Axes of the slice: x: 2, y: 2, z: 4, core: 2. Of those that a mesh axis runs over, the one named last changes fastest.
Arguments:
- hidden_in: bfloat16 [8192, 2048], P(('dp', 'tensor')), may hold values from -6 to 6
- segments: int32 [8, 1024], P('dp'), may hold values from 0 to 3, never falling along the last dimension, each value on 1 to 512 neighbouring positions
- ln_gain: bfloat16 [2048], P('dp'), may hold values from 0.099609375 to 1.8984375
- ln_bias: bfloat16 [2048], P('dp'), may hold values from -3 to 3
- qkv_weight: bfloat16 [2048, 3, 2048], P('dp', None, 'tensor'), may hold values from -1 to 1
- qkv_bias: bfloat16 [3, 2048], P(None, 'tensor'), may hold values from -3 to 3
- dense_weight: bfloat16 [2048, 2048], P('tensor', 'dp'), may hold values from -0.5 to 0.5
- dense_bias: bfloat16 [2048], P('dp'), may hold values from -3 to 3
- fc1_weight: bfloat16 [2048, 8192], P('dp', 'tensor'), may hold values from -0.125 to 0.125
- fc1_bias: bfloat16 [8192], P('tensor'), may hold values from -3 to 3
- fc2_weight: bfloat16 [8192, 2048], P('tensor', 'dp'), may hold values from -0.0625 to 0.0625
- fc2_bias: bfloat16 [2048], P('dp'), may hold values from -3 to 3
- cotangent: bfloat16 [8192, 2048], P(('dp', 'tensor')), may hold values from -6 to 6
Outputs:
- out: bfloat16 [8192, 2048], P(('dp', 'tensor'))
- hidden_grad: bfloat16 [8192, 2048], P(('dp', 'tensor'))
- ln_gain_grad: float32 [2048], P(('dp', 'tensor'))
- ln_bias_grad: float32 [2048], P(('dp', 'tensor'))
- qkv_weight_grad: float32 [2048, 3, 2048], P('dp', None, 'tensor')
- qkv_bias_grad: float32 [3, 2048], P(None, 'tensor')
- dense_weight_grad: float32 [2048, 2048], P('tensor', 'dp')
- dense_bias_grad: float32 [2048], P(('dp', 'tensor'))
- fc1_weight_grad: float32 [2048, 8192], P('dp', 'tensor')
- fc1_bias_grad: float32 [8192], P('tensor')
- fc2_weight_grad: float32 [8192, 2048], P('tensor', 'dp')
- fc2_bias_grad: float32 [2048], P(('dp', 'tensor'))
The draws below stay inside these ranges and needn't reach their ends.
Inputs may be any that keep to these rules, and one draw needn't show every extreme that they name: `segments`: segment numbers never fall along a sequence; each of the 4 documents of a sequence has 1 to 512 tokens, one exactly 512.
All inputs are finite; a program needn't handle non-finite values.
Results may differ from the reference program's by a relative error of at most 0.011.
Values may be sent and summed in bfloat16 or wider, within the bound.
A program may use at most 192 MiB of HBM per device.

```python
import math
import jax
import jax.numpy as jnp
import numpy as np
from jax import lax

D = 2048
HEADS = 32
HD = 64
ROT = 32
FF = 8192
LENGTH = 1024
SEGS = 4
ROWS = 8
TOKENS = 8192


def draw_qkv_weight(key, part):
    base = jax.random.truncated_normal(key, -6.0, 6.0, (D, 3, D), jnp.float32) * D ** (-0.5)
    return jnp.clip(base, -1.0, 1.0).astype(jnp.bfloat16)


def steps_of(stream_key, shape, split, low, largest):
    factor_of, own = 1.0, jax.random.fold_in(stream_key, 6)
    for axis_at, shards_of in split:
        steps = jnp.exp(jax.random.uniform(jax.random.fold_in(own, axis_at), (shards_of,), jnp.float32, low / len(split), largest / len(split)))
        factor_of = factor_of * jnp.repeat(steps, shape[axis_at] // shards_of).reshape([-1 if axis == axis_at else 1 for axis in range(len(shape))])
    return factor_of


def profile(number_of, total, limit, skew):
    weights = [(1 << 20) // math.isqrt(standing ** skew) + 1 for standing in range(2, number_of + 1)]
    spare, holding = total - limit - (number_of - 1), [1] * (number_of - 1)
    while spare > 0:
        free = [i for i in range(number_of - 1) if holding[i] < limit]
        mass, budget = sum([weights[i] for i in free]), spare
        for i in free:
            more = min(limit - holding[i], max(1, budget * weights[i] // mass), spare)
            holding[i] = holding[i] + more
            spare = spare - more
    return np.array([limit] + holding)


def ragged_sizes(key, count, total, bound, slope):
    if count == 2:
        one = jax.random.randint(key, (), max(1, total - bound), min(bound, total - 1) + 1)
        return jnp.stack([one, total - one])
    lengths = jnp.asarray(profile(count, total, bound, slope), jnp.int32)
    couples = (count - 1) // 2
    donor, receiver = lengths[1:1 + 2 * couples:2], lengths[2:2 + 2 * couples:2]
    room = jnp.minimum(donor - 1, bound - receiver)
    passed = jax.random.randint(jax.random.fold_in(key, 1), (couples,), 0, 1 << 20) % (room + 1)
    lengths = lengths.at[1:1 + 2 * couples:2].set(donor - passed).at[2:2 + 2 * couples:2].set(receiver + passed)
    return lengths[jax.random.permutation(jax.random.fold_in(key, 2), count)]


def noise(own_key, extent, scale, limit, cuts=(), held_as=jnp.bfloat16):
    values = scale * jax.random.normal(own_key, extent, jnp.float32)
    if cuts:
        values = values * steps_of(own_key, extent, cuts, -0.22, 0.18)
    return jnp.clip(values, -limit, limit).astype(held_as)


def setup_inputs(seed: int = 0) -> dict:
    key_list = jax.random.split(jax.random.key(seed), 14)
    hidden_in = noise(key_list[0], (TOKENS, D), 1.0, 6.0, ((0, 32),))
    segments = jax.vmap(lambda own: jnp.searchsorted(jnp.cumsum(ragged_sizes(own, SEGS, LENGTH, LENGTH // 2, 0)), jnp.arange(LENGTH), side="right"))(jax.random.split(key_list[1], ROWS)).reshape((ROWS, LENGTH)).astype(jnp.int32)
    ln_gain = jnp.clip(1.0 + 0.18 * jax.random.normal(key_list[2], (D,), jnp.float32), 0.099609375, 1.8984375).astype(jnp.bfloat16)
    ln_bias = noise(key_list[3], (D,), 0.5, 3.0, ((0, 8),))
    qkv_weight = draw_qkv_weight(jax.random.fold_in(key_list[13], 71), 0)
    qkv_bias = noise(key_list[5], (3, D), 0.5, 3.0, ((1, 4),))
    dense_weight = noise(key_list[6], (D, D), (D // 16) ** -0.5, 0.5, ((0, 4), (1, 8)))
    dense_bias = noise(key_list[7], (D,), 0.5, 3.0, ((0, 8),))
    fc1_weight = noise(key_list[8], (D, FF), D ** -0.5, 0.125, ((0, 8), (1, 4)))
    fc1_bias = noise(key_list[9], (FF,), 0.5, 3.0, ((0, 4),))
    fc2_weight = noise(key_list[10], (FF, D), FF ** -0.5, 0.0625, ((0, 4), (1, 8)))
    fc2_bias = noise(key_list[11], (D,), 0.5, 3.0, ((0, 8),))
    cotangent = noise(key_list[12], (TOKENS, D), 1.0, 6.0, ((0, 32),))
    return {"hidden_in": hidden_in, "segments": segments, "ln_gain": ln_gain, "ln_bias": ln_bias, "qkv_weight": qkv_weight, "qkv_bias": qkv_bias, "dense_weight": dense_weight, "dense_bias": dense_bias, "fc1_weight": fc1_weight, "fc1_bias": fc1_bias, "fc2_weight": fc2_weight, "fc2_bias": fc2_bias, "cotangent": cotangent}


@jax.custom_vjp
def low(v):
    return lax.optimization_barrier(v.astype(jnp.bfloat16)).astype(jnp.float32)

@jax.custom_vjp
def low_back(v):
    return v

def low_keep(v):
    return (low(v), None)

def low_pass(kept, grad):
    return (grad,)

def back_keep(v):
    return (v, None)

def back_low(kept, grad):
    return (low(grad),)
low.defvjp(low_keep, low_pass)
low_back.defvjp(back_keep, back_low)
highest = lax.Precision.HIGHEST
layer_eps = 1e-05

def product(left, right):
    return jnp.dot(left, right, precision=highest, preferred_element_type=jnp.float32)

def positions_of(segments):
    length = segments.shape[-1]
    index_row = jnp.arange(length, dtype=jnp.int32)
    same_doc = segments[:, :, None] == segments[:, None, :]
    before = index_row[None, :] < index_row[:, None]
    return lax.optimization_barrier(jnp.sum((same_doc & before[None]).astype(jnp.int32), axis=-1))

def rotary_tables(positions):
    frequency = 1.0 / 10000.0 ** (jnp.arange(0, ROT, 2, dtype=jnp.float32) / ROT)
    angles = positions.astype(jnp.float32)[..., None] * frequency
    cosine = jnp.concatenate([jnp.cos(angles), jnp.cos(angles)], -1)[:, :, None, :]
    sine_table = jnp.concatenate([jnp.sin(angles), jnp.sin(angles)], -1)[:, :, None, :]
    return (cosine, sine_table)

def rotate(fields, cosine, sine_table):
    half_rot = ROT // 2
    rotated_part = fields[..., :ROT]
    turned = jnp.concatenate([-rotated_part[..., half_rot:], rotated_part[..., :half_rot]], -1)
    return jnp.concatenate([rotated_part * cosine + turned * sine_table, fields[..., ROT:]], -1)

def attend_row(inputs):
    query_rows, key_rows, value_rows, seg_row = inputs
    length = query_rows.shape[0]
    scaling = query_rows.shape[-1] ** (-0.5)
    raw_scores = jnp.einsum('qhd,khd->hqk', query_rows, key_rows, precision=highest, preferred_element_type=jnp.float32) * scaling
    raw_scores = low_back(raw_scores)
    index_row = jnp.arange(length, dtype=jnp.int32)
    allowed = (index_row[None, :] <= index_row[:, None]) & (seg_row[:, None] == seg_row[None, :])
    scores = jnp.where(allowed[None], raw_scores, -1e+30)
    row_max = lax.optimization_barrier(jnp.max(scores, -1, keepdims=True))
    exponent = jnp.exp(scores - row_max)
    attn_probs = exponent / lax.optimization_barrier(jnp.sum(exponent, -1, keepdims=True))
    return jnp.einsum('hqk,khd->qhd', low(attn_probs), value_rows, precision=highest, preferred_element_type=jnp.float32)

def reference(hidden_in, segments, ln_gain, ln_bias, qkv_weight, qkv_bias, dense_weight, dense_bias, fc1_weight, fc1_bias, fc2_weight, fc2_bias, cotangent):
    num_rows = segments.shape[0]
    length = segments.shape[1]
    tokens_all = hidden_in.shape[0]
    cosine, sine_table = rotary_tables(positions_of(segments))

    def forward(resid_in, gain_full, beta_full, w_qkv, b_qkv, w_dense, b_dense, w_fc1, b_fc1, w_fc2, b_fc2):
        average = lax.optimization_barrier(jnp.mean(resid_in, -1, keepdims=True))
        centred = resid_in - average
        spread = lax.optimization_barrier(jnp.mean(centred * centred, -1, keepdims=True))
        normed = low(centred * lax.rsqrt(spread + layer_eps) * gain_full + beta_full)
        qkv_proj = low_back(product(normed, w_qkv.reshape(D, 3 * D)) + b_qkv.reshape(3 * D))
        qkv_proj = qkv_proj.reshape(num_rows, length, 3, HEADS, HD)
        query_rows = low(rotate(qkv_proj[:, :, 0], cosine, sine_table))
        key_rows = low(rotate(qkv_proj[:, :, 1], cosine, sine_table))
        value_rows = low(qkv_proj[:, :, 2])
        attended = lax.map(jax.checkpoint(attend_row), (query_rows, key_rows, value_rows, segments))
        attn_vec = low(low_back(attended)).reshape(tokens_all, D)
        pre_act = low_back(product(normed, w_fc1) + b_fc1)
        act_vals = low(jax.nn.gelu(pre_act, approximate=True))
        return resid_in + product(attn_vec, w_dense) + product(act_vals, w_fc2) + b_dense + b_fc2
    out_full, pull = jax.vjp(forward, hidden_in.astype(jnp.float32), ln_gain.astype(jnp.float32), ln_bias.astype(jnp.float32), qkv_weight.astype(jnp.float32), qkv_bias.astype(jnp.float32), dense_weight.astype(jnp.float32), dense_bias.astype(jnp.float32), fc1_weight.astype(jnp.float32), fc1_bias.astype(jnp.float32), fc2_weight.astype(jnp.float32), fc2_bias.astype(jnp.float32))
    grads = pull(cotangent.astype(jnp.float32))
    return (out_full.astype(jnp.bfloat16), grads[0].astype(jnp.bfloat16), grads[1], grads[2], grads[3], grads[4], grads[5], grads[6], grads[7], grads[8], grads[9], grads[10])
```

```python
import functools

import jax
import jax.numpy as jnp
from jax import lax
from jax.experimental import pallas as pl
from jax.experimental.pallas import tpu as pltpu
from jax.sharding import PartitionSpec as P

HD = 64
ROT = 32
BLOCK = 256
MAX_DOC = 512
VMEM_LIMIT = 66_000_000
MESH = pl.DeviceIdType.MESH
ANY = pl.BlockSpec(memory_space=pl.ANY)
VMEM = pl.BlockSpec(memory_space=pltpu.VMEM)

layer_eps = 1e-05
f32 = jnp.float32
bf16 = jnp.bfloat16


def dot_nn(a, b):
    return lax.dot_general(a, b, (((1,), (0,)), ((), ())), preferred_element_type=f32)


def dot_nt(a, b):
    return lax.dot_general(a, b, (((1,), (1,)), ((), ())), preferred_element_type=f32)


def dot_tn(a, b):
    return lax.dot_general(a, b, (((0,), (0,)), ((), ())), preferred_element_type=f32)


def flip(index, bit):
    step = 1 << bit
    return index + step * (1 - 2 * (lax.div(index, step) % 2))


def relative(index, offset):
    bit = 0
    while offset >> bit:
        if (offset >> bit) & 1:
            index = flip(index, bit)
        bit += 1
    return index


def stages_of(order):
    held, stages = [0], []
    for bit in order:
        got = [r ^ (1 << bit) for r in held]
        stages.append((bit, list(held), got))
        held = held + got
    return stages


class Sems:
    def __init__(self):
        self.count = 0

    def take(self):
        self.count += 1
        return self.count - 1


class CubeGather:
    def __init__(self, sems, orders):
        self.plans = [stages_of(order) for order in orders]
        self.ids = {
            (h, j, i): sems.take()
            for h, stages in enumerate(self.plans)
            for j, (_, held, _) in enumerate(stages)
            for i in range(len(held))
        }

    def bind(self, me, other, own, window, send_sem, recv_sem):
        self.me, self.other, self.own, self.window = me, other, own, window
        self.send_sem, self.recv_sem = send_sem, recv_sem
        return self

    def copy(self, h, j, i):
        bit, held, _ = self.plans[h][j]
        slot = relative(self.me, held[i])
        target = self.window(slot, h)
        source = self.own(h) if held[i] == 0 else target
        k = self.ids[h, j, i]
        return pltpu.make_async_remote_copy(
            src_ref=source,
            dst_ref=target,
            send_sem=self.send_sem.at[k],
            recv_sem=self.recv_sem.at[k],
            device_id=(flip(self.me, bit), self.other),
            device_id_type=MESH,
        )

    def start(self):
        depth = len(self.plans[0])
        for j in range(depth):
            for h in range(len(self.plans)):
                self.copy(h, j, 0).start()

    def advance(self, j):
        for i in range(len(self.plans[0][j][1])):
            for h, stages in enumerate(self.plans):
                self.copy(h, j, i).wait_recv()
                slot = stages[j][2][i]
                for later in range(j + 1, len(stages)):
                    self.copy(h, later, stages[later][1].index(slot)).start()

    def finish(self):
        for h, j, i in self.ids:
            self.copy(h, j, i).wait_send()


class LineGather:
    def __init__(self, sems, size, subs):
        self.size, self.subs = size, subs
        self.ids = {
            (way, s, u): sems.take()
            for way in (0, 1)
            for s in range(size - 1)
            for u in range(subs)
        }

    def bind(self, me, other, own, window, send_sem, recv_sem):
        self.me, self.other, self.own, self.window = me, other, own, window
        self.send_sem, self.recv_sem = send_sem, recv_sem
        return self

    def copy(self, way, s, u):
        block = self.me - s if way == 0 else self.me + s
        target = self.window(block, u)
        k = self.ids[way, s, u]
        return pltpu.make_async_remote_copy(
            src_ref=self.own(u) if s == 0 else target,
            dst_ref=target,
            send_sem=self.send_sem.at[k],
            recv_sem=self.recv_sem.at[k],
            device_id=(self.other, self.me + 1 if way == 0 else self.me - 1),
            device_id_type=MESH,
        )

    def sends(self, way, s):
        if way == 0:
            return (self.me >= s) & (self.me < self.size - 1)
        return (self.me + s < self.size) & (self.me > 0)

    def gets(self, way, s):
        if way == 0:
            return self.me - 1 - s >= 0
        return self.me + 1 + s < self.size

    def start(self, u):
        for way in (0, 1):

            @pl.when(self.sends(way, 0))
            def _():
                self.copy(way, 0, u).start()

    def advance(self, s, u):
        for way in (0, 1):

            @pl.when(self.gets(way, s))
            def _():
                self.copy(way, s, u).wait_recv()

            if s + 1 < self.size - 1:

                @pl.when(self.sends(way, s + 1))
                def _():
                    self.copy(way, s + 1, u).start()

    def finish(self):
        for way, s, u in self.ids:

            @pl.when(self.sends(way, s))
            def _():
                self.copy(way, s, u).wait_send()


def greet(dp, me, tensor, line):
    barrier = pltpu.get_barrier_semaphore()
    bits = dp.bit_length() - 1
    for bit in range(bits):
        pl.semaphore_signal(barrier, inc=1, device_id=(flip(me, bit), line), device_id_type=MESH)

    @pl.when(line > 0)
    def _():
        pl.semaphore_signal(barrier, inc=1, device_id=(me, line - 1), device_id_type=MESH)

    @pl.when(line < tensor - 1)
    def _():
        pl.semaphore_signal(barrier, inc=1, device_id=(me, line + 1), device_id_type=MESH)

    left, right = jnp.minimum(line, 1), jnp.minimum(tensor - 1 - line, 1)
    pl.semaphore_wait(barrier, bits + left + right)


def orders_of(dp):
    bits = list(range(1, dp.bit_length() - 1))
    return [bits + [0], bits[::-1] + [0]]


def gather_call(dp, tensor, hidden, cotangent, w_qkv, w_dense, w_fc1, w_fc2, vectors):
    rows, width = hidden.shape
    local = w_qkv.shape[2]
    hidden_units = w_fc1.shape[1]
    part = width // dp
    sems = Sems()
    orders = orders_of(dp)
    plan_vec = CubeGather(sems, orders[:1])
    plan_qkv, plan_dense, plan_fc1, plan_fc2 = (CubeGather(sems, orders) for _ in range(4))
    plan_n, plan_c = LineGather(sems, tensor, 2), LineGather(sems, tensor, 2)

    def kernel(
        x_ref, c_ref, wq_ref, wd_ref, w1_ref, w2_ref, vec_ref,
        gq_ref, gd_ref, g1_ref, g2_ref, gn_ref, gc_ref, gvec_ref,
        x_buf, n_buf, vec_buf, send_sem, recv_sem, local_sem,
    ):
        me, line = lax.axis_index("dp"), lax.axis_index("tensor")
        half = part // 2

        def cols(a):
            return pl.ds(pl.multiple_of(a * part, part), part)

        def half_rows(a, h):
            return pl.ds(pl.multiple_of(a * part + h * half, half), half)

        def tok(b, u):
            return pl.ds(pl.multiple_of(b * rows + u * (rows // 2), rows // 2), rows // 2)

        def sub(u):
            return pl.ds(u * (rows // 2), rows // 2)

        def piece(n, h):
            return pl.ds(h * (n // 2), n // 2)

        pair = (send_sem, recv_sem)
        vec = plan_vec.bind(me, line, lambda h: vec_ref, lambda a, h: vec_buf.at[:, cols(a)], *pair)
        qkv = plan_qkv.bind(
            me, line,
            lambda h: wq_ref.at[:, pl.ds(h * half, half), :],
            lambda a, h: gq_ref.at[:, half_rows(a, h), :], *pair)
        fc1 = plan_fc1.bind(
            me, line,
            lambda h: w1_ref.at[pl.ds(h * half, half), :],
            lambda a, h: g1_ref.at[half_rows(a, h), :], *pair)
        dense = plan_dense.bind(
            me, line,
            lambda h: wd_ref.at[piece(local, h), :],
            lambda a, h: gd_ref.at[piece(local, h), cols(a)], *pair)
        fc2 = plan_fc2.bind(
            me, line,
            lambda h: w2_ref.at[piece(hidden_units, h), :],
            lambda a, h: g2_ref.at[piece(hidden_units, h), cols(a)], *pair)
        norm = plan_n.bind(
            line, me, lambda u: n_buf.at[sub(u)], lambda b, u: gn_ref.at[tok(b, u)], *pair)
        cot = plan_c.bind(
            line, me, lambda u: c_ref.at[sub(u)], lambda b, u: gc_ref.at[tok(b, u)], *pair)

        keep = [
            (x_ref, x_buf),
            (vec_ref, vec_buf.at[:, cols(me)]),
            (wq_ref, gq_ref.at[:, pl.ds(pl.multiple_of(me * part, part), part), :]),
            (w1_ref, g1_ref.at[pl.ds(pl.multiple_of(me * part, part), part), :]),
            (wd_ref, gd_ref.at[:, cols(me)]),
            (w2_ref, g2_ref.at[:, cols(me)]),
            (c_ref, gc_ref.at[pl.ds(pl.multiple_of(line * rows, rows), rows), :]),
        ]
        keeps = [
            pltpu.make_async_copy(a, b, local_sem.at[k]) for k, (a, b) in enumerate(keep)
        ]
        keeps[0].start()
        greet(dp, me, tensor, line)
        vec.start()
        qkv.start()
        for copy in keeps[1:]:
            copy.start()
        stages = dp.bit_length() - 1
        for j in range(stages):
            vec.advance(j)
        keeps[0].wait()
        keeps[1].wait()

        @pl.loop(0, rows, step=32)
        def _(r):
            x = x_buf[pl.ds(r, 32), :].astype(f32)
            centred = x - jnp.mean(x, -1, keepdims=True)
            spread = jnp.mean(centred * centred, -1, keepdims=True)
            unit = centred * lax.rsqrt(spread + layer_eps)
            n_buf[pl.ds(r, 32), :] = (unit * vec_buf[0:1, :] + vec_buf[1:2, :]).astype(bf16)

        norm.start(0)
        norm.start(1)
        own_n = pltpu.make_async_copy(
            n_buf, gn_ref.at[pl.ds(pl.multiple_of(line * rows, rows), rows), :], local_sem.at[len(keep)])
        own_n.start()
        gvec_ref[...] = vec_buf[...]
        qkv.advance(0)
        fc1.start()
        norm.advance(0, 0)
        for j in range(1, stages - 1):
            qkv.advance(j)
        norm.advance(0, 1)
        fc1.advance(0)
        dense.start()
        fc2.start()
        qkv.advance(stages - 1)
        norm.advance(1, 0)
        norm.advance(1, 1)
        cot.start(0)
        cot.start(1)
        for j in range(1, stages - 1):
            fc1.advance(j)
        dense.advance(0)
        norm.advance(2, 0)
        norm.advance(2, 1)
        fc1.advance(stages - 1)
        fc2.advance(0)
        cot.advance(0, 0)
        for j in range(1, stages - 1):
            dense.advance(j)
        cot.advance(0, 1)
        for j in range(1, stages - 1):
            fc2.advance(j)
        dense.advance(stages - 1)
        fc2.advance(stages - 1)
        for s in (1, 2):
            for u in (0, 1):
                cot.advance(s, u)
        for copy in keeps[2:]:
            copy.wait()
        own_n.wait()
        for plan in (vec, qkv, fc1, dense, fc2, norm, cot):
            plan.finish()

    tokens = rows * tensor
    return pl.pallas_call(
        kernel,
        out_shape=(
            jax.ShapeDtypeStruct((3, width, local), bf16),
            jax.ShapeDtypeStruct((local, width), bf16),
            jax.ShapeDtypeStruct((width, hidden_units), bf16),
            jax.ShapeDtypeStruct((hidden_units, width), bf16),
            jax.ShapeDtypeStruct((tokens, width), bf16),
            jax.ShapeDtypeStruct((tokens, width), bf16),
            jax.ShapeDtypeStruct((8, width), f32),
        ),
        in_specs=[ANY] * 7,
        out_specs=(ANY,) * 6 + (VMEM,),
        scratch_shapes=[
            pltpu.VMEM((rows, width), bf16),
            pltpu.VMEM((rows, width), bf16),
            pltpu.VMEM((8, width), f32),
            pltpu.SemaphoreType.DMA((sems.count,)),
            pltpu.SemaphoreType.DMA((sems.count,)),
            pltpu.SemaphoreType.DMA((8,)),
        ],
        compiler_params=pltpu.CompilerParams(
            collective_id=0, has_side_effects=True, vmem_limit_bytes=VMEM_LIMIT
        ),
        name="gather",
    )(hidden, cotangent, w_qkv, w_dense, w_fc1, w_fc2, vectors)


def normalize(x, gain, bias):
    centred = x - jnp.mean(x, -1, keepdims=True)
    spread = jnp.mean(centred * centred, -1, keepdims=True)
    unit = centred * lax.rsqrt(spread + layer_eps)
    return (unit * gain + bias).astype(bf16)


def gather_plain(hidden, cotangent, w_qkv, w_dense, w_fc1, w_fc2, vectors):
    vec = lax.all_gather(vectors, "dp", axis=1, tiled=True)
    normed = normalize(hidden.astype(f32), vec[0:1], vec[1:2])
    return (
        lax.all_gather(w_qkv, "dp", axis=1, tiled=True),
        lax.all_gather(w_dense, "dp", axis=1, tiled=True),
        lax.all_gather(w_fc1, "dp", axis=0, tiled=True),
        lax.all_gather(w_fc2, "dp", axis=1, tiled=True),
        lax.all_gather(normed, "tensor", axis=0, tiled=True),
        lax.all_gather(cotangent, "tensor", axis=0, tiled=True),
        vec,
    )


def spans_of(length):
    back = -(-(MAX_DOC - 1) // BLOCK)
    spans, at = [], 0
    for i in range(length // BLOCK):
        low = max(0, i - back) * BLOCK
        spans.append((low, (i + 1) * BLOCK, at))
        at += (i + 1) * BLOCK - low
    return spans, at


def turn(x, cosine, sine_lo, sine_hi):
    return x * cosine + pltpu.roll(x, 128 - ROT // 2, 1) * sine_lo + pltpu.roll(x, ROT // 2, 1) * sine_hi


def head_lanes(shape, e):
    lane = lax.broadcasted_iota(jnp.int32, shape, 1)
    return (lane >= e * HD) & (lane < (e + 1) * HD)


def only(x, e):
    return jnp.where(head_lanes(x.shape, e), x, jnp.zeros_like(x))


def attend_kernel(
    q_ref, k_ref, v_ref, bias_ref, cos_ref, slo_ref, shi_ref, segc_ref, segr_ref,
    qs_ref, ks_ref, vs_ref, o_ref, p_ref, mask_ref,
):
    length = q_ref.shape[0]
    spans, _ = spans_of(length)

    @pl.when(pl.program_id(1) == 0)
    def _():
        for i, (low, high, at) in enumerate(spans):
            keys = lax.broadcasted_iota(jnp.int32, (high - low, BLOCK), 0) + low
            queries = lax.broadcasted_iota(jnp.int32, (high - low, BLOCK), 1) + i * BLOCK
            same = segc_ref[low:high, :] == segr_ref[:, i * BLOCK : (i + 1) * BLOCK]
            mask_ref[at : at + high - low, :] = jnp.where((keys <= queries) & same, 0.0, -1e30)

    cosine, slo, shi = cos_ref[...], slo_ref[...], shi_ref[...]
    query = turn(q_ref[...] + bias_ref[0:1, :], cosine, slo, shi).astype(bf16) * bf16(HD**-0.5)
    key = turn(k_ref[...] + bias_ref[1:2, :], cosine, slo, shi).astype(bf16)
    value = (v_ref[...] + bias_ref[2:3, :]).astype(bf16)
    qs_ref[...] = query
    ks_ref[...] = key
    vs_ref[...] = value
    heads = 128 // HD
    for i, (low, high, at) in enumerate(spans):
        q_i = query[i * BLOCK : (i + 1) * BLOCK]
        total = jnp.zeros((BLOCK, 128), f32)
        for e in range(heads):
            scores = dot_nt(only(key[low:high], e), q_i) + mask_ref[at : at + high - low, :]
            exponent = jnp.exp(scores - jnp.max(scores, 0, keepdims=True))
            inverse = 1.0 / jnp.sum(exponent, 0, keepdims=True)
            probs = (exponent * inverse).astype(bf16)
            p_ref[e, at : at + high - low, :] = probs
            total = total + dot_tn(probs, only(value[low:high], e))
        o_ref[i * BLOCK : (i + 1) * BLOCK, :] = total.astype(bf16)


def attend(q, k, v, qkv_bias, tables, segments, rows):
    tokens, local = q.shape
    length = tokens // rows
    pairs = local // 128
    _, stored = spans_of(length)
    block = pl.BlockSpec((length, 128), lambda r, h: (r, h))
    table = pl.BlockSpec((length, 128), lambda r, h: (r, 0))
    shape = jax.ShapeDtypeStruct((tokens, local), bf16)
    return pl.pallas_call(
        attend_kernel,
        grid=(rows, pairs),
        out_shape=(shape,) * 4 + (jax.ShapeDtypeStruct((rows, local // HD, stored, BLOCK), bf16),),
        in_specs=[block] * 3
        + [pl.BlockSpec((8, 128), lambda r, h: (0, h))]
        + [table] * 3
        + [
            pl.BlockSpec((length, 1), lambda r, h: (r, 0)),
            pl.BlockSpec((pl.Squeezed(), 1, length), lambda r, h: (r, 0, 0)),
        ],
        out_specs=(block,) * 4
        + (pl.BlockSpec((pl.Squeezed(), 128 // HD, stored, BLOCK), lambda r, h: (r, h, 0, 0)),),
        scratch_shapes=[pltpu.VMEM((stored, BLOCK), f32)],
        compiler_params=pltpu.CompilerParams(vmem_limit_bytes=VMEM_LIMIT),
        cost_estimate=pl.CostEstimate(
            flops=16 * tokens * 768 * local, bytes_accessed=24 << 20, transcendentals=0
        ),
        name="attend",
    )(q, k, v, qkv_bias, *tables, segments.reshape(tokens, 1), segments.reshape(rows, 1, length))


def attend_back_kernel(
    q_ref, k_ref, v_ref, g_ref, o_ref, p_ref, cos_ref, slo_ref, shi_ref,
    dq_ref, dk_ref, dv_ref, bias_ref, kacc_ref, vacc_ref,
):
    length = q_ref.shape[0]
    spans, _ = spans_of(length)
    heads = 128 // HD
    grad = g_ref[...]
    inner = grad.astype(f32) * o_ref[...].astype(f32)
    lane = lax.broadcasted_iota(jnp.int32, (8, 128), 1)
    row = lax.broadcasted_iota(jnp.int32, (8, 128), 0)
    pick = jnp.where(lax.div(lane, HD) == row, 1.0, 0.0)
    delta = lax.dot_general(
        pick, inner, (((1,), (1,)), ((), ())),
        precision=lax.Precision.HIGHEST, preferred_element_type=f32)
    query, key, value = q_ref[...], k_ref[...], v_ref[...]
    kacc_ref[...] = jnp.zeros_like(kacc_ref)
    vacc_ref[...] = jnp.zeros_like(vacc_ref)
    cosine, slo, shi = cos_ref[...], slo_ref[...], shi_ref[...]
    first = jnp.zeros((1, 128), f32)
    for i, (low, high, at) in enumerate(spans):
        mine = slice(i * BLOCK, (i + 1) * BLOCK)
        g_i, q_i = grad[mine], query[mine]
        dq = jnp.zeros((BLOCK, 128), f32)
        ps, dss = [], []
        for e in range(heads):
            probs = p_ref[e, at : at + high - low, :]
            dprobs = dot_nt(only(value[low:high], e), g_i)
            ds = (probs.astype(f32) * (dprobs - delta[e : e + 1, mine])).astype(bf16)
            dq = dq + dot_tn(ds, only(key[low:high], e))
            ps.append(probs)
            dss.append(ds)
        g_cat = jnp.concatenate([only(g_i, e) for e in range(heads)], 0)
        q_cat = jnp.concatenate([only(q_i, e) for e in range(heads)], 0)
        vacc_ref[low:high, :] += dot_nn(jnp.concatenate(ps, 1), g_cat)
        kacc_ref[low:high, :] += dot_nn(jnp.concatenate(dss, 1), q_cat)
        dq = dq * f32(HD**-0.5)
        dq = turn(dq, cosine[mine], -slo[mine], -shi[mine]).astype(bf16)
        dq_ref[mine, :] = dq
        first = first + jnp.sum(dq.astype(f32), 0, keepdims=True)
    dk = turn(kacc_ref[...], cosine, -slo, -shi).astype(bf16)
    dv = vacc_ref[...].astype(bf16)
    dk_ref[...] = dk
    dv_ref[...] = dv
    sums = [first, jnp.sum(dk.astype(f32), 0, keepdims=True), jnp.sum(dv.astype(f32), 0, keepdims=True)]
    sums = jnp.concatenate(sums + [jnp.zeros((5, 128), f32)], 0)

    @pl.when(pl.program_id(1) == 0)
    def _():
        bias_ref[...] = sums

    @pl.when(pl.program_id(1) > 0)
    def _():
        bias_ref[...] += sums


def attend_back(q, k, v, g, o, probs, tables, rows):
    tokens, local = q.shape
    length = tokens // rows
    pairs = local // 128
    stored = probs.shape[2]
    block = pl.BlockSpec((length, 128), lambda h, r: (r, h))
    table = pl.BlockSpec((length, 128), lambda h, r: (r, 0))
    shape = jax.ShapeDtypeStruct((tokens, local), bf16)
    return pl.pallas_call(
        attend_back_kernel,
        grid=(pairs, rows),
        out_shape=(shape,) * 3 + (jax.ShapeDtypeStruct((8, local), f32),),
        in_specs=[block] * 5
        + [pl.BlockSpec((pl.Squeezed(), 128 // HD, stored, BLOCK), lambda h, r: (r, h, 0, 0))]
        + [table] * 3,
        out_specs=(block,) * 3 + (pl.BlockSpec((8, 128), lambda h, r: (0, h)),),
        scratch_shapes=[pltpu.VMEM((length, 128), f32)] * 2,
        compiler_params=pltpu.CompilerParams(vmem_limit_bytes=VMEM_LIMIT),
        cost_estimate=pl.CostEstimate(
            flops=32 * tokens * 768 * local, bytes_accessed=24 << 20, transcendentals=0
        ),
        name="attend_back",
    )(q, k, v, g, o, probs, *tables)


def rotary_tables(segments):
    rows, length = segments.shape
    index = jnp.arange(length, dtype=jnp.int32)[None]
    start = jnp.zeros_like(segments)
    for number in range(1, 4):
        start = jnp.where(segments == number, jnp.sum(segments < number, -1, keepdims=True), start)
    position = (index - start).astype(f32).reshape(rows * length, 1)
    lane = jnp.arange(128, dtype=jnp.int32) % HD
    exponent = (2 * (lane % (ROT // 2))).astype(f32) / ROT
    angle = position * (1.0 / 10000.0**exponent)[None]
    cosine, sine = jnp.cos(angle), jnp.sin(angle)
    low, high = lane < ROT // 2, (lane >= ROT // 2) & (lane < ROT)
    return (
        jnp.where(lane < ROT, cosine, 1.0),
        jnp.where(low, -sine, 0.0),
        jnp.where(high, sine, 0.0),
    )


def matmul(a, b):
    return jnp.dot(a, b, preferred_element_type=f32)


def on_device(
    dp, tensor, fast,
    hidden_in, segments, ln_gain, ln_bias, qkv_weight, qkv_bias, dense_weight, dense_bias,
    fc1_weight, fc1_bias, fc2_weight, fc2_bias, cotangent,
):
    seqs = segments.shape[0]
    local = qkv_weight.shape[2]
    vectors = jnp.stack([ln_gain.astype(f32), ln_bias.astype(f32), dense_bias.astype(f32) + fc2_bias.astype(f32)])
    vectors = jnp.pad(vectors, ((0, 5), (0, 0)))
    mine = (
        hidden_in, cotangent, qkv_weight.transpose(1, 0, 2),
        dense_weight, fc1_weight, fc2_weight, vectors,
    )
    gathered = gather_call(dp, tensor, *mine) if fast else gather_plain(*mine)
    w_qkv, w_dense, w_fc1, w_fc2, normed, grad_out, vec = gathered
    gain, out_bias = vec[0:1], vec[2:3]
    resid_in = hidden_in.astype(f32)
    cot_float = cotangent.astype(f32)
    centred = resid_in - jnp.mean(resid_in, -1, keepdims=True)
    spread = jnp.mean(centred * centred, -1, keepdims=True)
    inv_std = lax.rsqrt(spread + layer_eps)
    unit_rows = centred * inv_std

    tables = rotary_tables(segments)
    bias = jnp.pad(qkv_bias.astype(f32), ((0, 5), (0, 0)))
    query, key, value, attn_vec, probs = attend(
        *(matmul(normed, w_qkv[i]) for i in range(3)), bias, tables, segments, seqs
    )
    pre_act = matmul(normed, w_fc1) + fc1_bias.astype(f32)
    act_vals, gelu_pull = jax.vjp(lambda pre: jax.nn.gelu(pre, approximate=True), pre_act)
    act_vals = act_vals.astype(bf16)
    branches = matmul(attn_vec, w_dense) + matmul(act_vals, w_fc2)
    summed = lax.psum_scatter(branches.astype(bf16), "tensor", scatter_dimension=0, tiled=True)
    out = (resid_in + summed.astype(f32) + out_bias).astype(bf16)

    out_bias_part = jnp.sum(cot_float, 0)
    grad_fc2 = matmul(act_vals.T, grad_out)
    grad_dense = matmul(attn_vec.T, grad_out)
    grad_pre = gelu_pull(matmul(grad_out, w_fc2.T))[0].astype(bf16)
    fc1_bias_part = jnp.sum(grad_pre.astype(f32), 0)
    grad_fc1 = matmul(normed.T, grad_pre)
    grad_attn = matmul(grad_out, w_dense.T).astype(bf16)
    *grads, qkv_bias_part = attend_back(query, key, value, grad_attn, attn_vec, probs, tables, seqs)
    grad_wqkv = jnp.stack([matmul(normed.T, g) for g in grads])
    grad_normed = matmul(grad_pre, w_fc1.T) + sum(matmul(g, w.T) for g, w in zip(grads, w_qkv))
    sent_qkv, sent_dense, sent_fc1, sent_fc2 = (
        lax.psum_scatter(grad_wqkv.astype(bf16), "dp", scatter_dimension=1, tiled=True),
        lax.psum_scatter(grad_dense.astype(bf16), "dp", scatter_dimension=1, tiled=True),
        lax.psum_scatter(grad_fc1.astype(bf16), "dp", scatter_dimension=0, tiled=True),
        lax.psum_scatter(grad_fc2.astype(bf16), "dp", scatter_dimension=1, tiled=True),
    )
    grad_local = lax.psum_scatter(
        grad_normed.astype(bf16), "tensor", scatter_dimension=0, tiled=True
    ).astype(f32)
    gain_part = jnp.sum(grad_local * unit_rows, 0)
    beta_part = jnp.sum(grad_local, 0)
    scaled_grad = grad_local * gain
    first_mean = jnp.mean(scaled_grad, -1, keepdims=True)
    second_mean = jnp.mean(scaled_grad * unit_rows, -1, keepdims=True)
    hidden_grad = (
        cot_float + inv_std * (scaled_grad - first_mean - unit_rows * second_mean)
    ).astype(bf16)
    gain_grad, beta_grad, out_bias_grad = (
        lax.psum_scatter(gain_part, ("dp", "tensor"), scatter_dimension=0, tiled=True),
        lax.psum_scatter(beta_part, ("dp", "tensor"), scatter_dimension=0, tiled=True),
        lax.psum_scatter(out_bias_part, ("dp", "tensor"), scatter_dimension=0, tiled=True),
    )
    qkv_bias_grad, fc1_bias_grad = lax.psum((qkv_bias_part[:3], fc1_bias_part), "dp")
    return (
        out,
        hidden_grad,
        gain_grad,
        beta_grad,
        sent_qkv.transpose(1, 0, 2).astype(f32),
        qkv_bias_grad,
        sent_dense.astype(f32),
        out_bias_grad,
        sent_fc1.astype(f32),
        fc1_bias_grad,
        sent_fc2.astype(f32),
        out_bias_grad,
    )


def solution(mesh):
    dp, tensor = mesh.shape["dp"], mesh.shape["tensor"]
    fast = dp == 8 and tensor == 4
    placed = (
        P(("dp", "tensor"), None),
        P("dp", None),
        P("dp"),
        P("dp"),
        P("dp", None, "tensor"),
        P(None, "tensor"),
        P("tensor", "dp"),
        P("dp"),
        P("dp", "tensor"),
        P("tensor"),
        P("tensor", "dp"),
        P("dp"),
        P(("dp", "tensor"), None),
    )
    return jax.shard_map(
        functools.partial(on_device, dp, tensor, fast),
        mesh=mesh,
        in_specs=placed,
        out_specs=(
            P(("dp", "tensor"), None),
            P(("dp", "tensor"), None),
            P(("dp", "tensor")),
            P(("dp", "tensor")),
            P("dp", None, "tensor"),
            P(None, "tensor"),
            P("tensor", "dp"),
            P(("dp", "tensor")),
            P("dp", "tensor"),
            P("tensor"),
            P("tensor", "dp"),
            P(("dp", "tensor")),
        ),
        check_vma=False,
    )
```

```python
import functools

import jax
import jax.numpy as jnp
from jax import lax
from jax.experimental import pallas as pl
from jax.experimental.pallas import tpu as pltpu
from jax.sharding import PartitionSpec as P

HD = 64
ROT = 32
BLOCK = 256
MAX_DOC = 512
VMEM_LIMIT = 66_000_000
MESH = pl.DeviceIdType.MESH
ANY = pl.BlockSpec(memory_space=pl.ANY)
VMEM = pl.BlockSpec(memory_space=pltpu.VMEM)

layer_eps = 1e-05
f32 = jnp.float32
bf16 = jnp.bfloat16


def dot_nn(a, b):
    return lax.dot_general(a, b, (((1,), (0,)), ((), ())), preferred_element_type=f32)


def dot_nt(a, b):
    return lax.dot_general(a, b, (((1,), (1,)), ((), ())), preferred_element_type=f32)


def dot_tn(a, b):
    return lax.dot_general(a, b, (((0,), (0,)), ((), ())), preferred_element_type=f32)


def flip(index, bit):
    step = 1 << bit
    return index + step * (1 - 2 * (lax.div(index, step) % 2))


def relative(index, offset):
    bit = 0
    while offset >> bit:
        if (offset >> bit) & 1:
            index = flip(index, bit)
        bit += 1
    return index


def stages_of(order):
    held, stages = [0], []
    for bit in order:
        got = [r ^ (1 << bit) for r in held]
        stages.append((bit, list(held), got))
        held = held + got
    return stages


class Sems:
    def __init__(self):
        self.count = 0

    def take(self):
        self.count += 1
        return self.count - 1


class CubeGather:
    def __init__(self, sems, orders):
        self.plans = [stages_of(order) for order in orders]
        self.ids = {
            (h, j, i): sems.take()
            for h, stages in enumerate(self.plans)
            for j, (_, held, _) in enumerate(stages)
            for i in range(len(held))
        }

    def bind(self, me, other, own, window, send_sem, recv_sem):
        self.me, self.other, self.own, self.window = me, other, own, window
        self.send_sem, self.recv_sem = send_sem, recv_sem
        return self

    def copy(self, h, j, i):
        bit, held, _ = self.plans[h][j]
        slot = relative(self.me, held[i])
        target = self.window(slot, h)
        source = self.own(h) if held[i] == 0 else target
        k = self.ids[h, j, i]
        return pltpu.make_async_remote_copy(
            src_ref=source,
            dst_ref=target,
            send_sem=self.send_sem.at[k],
            recv_sem=self.recv_sem.at[k],
            device_id=(flip(self.me, bit), self.other),
            device_id_type=MESH,
        )

    def start(self):
        depth = len(self.plans[0])
        for j in range(depth):
            for h in range(len(self.plans)):
                self.copy(h, j, 0).start()

    def advance(self, j):
        for i in range(len(self.plans[0][j][1])):
            for h, stages in enumerate(self.plans):
                self.copy(h, j, i).wait_recv()
                slot = stages[j][2][i]
                for later in range(j + 1, len(stages)):
                    self.copy(h, later, stages[later][1].index(slot)).start()

    def finish(self):
        for h, j, i in self.ids:
            self.copy(h, j, i).wait_send()


class LineGather:
    def __init__(self, sems, size, subs):
        self.size, self.subs = size, subs
        self.ids = {
            (way, s, u): sems.take()
            for way in (0, 1)
            for s in range(size - 1)
            for u in range(subs)
        }

    def bind(self, me, other, own, window, send_sem, recv_sem):
        self.me, self.other, self.own, self.window = me, other, own, window
        self.send_sem, self.recv_sem = send_sem, recv_sem
        return self

    def copy(self, way, s, u):
        block = self.me - s if way == 0 else self.me + s
        target = self.window(block, u)
        k = self.ids[way, s, u]
        return pltpu.make_async_remote_copy(
            src_ref=self.own(u) if s == 0 else target,
            dst_ref=target,
            send_sem=self.send_sem.at[k],
            recv_sem=self.recv_sem.at[k],
            device_id=(self.other, self.me + 1 if way == 0 else self.me - 1),
            device_id_type=MESH,
        )

    def sends(self, way, s):
        if way == 0:
            return (self.me >= s) & (self.me < self.size - 1)
        return (self.me + s < self.size) & (self.me > 0)

    def gets(self, way, s):
        if way == 0:
            return self.me - 1 - s >= 0
        return self.me + 1 + s < self.size

    def start(self, u):
        for way in (0, 1):

            @pl.when(self.sends(way, 0))
            def _():
                self.copy(way, 0, u).start()

    def advance(self, s, u):
        for way in (0, 1):

            @pl.when(self.gets(way, s))
            def _():
                self.copy(way, s, u).wait_recv()

            if s + 1 < self.size - 1:

                @pl.when(self.sends(way, s + 1))
                def _():
                    self.copy(way, s + 1, u).start()

    def finish(self):
        for way, s, u in self.ids:

            @pl.when(self.sends(way, s))
            def _():
                self.copy(way, s, u).wait_send()


def greet(dp, me, tensor, line, wide=False):
    barrier = pltpu.get_barrier_semaphore()

    def hello(a, b):
        pl.semaphore_signal(barrier, inc=1, device_id=(a, b), device_id_type=MESH)

    if wide:
        for r in range(1, dp):
            hello(relative(me, r), line)
        for k in range(1, tensor):
            hello(me, lax.rem(line + k, tensor))
        pl.semaphore_wait(barrier, dp + tensor - 2)
        return
    bits = dp.bit_length() - 1
    for bit in range(bits):
        hello(flip(me, bit), line)

    @pl.when(line > 0)
    def _():
        hello(me, line - 1)

    @pl.when(line < tensor - 1)
    def _():
        hello(me, line + 1)

    left, right = jnp.minimum(line, 1), jnp.minimum(tensor - 1 - line, 1)
    pl.semaphore_wait(barrier, bits + left + right)


def orders_of(dp):
    bits = list(range(1, dp.bit_length() - 1))
    return [bits + [0], bits[::-1] + [0]]


def gather_call(dp, tensor, hidden, cotangent, w_qkv, w_dense, w_fc1, w_fc2, vectors):
    rows, width = hidden.shape
    local = w_qkv.shape[2]
    hidden_units = w_fc1.shape[1]
    part = width // dp
    sems = Sems()
    orders = orders_of(dp)
    plan_vec = CubeGather(sems, orders[:1])
    plan_qkv, plan_dense, plan_fc1, plan_fc2 = (CubeGather(sems, orders) for _ in range(4))
    plan_n, plan_c = LineGather(sems, tensor, 2), LineGather(sems, tensor, 2)

    def kernel(
        x_ref, c_ref, wq_ref, wd_ref, w1_ref, w2_ref, vec_ref,
        gq_ref, gd_ref, g1_ref, g2_ref, gn_ref, gc_ref, gvec_ref,
        x_buf, n_buf, vec_buf, send_sem, recv_sem, local_sem,
    ):
        me, line = lax.axis_index("dp"), lax.axis_index("tensor")
        half = part // 2

        def cols(a):
            return pl.ds(pl.multiple_of(a * part, part), part)

        def half_rows(a, h):
            return pl.ds(pl.multiple_of(a * part + h * half, half), half)

        def tok(b, u):
            return pl.ds(pl.multiple_of(b * rows + u * (rows // 2), rows // 2), rows // 2)

        def sub(u):
            return pl.ds(u * (rows // 2), rows // 2)

        def piece(n, h):
            return pl.ds(h * (n // 2), n // 2)

        pair = (send_sem, recv_sem)
        vec = plan_vec.bind(me, line, lambda h: vec_ref, lambda a, h: vec_buf.at[:, cols(a)], *pair)
        qkv = plan_qkv.bind(
            me, line,
            lambda h: wq_ref.at[:, pl.ds(h * half, half), :],
            lambda a, h: gq_ref.at[:, half_rows(a, h), :], *pair)
        fc1 = plan_fc1.bind(
            me, line,
            lambda h: w1_ref.at[pl.ds(h * half, half), :],
            lambda a, h: g1_ref.at[half_rows(a, h), :], *pair)
        dense = plan_dense.bind(
            me, line,
            lambda h: wd_ref.at[piece(local, h), :],
            lambda a, h: gd_ref.at[piece(local, h), cols(a)], *pair)
        fc2 = plan_fc2.bind(
            me, line,
            lambda h: w2_ref.at[piece(hidden_units, h), :],
            lambda a, h: g2_ref.at[piece(hidden_units, h), cols(a)], *pair)
        norm = plan_n.bind(
            line, me, lambda u: n_buf.at[sub(u)], lambda b, u: gn_ref.at[tok(b, u)], *pair)
        cot = plan_c.bind(
            line, me, lambda u: c_ref.at[sub(u)], lambda b, u: gc_ref.at[tok(b, u)], *pair)

        keep = [
            (x_ref, x_buf),
            (vec_ref, vec_buf.at[:, cols(me)]),
            (wq_ref, gq_ref.at[:, pl.ds(pl.multiple_of(me * part, part), part), :]),
            (w1_ref, g1_ref.at[pl.ds(pl.multiple_of(me * part, part), part), :]),
            (wd_ref, gd_ref.at[:, cols(me)]),
            (w2_ref, g2_ref.at[:, cols(me)]),
            (c_ref, gc_ref.at[pl.ds(pl.multiple_of(line * rows, rows), rows), :]),
        ]
        keeps = [
            pltpu.make_async_copy(a, b, local_sem.at[k]) for k, (a, b) in enumerate(keep)
        ]
        keeps[0].start()
        greet(dp, me, tensor, line)
        vec.start()
        qkv.start()
        for copy in keeps[1:]:
            copy.start()
        stages = dp.bit_length() - 1
        for j in range(stages):
            vec.advance(j)
        keeps[0].wait()
        keeps[1].wait()

        @pl.loop(0, rows, step=32)
        def _(r):
            x = x_buf[pl.ds(r, 32), :].astype(f32)
            centred = x - jnp.mean(x, -1, keepdims=True)
            spread = jnp.mean(centred * centred, -1, keepdims=True)
            unit = centred * lax.rsqrt(spread + layer_eps)
            n_buf[pl.ds(r, 32), :] = (unit * vec_buf[0:1, :] + vec_buf[1:2, :]).astype(bf16)

        norm.start(0)
        norm.start(1)
        own_n = pltpu.make_async_copy(
            n_buf, gn_ref.at[pl.ds(pl.multiple_of(line * rows, rows), rows), :], local_sem.at[len(keep)])
        own_n.start()
        gvec_ref[...] = vec_buf[...]
        qkv.advance(0)
        fc1.start()
        norm.advance(0, 0)
        for j in range(1, stages - 1):
            qkv.advance(j)
        norm.advance(0, 1)
        fc1.advance(0)
        dense.start()
        fc2.start()
        qkv.advance(stages - 1)
        norm.advance(1, 0)
        norm.advance(1, 1)
        cot.start(0)
        cot.start(1)
        for j in range(1, stages - 1):
            fc1.advance(j)
        dense.advance(0)
        norm.advance(2, 0)
        norm.advance(2, 1)
        fc1.advance(stages - 1)
        fc2.advance(0)
        cot.advance(0, 0)
        for j in range(1, stages - 1):
            dense.advance(j)
        cot.advance(0, 1)
        for j in range(1, stages - 1):
            fc2.advance(j)
        dense.advance(stages - 1)
        fc2.advance(stages - 1)
        for s in (1, 2):
            for u in (0, 1):
                cot.advance(s, u)
        for copy in keeps[2:]:
            copy.wait()
        own_n.wait()
        for plan in (vec, qkv, fc1, dense, fc2, norm, cot):
            plan.finish()

    tokens = rows * tensor
    return pl.pallas_call(
        kernel,
        out_shape=(
            jax.ShapeDtypeStruct((3, width, local), bf16),
            jax.ShapeDtypeStruct((local, width), bf16),
            jax.ShapeDtypeStruct((width, hidden_units), bf16),
            jax.ShapeDtypeStruct((hidden_units, width), bf16),
            jax.ShapeDtypeStruct((tokens, width), bf16),
            jax.ShapeDtypeStruct((tokens, width), bf16),
            jax.ShapeDtypeStruct((8, width), f32),
        ),
        in_specs=[ANY] * 7,
        out_specs=(ANY,) * 6 + (VMEM,),
        scratch_shapes=[
            pltpu.VMEM((rows, width), bf16),
            pltpu.VMEM((rows, width), bf16),
            pltpu.VMEM((8, width), f32),
            pltpu.SemaphoreType.DMA((sems.count,)),
            pltpu.SemaphoreType.DMA((sems.count,)),
            pltpu.SemaphoreType.DMA((8,)),
        ],
        compiler_params=pltpu.CompilerParams(
            collective_id=0, has_side_effects=True, vmem_limit_bytes=VMEM_LIMIT
        ),
        name="gather",
    )(hidden, cotangent, w_qkv, w_dense, w_fc1, w_fc2, vectors)


def normalize(x, gain, bias):
    centred = x - jnp.mean(x, -1, keepdims=True)
    spread = jnp.mean(centred * centred, -1, keepdims=True)
    unit = centred * lax.rsqrt(spread + layer_eps)
    return (unit * gain + bias).astype(bf16)


def gather_plain(hidden, cotangent, w_qkv, w_dense, w_fc1, w_fc2, vectors):
    vec = lax.all_gather(vectors, "dp", axis=1, tiled=True)
    normed = normalize(hidden.astype(f32), vec[0:1], vec[1:2])
    return (
        lax.all_gather(w_qkv, "dp", axis=1, tiled=True),
        lax.all_gather(w_dense, "dp", axis=1, tiled=True),
        lax.all_gather(w_fc1, "dp", axis=0, tiled=True),
        lax.all_gather(w_fc2, "dp", axis=1, tiled=True),
        lax.all_gather(normed, "tensor", axis=0, tiled=True),
        lax.all_gather(cotangent, "tensor", axis=0, tiled=True),
        vec,
    )


class ChipReduce:
    COUNT = 6

    def __init__(self, sems):
        self.ids = [sems.take() for _ in range(self.COUNT)]

    def bind(self, me, other, parts, landing, send_sem, recv_sem):
        self.me, self.other, self.parts, self.landing = me, other, parts, landing
        self.send_sem, self.recv_sem = send_sem, recv_sem
        self.half = parts.shape[-1] // 2
        return self

    def view(self, r, h):
        return self.parts.at[r, :, pl.ds(h * self.half, self.half)]

    def copy(self, slot):
        r, h, bit = [(2, 0, 2), (3, 0, 2), (1, 0, 1), (1, 1, 1), (3, 1, 1), (2, 1, 2)][slot]
        k = self.ids[slot]
        return pltpu.make_async_remote_copy(
            src_ref=self.view(r, h),
            dst_ref=self.landing.at[slot],
            send_sem=self.send_sem.at[k],
            recv_sem=self.recv_sem.at[k],
            device_id=(flip(self.me, bit), self.other),
            device_id_type=MESH,
        )

    def start(self, r):
        for slot in {3: (1, 4), 2: (0,), 1: (3,), 0: ()}[r]:
            self.copy(slot).start()

    def middle(self):
        for slot, r, h, last in ((1, 1, 0, 2), (4, 2, 1, 5)):
            self.copy(slot).wait_recv()
            view = self.view(r, h)
            view[...] = (view[...].astype(f32) + self.landing[slot].astype(f32)).astype(bf16)
            self.copy(last).start()

    def final(self):
        for h in (0, 1):
            for slot in ((0, 2), (3, 5))[h]:
                self.copy(slot).wait_recv()
            a, b = ((0, 2), (3, 5))[h]
            view = self.view(0, h)
            total = view[...].astype(f32) + self.landing[a].astype(f32) + self.landing[b].astype(f32)
            view[...] = total.astype(bf16)

    def finish(self):
        for slot in range(self.COUNT):
            self.copy(slot).wait_send()


class LineReduce:
    def __init__(self, sems, size):
        self.size = size
        self.ids = {(way, i): sems.take() for way in (0, 1) for i in range(size - 1)}

    def bind(self, me, other, own, landing, send_sem, recv_sem):
        self.me, self.other, self.own, self.landing = me, other, own, landing
        self.send_sem, self.recv_sem = send_sem, recv_sem
        return self

    def target(self, way, i):
        return self.size - 1 - i if way == 0 else i

    def copy(self, way, i, edge):
        k = self.ids[way, i]
        here = self.landing.at[way, i]
        return pltpu.make_async_remote_copy(
            src_ref=self.own(self.target(way, i)) if edge else here,
            dst_ref=here,
            send_sem=self.send_sem.at[k],
            recv_sem=self.recv_sem.at[k],
            device_id=(self.other, self.me + 1 if way == 0 else self.me - 1),
            device_id_type=MESH,
        )

    def edge(self, way):
        return self.me == (0 if way == 0 else self.size - 1)

    def passes(self, way, i):
        d = self.target(way, i)
        return (self.me > 0) & (self.me < d) if way == 0 else (self.me < self.size - 1) & (self.me > d)

    def start(self, way, i):
        @pl.when(self.edge(way))
        def _():
            self.copy(way, i, True).start()

    def advance(self, step, add):
        for way in (0, 1):
            steps_from_edge = self.me if way == 0 else self.size - 1 - self.me
            for i in range(step):

                @pl.when(self.passes(way, i) & (steps_from_edge == step - i))
                def _():
                    self.copy(way, i, False).wait_recv()
                    add(self.landing.at[way, i], self.own(self.target(way, i)))
                    self.copy(way, i, False).start()

    def arrive(self):
        for way in (0, 1):
            for i in range(self.size - 1):

                @pl.when(self.me == self.target(way, i))
                def _():
                    self.copy(way, i, False).wait_recv()

    def finish(self):
        for way, i in self.ids:

            @pl.when(self.edge(way))
            def _():
                self.copy(way, i, True).wait_send()

            @pl.when(self.passes(way, i))
            def _():
                self.copy(way, i, False).wait_send()

    def total(self, own, rows):
        last = self.size - 1
        value = own.astype(f32)
        lefts = jnp.clip(last - self.me, 0, last - 1)
        rights = jnp.clip(self.me, 0, last - 1)
        from_left = self.landing[0, lefts, rows, :].astype(f32)
        from_right = self.landing[1, rights, rows, :].astype(f32)
        value = value + jnp.where(self.me > 0, from_left, 0.0)
        return value + jnp.where(self.me < last, from_right, 0.0)


def add_into(landing, own):
    rows = landing.shape[0]

    @pl.loop(0, rows, step=64)
    def _(r):
        at = pl.ds(r, 64)
        landing[at, :] = (landing[at, :].astype(f32) + own[at, :].astype(f32)).astype(bf16)


def first_call(dp, tensor, arrays):
    hidden, vec, branches, grad_out, act, slope, attn, w_fc2 = arrays
    rows, width = hidden.shape
    tokens, units = act.shape
    local = attn.shape[1]
    part = width // dp
    chips = dp // 2
    sems = Sems()
    reduce_fc2, reduce_dense = ChipReduce(sems), ChipReduce(sems)
    line_out = LineReduce(sems, tensor)
    swaps = [sems.take() for _ in range(chips + 2)]

    def kernel(
        x_ref, vec_ref, b_ref, c_ref, a_ref, d_ref, t_ref, w2_ref,
        out_ref, gp_ref, sum_ref, s2_out, sd_out,
        x_buf, c_buf, cx_buf, a_buf, ax_buf, t_buf, tx_buf, w2_buf, d_buf, own_buf,
        s2, sd, r2, rd, rz, send_sem, recv_sem, local_sem,
    ):
        me, line = lax.axis_index("dp"), lax.axis_index("tensor")
        twin = flip(me, 0)

        def cols(a):
            return pl.ds(pl.multiple_of(a * part, part), part)

        def block(d):
            return pl.ds(pl.multiple_of(d * rows, rows), rows)

        pair = (send_sem, recv_sem)
        fc2 = reduce_fc2.bind(me, line, s2, r2, *pair)
        dense = reduce_dense.bind(me, line, sd, rd, *pair)
        outs = line_out.bind(line, me, lambda d: b_ref.at[pl.ds(d * rows, rows), :], rz, *pair)

        def swap(k, source, target):
            return pltpu.make_async_remote_copy(
                src_ref=source, dst_ref=target,
                send_sem=send_sem.at[swaps[k]], recv_sem=recv_sem.at[swaps[k]],
                device_id=(twin, line), device_id_type=MESH)

        crossing = [
            swap(r, c_ref.at[:, cols(relative(twin, r << 1))], cx_buf.at[r]) for r in range(chips)
        ] + [swap(chips, a_ref, ax_buf), swap(chips + 1, t_ref, tx_buf)]
        loads = [
            pltpu.make_async_copy(a, b, local_sem.at[k])
            for k, (a, b) in enumerate([
                (c_ref, c_buf), (a_ref, a_buf), (t_ref, t_buf), (w2_ref, w2_buf), (d_ref, d_buf),
                (x_ref, x_buf), (b_ref.at[block(line), :], own_buf),
            ])
        ]
        loads[0].start()
        loads[1].start()
        greet(dp, me, tensor, line)
        for copy in (crossing[3], crossing[chips]):
            copy.start()
        for i in range(tensor - 1):
            outs.start(0, i)
            outs.start(1, i)
        for copy in crossing[:3] + crossing[chips + 1 :]:
            copy.start()
        for copy in loads[2:]:
            copy.start()
        loads[0].wait()
        loads[1].wait()
        crossing[chips].wait_recv()

        @pl.loop(0, chips)
        def _(i):
            r = chips - 1 - i
            slot = me + 2 * ((r % 2) * (1 - 2 * (lax.div(me, 2) % 2))) + 4 * (
                lax.div(r, 2) * (1 - 2 * (lax.div(me, 4) % 2)))
            for k in range(chips):

                @pl.when(r == k)
                def _():
                    crossing[k].wait_recv()

            @pl.loop(0, units, step=1024)
            def _(n):
                at = pl.ds(pl.multiple_of(n, 1024), 1024)
                value = dot_tn(c_buf[:, cols(slot)], a_buf[:, at])
                value = value + dot_tn(cx_buf[r], ax_buf[:, at])
                s2[r, :, at] = value.astype(bf16)

            for k in range(1, chips):

                @pl.when(r == k)
                def _():
                    fc2.start(k)

        loads[2].wait()
        crossing[chips + 1].wait_recv()

        @pl.loop(0, chips)
        def _(i):
            r = chips - 1 - i
            slot = me + 2 * ((r % 2) * (1 - 2 * (lax.div(me, 2) % 2))) + 4 * (
                lax.div(r, 2) * (1 - 2 * (lax.div(me, 4) % 2)))
            value = dot_tn(c_buf[:, cols(slot)], t_buf[...]) + dot_tn(cx_buf[r], tx_buf[...])
            sd[r] = value.astype(bf16)
            for k in range(1, chips):

                @pl.when(r == k)
                def _():
                    dense.start(k)

        loads[3].wait()
        loads[4].wait()

        def slope_tile(n):
            at = pl.ds(pl.multiple_of(n, 512), 512)
            value = dot_nt(c_buf[...], w2_buf[at, :]) * d_buf[:, at].astype(f32)
            value = value.astype(bf16)
            d_buf[:, at] = value
            sum_ref[0:1, at] = jnp.sum(value.astype(f32), 0, keepdims=True)

        @pl.loop(0, units, step=512)
        def _(n):
            slope_tile(n)

        store = pltpu.make_async_copy(d_buf, gp_ref, local_sem.at[len(loads)])
        store.start()

        def add_out(landing, own):
            copy = pltpu.make_async_copy(own, a_buf.at[pl.ds(0, rows), :], local_sem.at[len(loads) + 1])
            copy.start()
            copy.wait()
            add_into(landing, a_buf.at[pl.ds(0, rows), :])

        outs.advance(1, add_out)
        fc2.middle()
        outs.advance(2, add_out)
        dense.middle()
        fc2.final()
        dense.final()
        store2 = pltpu.make_async_copy(s2.at[0], s2_out, local_sem.at[len(loads) + 2])
        stored = pltpu.make_async_copy(sd.at[0], sd_out, local_sem.at[len(loads) + 3])
        store2.start()
        stored.start()
        for copy in loads[5:]:
            copy.wait()
        outs.arrive()

        @pl.loop(0, rows, step=32)
        def _(r):
            at = pl.ds(r, 32)
            total = x_buf[at, :].astype(f32) + outs.total(own_buf[at, :], at) + vec_ref[2:3, :]
            x_buf[at, :] = total.astype(bf16)

        last = pltpu.make_async_copy(x_buf, out_ref, local_sem.at[len(loads) + 4])
        last.start()
        for copy in crossing:
            copy.wait_send()
        for plan in (fc2, dense, outs):
            plan.finish()
        for copy in (store, store2, stored, last):
            copy.wait()

    return pl.pallas_call(
        kernel,
        out_shape=(
            jax.ShapeDtypeStruct((rows, width), bf16),
            jax.ShapeDtypeStruct((tokens, units), bf16),
            jax.ShapeDtypeStruct((8, units), f32),
            jax.ShapeDtypeStruct((part, units), bf16),
            jax.ShapeDtypeStruct((part, local), bf16),
        ),
        in_specs=[ANY, VMEM] + [ANY] * 6,
        out_specs=(ANY, ANY, VMEM, ANY, ANY),
        scratch_shapes=[
            pltpu.VMEM((rows, width), bf16),
            pltpu.VMEM((tokens, width), bf16),
            pltpu.VMEM((chips, tokens, part), bf16),
            pltpu.VMEM((tokens, units), bf16),
            pltpu.VMEM((tokens, units), bf16),
            pltpu.VMEM((tokens, local), bf16),
            pltpu.VMEM((tokens, local), bf16),
            pltpu.VMEM((units, width), bf16),
            pltpu.VMEM((tokens, units), bf16),
            pltpu.VMEM((rows, width), bf16),
            pltpu.VMEM((chips, part, units), bf16),
            pltpu.VMEM((chips, part, local), bf16),
            pltpu.VMEM((6, part, units // 2), bf16),
            pltpu.VMEM((6, part, local // 2), bf16),
            pltpu.VMEM((2, tensor - 1, rows, width), bf16),
            pltpu.SemaphoreType.DMA((sems.count,)),
            pltpu.SemaphoreType.DMA((sems.count,)),
            pltpu.SemaphoreType.DMA((12,)),
        ],
        compiler_params=pltpu.CompilerParams(
            collective_id=1, has_side_effects=True, vmem_limit_bytes=VMEM_LIMIT
        ),
        name="first_back",
    )(*arrays)


def second_call(dp, tensor, arrays):
    hidden, cotangent, vec, sums, normed, grad_pre, dq, dk, dv, w_qkv, w_fc1 = arrays
    rows, width = hidden.shape
    tokens, units = grad_pre.shape
    local = dq.shape[1]
    wide = 3 * local
    part = width // dp
    chips = dp // 2
    sems = Sems()
    reduce_fc1, reduce_qkv = ChipReduce(sems), ChipReduce(sems)
    line_in = LineReduce(sems, tensor)
    swaps = [sems.take() for _ in range(chips + 4)]
    tells = [sems.take() for _ in range(2 * (dp - 1) + tensor - 1)]

    def kernel(
        x_ref, c_ref, vec_ref, sum_ref, n_ref, gp_in, dq_in, dk_in, dv_in, wq_ref, w1_ref,
        hid_ref, s1_out, sq_out, vout_ref, bout_ref,
        x_buf, c_buf, n_buf, nx_buf, gp, gpx, gq, gqx, wq, w1, gn,
        s1, sq, r1, rq, rz, parts, tell_v, tell_b, tell_z, send_sem, recv_sem, local_sem,
    ):
        me, line = lax.axis_index("dp"), lax.axis_index("tensor")
        twin = flip(me, 0)

        def cols(a):
            return pl.ds(pl.multiple_of(a * part, part), part)

        pair = (send_sem, recv_sem)
        fc1 = reduce_fc1.bind(me, line, s1, r1, *pair)
        qkv = reduce_qkv.bind(me, line, sq, rq, *pair)
        ins = line_in.bind(line, me, lambda d: gn.at[pl.ds(d * rows, rows), :], rz, *pair)

        def remote(k, source, target, device):
            return pltpu.make_async_remote_copy(
                src_ref=source, dst_ref=target,
                send_sem=send_sem.at[k], recv_sem=recv_sem.at[k],
                device_id=device, device_id_type=MESH)

        grads_in = (dq_in, dk_in, dv_in)

        def third(i):
            return pl.ds(i * local, local)

        crossing = [
            remote(swaps[r], n_ref.at[:, cols(relative(twin, r << 1))], nx_buf.at[r], (twin, line))
            for r in range(chips)
        ] + [remote(swaps[chips], gp_in, gpx, (twin, line))] + [
            remote(swaps[chips + 1 + i], grads_in[i], gqx.at[:, third(i)], (twin, line))
            for i in range(3)
        ]
        bias_tells = [
            remote(tells[r - 1], sum_ref, tell_b.at[r], (relative(me, r), line)) for r in range(1, dp)
        ]
        vec_tells = [
            remote(tells[dp - 2 + r], parts.at[:, cols(relative(me, r))], tell_v.at[r],
                   (relative(me, r), line))
            for r in range(1, dp)
        ]
        line_tells = [
            remote(tells[2 * dp - 3 + k], tell_z.at[0], tell_z.at[k],
                   (me, lax.rem(line + k, tensor)))
            for k in range(1, tensor)
        ]
        tile = 512
        pieces = (
            [(gp_in, gp)]
            + [(grads_in[i], gq.at[:, third(i)]) for i in range(3)]
            + [(w1_ref.at[pl.ds(n, tile), :], w1.at[pl.ds(n, tile), :]) for n in range(0, width, tile)]
            + [
                (wq_ref.at[i, pl.ds(n, tile), :], wq.at[pl.ds(n, tile), third(i)])
                for n in range(0, width, tile) for i in range(3)
            ]
            + [(n_ref, n_buf), (x_ref, x_buf), (c_ref, c_buf)]
        )
        loads = [pltpu.make_async_copy(a, b, local_sem.at[k]) for k, (a, b) in enumerate(pieces)]
        tiles = width // tile
        for copy in loads[:4]:
            copy.start()
        for n in range(tiles):
            loads[4 + n].start()
            for i in range(3):
                loads[4 + tiles + 3 * n + i].start()
        greet(dp, me, tensor, line, wide=True)
        for copy in loads[4 + 4 * tiles :]:
            copy.start()
        for copy in crossing:
            copy.start()
        for copy in bias_tells:
            copy.start()
        for copy in loads[:4]:
            copy.wait()
        for n in range(tiles):
            loads[4 + n].wait()
            for i in range(3):
                loads[4 + tiles + 3 * n + i].wait()

        upper = lax.div(line, tensor // 2)

        @pl.loop(0, tensor)
        def _(i):
            d = (1 - upper) * (tensor - 1 - i) + upper * i
            at = pl.ds(pl.multiple_of(d * rows, rows), rows)

            @pl.loop(0, width, step=1024)
            def _(n):
                to = pl.ds(pl.multiple_of(n, 1024), 1024)
                value = dot_nt(gp[at, :], w1[to, :]) + dot_nt(gq[at, :], wq[to, :])
                gn[at, to] = value.astype(bf16)

            for k in range(tensor - 1):

                @pl.when(i == k)
                def _():
                    ins.start(0, k)
                    ins.start(1, k)

        loads[4 + 4 * tiles].wait()

        def weight_grad(target, plan, own, crossed, size, step):
            @pl.loop(0, chips)
            def _(i):
                r = chips - 1 - i
                slot = me + 2 * ((r % 2) * (1 - 2 * (lax.div(me, 2) % 2))) + 4 * (
                    lax.div(r, 2) * (1 - 2 * (lax.div(me, 4) % 2)))

                @pl.loop(0, size, step=step)
                def _(n):
                    at = pl.ds(pl.multiple_of(n, step), step)
                    value = dot_tn(n_buf[:, cols(slot)], own[:, at])
                    value = value + dot_tn(nx_buf[r], crossed[:, at])
                    target[r, :, at] = value.astype(bf16)

                for k in range(1, chips):

                    @pl.when(r == k)
                    def _():
                        plan.start(k)

        for copy in crossing:
            copy.wait_recv()
        weight_grad(s1, fc1, gp, gpx, units, 1024)
        ins.advance(1, add_into)
        weight_grad(sq, qkv, gq, gqx, wide, 768)
        ins.advance(2, add_into)
        fc1.middle()
        for copy in bias_tells:
            copy.wait_recv()
        total = sum_ref[...]
        for r in range(1, dp):
            total = total + tell_b[r]
        bout_ref[...] = total
        for copy in loads[5 + 4 * tiles :]:
            copy.wait()
        qkv.middle()
        ins.arrive()
        parts[...] = jnp.zeros_like(parts)

        @pl.loop(0, rows, step=32)
        def _(r):
            at = pl.ds(r, 32)
            x = x_buf[at, :].astype(f32)
            centred = x - jnp.mean(x, -1, keepdims=True)
            inv_std = lax.rsqrt(jnp.mean(centred * centred, -1, keepdims=True) + layer_eps)
            unit = centred * inv_std
            own = pl.ds(pl.multiple_of(line * rows + r, 32), 32)
            grad = ins.total(gn[own, :], at)
            cot = c_buf[at, :].astype(f32)
            scaled = grad * vec_ref[0:1, :]
            first = jnp.mean(scaled, -1, keepdims=True)
            second = jnp.mean(scaled * unit, -1, keepdims=True)
            c_buf[at, :] = (cot + inv_std * (scaled - first - unit * second)).astype(bf16)
            parts[0:1, :] += jnp.sum(grad * unit, 0, keepdims=True)
            parts[1:2, :] += jnp.sum(grad, 0, keepdims=True)
            parts[2:3, :] += jnp.sum(cot, 0, keepdims=True)

        last = pltpu.make_async_copy(c_buf, hid_ref, local_sem.at[len(loads)])
        last.start()
        for copy in vec_tells:
            copy.start()
        fc1.final()
        store1 = pltpu.make_async_copy(s1.at[0], s1_out, local_sem.at[len(loads) + 1])
        store1.start()
        for copy in vec_tells:
            copy.wait_recv()
        total_v = parts[:, cols(me)]
        for r in range(1, dp):
            total_v = total_v + tell_v[r]
        tell_z[0] = total_v
        for copy in line_tells:
            copy.start()
        qkv.final()
        storeq = pltpu.make_async_copy(sq.at[0], sq_out, local_sem.at[len(loads) + 2])
        storeq.start()
        for copy in line_tells:
            copy.wait_recv()
        total_z = tell_z[0]
        for k in range(1, tensor):
            total_z = total_z + tell_z[k]
        vout_ref[...] = total_z
        for copy in crossing + bias_tells + vec_tells + line_tells:
            copy.wait_send()
        for plan in (fc1, qkv, ins):
            plan.finish()
        for copy in (last, store1, storeq):
            copy.wait()

    return pl.pallas_call(
        kernel,
        out_shape=(
            jax.ShapeDtypeStruct((rows, width), bf16),
            jax.ShapeDtypeStruct((part, units), bf16),
            jax.ShapeDtypeStruct((part, wide), bf16),
            jax.ShapeDtypeStruct((8, part), f32),
            jax.ShapeDtypeStruct((8, local), f32),
        ),
        in_specs=[ANY] * 2 + [VMEM] * 2 + [ANY] * 7,
        out_specs=(ANY, ANY, ANY, VMEM, VMEM),
        scratch_shapes=[
            pltpu.VMEM((rows, width), bf16),
            pltpu.VMEM((rows, width), bf16),
            pltpu.VMEM((tokens, width), bf16),
            pltpu.VMEM((chips, tokens, part), bf16),
            pltpu.VMEM((tokens, units), bf16),
            pltpu.VMEM((tokens, units), bf16),
            pltpu.VMEM((tokens, wide), bf16),
            pltpu.VMEM((tokens, wide), bf16),
            pltpu.VMEM((width, wide), bf16),
            pltpu.VMEM((width, units), bf16),
            pltpu.VMEM((tokens, width), bf16),
            pltpu.VMEM((chips, part, units), bf16),
            pltpu.VMEM((chips, part, wide), bf16),
            pltpu.VMEM((6, part, units // 2), bf16),
            pltpu.VMEM((6, part, wide // 2), bf16),
            pltpu.VMEM((2, tensor - 1, rows, width), bf16),
            pltpu.VMEM((8, width), f32),
            pltpu.VMEM((dp, 8, part), f32),
            pltpu.VMEM((dp, 8, local), f32),
            pltpu.VMEM((tensor, 8, part), f32),
            pltpu.SemaphoreType.DMA((sems.count,)),
            pltpu.SemaphoreType.DMA((sems.count,)),
            pltpu.SemaphoreType.DMA((30,)),
        ],
        compiler_params=pltpu.CompilerParams(
            collective_id=2, has_side_effects=True, vmem_limit_bytes=VMEM_LIMIT
        ),
        name="second_back",
    )(*arrays)


def spans_of(length):
    back = -(-(MAX_DOC - 1) // BLOCK)
    spans, at = [], 0
    for i in range(length // BLOCK):
        low = max(0, i - back) * BLOCK
        spans.append((low, (i + 1) * BLOCK, at))
        at += (i + 1) * BLOCK - low
    return spans, at


def turn(x, cosine, sine_lo, sine_hi):
    return x * cosine + pltpu.roll(x, 128 - ROT // 2, 1) * sine_lo + pltpu.roll(x, ROT // 2, 1) * sine_hi


def head_lanes(shape, e):
    lane = lax.broadcasted_iota(jnp.int32, shape, 1)
    return (lane >= e * HD) & (lane < (e + 1) * HD)


def only(x, e):
    return jnp.where(head_lanes(x.shape, e), x, jnp.zeros_like(x))


def attend_kernel(
    q_ref, k_ref, v_ref, bias_ref, cos_ref, slo_ref, shi_ref, segc_ref, segr_ref,
    qs_ref, ks_ref, vs_ref, o_ref, p_ref, mask_ref,
):
    length = q_ref.shape[0]
    spans, _ = spans_of(length)

    @pl.when(pl.program_id(1) == 0)
    def _():
        for i, (low, high, at) in enumerate(spans):
            keys = lax.broadcasted_iota(jnp.int32, (high - low, BLOCK), 0) + low
            queries = lax.broadcasted_iota(jnp.int32, (high - low, BLOCK), 1) + i * BLOCK
            same = segc_ref[low:high, :] == segr_ref[:, i * BLOCK : (i + 1) * BLOCK]
            mask_ref[at : at + high - low, :] = jnp.where((keys <= queries) & same, 0.0, -1e30)

    cosine, slo, shi = cos_ref[...], slo_ref[...], shi_ref[...]
    query = turn(q_ref[...] + bias_ref[0:1, :], cosine, slo, shi).astype(bf16) * bf16(HD**-0.5)
    key = turn(k_ref[...] + bias_ref[1:2, :], cosine, slo, shi).astype(bf16)
    value = (v_ref[...] + bias_ref[2:3, :]).astype(bf16)
    qs_ref[...] = query
    ks_ref[...] = key
    vs_ref[...] = value
    heads = 128 // HD
    for i, (low, high, at) in enumerate(spans):
        q_i = query[i * BLOCK : (i + 1) * BLOCK]
        total = jnp.zeros((BLOCK, 128), f32)
        for e in range(heads):
            scores = dot_nt(only(key[low:high], e), q_i) + mask_ref[at : at + high - low, :]
            exponent = jnp.exp(scores - jnp.max(scores, 0, keepdims=True))
            inverse = 1.0 / jnp.sum(exponent, 0, keepdims=True)
            probs = (exponent * inverse).astype(bf16)
            p_ref[e, at : at + high - low, :] = probs
            total = total + dot_tn(probs, only(value[low:high], e))
        o_ref[i * BLOCK : (i + 1) * BLOCK, :] = total.astype(bf16)


def attend(q, k, v, qkv_bias, tables, segments, rows):
    tokens, local = q.shape
    length = tokens // rows
    pairs = local // 128
    _, stored = spans_of(length)
    block = pl.BlockSpec((length, 128), lambda r, h: (r, h))
    table = pl.BlockSpec((length, 128), lambda r, h: (r, 0))
    shape = jax.ShapeDtypeStruct((tokens, local), bf16)
    return pl.pallas_call(
        attend_kernel,
        grid=(rows, pairs),
        out_shape=(shape,) * 4 + (jax.ShapeDtypeStruct((rows, local // HD, stored, BLOCK), bf16),),
        in_specs=[block] * 3
        + [pl.BlockSpec((8, 128), lambda r, h: (0, h))]
        + [table] * 3
        + [
            pl.BlockSpec((length, 1), lambda r, h: (r, 0)),
            pl.BlockSpec((pl.Squeezed(), 1, length), lambda r, h: (r, 0, 0)),
        ],
        out_specs=(block,) * 4
        + (pl.BlockSpec((pl.Squeezed(), 128 // HD, stored, BLOCK), lambda r, h: (r, h, 0, 0)),),
        scratch_shapes=[pltpu.VMEM((stored, BLOCK), f32)],
        compiler_params=pltpu.CompilerParams(vmem_limit_bytes=VMEM_LIMIT),
        cost_estimate=pl.CostEstimate(
            flops=16 * tokens * 768 * local, bytes_accessed=24 << 20, transcendentals=0
        ),
        name="attend",
    )(q, k, v, qkv_bias, *tables, segments.reshape(tokens, 1), segments.reshape(rows, 1, length))


def attend_back_kernel(
    q_ref, k_ref, v_ref, g_ref, o_ref, p_ref, cos_ref, slo_ref, shi_ref,
    dq_ref, dk_ref, dv_ref, bias_ref, kacc_ref, vacc_ref,
):
    length = q_ref.shape[0]
    spans, _ = spans_of(length)
    heads = 128 // HD
    grad = g_ref[...]
    inner = grad.astype(f32) * o_ref[...].astype(f32)
    lane = lax.broadcasted_iota(jnp.int32, (8, 128), 1)
    row = lax.broadcasted_iota(jnp.int32, (8, 128), 0)
    pick = jnp.where(lax.div(lane, HD) == row, 1.0, 0.0)
    delta = lax.dot_general(
        pick, inner, (((1,), (1,)), ((), ())),
        precision=lax.Precision.HIGHEST, preferred_element_type=f32)
    query, key, value = q_ref[...], k_ref[...], v_ref[...]
    kacc_ref[...] = jnp.zeros_like(kacc_ref)
    vacc_ref[...] = jnp.zeros_like(vacc_ref)
    cosine, slo, shi = cos_ref[...], slo_ref[...], shi_ref[...]
    first = jnp.zeros((1, 128), f32)
    for i, (low, high, at) in enumerate(spans):
        mine = slice(i * BLOCK, (i + 1) * BLOCK)
        g_i, q_i = grad[mine], query[mine]
        dq = jnp.zeros((BLOCK, 128), f32)
        ps, dss = [], []
        for e in range(heads):
            probs = p_ref[e, at : at + high - low, :]
            dprobs = dot_nt(only(value[low:high], e), g_i)
            ds = (probs.astype(f32) * (dprobs - delta[e : e + 1, mine])).astype(bf16)
            dq = dq + dot_tn(ds, only(key[low:high], e))
            ps.append(probs)
            dss.append(ds)
        g_cat = jnp.concatenate([only(g_i, e) for e in range(heads)], 0)
        q_cat = jnp.concatenate([only(q_i, e) for e in range(heads)], 0)
        vacc_ref[low:high, :] += dot_nn(jnp.concatenate(ps, 1), g_cat)
        kacc_ref[low:high, :] += dot_nn(jnp.concatenate(dss, 1), q_cat)
        dq = dq * f32(HD**-0.5)
        dq = turn(dq, cosine[mine], -slo[mine], -shi[mine]).astype(bf16)
        dq_ref[mine, :] = dq
        first = first + jnp.sum(dq.astype(f32), 0, keepdims=True)
    dk = turn(kacc_ref[...], cosine, -slo, -shi).astype(bf16)
    dv = vacc_ref[...].astype(bf16)
    dk_ref[...] = dk
    dv_ref[...] = dv
    sums = [first, jnp.sum(dk.astype(f32), 0, keepdims=True), jnp.sum(dv.astype(f32), 0, keepdims=True)]
    sums = jnp.concatenate(sums + [jnp.zeros((5, 128), f32)], 0)

    @pl.when(pl.program_id(1) == 0)
    def _():
        bias_ref[...] = sums

    @pl.when(pl.program_id(1) > 0)
    def _():
        bias_ref[...] += sums


def attend_back(q, k, v, g, o, probs, tables, rows):
    tokens, local = q.shape
    length = tokens // rows
    pairs = local // 128
    stored = probs.shape[2]
    block = pl.BlockSpec((length, 128), lambda h, r: (r, h))
    table = pl.BlockSpec((length, 128), lambda h, r: (r, 0))
    shape = jax.ShapeDtypeStruct((tokens, local), bf16)
    return pl.pallas_call(
        attend_back_kernel,
        grid=(pairs, rows),
        out_shape=(shape,) * 3 + (jax.ShapeDtypeStruct((8, local), f32),),
        in_specs=[block] * 5
        + [pl.BlockSpec((pl.Squeezed(), 128 // HD, stored, BLOCK), lambda h, r: (r, h, 0, 0))]
        + [table] * 3,
        out_specs=(block,) * 3 + (pl.BlockSpec((8, 128), lambda h, r: (0, h)),),
        scratch_shapes=[pltpu.VMEM((length, 128), f32)] * 2,
        compiler_params=pltpu.CompilerParams(vmem_limit_bytes=VMEM_LIMIT),
        cost_estimate=pl.CostEstimate(
            flops=32 * tokens * 768 * local, bytes_accessed=24 << 20, transcendentals=0
        ),
        name="attend_back",
    )(q, k, v, g, o, probs, *tables)


def rotary_tables(segments):
    rows, length = segments.shape
    index = jnp.arange(length, dtype=jnp.int32)[None]
    start = jnp.zeros_like(segments)
    for number in range(1, 4):
        start = jnp.where(segments == number, jnp.sum(segments < number, -1, keepdims=True), start)
    position = (index - start).astype(f32).reshape(rows * length, 1)
    lane = jnp.arange(128, dtype=jnp.int32) % HD
    exponent = (2 * (lane % (ROT // 2))).astype(f32) / ROT
    angle = position * (1.0 / 10000.0**exponent)[None]
    cosine, sine = jnp.cos(angle), jnp.sin(angle)
    low, high = lane < ROT // 2, (lane >= ROT // 2) & (lane < ROT)
    return (
        jnp.where(lane < ROT, cosine, 1.0),
        jnp.where(low, -sine, 0.0),
        jnp.where(high, sine, 0.0),
    )


def matmul(a, b):
    return jnp.dot(a, b, preferred_element_type=f32)


def on_device(
    dp, tensor, fast,
    hidden_in, segments, ln_gain, ln_bias, qkv_weight, qkv_bias, dense_weight, dense_bias,
    fc1_weight, fc1_bias, fc2_weight, fc2_bias, cotangent,
):
    seqs = segments.shape[0]
    local = qkv_weight.shape[2]
    vectors = jnp.stack([ln_gain.astype(f32), ln_bias.astype(f32), dense_bias.astype(f32) + fc2_bias.astype(f32)])
    vectors = jnp.pad(vectors, ((0, 5), (0, 0)))
    mine = (
        hidden_in, cotangent, qkv_weight.transpose(1, 0, 2),
        dense_weight, fc1_weight, fc2_weight, vectors,
    )
    gathered = gather_call(dp, tensor, *mine) if fast else gather_plain(*mine)
    w_qkv, w_dense, w_fc1, w_fc2, normed, grad_out, vec = gathered
    gain, out_bias = vec[0:1], vec[2:3]
    tables = rotary_tables(segments)
    bias = jnp.pad(qkv_bias.astype(f32), ((0, 5), (0, 0)))
    query, key, value, attn_vec, probs = attend(
        *(matmul(normed, w_qkv[i]) for i in range(3)), bias, tables, segments, seqs
    )
    pre_act = matmul(normed, w_fc1) + fc1_bias.astype(f32)
    act_vals, gelu_pull = jax.vjp(lambda pre: jax.nn.gelu(pre, approximate=True), pre_act)
    act_vals = act_vals.astype(bf16)
    slope = gelu_pull(jnp.ones_like(pre_act))[0].astype(bf16)
    branches = matmul(attn_vec, w_dense) + matmul(act_vals, w_fc2)
    grad_attn = matmul(grad_out, w_dense.T).astype(bf16)
    *grads, qkv_sums = attend_back(query, key, value, grad_attn, attn_vec, probs, tables, seqs)
    if fast:
        out, grad_pre, fc1_sums, sent_fc2, sent_dense = first_call(
            dp, tensor,
            (hidden_in, vec, branches.astype(bf16), grad_out, act_vals, slope, attn_vec, w_fc2))
        sums = jnp.concatenate([fc1_sums[0].reshape(4, local), qkv_sums[:3], jnp.zeros((1, local), f32)], 0)
        hidden_grad, sent_fc1, sent_qkv, vec_sums, all_sums = second_call(
            dp, tensor,
            (hidden_in, cotangent, vec, sums, normed, grad_pre, *grads, w_qkv, w_fc1))
        quarter = vec_sums.shape[1] // tensor
        at = lax.axis_index("tensor") * quarter
        small = lax.dynamic_slice(vec_sums, (0, at), (3, quarter))
        return (
            out,
            hidden_grad,
            small[0],
            small[1],
            sent_qkv.astype(f32).reshape(-1, 3, local),
            all_sums[4:7],
            sent_dense.T.astype(f32),
            small[2],
            sent_fc1.astype(f32),
            all_sums[:4].reshape(-1),
            sent_fc2.T.astype(f32),
            small[2],
        )

    resid_in = hidden_in.astype(f32)
    cot_float = cotangent.astype(f32)
    centred = resid_in - jnp.mean(resid_in, -1, keepdims=True)
    spread = jnp.mean(centred * centred, -1, keepdims=True)
    inv_std = lax.rsqrt(spread + layer_eps)
    unit_rows = centred * inv_std
    summed = lax.psum_scatter(branches.astype(bf16), "tensor", scatter_dimension=0, tiled=True)
    out = (resid_in + summed.astype(f32) + out_bias).astype(bf16)
    out_bias_part = jnp.sum(cot_float, 0)
    grad_fc2 = matmul(act_vals.T, grad_out)
    grad_dense = matmul(attn_vec.T, grad_out)
    grad_pre = (matmul(grad_out, w_fc2.T) * slope.astype(f32)).astype(bf16)
    fc1_bias_part = jnp.sum(grad_pre.astype(f32), 0)
    grad_fc1 = matmul(normed.T, grad_pre)
    grad_wqkv = jnp.stack([matmul(normed.T, g) for g in grads])
    grad_normed = matmul(grad_pre, w_fc1.T) + sum(matmul(g, w.T) for g, w in zip(grads, w_qkv))
    sent_qkv, sent_dense, sent_fc1, sent_fc2 = (
        lax.psum_scatter(grad_wqkv.astype(bf16), "dp", scatter_dimension=1, tiled=True),
        lax.psum_scatter(grad_dense.astype(bf16), "dp", scatter_dimension=1, tiled=True),
        lax.psum_scatter(grad_fc1.astype(bf16), "dp", scatter_dimension=0, tiled=True),
        lax.psum_scatter(grad_fc2.astype(bf16), "dp", scatter_dimension=1, tiled=True),
    )
    grad_local = lax.psum_scatter(
        grad_normed.astype(bf16), "tensor", scatter_dimension=0, tiled=True
    ).astype(f32)
    gain_part = jnp.sum(grad_local * unit_rows, 0)
    beta_part = jnp.sum(grad_local, 0)
    scaled_grad = grad_local * gain
    first_mean = jnp.mean(scaled_grad, -1, keepdims=True)
    second_mean = jnp.mean(scaled_grad * unit_rows, -1, keepdims=True)
    hidden_grad = (
        cot_float + inv_std * (scaled_grad - first_mean - unit_rows * second_mean)
    ).astype(bf16)
    gain_grad, beta_grad, out_bias_grad = (
        lax.psum_scatter(gain_part, ("dp", "tensor"), scatter_dimension=0, tiled=True),
        lax.psum_scatter(beta_part, ("dp", "tensor"), scatter_dimension=0, tiled=True),
        lax.psum_scatter(out_bias_part, ("dp", "tensor"), scatter_dimension=0, tiled=True),
    )
    qkv_bias_grad, fc1_bias_grad = lax.psum((qkv_sums[:3], fc1_bias_part), "dp")
    return (
        out,
        hidden_grad,
        gain_grad,
        beta_grad,
        sent_qkv.transpose(1, 0, 2).astype(f32),
        qkv_bias_grad,
        sent_dense.astype(f32),
        out_bias_grad,
        sent_fc1.astype(f32),
        fc1_bias_grad,
        sent_fc2.astype(f32),
        out_bias_grad,
    )


def solution(mesh):
    dp, tensor = mesh.shape["dp"], mesh.shape["tensor"]
    fast = dp == 8 and tensor == 4
    placed = (
        P(("dp", "tensor"), None),
        P("dp", None),
        P("dp"),
        P("dp"),
        P("dp", None, "tensor"),
        P(None, "tensor"),
        P("tensor", "dp"),
        P("dp"),
        P("dp", "tensor"),
        P("tensor"),
        P("tensor", "dp"),
        P("dp"),
        P(("dp", "tensor"), None),
    )
    return jax.shard_map(
        functools.partial(on_device, dp, tensor, fast),
        mesh=mesh,
        in_specs=placed,
        out_specs=(
            P(("dp", "tensor"), None),
            P(("dp", "tensor"), None),
            P(("dp", "tensor")),
            P(("dp", "tensor")),
            P("dp", None, "tensor"),
            P(None, "tensor"),
            P("tensor", "dp"),
            P(("dp", "tensor")),
            P("dp", "tensor"),
            P("tensor"),
            P("tensor", "dp"),
            P(("dp", "tensor")),
        ),
        check_vma=False,
    )
```

```python
import functools

import jax
import jax.numpy as jnp
from jax import lax
from jax.experimental import pallas as pl
from jax.experimental.pallas import tpu as pltpu
from jax.sharding import PartitionSpec as P

HD = 64
ROT = 32
BLOCK = 256
MAX_DOC = 512
VMEM_LIMIT = 66_000_000
MESH = pl.DeviceIdType.MESH
ANY = pl.BlockSpec(memory_space=pl.ANY)
VMEM = pl.BlockSpec(memory_space=pltpu.VMEM)

layer_eps = 1e-05
f32 = jnp.float32
bf16 = jnp.bfloat16


def dot_nn(a, b):
    return lax.dot_general(a, b, (((1,), (0,)), ((), ())), preferred_element_type=f32)


def dot_nt(a, b):
    return lax.dot_general(a, b, (((1,), (1,)), ((), ())), preferred_element_type=f32)


def dot_tn(a, b):
    return lax.dot_general(a, b, (((0,), (0,)), ((), ())), preferred_element_type=f32)


def flip(index, bit):
    step = 1 << bit
    return index + step * (1 - 2 * (lax.div(index, step) % 2))


def relative(index, offset):
    bit = 0
    while offset >> bit:
        if (offset >> bit) & 1:
            index = flip(index, bit)
        bit += 1
    return index


def stages_of(order):
    held, stages = [0], []
    for bit in order:
        got = [r ^ (1 << bit) for r in held]
        stages.append((bit, list(held), got))
        held = held + got
    return stages


class Sems:
    def __init__(self):
        self.count = 0

    def take(self):
        self.count += 1
        return self.count - 1


class CubeGather:
    def __init__(self, sems, orders):
        self.plans = [stages_of(order) for order in orders]
        self.ids = {
            (h, j, i): sems.take()
            for h, stages in enumerate(self.plans)
            for j, (_, held, _) in enumerate(stages)
            for i in range(len(held))
        }

    def bind(self, me, other, own, window, send_sem, recv_sem):
        self.me, self.other, self.own, self.window = me, other, own, window
        self.send_sem, self.recv_sem = send_sem, recv_sem
        return self

    def copy(self, h, j, i):
        bit, held, _ = self.plans[h][j]
        slot = relative(self.me, held[i])
        target = self.window(slot, h)
        source = self.own(h) if held[i] == 0 else target
        k = self.ids[h, j, i]
        return pltpu.make_async_remote_copy(
            src_ref=source,
            dst_ref=target,
            send_sem=self.send_sem.at[k],
            recv_sem=self.recv_sem.at[k],
            device_id=(flip(self.me, bit), self.other),
            device_id_type=MESH,
        )

    def start(self):
        depth = len(self.plans[0])
        for j in range(depth):
            for h in range(len(self.plans)):
                self.copy(h, j, 0).start()

    def advance(self, j):
        for i in range(len(self.plans[0][j][1])):
            for h, stages in enumerate(self.plans):
                self.copy(h, j, i).wait_recv()
                slot = stages[j][2][i]
                for later in range(j + 1, len(stages)):
                    self.copy(h, later, stages[later][1].index(slot)).start()

    def finish(self):
        for h, j, i in self.ids:
            self.copy(h, j, i).wait_send()


class LineGather:
    def __init__(self, sems, size, subs):
        self.size, self.subs = size, subs
        self.ids = {
            (way, s, u): sems.take()
            for way in (0, 1)
            for s in range(size - 1)
            for u in range(subs)
        }

    def bind(self, me, other, own, window, send_sem, recv_sem):
        self.me, self.other, self.own, self.window = me, other, own, window
        self.send_sem, self.recv_sem = send_sem, recv_sem
        return self

    def copy(self, way, s, u):
        block = self.me - s if way == 0 else self.me + s
        target = self.window(block, u)
        k = self.ids[way, s, u]
        return pltpu.make_async_remote_copy(
            src_ref=self.own(u) if s == 0 else target,
            dst_ref=target,
            send_sem=self.send_sem.at[k],
            recv_sem=self.recv_sem.at[k],
            device_id=(self.other, self.me + 1 if way == 0 else self.me - 1),
            device_id_type=MESH,
        )

    def sends(self, way, s):
        if way == 0:
            return (self.me >= s) & (self.me < self.size - 1)
        return (self.me + s < self.size) & (self.me > 0)

    def gets(self, way, s):
        if way == 0:
            return self.me - 1 - s >= 0
        return self.me + 1 + s < self.size

    def start(self, u):
        for way in (0, 1):

            @pl.when(self.sends(way, 0))
            def _():
                self.copy(way, 0, u).start()

    def advance(self, s, u):
        for way in (0, 1):

            @pl.when(self.gets(way, s))
            def _():
                self.copy(way, s, u).wait_recv()

            if s + 1 < self.size - 1:

                @pl.when(self.sends(way, s + 1))
                def _():
                    self.copy(way, s + 1, u).start()

    def finish(self):
        for way, s, u in self.ids:

            @pl.when(self.sends(way, s))
            def _():
                self.copy(way, s, u).wait_send()


def greet(dp, me, tensor, line, wide=False):
    barrier = pltpu.get_barrier_semaphore()

    def hello(a, b):
        pl.semaphore_signal(barrier, inc=1, device_id=(a, b), device_id_type=MESH)

    if wide:
        for r in range(1, dp):
            hello(relative(me, r), line)
        for k in range(1, tensor):
            hello(me, lax.rem(line + k, tensor))
        pl.semaphore_wait(barrier, dp + tensor - 2)
        return
    bits = dp.bit_length() - 1
    for bit in range(bits):
        hello(flip(me, bit), line)

    @pl.when(line > 0)
    def _():
        hello(me, line - 1)

    @pl.when(line < tensor - 1)
    def _():
        hello(me, line + 1)

    left, right = jnp.minimum(line, 1), jnp.minimum(tensor - 1 - line, 1)
    pl.semaphore_wait(barrier, bits + left + right)


def orders_of(dp):
    bits = list(range(1, dp.bit_length() - 1))
    return [bits + [0], bits[::-1] + [0]]


def normalize(x, gain, bias):
    centred = x - jnp.mean(x, -1, keepdims=True)
    spread = jnp.mean(centred * centred, -1, keepdims=True)
    unit = centred * lax.rsqrt(spread + layer_eps)
    return (unit * gain + bias).astype(bf16)


def gather_plain(hidden, cotangent, w_qkv, w_dense, w_fc1, w_fc2, vectors):
    vec = lax.all_gather(vectors, "dp", axis=1, tiled=True)
    normed = normalize(hidden.astype(f32), vec[0:1], vec[1:2])
    return (
        lax.all_gather(w_qkv, "dp", axis=1, tiled=True),
        lax.all_gather(w_dense, "dp", axis=1, tiled=True),
        lax.all_gather(w_fc1, "dp", axis=0, tiled=True),
        lax.all_gather(w_fc2, "dp", axis=1, tiled=True),
        lax.all_gather(normed, "tensor", axis=0, tiled=True),
        lax.all_gather(cotangent, "tensor", axis=0, tiled=True),
        vec,
    )


class ChipReduce:
    COUNT = 6

    def __init__(self, sems):
        self.ids = [sems.take() for _ in range(self.COUNT)]

    def bind(self, me, other, parts, landing, send_sem, recv_sem):
        self.me, self.other, self.parts, self.landing = me, other, parts, landing
        self.send_sem, self.recv_sem = send_sem, recv_sem
        self.half = parts.shape[-1] // 2
        return self

    def view(self, r, h):
        return self.parts.at[r, :, pl.ds(h * self.half, self.half)]

    def copy(self, slot):
        r, h, bit = [(2, 0, 2), (3, 0, 2), (1, 0, 1), (1, 1, 1), (3, 1, 1), (2, 1, 2)][slot]
        k = self.ids[slot]
        return pltpu.make_async_remote_copy(
            src_ref=self.view(r, h),
            dst_ref=self.landing.at[slot],
            send_sem=self.send_sem.at[k],
            recv_sem=self.recv_sem.at[k],
            device_id=(flip(self.me, bit), self.other),
            device_id_type=MESH,
        )

    def start(self, r):
        for slot in {3: (1, 4), 2: (0,), 1: (3,), 0: ()}[r]:
            self.copy(slot).start()

    def middle(self):
        for slot, r, h, last in ((1, 1, 0, 2), (4, 2, 1, 5)):
            self.copy(slot).wait_recv()
            view = self.view(r, h)
            view[...] = (view[...].astype(f32) + self.landing[slot].astype(f32)).astype(bf16)
            self.copy(last).start()

    def final(self):
        for h in (0, 1):
            for slot in ((0, 2), (3, 5))[h]:
                self.copy(slot).wait_recv()
            a, b = ((0, 2), (3, 5))[h]
            view = self.view(0, h)
            total = view[...].astype(f32) + self.landing[a].astype(f32) + self.landing[b].astype(f32)
            view[...] = total.astype(bf16)

    def finish(self):
        for slot in range(self.COUNT):
            self.copy(slot).wait_send()


class LineReduce:
    def __init__(self, sems, size):
        self.size = size
        self.ids = {(way, i): sems.take() for way in (0, 1) for i in range(size - 1)}

    def bind(self, me, other, own, landing, send_sem, recv_sem):
        self.me, self.other, self.own, self.landing = me, other, own, landing
        self.send_sem, self.recv_sem = send_sem, recv_sem
        return self

    def target(self, way, i):
        return self.size - 1 - i if way == 0 else i

    def place(self, way, i):
        return i if way == 0 else 2 * self.size - 4 - i

    def copy(self, way, i, edge):
        k = self.ids[way, i]
        here = self.landing.at[self.place(way, i)]
        return pltpu.make_async_remote_copy(
            src_ref=self.own(self.target(way, i)) if edge else here,
            dst_ref=here,
            send_sem=self.send_sem.at[k],
            recv_sem=self.recv_sem.at[k],
            device_id=(self.other, self.me + 1 if way == 0 else self.me - 1),
            device_id_type=MESH,
        )

    def edge(self, way):
        return self.me == (0 if way == 0 else self.size - 1)

    def passes(self, way, i):
        d = self.target(way, i)
        return (self.me > 0) & (self.me < d) if way == 0 else (self.me < self.size - 1) & (self.me > d)

    def start(self, way, i):
        @pl.when(self.edge(way))
        def _():
            self.copy(way, i, True).start()

    def advance(self, step, add):
        for way in (0, 1):
            steps_from_edge = self.me if way == 0 else self.size - 1 - self.me
            for i in range(step):

                @pl.when(self.passes(way, i) & (steps_from_edge == step - i))
                def _():
                    self.copy(way, i, False).wait_recv()
                    add(self.landing.at[self.place(way, i)], self.own(self.target(way, i)))
                    self.copy(way, i, False).start()

    def arrive(self):
        for way in (0, 1):
            for i in range(self.size - 1):

                @pl.when(self.me == self.target(way, i))
                def _():
                    self.copy(way, i, False).wait_recv()

    def finish(self):
        for way, i in self.ids:

            @pl.when(self.edge(way))
            def _():
                self.copy(way, i, True).wait_send()

            @pl.when(self.passes(way, i))
            def _():
                self.copy(way, i, False).wait_send()

    def total(self, own, rows):
        last = self.size - 1
        value = own.astype(f32)
        lefts = jnp.clip(last - self.me, 0, last - 1)
        rights = jnp.clip(self.me, 0, last - 1)
        from_left = self.landing[lefts, rows, :].astype(f32)
        from_right = self.landing[2 * self.size - 4 - rights, rows, :].astype(f32)
        value = value + jnp.where(self.me > 0, from_left, 0.0)
        return value + jnp.where(self.me < last, from_right, 0.0)


def add_into(landing, own):
    rows = landing.shape[0]

    @pl.loop(0, rows, step=64)
    def _(r):
        at = pl.ds(r, 64)
        landing[at, :] = (landing[at, :].astype(f32) + own[at, :].astype(f32)).astype(bf16)


def chip_slot(me, r):
    return (
        me
        + 2 * ((r % 2) * (1 - 2 * (lax.div(me, 2) % 2)))
        + 4 * (lax.div(r, 2) * (1 - 2 * (lax.div(me, 4) % 2)))
    )


def first_call(dp, tensor, arrays):
    grad_out, crossed_out, act, crossed_act, slope, attn, crossed_attn, w_fc2 = arrays
    tokens, width = grad_out.shape
    units = act.shape[1]
    local = attn.shape[1]
    part = width // dp
    chips = dp // 2
    sems = Sems()
    reduce_fc2, reduce_dense = ChipReduce(sems), ChipReduce(sems)
    swap_at = sems.take()

    def kernel(
        c_ref, cx_ref, a_ref, ax_ref, d_ref, t_ref, tx_ref, w2_ref,
        gp_ref, gpx_ref, sum_ref, s2_out, sd_out,
        c_buf, cx_buf, a_buf, ax_buf, t_buf, tx_buf, w2_buf, d_buf,
        s2, sd, r2, rd, send_sem, recv_sem, local_sem,
    ):
        me, line = lax.axis_index("dp"), lax.axis_index("tensor")

        def cols(a):
            return pl.ds(pl.multiple_of(a * part, part), part)

        pair = (send_sem, recv_sem)
        fc2 = reduce_fc2.bind(me, line, s2, r2, *pair)
        dense = reduce_dense.bind(me, line, sd, rd, *pair)
        loads = [
            pltpu.make_async_copy(a, b, local_sem.at[k])
            for k, (a, b) in enumerate([
                (c_ref, c_buf), (cx_ref, cx_buf), (a_ref, a_buf), (ax_ref, ax_buf),
                (t_ref, t_buf), (tx_ref, tx_buf), (w2_ref, w2_buf), (d_ref, d_buf),
            ])
        ]
        for copy in loads:
            copy.start()
        greet(dp, me, tensor, line)
        for copy in loads[:4]:
            copy.wait()

        def weight_grad(target, plan, own, crossed, size, step):
            @pl.loop(0, chips)
            def _(i):
                r = chips - 1 - i
                slot = chip_slot(me, r)

                @pl.loop(0, size, step=step)
                def _(n):
                    at = pl.ds(pl.multiple_of(n, step), step)
                    value = dot_tn(c_buf[:, cols(slot)], own[:, at])
                    value = value + dot_tn(cx_buf[r], crossed[:, at])
                    target[r, :, at] = value.astype(bf16)

                for k in range(1, chips):

                    @pl.when(r == k)
                    def _():
                        plan.start(k)

        weight_grad(s2, fc2, a_buf, ax_buf, units, 1024)
        for copy in loads[4:6]:
            copy.wait()
        weight_grad(sd, dense, t_buf, tx_buf, local, local)
        for copy in loads[6:]:
            copy.wait()

        @pl.loop(0, units, step=512)
        def _(n):
            at = pl.ds(pl.multiple_of(n, 512), 512)
            value = dot_nt(c_buf[...], w2_buf[at, :]) * d_buf[:, at].astype(f32)
            value = value.astype(bf16)
            d_buf[:, at] = value
            sum_ref[0:1, at] = jnp.sum(value.astype(f32), 0, keepdims=True)

        store = pltpu.make_async_copy(d_buf, gp_ref, local_sem.at[len(loads)])
        store.start()
        cross = pltpu.make_async_remote_copy(
            src_ref=d_buf, dst_ref=gpx_ref,
            send_sem=send_sem.at[swap_at], recv_sem=recv_sem.at[swap_at],
            device_id=(flip(me, 0), line), device_id_type=MESH)
        cross.start()
        fc2.middle()
        dense.middle()
        fc2.final()
        dense.final()
        store2 = pltpu.make_async_copy(s2.at[0], s2_out, local_sem.at[len(loads) + 1])
        stored = pltpu.make_async_copy(sd.at[0], sd_out, local_sem.at[len(loads) + 2])
        store2.start()
        stored.start()
        cross.wait()
        for plan in (fc2, dense):
            plan.finish()
        for copy in (store, store2, stored):
            copy.wait()

    return pl.pallas_call(
        kernel,
        out_shape=(
            jax.ShapeDtypeStruct((tokens, units), bf16),
            jax.ShapeDtypeStruct((tokens, units), bf16),
            jax.ShapeDtypeStruct((8, units), f32),
            jax.ShapeDtypeStruct((part, units), bf16),
            jax.ShapeDtypeStruct((part, local), bf16),
        ),
        in_specs=[ANY] * 8,
        out_specs=(ANY, ANY, VMEM, ANY, ANY),
        scratch_shapes=[
            pltpu.VMEM((tokens, width), bf16),
            pltpu.VMEM((chips, tokens, part), bf16),
            pltpu.VMEM((tokens, units), bf16),
            pltpu.VMEM((tokens, units), bf16),
            pltpu.VMEM((tokens, local), bf16),
            pltpu.VMEM((tokens, local), bf16),
            pltpu.VMEM((units, width), bf16),
            pltpu.VMEM((tokens, units), bf16),
            pltpu.VMEM((chips, part, units), bf16),
            pltpu.VMEM((chips, part, local), bf16),
            pltpu.VMEM((6, part, units // 2), bf16),
            pltpu.VMEM((6, part, local // 2), bf16),
            pltpu.SemaphoreType.DMA((sems.count,)),
            pltpu.SemaphoreType.DMA((sems.count,)),
            pltpu.SemaphoreType.DMA((12,)),
        ],
        compiler_params=pltpu.CompilerParams(
            collective_id=1, has_side_effects=True, vmem_limit_bytes=VMEM_LIMIT
        ),
        name="first_back",
    )(*arrays)


def second_call(dp, tensor, arrays):
    hidden, cotangent, vec, sums, normed, grad_pre, grad_qkv = arrays[:7]
    rows, width = hidden.shape
    tokens, units = grad_pre.shape
    wide = grad_qkv.shape[1]
    local = wide // 3
    part = width // dp
    chips = dp // 2
    sems = Sems()
    reduce_fc1, reduce_qkv = ChipReduce(sems), ChipReduce(sems)
    line_in = LineReduce(sems, tensor)
    tells = [sems.take() for _ in range(2 * (dp - 1) + tensor - 1)]

    def kernel(
        x_ref, c_ref, vec_ref, sum_ref, n_ref, gp_in, gq_in, nx_in, gpx_in, gqx_in, wq_ref, w1_ref,
        hid_ref, s1_out, sq_out, vout_ref, bout_ref,
        x_buf, c_buf, n_buf, nx_buf, gp, gpx, gq, gqx, wq, w1, gn,
        s1, sq, r1, rq, rz, parts, tell_v, tell_b, tell_z, send_sem, recv_sem, local_sem,
    ):
        me, line = lax.axis_index("dp"), lax.axis_index("tensor")
        twin = flip(me, 0)

        def cols(a):
            return pl.ds(pl.multiple_of(a * part, part), part)

        pair = (send_sem, recv_sem)
        fc1 = reduce_fc1.bind(me, line, s1, r1, *pair)
        qkv = reduce_qkv.bind(me, line, sq, rq, *pair)
        ins = line_in.bind(line, me, lambda d: gn.at[pl.ds(d * rows, rows), :], rz, *pair)

        def remote(k, source, target, device):
            return pltpu.make_async_remote_copy(
                src_ref=source, dst_ref=target,
                send_sem=send_sem.at[k], recv_sem=recv_sem.at[k],
                device_id=device, device_id_type=MESH)

        def third(i):
            return pl.ds(i * local, local)

        bias_tells = [
            remote(tells[r - 1], sum_ref, tell_b.at[r], (relative(me, r), line)) for r in range(1, dp)
        ]
        vec_tells = [
            remote(tells[dp - 2 + r], parts.at[:, cols(relative(me, r))], tell_v.at[r],
                   (relative(me, r), line))
            for r in range(1, dp)
        ]
        line_tells = [
            remote(tells[2 * dp - 3 + k], tell_z.at[0], tell_z.at[k],
                   (me, lax.rem(line + k, tensor)))
            for k in range(1, tensor)
        ]
        tile = 512
        pieces = (
            [(gp_in, gp), (gq_in, gq)]
            + [(w1_ref.at[pl.ds(n, tile), :], w1.at[pl.ds(n, tile), :]) for n in range(0, width, tile)]
            + [
                (wq_ref.at[i, pl.ds(n, tile), :], wq.at[pl.ds(n, tile), third(i)])
                for n in range(0, width, tile) for i in range(3)
            ]
            + [(n_ref, n_buf), (nx_in, nx_buf), (gpx_in, gpx), (gqx_in, gqx), (x_ref, x_buf), (c_ref, c_buf)]
        )
        loads = [pltpu.make_async_copy(a, b, local_sem.at[k]) for k, (a, b) in enumerate(pieces)]
        tiles = width // tile
        late = 2 + 4 * tiles
        for copy in loads:
            copy.start()
        greet(dp, me, tensor, line, wide=True)
        for copy in bias_tells:
            copy.start()
        for copy in loads[:late]:
            copy.wait()
        upper = lax.div(line, tensor // 2)

        @pl.loop(0, tensor)
        def _(i):
            d = (1 - upper) * (tensor - 1 - i) + upper * i
            at = pl.ds(pl.multiple_of(d * rows, rows), rows)

            @pl.loop(0, width, step=1024)
            def _(n):
                to = pl.ds(pl.multiple_of(n, 1024), 1024)
                value = dot_nt(gp[at, :], w1[to, :]) + dot_nt(gq[at, :], wq[to, :])
                gn[at, to] = value.astype(bf16)

            for k in range(tensor - 1):

                @pl.when(i == k)
                def _():
                    ins.start(0, k)
                    ins.start(1, k)

        for copy in loads[late : late + 4]:
            copy.wait()

        def weight_grad(target, plan, own, crossed, size, step):
            @pl.loop(0, chips)
            def _(i):
                r = chips - 1 - i
                slot = chip_slot(me, r)

                @pl.loop(0, size, step=step)
                def _(n):
                    at = pl.ds(pl.multiple_of(n, step), step)
                    value = dot_tn(n_buf[:, cols(slot)], own[:, at])
                    value = value + dot_tn(nx_buf[r], crossed[:, at])
                    target[r, :, at] = value.astype(bf16)

                for k in range(1, chips):

                    @pl.when(r == k)
                    def _():
                        plan.start(k)

        weight_grad(s1, fc1, gp, gpx, units, 1024)
        ins.advance(1, add_into)
        weight_grad(sq, qkv, gq, gqx, wide, 768)
        ins.advance(2, add_into)
        fc1.middle()
        for copy in bias_tells:
            copy.wait_recv()
        total = sum_ref[...]
        for r in range(1, dp):
            total = total + tell_b[r]
        bout_ref[...] = total
        for copy in loads[late + 4 :]:
            copy.wait()
        qkv.middle()
        ins.arrive()
        parts[...] = jnp.zeros_like(parts)

        @pl.loop(0, rows, step=32)
        def _(r):
            at = pl.ds(r, 32)
            x = x_buf[at, :].astype(f32)
            centred = x - jnp.mean(x, -1, keepdims=True)
            inv_std = lax.rsqrt(jnp.mean(centred * centred, -1, keepdims=True) + layer_eps)
            unit = centred * inv_std
            own = pl.ds(pl.multiple_of(line * rows + r, 32), 32)
            grad = ins.total(gn[own, :], at)
            cot = c_buf[at, :].astype(f32)
            scaled = grad * vec_ref[0:1, :]
            first = jnp.mean(scaled, -1, keepdims=True)
            second = jnp.mean(scaled * unit, -1, keepdims=True)
            c_buf[at, :] = (cot + inv_std * (scaled - first - unit * second)).astype(bf16)
            parts[0:1, :] += jnp.sum(grad * unit, 0, keepdims=True)
            parts[1:2, :] += jnp.sum(grad, 0, keepdims=True)
            parts[2:3, :] += jnp.sum(cot, 0, keepdims=True)

        last = pltpu.make_async_copy(c_buf, hid_ref, local_sem.at[len(loads)])
        last.start()
        for copy in vec_tells:
            copy.start()
        fc1.final()
        store1 = pltpu.make_async_copy(s1.at[0], s1_out, local_sem.at[len(loads) + 1])
        store1.start()
        for copy in vec_tells:
            copy.wait_recv()
        total_v = parts[:, cols(me)]
        for r in range(1, dp):
            total_v = total_v + tell_v[r]
        tell_z[0] = total_v
        for copy in line_tells:
            copy.start()
        qkv.final()
        storeq = pltpu.make_async_copy(sq.at[0], sq_out, local_sem.at[len(loads) + 2])
        storeq.start()
        for copy in line_tells:
            copy.wait_recv()
        total_z = tell_z[0]
        for k in range(1, tensor):
            total_z = total_z + tell_z[k]
        vout_ref[...] = total_z
        for copy in bias_tells + vec_tells + line_tells:
            copy.wait_send()
        for plan in (fc1, qkv, ins):
            plan.finish()
        for copy in (last, store1, storeq):
            copy.wait()

    return pl.pallas_call(
        kernel,
        out_shape=(
            jax.ShapeDtypeStruct((rows, width), bf16),
            jax.ShapeDtypeStruct((part, units), bf16),
            jax.ShapeDtypeStruct((part, wide), bf16),
            jax.ShapeDtypeStruct((8, part), f32),
            jax.ShapeDtypeStruct((8, local), f32),
        ),
        in_specs=[ANY] * 2 + [VMEM] * 2 + [ANY] * 8,
        out_specs=(ANY, ANY, ANY, VMEM, VMEM),
        scratch_shapes=[
            pltpu.VMEM((rows, width), bf16),
            pltpu.VMEM((rows, width), bf16),
            pltpu.VMEM((tokens, width), bf16),
            pltpu.VMEM((chips, tokens, part), bf16),
            pltpu.VMEM((tokens, units), bf16),
            pltpu.VMEM((tokens, units), bf16),
            pltpu.VMEM((tokens, wide), bf16),
            pltpu.VMEM((tokens, wide), bf16),
            pltpu.VMEM((width, wide), bf16),
            pltpu.VMEM((width, units), bf16),
            pltpu.VMEM((tokens, width), bf16),
            pltpu.VMEM((chips, part, units), bf16),
            pltpu.VMEM((chips, part, wide), bf16),
            pltpu.VMEM((6, part, units // 2), bf16),
            pltpu.VMEM((6, part, wide // 2), bf16),
            pltpu.VMEM((2 * tensor - 3, rows, width), bf16),
            pltpu.VMEM((8, width), f32),
            pltpu.VMEM((dp, 8, part), f32),
            pltpu.VMEM((dp, 8, local), f32),
            pltpu.VMEM((tensor, 8, part), f32),
            pltpu.SemaphoreType.DMA((sems.count,)),
            pltpu.SemaphoreType.DMA((sems.count,)),
            pltpu.SemaphoreType.DMA((30,)),
        ],
        compiler_params=pltpu.CompilerParams(
            collective_id=2, has_side_effects=True, vmem_limit_bytes=VMEM_LIMIT
        ),
        name="second_back",
    )(*arrays)


def spans_of(length):
    back = -(-(MAX_DOC - 1) // BLOCK)
    spans, at = [], 0
    for i in range(length // BLOCK):
        low = max(0, i - back) * BLOCK
        spans.append((low, (i + 1) * BLOCK, at))
        at += (i + 1) * BLOCK - low
    return spans, at


def turn(x, cosine, sine_lo, sine_hi):
    return x * cosine + pltpu.roll(x, 128 - ROT // 2, 1) * sine_lo + pltpu.roll(x, ROT // 2, 1) * sine_hi


def head_lanes(shape, e):
    lane = lax.broadcasted_iota(jnp.int32, shape, 1)
    return (lane >= e * HD) & (lane < (e + 1) * HD)


def only(x, e):
    return jnp.where(head_lanes(x.shape, e), x, jnp.zeros_like(x))


def attend_kernel(
    q_ref, k_ref, v_ref, bias_ref, cos_ref, slo_ref, shi_ref, segc_ref, segr_ref,
    qs_ref, ks_ref, vs_ref, o_ref, p_ref, mask_ref,
):
    @pl.when(pl.program_id(1) == 0)
    def _():
        fill_mask(mask_ref, segc_ref, segr_ref, q_ref.shape[0])

    cosine, slo, shi = cos_ref[...], slo_ref[...], shi_ref[...]
    query = turn(q_ref[...] + bias_ref[0:1, :], cosine, slo, shi).astype(bf16) * bf16(HD**-0.5)
    key = turn(k_ref[...] + bias_ref[1:2, :], cosine, slo, shi).astype(bf16)
    value = (v_ref[...] + bias_ref[2:3, :]).astype(bf16)
    qs_ref[...] = query
    ks_ref[...] = key
    vs_ref[...] = value

    def keep(e, at, probs):
        p_ref[e, at, :] = probs

    def write(at, result):
        o_ref[at, :] = result

    attend_pair(query, key, value, mask_ref, keep, write)


def attend(q, k, v, qkv_bias, tables, segments, rows):
    tokens, local = q.shape
    length = tokens // rows
    pairs = local // 128
    _, stored = spans_of(length)
    block = pl.BlockSpec((length, 128), lambda r, h: (r, h))
    table = pl.BlockSpec((length, 128), lambda r, h: (r, 0))
    shape = jax.ShapeDtypeStruct((tokens, local), bf16)
    return pl.pallas_call(
        attend_kernel,
        grid=(rows, pairs),
        out_shape=(shape,) * 4 + (jax.ShapeDtypeStruct((rows, local // HD, stored, BLOCK), bf16),),
        in_specs=[block] * 3
        + [pl.BlockSpec((8, 128), lambda r, h: (0, h))]
        + [table] * 3
        + [
            pl.BlockSpec((length, 1), lambda r, h: (r, 0)),
            pl.BlockSpec((pl.Squeezed(), 1, length), lambda r, h: (r, 0, 0)),
        ],
        out_specs=(block,) * 4
        + (pl.BlockSpec((pl.Squeezed(), 128 // HD, stored, BLOCK), lambda r, h: (r, h, 0, 0)),),
        scratch_shapes=[pltpu.VMEM((stored, BLOCK), f32)],
        compiler_params=pltpu.CompilerParams(vmem_limit_bytes=VMEM_LIMIT),
        cost_estimate=pl.CostEstimate(
            flops=16 * tokens * 768 * local, bytes_accessed=24 << 20, transcendentals=0
        ),
        name="attend",
    )(q, k, v, qkv_bias, *tables, segments.reshape(tokens, 1), segments.reshape(rows, 1, length))


def attend_back_kernel(
    q_ref, k_ref, v_ref, g_ref, o_ref, p_ref, cos_ref, slo_ref, shi_ref,
    dq_ref, dk_ref, dv_ref, bias_ref, kacc_ref, vacc_ref,
):
    def write(which, at, value):
        (dq_ref, dk_ref, dv_ref)[which][at, :] = value

    sums = attend_back_pair(
        q_ref[...], k_ref[...], v_ref[...], g_ref[...], o_ref[...],
        lambda e, at: p_ref[e, at, :], (cos_ref, slo_ref, shi_ref), kacc_ref, vacc_ref, write)
    sums = jnp.concatenate(list(sums) + [jnp.zeros((5, 128), f32)], 0)

    @pl.when(pl.program_id(1) == 0)
    def _():
        bias_ref[...] = sums

    @pl.when(pl.program_id(1) > 0)
    def _():
        bias_ref[...] += sums


def attend_back(q, k, v, g, o, probs, tables, rows):
    tokens, local = q.shape
    length = tokens // rows
    pairs = local // 128
    stored = probs.shape[2]
    block = pl.BlockSpec((length, 128), lambda h, r: (r, h))
    table = pl.BlockSpec((length, 128), lambda h, r: (r, 0))
    shape = jax.ShapeDtypeStruct((tokens, local), bf16)
    return pl.pallas_call(
        attend_back_kernel,
        grid=(pairs, rows),
        out_shape=(shape,) * 3 + (jax.ShapeDtypeStruct((8, local), f32),),
        in_specs=[block] * 5
        + [pl.BlockSpec((pl.Squeezed(), 128 // HD, stored, BLOCK), lambda h, r: (r, h, 0, 0))]
        + [table] * 3,
        out_specs=(block,) * 3 + (pl.BlockSpec((8, 128), lambda h, r: (0, h)),),
        scratch_shapes=[pltpu.VMEM((length, 128), f32)] * 2,
        compiler_params=pltpu.CompilerParams(vmem_limit_bytes=VMEM_LIMIT),
        cost_estimate=pl.CostEstimate(
            flops=32 * tokens * 768 * local, bytes_accessed=24 << 20, transcendentals=0
        ),
        name="attend_back",
    )(q, k, v, g, o, probs, *tables)


def attend_pair(query, key, value, mask_ref, keep, write):
    length = query.shape[0]
    spans, _ = spans_of(length)
    for i, (low, high, at) in enumerate(spans):
        mine = slice(i * BLOCK, (i + 1) * BLOCK)
        total = jnp.zeros((BLOCK, 128), f32)
        for e in range(128 // HD):
            scores = dot_nt(only(key[low:high], e), query[mine]) + mask_ref[at : at + high - low, :]
            exponent = jnp.exp(scores - jnp.max(scores, 0, keepdims=True))
            inverse = 1.0 / jnp.sum(exponent, 0, keepdims=True)
            probs = (exponent * inverse).astype(bf16)
            keep(e, slice(at, at + high - low), probs)
            total = total + dot_tn(probs, only(value[low:high], e))
        write(mine, total.astype(bf16))


def fill_mask(mask_ref, segc_ref, segr_ref, length):
    for i, (low, high, at) in enumerate(spans_of(length)[0]):
        keys = lax.broadcasted_iota(jnp.int32, (high - low, BLOCK), 0) + low
        queries = lax.broadcasted_iota(jnp.int32, (high - low, BLOCK), 1) + i * BLOCK
        same = segc_ref[low:high, :] == segr_ref[:, i * BLOCK : (i + 1) * BLOCK]
        mask_ref[at : at + high - low, :] = jnp.where((keys <= queries) & same, 0.0, -1e30)


def attend_back_pair(query, key, value, grad, result, probs_of, tables, kacc_ref, vacc_ref, write):
    length = query.shape[0]
    spans, _ = spans_of(length)
    heads = 128 // HD
    inner = grad.astype(f32) * result.astype(f32)
    lane = lax.broadcasted_iota(jnp.int32, (8, 128), 1)
    row = lax.broadcasted_iota(jnp.int32, (8, 128), 0)
    pick = jnp.where(lax.div(lane, HD) == row, 1.0, 0.0)
    delta = lax.dot_general(
        pick, inner, (((1,), (1,)), ((), ())),
        precision=lax.Precision.HIGHEST, preferred_element_type=f32)
    kacc_ref[...] = jnp.zeros_like(kacc_ref)
    vacc_ref[...] = jnp.zeros_like(vacc_ref)
    cos_ref, slo_ref, shi_ref = tables
    first = jnp.zeros((1, 128), f32)
    for i, (low, high, at) in enumerate(spans):
        mine = slice(i * BLOCK, (i + 1) * BLOCK)
        g_i, q_i = grad[mine], query[mine]
        dq = jnp.zeros((BLOCK, 128), f32)
        ps, dss = [], []
        for e in range(heads):
            probs = probs_of(e, slice(at, at + high - low))
            dprobs = dot_nt(only(value[low:high], e), g_i)
            ds = (probs.astype(f32) * (dprobs - delta[e : e + 1, mine])).astype(bf16)
            dq = dq + dot_tn(ds, only(key[low:high], e))
            ps.append(probs)
            dss.append(ds)
        g_cat = jnp.concatenate([only(g_i, e) for e in range(heads)], 0)
        q_cat = jnp.concatenate([only(q_i, e) for e in range(heads)], 0)
        vacc_ref[low:high, :] += dot_nn(jnp.concatenate(ps, 1), g_cat)
        kacc_ref[low:high, :] += dot_nn(jnp.concatenate(dss, 1), q_cat)
        dq = dq * f32(HD**-0.5)
        dq = turn(dq, cos_ref[mine, :], -slo_ref[mine, :], -shi_ref[mine, :]).astype(bf16)
        write(0, mine, dq)
        first = first + jnp.sum(dq.astype(f32), 0, keepdims=True)
    everything = slice(0, length)
    dk = turn(kacc_ref[...], cos_ref[...], -slo_ref[...], -shi_ref[...]).astype(bf16)
    dv = vacc_ref[...].astype(bf16)
    write(1, everything, dk)
    write(2, everything, dv)
    return first, jnp.sum(dk.astype(f32), 0, keepdims=True), jnp.sum(dv.astype(f32), 0, keepdims=True)


def forward_call(dp, tensor, arrays):
    hidden, cotangent, w_qkv, w_dense, w_fc1, w_fc2, vectors = arrays[:7]
    rows, width = hidden.shape
    local = w_qkv.shape[2]
    units = w_fc1.shape[1]
    part = width // dp
    chips = dp // 2
    tokens = rows * tensor
    pairs = local // 128
    stored = spans_of(tokens)[1]
    sems = Sems()
    orders = orders_of(dp)
    plan_vec = CubeGather(sems, orders[:1])
    plan_qkv, plan_dense, plan_fc1, plan_fc2 = (CubeGather(sems, orders) for _ in range(4))
    plan_n, plan_c = LineGather(sems, tensor, 2), LineGather(sems, tensor, 2)
    line_out = LineReduce(sems, tensor)
    swaps = [sems.take() for _ in range(2 * chips + 3)]

    def kernel(
        x_ref, c_ref, wq_ref, wd_ref, w1_ref, w2_ref, vec_ref,
        qb_ref, fb_ref, cos_ref, slo_ref, shi_ref, segc_ref, segr_ref,
        out_ref, gq_ref, g1_ref, g2_ref, n_out, nx_out, c_out, cx_out, a_out, ax_out, d_out,
        t_out, tx_out, dq_out, dqx_out, gvec_ref, qsum_ref,
        x_buf, vec_buf, nv, wa, wb, wd, act, slope, qkv3, attn, pb, mask, g_buf, kacc, vacc, rz,
        send_sem, recv_sem, local_sem,
    ):
        me, line = lax.axis_index("dp"), lax.axis_index("tensor")
        twin = flip(me, 0)
        half = part // 2
        local_count = [0]

        def cols(a):
            return pl.ds(pl.multiple_of(a * part, part), part)

        def half_rows(a, h):
            return pl.ds(pl.multiple_of(a * part + h * half, half), half)

        def tok(b, u):
            return pl.ds(pl.multiple_of(b * rows + u * (rows // 2), rows // 2), rows // 2)

        def block(b):
            return pl.ds(pl.multiple_of(b * rows, rows), rows)

        def piece(n, h):
            return pl.ds(h * (n // 2), n // 2)

        def copy_of(a, b):
            local_count[0] += 1
            return pltpu.make_async_copy(a, b, local_sem.at[local_count[0] - 1])

        def to_twin(k, source, target):
            return pltpu.make_async_remote_copy(
                src_ref=source, dst_ref=target,
                send_sem=send_sem.at[swaps[k]], recv_sem=recv_sem.at[swaps[k]],
                device_id=(twin, line), device_id_type=MESH)

        pair = (send_sem, recv_sem)
        vec = plan_vec.bind(me, line, lambda h: vec_ref, lambda a, h: vec_buf.at[:, cols(a)], *pair)
        qkv = plan_qkv.bind(
            me, line,
            lambda h: wq_ref.at[:, pl.ds(h * half, half), :],
            lambda a, h: gq_ref.at[:, half_rows(a, h), :], *pair)
        fc1 = plan_fc1.bind(
            me, line,
            lambda h: w1_ref.at[pl.ds(h * half, half), :],
            lambda a, h: g1_ref.at[half_rows(a, h), :], *pair)
        dense = plan_dense.bind(
            me, line,
            lambda h: wd_ref.at[piece(local, h), :],
            lambda a, h: wd.at[piece(local, h), cols(a)], *pair)
        fc2 = plan_fc2.bind(
            me, line,
            lambda h: w2_ref.at[piece(units, h), :],
            lambda a, h: g2_ref.at[piece(units, h), cols(a)], *pair)
        norm = plan_n.bind(
            line, me, lambda u: nv.at[tok(line, u)], lambda b, u: nv.at[tok(b, u)], *pair)
        cot = plan_c.bind(
            line, me, lambda u: c_ref.at[piece(rows, u)], lambda b, u: c_out.at[tok(b, u)], *pair)
        outs = line_out.bind(line, me, lambda d: nv.at[pl.ds(d * rows, rows), :], rz, *pair)
        stages = dp.bit_length() - 1

        keeps = [
            copy_of(x_ref, x_buf),
            copy_of(vec_ref, vec_buf.at[:, cols(me)]),
            copy_of(wq_ref, gq_ref.at[:, cols(me), :]),
            copy_of(w1_ref, g1_ref.at[cols(me), :]),
            copy_of(wd_ref, wd.at[:, cols(me)]),
            copy_of(w2_ref, g2_ref.at[:, cols(me)]),
            copy_of(c_ref, c_out.at[block(line), :]),
        ]
        keeps[0].start()
        greet(dp, me, tensor, line)
        vec.start()
        qkv.start()
        cot.start(0)
        for copy in keeps[1:]:
            copy.start()
        for j in range(stages):
            vec.advance(j)
        keeps[0].wait()
        keeps[1].wait()

        @pl.loop(0, rows, step=32)
        def _(r):
            x = x_buf[pl.ds(r, 32), :].astype(f32)
            centred = x - jnp.mean(x, -1, keepdims=True)
            spread = jnp.mean(centred * centred, -1, keepdims=True)
            unit = centred * lax.rsqrt(spread + layer_eps)
            at = pl.ds(pl.multiple_of(line * rows + r, 32), 32)
            nv[at, :] = (unit * vec_buf[0:1, :] + vec_buf[1:2, :]).astype(bf16)

        norm.start(0)
        norm.start(1)
        gvec_ref[...] = vec_buf[...]
        qkv.advance(0)
        fc1.start()
        fill_mask(mask, segc_ref, segr_ref, tokens)

        def project(b):
            at = block(b)
            cosine, slo, shi = cos_ref[at, :], slo_ref[at, :], shi_ref[at, :]
            for i in range(3):
                value = dot_nn(nv[at, :], wa[:, i * local : (i + 1) * local]) + qb_ref[i : i + 1, :]
                if i == 2:
                    qkv3[2, at, :] = value.astype(bf16)
                    continue
                for h in range(pairs):
                    lanes = slice(h * 128, (h + 1) * 128)
                    turned = turn(value[:, lanes], cosine, slo, shi).astype(bf16)
                    if i == 0:
                        turned = turned * bf16(HD**-0.5)
                    qkv3[i, at, lanes] = turned

        def hidden_layer(b):
            at = block(b)

            @pl.loop(0, units, step=512)
            def _(n):
                to = pl.ds(pl.multiple_of(n, 512), 512)
                pre = dot_nn(nv[at, :], wb[:, to]) + fb_ref[0:1, to]
                square = pre * pre
                bend = jnp.tanh(0.7978845608028654 * pre * (1.0 + 0.044715 * square))
                act[at, to] = (0.5 * pre * (1.0 + bend)).astype(bf16)
                rise = 0.7978845608028654 * (1.0 + 3 * 0.044715 * square)
                slope[at, to] = (
                    0.5 * (1.0 + bend) + 0.5 * pre * (1.0 - bend * bend) * rise
                ).astype(bf16)

        norm.advance(0, 0)
        for j in range(1, stages - 1):
            qkv.advance(j)
        norm.advance(0, 1)
        qkv.advance(stages - 1)
        keeps[2].wait()
        load_q = [
            copy_of(gq_ref.at[i], wa.at[:, pl.ds(i * local, local)]) for i in range(3)
        ]
        for copy in load_q:
            copy.start()
        fc1.advance(0)
        dense.start()
        fc2.start()
        for copy in load_q:
            copy.wait()

        @pl.loop(0, 4)
        def _(i):
            s = i - 1

            @pl.when(i == 2)
            def _():
                norm.advance(1, 0)
                norm.advance(1, 1)
                cot.start(1)

            @pl.when(i == 3)
            def _():
                for j in range(1, stages):
                    fc1.advance(j)
                dense.advance(0)
                norm.advance(2, 0)
                norm.advance(2, 1)

            @pl.loop(0, 2)
            def _(way):
                b = line + (2 * way - 1) * (1 + s)

                @pl.when((b >= 0) & (b < tensor) & ((i > 0) | (way == 0)))
                def _():
                    project(b)

        keeps[3].wait()
        load_1 = copy_of(g1_ref, wb)
        load_1.start()
        n_store = copy_of(nv, n_out)
        n_store.start()
        cross_n = [
            to_twin(r, nv.at[:, cols(relative(twin, r << 1))], nx_out.at[r]) for r in range(chips)
        ]
        for copy in cross_n:
            copy.start()
        fc2.advance(0)
        cot.advance(0, 0)
        load_1.wait()

        @pl.loop(0, tensor)
        def _(b):
            hidden_layer(b)

            @pl.when(b == 1)
            def _():
                cot.advance(0, 1)
                for j in range(1, stages - 1):
                    dense.advance(j)

        for j in range(1, stages - 1):
            fc2.advance(j)
        stores = [copy_of(act, a_out), copy_of(slope, d_out)]
        cross_a = to_twin(chips, act, ax_out)
        for copy in stores + [cross_a]:
            copy.start()
        dense.advance(stages - 1)
        fc2.advance(stages - 1)
        keeps[4].wait()
        keeps[5].wait()
        load_2 = copy_of(g2_ref, wa)
        load_2.start()

        @pl.loop(0, pairs)
        def _(h):
            lanes = pl.ds(pl.multiple_of(h * 128, 128), 128)

            def keep(e, at, value):
                pb[2 * h + e, at, :] = value

            def write(at, value):
                attn[at, lanes] = value

            attend_pair(
                qkv3[0, :, lanes], qkv3[1, :, lanes], qkv3[2, :, lanes], mask, keep, write)

            @pl.when(h == 1)
            def _():
                cot.advance(1, 0)

        cross_t = to_twin(chips + 1, attn, tx_out)
        stores.append(copy_of(attn, t_out))
        stores[-1].start()
        cross_t.start()
        cot.advance(1, 1)
        load_2.wait()
        norm.finish()
        n_store.wait()
        for copy in cross_n:
            copy.wait_send()
        upper = lax.div(line, tensor // 2)

        @pl.loop(0, tensor)
        def _(i):
            d = (1 - upper) * (tensor - 1 - i) + upper * i
            at = block(d)

            @pl.loop(0, width, step=1024)
            def _(n):
                to = pl.ds(pl.multiple_of(n, 1024), 1024)
                value = dot_nn(act[at, :], wa[:, to]) + dot_nn(attn[at, :], wd[:, to])
                nv[at, to] = value.astype(bf16)

            for k in range(tensor - 1):

                @pl.when(i == k)
                def _():
                    outs.start(0, k)
                    outs.start(1, k)

        cot.advance(2, 0)
        outs.advance(1, add_into)
        cot.advance(2, 1)
        keeps[6].wait()
        grad = wa.at[pl.ds(0, tokens), :]
        load_c = copy_of(c_out, grad)
        load_c.start()
        cross_c = [
            to_twin(chips + 2 + r, c_out.at[:, cols(relative(twin, r << 1))], cx_out.at[r])
            for r in range(chips)
        ]
        for copy in cross_c:
            copy.start()
        load_c.wait()
        g_buf[...] = dot_nt(grad[...], wd[...]).astype(bf16)
        outs.advance(2, add_into)
        qsum_ref[...] = jnp.zeros_like(qsum_ref)

        @pl.loop(0, pairs)
        def _(h):
            lanes = pl.ds(pl.multiple_of(h * 128, 128), 128)

            def write(which, at, value):
                wb[at, pl.ds(pl.multiple_of(which * local + h * 128, 128), 128)] = value

            sums = attend_back_pair(
                qkv3[0, :, lanes], qkv3[1, :, lanes], qkv3[2, :, lanes],
                g_buf[:, lanes], attn[:, lanes], lambda e, at: pb[2 * h + e, at, :],
                (cos_ref, slo_ref, shi_ref), kacc, vacc, write)
            for k in range(3):
                qsum_ref[k : k + 1, lanes] = sums[k]

        back = wb.at[pl.ds(0, tokens), pl.ds(0, 3 * local)]
        stores.append(copy_of(back, dq_out))
        stores[-1].start()
        cross_d = to_twin(2 * chips + 2, back, dqx_out)
        cross_d.start()
        outs.arrive()

        @pl.loop(0, rows, step=32)
        def _(r):
            at = pl.ds(r, 32)
            own = pl.ds(pl.multiple_of(line * rows + r, 32), 32)
            total = x_buf[at, :].astype(f32) + outs.total(nv[own, :], at) + vec_buf[2:3, :]
            x_buf[at, :] = total.astype(bf16)

        stores.append(copy_of(x_buf, out_ref))
        stores[-1].start()
        crossed = cross_n + [cross_a, cross_t] + cross_c + [cross_d]
        for copy in crossed:
            copy.wait_recv()
        for copy in crossed[chips:]:
            copy.wait_send()
        for plan in (vec, qkv, fc1, dense, fc2, cot, outs):
            plan.finish()
        for copy in stores:
            copy.wait()

    def shape(*dims):
        return jax.ShapeDtypeStruct(dims, bf16)

    return pl.pallas_call(
        kernel,
        out_shape=(
            shape(rows, width),
            shape(3, width, local),
            shape(width, units),
            shape(units, width),
            shape(tokens, width),
            shape(chips, tokens, part),
            shape(tokens, width),
            shape(chips, tokens, part),
            shape(tokens, units),
            shape(tokens, units),
            shape(tokens, units),
            shape(tokens, local),
            shape(tokens, local),
            shape(tokens, 3 * local),
            shape(tokens, 3 * local),
            jax.ShapeDtypeStruct((8, width), f32),
            jax.ShapeDtypeStruct((8, local), f32),
        ),
        in_specs=[ANY] * 7 + [VMEM] * 7,
        out_specs=(ANY,) * 15 + (VMEM,) * 2,
        scratch_shapes=[
            pltpu.VMEM((rows, width), bf16),
            pltpu.VMEM((8, width), f32),
            pltpu.VMEM((tokens, width), bf16),
            pltpu.VMEM((width, width), bf16),
            pltpu.VMEM((width, units), bf16),
            pltpu.VMEM((local, width), bf16),
            pltpu.VMEM((tokens, units), bf16),
            pltpu.VMEM((tokens, units), bf16),
            pltpu.VMEM((3, tokens, local), bf16),
            pltpu.VMEM((tokens, local), bf16),
            pltpu.VMEM((local // HD, stored, BLOCK), bf16),
            pltpu.VMEM((stored, BLOCK), f32),
            pltpu.VMEM((tokens, local), bf16),
            pltpu.VMEM((tokens, 128), f32),
            pltpu.VMEM((tokens, 128), f32),
            pltpu.VMEM((2 * tensor - 3, rows, width), bf16),
            pltpu.SemaphoreType.DMA((sems.count,)),
            pltpu.SemaphoreType.DMA((sems.count,)),
            pltpu.SemaphoreType.DMA((24,)),
        ],
        compiler_params=pltpu.CompilerParams(
            collective_id=0, has_side_effects=True, vmem_limit_bytes=VMEM_LIMIT
        ),
        name="forward",
    )(*arrays)


def rotary_tables(segments):
    rows, length = segments.shape
    index = jnp.arange(length, dtype=jnp.int32)[None]
    start = jnp.zeros_like(segments)
    for number in range(1, 4):
        start = jnp.where(segments == number, jnp.sum(segments < number, -1, keepdims=True), start)
    position = (index - start).astype(f32).reshape(rows * length, 1)
    lane = jnp.arange(128, dtype=jnp.int32) % HD
    exponent = (2 * (lane % (ROT // 2))).astype(f32) / ROT
    angle = position * (1.0 / 10000.0**exponent)[None]
    cosine, sine = jnp.cos(angle), jnp.sin(angle)
    low, high = lane < ROT // 2, (lane >= ROT // 2) & (lane < ROT)
    return (
        jnp.where(lane < ROT, cosine, 1.0),
        jnp.where(low, -sine, 0.0),
        jnp.where(high, sine, 0.0),
    )


def matmul(a, b):
    return jnp.dot(a, b, preferred_element_type=f32)


def on_device(
    dp, tensor, fast,
    hidden_in, segments, ln_gain, ln_bias, qkv_weight, qkv_bias, dense_weight, dense_bias,
    fc1_weight, fc1_bias, fc2_weight, fc2_bias, cotangent,
):
    seqs = segments.shape[0]
    local = qkv_weight.shape[2]
    vectors = jnp.stack([ln_gain.astype(f32), ln_bias.astype(f32), dense_bias.astype(f32) + fc2_bias.astype(f32)])
    vectors = jnp.pad(vectors, ((0, 5), (0, 0)))
    mine = (
        hidden_in, cotangent, qkv_weight.transpose(1, 0, 2),
        dense_weight, fc1_weight, fc2_weight, vectors,
    )
    tables = rotary_tables(segments)
    bias = jnp.pad(qkv_bias.astype(f32), ((0, 5), (0, 0)))
    if fast:
        (
            out, w_qkv, w_fc1, w_fc2, normed, crossed_normed, grad_out, crossed_out,
            act, crossed_act, slope, attn, crossed_attn, grad_qkv, crossed_qkv, vec, qkv_sums,
        ) = forward_call(
            dp, tensor,
            (*mine, bias, fc1_bias.astype(f32)[None], *tables,
             segments.reshape(-1, 1), segments.reshape(1, -1)))
        grad_pre, crossed_pre, fc1_sums, sent_fc2, sent_dense = first_call(
            dp, tensor,
            (grad_out, crossed_out, act, crossed_act, slope, attn, crossed_attn, w_fc2))
        sums = jnp.concatenate([fc1_sums[0].reshape(4, local), qkv_sums[:3], jnp.zeros((1, local), f32)], 0)
        hidden_grad, sent_fc1, sent_qkv, vec_sums, all_sums = second_call(
            dp, tensor,
            (hidden_in, cotangent, vec, sums, normed, grad_pre, grad_qkv,
             crossed_normed, crossed_pre, crossed_qkv, w_qkv, w_fc1))
        quarter = vec_sums.shape[1] // tensor
        at = lax.axis_index("tensor") * quarter
        small = lax.dynamic_slice(vec_sums, (0, at), (3, quarter))
        return (
            out,
            hidden_grad,
            small[0],
            small[1],
            sent_qkv.astype(f32).reshape(-1, 3, local),
            all_sums[4:7],
            sent_dense.T.astype(f32),
            small[2],
            sent_fc1.astype(f32),
            all_sums[:4].reshape(-1),
            sent_fc2.T.astype(f32),
            small[2],
        )

    w_qkv, w_dense, w_fc1, w_fc2, normed, grad_out, vec = gather_plain(*mine)
    gain, out_bias = vec[0:1], vec[2:3]
    query, key, value, attn_vec, probs = attend(
        *(matmul(normed, w_qkv[i]) for i in range(3)), bias, tables, segments, seqs
    )
    pre_act = matmul(normed, w_fc1) + fc1_bias.astype(f32)
    act_vals, gelu_pull = jax.vjp(lambda pre: jax.nn.gelu(pre, approximate=True), pre_act)
    act_vals = act_vals.astype(bf16)
    slope = gelu_pull(jnp.ones_like(pre_act))[0].astype(bf16)
    branches = matmul(attn_vec, w_dense) + matmul(act_vals, w_fc2)
    grad_attn = matmul(grad_out, w_dense.T).astype(bf16)
    *grads, qkv_sums = attend_back(query, key, value, grad_attn, attn_vec, probs, tables, seqs)
    resid_in = hidden_in.astype(f32)
    cot_float = cotangent.astype(f32)
    centred = resid_in - jnp.mean(resid_in, -1, keepdims=True)
    spread = jnp.mean(centred * centred, -1, keepdims=True)
    inv_std = lax.rsqrt(spread + layer_eps)
    unit_rows = centred * inv_std
    summed = lax.psum_scatter(branches.astype(bf16), "tensor", scatter_dimension=0, tiled=True)
    out = (resid_in + summed.astype(f32) + out_bias).astype(bf16)
    out_bias_part = jnp.sum(cot_float, 0)
    grad_fc2 = matmul(act_vals.T, grad_out)
    grad_dense = matmul(attn_vec.T, grad_out)
    grad_pre = (matmul(grad_out, w_fc2.T) * slope.astype(f32)).astype(bf16)
    fc1_bias_part = jnp.sum(grad_pre.astype(f32), 0)
    grad_fc1 = matmul(normed.T, grad_pre)
    grad_wqkv = jnp.stack([matmul(normed.T, g) for g in grads])
    grad_normed = matmul(grad_pre, w_fc1.T) + sum(matmul(g, w.T) for g, w in zip(grads, w_qkv))
    sent_qkv, sent_dense, sent_fc1, sent_fc2 = (
        lax.psum_scatter(grad_wqkv.astype(bf16), "dp", scatter_dimension=1, tiled=True),
        lax.psum_scatter(grad_dense.astype(bf16), "dp", scatter_dimension=1, tiled=True),
        lax.psum_scatter(grad_fc1.astype(bf16), "dp", scatter_dimension=0, tiled=True),
        lax.psum_scatter(grad_fc2.astype(bf16), "dp", scatter_dimension=1, tiled=True),
    )
    grad_local = lax.psum_scatter(
        grad_normed.astype(bf16), "tensor", scatter_dimension=0, tiled=True
    ).astype(f32)
    gain_part = jnp.sum(grad_local * unit_rows, 0)
    beta_part = jnp.sum(grad_local, 0)
    scaled_grad = grad_local * gain
    first_mean = jnp.mean(scaled_grad, -1, keepdims=True)
    second_mean = jnp.mean(scaled_grad * unit_rows, -1, keepdims=True)
    hidden_grad = (
        cot_float + inv_std * (scaled_grad - first_mean - unit_rows * second_mean)
    ).astype(bf16)
    gain_grad, beta_grad, out_bias_grad = (
        lax.psum_scatter(gain_part, ("dp", "tensor"), scatter_dimension=0, tiled=True),
        lax.psum_scatter(beta_part, ("dp", "tensor"), scatter_dimension=0, tiled=True),
        lax.psum_scatter(out_bias_part, ("dp", "tensor"), scatter_dimension=0, tiled=True),
    )
    qkv_bias_grad, fc1_bias_grad = lax.psum((qkv_sums[:3], fc1_bias_part), "dp")
    return (
        out,
        hidden_grad,
        gain_grad,
        beta_grad,
        sent_qkv.transpose(1, 0, 2).astype(f32),
        qkv_bias_grad,
        sent_dense.astype(f32),
        out_bias_grad,
        sent_fc1.astype(f32),
        fc1_bias_grad,
        sent_fc2.astype(f32),
        out_bias_grad,
    )


def solution(mesh):
    dp, tensor = mesh.shape["dp"], mesh.shape["tensor"]
    fast = dp == 8 and tensor == 4
    placed = (
        P(("dp", "tensor"), None),
        P("dp", None),
        P("dp"),
        P("dp"),
        P("dp", None, "tensor"),
        P(None, "tensor"),
        P("tensor", "dp"),
        P("dp"),
        P("dp", "tensor"),
        P("tensor"),
        P("tensor", "dp"),
        P("dp"),
        P(("dp", "tensor"), None),
    )
    return jax.shard_map(
        functools.partial(on_device, dp, tensor, fast),
        mesh=mesh,
        in_specs=placed,
        out_specs=(
            P(("dp", "tensor"), None),
            P(("dp", "tensor"), None),
            P(("dp", "tensor")),
            P(("dp", "tensor")),
            P("dp", None, "tensor"),
            P(None, "tensor"),
            P("tensor", "dp"),
            P(("dp", "tensor")),
            P("dp", "tensor"),
            P("tensor"),
            P("tensor", "dp"),
            P(("dp", "tensor")),
        ),
        check_vma=False,
    )
```

```python
import functools

import jax
import jax.numpy as jnp
from jax import lax
from jax.experimental import pallas as pl
from jax.experimental.pallas import tpu as pltpu
from jax.sharding import PartitionSpec as P

HD = 64
ROT = 32
BLOCK = 256
MAX_DOC = 512
VMEM_LIMIT = 66_000_000
MESH = pl.DeviceIdType.MESH
ANY = pl.BlockSpec(memory_space=pl.ANY)
VMEM = pl.BlockSpec(memory_space=pltpu.VMEM)

layer_eps = 1e-05
f32 = jnp.float32
bf16 = jnp.bfloat16


def dot_nn(a, b):
    return lax.dot_general(a, b, (((1,), (0,)), ((), ())), preferred_element_type=f32)


def dot_nt(a, b):
    return lax.dot_general(a, b, (((1,), (1,)), ((), ())), preferred_element_type=f32)


def dot_tn(a, b):
    return lax.dot_general(a, b, (((0,), (0,)), ((), ())), preferred_element_type=f32)


def flip(index, bit):
    step = 1 << bit
    return index + step * (1 - 2 * (lax.div(index, step) % 2))


def relative(index, offset):
    bit = 0
    while offset >> bit:
        if (offset >> bit) & 1:
            index = flip(index, bit)
        bit += 1
    return index


def stages_of(order):
    held, stages = [0], []
    for bit in order:
        got = [r ^ (1 << bit) for r in held]
        stages.append((bit, list(held), got))
        held = held + got
    return stages


class Sems:
    def __init__(self):
        self.count = 0

    def take(self):
        self.count += 1
        return self.count - 1


class CubeGather:
    def __init__(self, sems, orders):
        self.plans = [stages_of(order) for order in orders]
        self.ids = {
            (h, j, i): sems.take()
            for h, stages in enumerate(self.plans)
            for j, (_, held, _) in enumerate(stages)
            for i in range(len(held))
        }

    def bind(self, me, other, own, window, send_sem, recv_sem):
        self.me, self.other, self.own, self.window = me, other, own, window
        self.send_sem, self.recv_sem = send_sem, recv_sem
        return self

    def copy(self, h, j, i):
        bit, held, _ = self.plans[h][j]
        slot = relative(self.me, held[i])
        target = self.window(slot, h)
        source = self.own(h) if held[i] == 0 else target
        k = self.ids[h, j, i]
        return pltpu.make_async_remote_copy(
            src_ref=source,
            dst_ref=target,
            send_sem=self.send_sem.at[k],
            recv_sem=self.recv_sem.at[k],
            device_id=(flip(self.me, bit), self.other),
            device_id_type=MESH,
        )

    def start(self):
        depth = len(self.plans[0])
        for j in range(depth):
            for h in range(len(self.plans)):
                self.copy(h, j, 0).start()

    def advance(self, j):
        for i in range(len(self.plans[0][j][1])):
            for h, stages in enumerate(self.plans):
                self.copy(h, j, i).wait_recv()
                slot = stages[j][2][i]
                for later in range(j + 1, len(stages)):
                    self.copy(h, later, stages[later][1].index(slot)).start()

    def finish(self):
        for h, j, i in self.ids:
            self.copy(h, j, i).wait_send()


class LineGather:
    def __init__(self, sems, size, subs):
        self.size, self.subs = size, subs
        self.ids = {
            (way, s, u): sems.take()
            for way in (0, 1)
            for s in range(size - 1)
            for u in range(subs)
        }

    def bind(self, me, other, own, window, send_sem, recv_sem):
        self.me, self.other, self.own, self.window = me, other, own, window
        self.send_sem, self.recv_sem = send_sem, recv_sem
        return self

    def copy(self, way, s, u):
        block = self.me - s if way == 0 else self.me + s
        target = self.window(block, u)
        k = self.ids[way, s, u]
        return pltpu.make_async_remote_copy(
            src_ref=self.own(u) if s == 0 else target,
            dst_ref=target,
            send_sem=self.send_sem.at[k],
            recv_sem=self.recv_sem.at[k],
            device_id=(self.other, self.me + 1 if way == 0 else self.me - 1),
            device_id_type=MESH,
        )

    def sends(self, way, s):
        if way == 0:
            return (self.me >= s) & (self.me < self.size - 1)
        return (self.me + s < self.size) & (self.me > 0)

    def gets(self, way, s):
        if way == 0:
            return self.me - 1 - s >= 0
        return self.me + 1 + s < self.size

    def start(self, u):
        for way in (0, 1):

            @pl.when(self.sends(way, 0))
            def _():
                self.copy(way, 0, u).start()

    def advance(self, s, u):
        for way in (0, 1):

            @pl.when(self.gets(way, s))
            def _():
                self.copy(way, s, u).wait_recv()

            if s + 1 < self.size - 1:

                @pl.when(self.sends(way, s + 1))
                def _():
                    self.copy(way, s + 1, u).start()

    def finish(self):
        for way, s, u in self.ids:

            @pl.when(self.sends(way, s))
            def _():
                self.copy(way, s, u).wait_send()


def greet(dp, me, tensor, line, all_tensor):
    barrier = pltpu.get_barrier_semaphore()

    def hello(a, b):
        pl.semaphore_signal(barrier, inc=1, device_id=(a, b), device_id_type=MESH)

    for r in range(1, dp):
        hello(relative(me, r), line)
    if all_tensor:
        for k in range(1, tensor):
            hello(me, lax.rem(line + k, tensor))
        pl.semaphore_wait(barrier, dp + tensor - 2)
        return

    @pl.when(line > 0)
    def _():
        hello(me, line - 1)

    @pl.when(line < tensor - 1)
    def _():
        hello(me, line + 1)

    left, right = jnp.minimum(line, 1), jnp.minimum(tensor - 1 - line, 1)
    pl.semaphore_wait(barrier, dp - 1 + left + right)


def orders_of(dp):
    bits = list(range(1, dp.bit_length() - 1))
    return [bits + [0], bits[::-1] + [0]]


def normalize(x, gain, bias):
    centred = x - jnp.mean(x, -1, keepdims=True)
    spread = jnp.mean(centred * centred, -1, keepdims=True)
    unit = centred * lax.rsqrt(spread + layer_eps)
    return (unit * gain + bias).astype(bf16)


def gather_plain(hidden, cotangent, w_qkv, w_dense, w_fc1, w_fc2, vectors):
    vec = lax.all_gather(vectors, "dp", axis=1, tiled=True)
    normed = normalize(hidden.astype(f32), vec[0:1], vec[1:2])
    return (
        lax.all_gather(w_qkv, "dp", axis=1, tiled=True),
        lax.all_gather(w_dense, "dp", axis=1, tiled=True),
        lax.all_gather(w_fc1, "dp", axis=0, tiled=True),
        lax.all_gather(w_fc2, "dp", axis=1, tiled=True),
        lax.all_gather(normed, "tensor", axis=0, tiled=True),
        lax.all_gather(cotangent, "tensor", axis=0, tiled=True),
        vec,
    )


class ChipReduce:
    COUNT = 6

    def __init__(self, sems):
        self.ids = [sems.take() for _ in range(self.COUNT)]

    def bind(self, me, other, view, landing, send_sem, recv_sem):
        self.me, self.other, self.view, self.landing = me, other, view, landing
        self.send_sem, self.recv_sem = send_sem, recv_sem
        return self

    def copy(self, slot):
        r, h, bit = [(2, 0, 2), (3, 0, 2), (1, 0, 1), (1, 1, 1), (3, 1, 1), (2, 1, 2)][slot]
        k = self.ids[slot]
        return pltpu.make_async_remote_copy(
            src_ref=self.view(r, h),
            dst_ref=self.landing.at[slot],
            send_sem=self.send_sem.at[k],
            recv_sem=self.recv_sem.at[k],
            device_id=(flip(self.me, bit), self.other),
            device_id_type=MESH,
        )

    def start(self, r):
        for slot in {3: (1, 4), 2: (0,), 1: (3,), 0: ()}[r]:
            self.copy(slot).start()

    def middle(self):
        for slot, r, h, last in ((1, 1, 0, 2), (4, 2, 1, 5)):
            self.copy(slot).wait_recv()
            view = self.view(r, h)
            view[...] = (view[...].astype(f32) + self.landing[slot].astype(f32)).astype(bf16)
            self.copy(last).start()

    def final(self):
        for h in (0, 1):
            for slot in ((0, 2), (3, 5))[h]:
                self.copy(slot).wait_recv()
            a, b = ((0, 2), (3, 5))[h]
            view = self.view(0, h)
            total = view[...].astype(f32) + self.landing[a].astype(f32) + self.landing[b].astype(f32)
            view[...] = total.astype(bf16)

    def finish(self):
        for slot in range(self.COUNT):
            self.copy(slot).wait_send()


def halves_of(parts):
    half = parts.shape[-1] // 2
    return lambda r, h: parts.at[r, :, pl.ds(h * half, half)]


class LineReduce:
    def __init__(self, sems, size):
        self.size = size
        self.ids = {(way, i): sems.take() for way in (0, 1) for i in range(size - 1)}

    def bind(self, me, other, own, landing, send_sem, recv_sem):
        self.me, self.other, self.own, self.landing = me, other, own, landing
        self.send_sem, self.recv_sem = send_sem, recv_sem
        return self

    def target(self, way, i):
        return self.size - 1 - i if way == 0 else i

    def place(self, way, i):
        return i if way == 0 else 2 * self.size - 4 - i

    def copy(self, way, i, edge):
        k = self.ids[way, i]
        here = self.landing.at[self.place(way, i)]
        return pltpu.make_async_remote_copy(
            src_ref=self.own(self.target(way, i)) if edge else here,
            dst_ref=here,
            send_sem=self.send_sem.at[k],
            recv_sem=self.recv_sem.at[k],
            device_id=(self.other, self.me + 1 if way == 0 else self.me - 1),
            device_id_type=MESH,
        )

    def edge(self, way):
        return self.me == (0 if way == 0 else self.size - 1)

    def passes(self, way, i):
        d = self.target(way, i)
        return (self.me > 0) & (self.me < d) if way == 0 else (self.me < self.size - 1) & (self.me > d)

    def start(self, way, i):
        @pl.when(self.edge(way))
        def _():
            self.copy(way, i, True).start()

    def advance(self, step, add):
        for way in (0, 1):
            steps_from_edge = self.me if way == 0 else self.size - 1 - self.me
            for i in range(step):

                @pl.when(self.passes(way, i) & (steps_from_edge == step - i))
                def _():
                    self.copy(way, i, False).wait_recv()
                    add(self.landing.at[self.place(way, i)], self.own(self.target(way, i)))
                    self.copy(way, i, False).start()

    def arrive(self):
        for way in (0, 1):
            for i in range(self.size - 1):

                @pl.when(self.me == self.target(way, i))
                def _():
                    self.copy(way, i, False).wait_recv()

    def finish(self):
        for way, i in self.ids:

            @pl.when(self.edge(way))
            def _():
                self.copy(way, i, True).wait_send()

            @pl.when(self.passes(way, i))
            def _():
                self.copy(way, i, False).wait_send()

    def total(self, own, rows):
        last = self.size - 1
        value = own.astype(f32)
        lefts = jnp.clip(last - self.me, 0, last - 1)
        rights = jnp.clip(self.me, 0, last - 1)
        from_left = self.landing[lefts, rows, :].astype(f32)
        from_right = self.landing[2 * self.size - 4 - rights, rows, :].astype(f32)
        value = value + jnp.where(self.me > 0, from_left, 0.0)
        return value + jnp.where(self.me < last, from_right, 0.0)


def add_into(landing, own):
    rows = landing.shape[0]

    @pl.loop(0, rows, step=64)
    def _(r):
        at = pl.ds(r, 64)
        landing[at, :] = (landing[at, :].astype(f32) + own[at, :].astype(f32)).astype(bf16)


def chip_slot(me, r):
    return (
        me
        + 2 * ((r % 2) * (1 - 2 * (lax.div(me, 2) % 2)))
        + 4 * (lax.div(r, 2) * (1 - 2 * (lax.div(me, 4) % 2)))
    )


def second_call(dp, tensor, arrays):
    hidden, cotangent, vec, sums, normed, grad_pre, grad_qkv = arrays[:7]
    rows, width = hidden.shape
    tokens, units = grad_pre.shape
    wide = grad_qkv.shape[1]
    local = wide // 3
    part = width // dp
    chips = dp // 2
    sems = Sems()
    reduce_fc1, reduce_qkv = ChipReduce(sems), ChipReduce(sems)
    line_in = LineReduce(sems, tensor)
    tells = [sems.take() for _ in range(2 * (dp - 1) + tensor - 1)]

    def kernel(
        x_ref, c_ref, vec_ref, sum_ref, n_ref, gp_in, gq_in, nx_in, gpx_in, gqx_in, wq_ref, w1_ref,
        hid_ref, s1_out, sq_out, vout_ref, bout_ref,
        x_buf, c_buf, n_buf, nx_buf, gp, gpx, gq, gqx, wq, w1, gn,
        s1, sq, r1, rq, rz, parts, tell_v, tell_b, tell_z, send_sem, recv_sem, local_sem,
    ):
        me, line = lax.axis_index("dp"), lax.axis_index("tensor")
        twin = flip(me, 0)

        def cols(a):
            return pl.ds(pl.multiple_of(a * part, part), part)

        pair = (send_sem, recv_sem)
        fc1 = reduce_fc1.bind(me, line, halves_of(s1), r1, *pair)
        qkv = reduce_qkv.bind(me, line, halves_of(sq), rq, *pair)
        ins = line_in.bind(line, me, lambda d: gn.at[pl.ds(d * rows, rows), :], rz, *pair)

        def remote(k, source, target, device):
            return pltpu.make_async_remote_copy(
                src_ref=source, dst_ref=target,
                send_sem=send_sem.at[k], recv_sem=recv_sem.at[k],
                device_id=device, device_id_type=MESH)

        def third(i):
            return pl.ds(i * local, local)

        bias_tells = [
            remote(tells[r - 1], sum_ref, tell_b.at[r], (relative(me, r), line)) for r in range(1, dp)
        ]
        vec_tells = [
            remote(tells[dp - 2 + r], parts.at[:, cols(relative(me, r))], tell_v.at[r],
                   (relative(me, r), line))
            for r in range(1, dp)
        ]
        line_tells = [
            remote(tells[2 * dp - 3 + k], tell_z.at[0], tell_z.at[k],
                   (me, lax.rem(line + k, tensor)))
            for k in range(1, tensor)
        ]
        tile = 512
        pieces = (
            [(gp_in, gp), (gq_in, gq)]
            + [(w1_ref.at[pl.ds(n, tile), :], w1.at[pl.ds(n, tile), :]) for n in range(0, width, tile)]
            + [
                (wq_ref.at[i, pl.ds(n, tile), :], wq.at[pl.ds(n, tile), third(i)])
                for n in range(0, width, tile) for i in range(3)
            ]
            + [(n_ref, n_buf), (nx_in, nx_buf), (gpx_in, gpx), (gqx_in, gqx), (x_ref, x_buf), (c_ref, c_buf)]
        )
        loads = [pltpu.make_async_copy(a, b, local_sem.at[k]) for k, (a, b) in enumerate(pieces)]
        tiles = width // tile
        late = 2 + 4 * tiles
        for copy in loads:
            copy.start()
        greet(dp, me, tensor, line, True)
        for copy in bias_tells:
            copy.start()
        for copy in loads[:late]:
            copy.wait()
        upper = lax.div(line, tensor // 2)

        @pl.loop(0, tensor)
        def _(i):
            d = (1 - upper) * (tensor - 1 - i) + upper * i
            at = pl.ds(pl.multiple_of(d * rows, rows), rows)

            @pl.loop(0, width, step=1024)
            def _(n):
                to = pl.ds(pl.multiple_of(n, 1024), 1024)
                value = dot_nt(gp[at, :], w1[to, :]) + dot_nt(gq[at, :], wq[to, :])
                gn[at, to] = value.astype(bf16)

            for k in range(tensor - 1):

                @pl.when(i == k)
                def _():
                    ins.start(0, k)
                    ins.start(1, k)

        for copy in loads[late : late + 4]:
            copy.wait()

        def weight_grad(target, plan, own, crossed, size, step):
            @pl.loop(0, chips)
            def _(i):
                r = chips - 1 - i
                slot = chip_slot(me, r)

                @pl.loop(0, size, step=step)
                def _(n):
                    at = pl.ds(pl.multiple_of(n, step), step)
                    value = dot_tn(n_buf[:, cols(slot)], own[:, at])
                    value = value + dot_tn(nx_buf[r], crossed[:, at])
                    target[r, :, at] = value.astype(bf16)

                for k in range(1, chips):

                    @pl.when(r == k)
                    def _():
                        plan.start(k)

        weight_grad(s1, fc1, gp, gpx, units, 1024)
        ins.advance(1, add_into)
        weight_grad(sq, qkv, gq, gqx, wide, 768)
        ins.advance(2, add_into)
        fc1.middle()
        for copy in bias_tells:
            copy.wait_recv()
        total = sum_ref[...]
        for r in range(1, dp):
            total = total + tell_b[r]
        bout_ref[...] = total
        for copy in loads[late + 4 :]:
            copy.wait()
        qkv.middle()
        ins.arrive()
        parts[...] = jnp.zeros_like(parts)

        @pl.loop(0, rows, step=32)
        def _(r):
            at = pl.ds(r, 32)
            x = x_buf[at, :].astype(f32)
            centred = x - jnp.mean(x, -1, keepdims=True)
            inv_std = lax.rsqrt(jnp.mean(centred * centred, -1, keepdims=True) + layer_eps)
            unit = centred * inv_std
            own = pl.ds(pl.multiple_of(line * rows + r, 32), 32)
            grad = ins.total(gn[own, :], at)
            cot = c_buf[at, :].astype(f32)
            scaled = grad * vec_ref[0:1, :]
            first = jnp.mean(scaled, -1, keepdims=True)
            second = jnp.mean(scaled * unit, -1, keepdims=True)
            c_buf[at, :] = (cot + inv_std * (scaled - first - unit * second)).astype(bf16)
            parts[0:1, :] += jnp.sum(grad * unit, 0, keepdims=True)
            parts[1:2, :] += jnp.sum(grad, 0, keepdims=True)
            parts[2:3, :] += jnp.sum(cot, 0, keepdims=True)

        last = pltpu.make_async_copy(c_buf, hid_ref, local_sem.at[len(loads)])
        last.start()
        for copy in vec_tells:
            copy.start()
        fc1.final()
        store1 = pltpu.make_async_copy(s1.at[0], s1_out, local_sem.at[len(loads) + 1])
        store1.start()
        for copy in vec_tells:
            copy.wait_recv()
        total_v = parts[:, cols(me)]
        for r in range(1, dp):
            total_v = total_v + tell_v[r]
        tell_z[0] = total_v
        for copy in line_tells:
            copy.start()
        qkv.final()
        storeq = pltpu.make_async_copy(sq.at[0], sq_out, local_sem.at[len(loads) + 2])
        storeq.start()
        for copy in line_tells:
            copy.wait_recv()
        total_z = tell_z[0]
        for k in range(1, tensor):
            total_z = total_z + tell_z[k]
        vout_ref[...] = total_z
        for copy in bias_tells + vec_tells + line_tells:
            copy.wait_send()
        for plan in (fc1, qkv, ins):
            plan.finish()
        for copy in (last, store1, storeq):
            copy.wait()

    return pl.pallas_call(
        kernel,
        out_shape=(
            jax.ShapeDtypeStruct((rows, width), bf16),
            jax.ShapeDtypeStruct((part, units), bf16),
            jax.ShapeDtypeStruct((part, wide), bf16),
            jax.ShapeDtypeStruct((8, part), f32),
            jax.ShapeDtypeStruct((8, local), f32),
        ),
        in_specs=[ANY] * 2 + [VMEM] * 2 + [ANY] * 8,
        out_specs=(ANY, ANY, ANY, VMEM, VMEM),
        scratch_shapes=[
            pltpu.VMEM((rows, width), bf16),
            pltpu.VMEM((rows, width), bf16),
            pltpu.VMEM((tokens, width), bf16),
            pltpu.VMEM((chips, tokens, part), bf16),
            pltpu.VMEM((tokens, units), bf16),
            pltpu.VMEM((tokens, units), bf16),
            pltpu.VMEM((tokens, wide), bf16),
            pltpu.VMEM((tokens, wide), bf16),
            pltpu.VMEM((width, wide), bf16),
            pltpu.VMEM((width, units), bf16),
            pltpu.VMEM((tokens, width), bf16),
            pltpu.VMEM((chips, part, units), bf16),
            pltpu.VMEM((chips, part, wide), bf16),
            pltpu.VMEM((6, part, units // 2), bf16),
            pltpu.VMEM((6, part, wide // 2), bf16),
            pltpu.VMEM((2 * tensor - 3, rows, width), bf16),
            pltpu.VMEM((8, width), f32),
            pltpu.VMEM((dp, 8, part), f32),
            pltpu.VMEM((dp, 8, local), f32),
            pltpu.VMEM((tensor, 8, part), f32),
            pltpu.SemaphoreType.DMA((sems.count,)),
            pltpu.SemaphoreType.DMA((sems.count,)),
            pltpu.SemaphoreType.DMA((30,)),
        ],
        compiler_params=pltpu.CompilerParams(
            collective_id=2, has_side_effects=True, vmem_limit_bytes=VMEM_LIMIT
        ),
        name="second_back",
    )(*arrays)


def spans_of(length):
    back = -(-(MAX_DOC - 1) // BLOCK)
    spans, at = [], 0
    for i in range(length // BLOCK):
        low = max(0, i - back) * BLOCK
        spans.append((low, (i + 1) * BLOCK, at))
        at += (i + 1) * BLOCK - low
    return spans, at


def turn(x, cosine, sine_lo, sine_hi):
    return x * cosine + pltpu.roll(x, 128 - ROT // 2, 1) * sine_lo + pltpu.roll(x, ROT // 2, 1) * sine_hi


def head_lanes(shape, e):
    lane = lax.broadcasted_iota(jnp.int32, shape, 1)
    return (lane >= e * HD) & (lane < (e + 1) * HD)


def only(x, e):
    return jnp.where(head_lanes(x.shape, e), x, jnp.zeros_like(x))


def attend_kernel(
    q_ref, k_ref, v_ref, bias_ref, cos_ref, slo_ref, shi_ref, segc_ref, segr_ref,
    qs_ref, ks_ref, vs_ref, o_ref, p_ref, mask_ref,
):
    @pl.when(pl.program_id(1) == 0)
    def _():
        fill_mask(mask_ref, segc_ref, segr_ref, q_ref.shape[0])

    cosine, slo, shi = cos_ref[...], slo_ref[...], shi_ref[...]
    query = turn(q_ref[...] + bias_ref[0:1, :], cosine, slo, shi).astype(bf16) * bf16(HD**-0.5)
    key = turn(k_ref[...] + bias_ref[1:2, :], cosine, slo, shi).astype(bf16)
    value = (v_ref[...] + bias_ref[2:3, :]).astype(bf16)
    qs_ref[...] = query
    ks_ref[...] = key
    vs_ref[...] = value

    def keep(e, at, probs):
        p_ref[e, at, :] = probs

    def write(at, result):
        o_ref[at, :] = result

    attend_pair(query, key, value, mask_ref, keep, write)


def attend(q, k, v, qkv_bias, tables, segments, rows):
    tokens, local = q.shape
    length = tokens // rows
    pairs = local // 128
    _, stored = spans_of(length)
    block = pl.BlockSpec((length, 128), lambda r, h: (r, h))
    table = pl.BlockSpec((length, 128), lambda r, h: (r, 0))
    shape = jax.ShapeDtypeStruct((tokens, local), bf16)
    return pl.pallas_call(
        attend_kernel,
        grid=(rows, pairs),
        out_shape=(shape,) * 4 + (jax.ShapeDtypeStruct((rows, local // HD, stored, BLOCK), bf16),),
        in_specs=[block] * 3
        + [pl.BlockSpec((8, 128), lambda r, h: (0, h))]
        + [table] * 3
        + [
            pl.BlockSpec((length, 1), lambda r, h: (r, 0)),
            pl.BlockSpec((pl.Squeezed(), 1, length), lambda r, h: (r, 0, 0)),
        ],
        out_specs=(block,) * 4
        + (pl.BlockSpec((pl.Squeezed(), 128 // HD, stored, BLOCK), lambda r, h: (r, h, 0, 0)),),
        scratch_shapes=[pltpu.VMEM((stored, BLOCK), f32)],
        compiler_params=pltpu.CompilerParams(vmem_limit_bytes=VMEM_LIMIT),
        cost_estimate=pl.CostEstimate(
            flops=16 * tokens * 768 * local, bytes_accessed=24 << 20, transcendentals=0
        ),
        name="attend",
    )(q, k, v, qkv_bias, *tables, segments.reshape(tokens, 1), segments.reshape(rows, 1, length))


def attend_back_kernel(
    q_ref, k_ref, v_ref, g_ref, o_ref, p_ref, cos_ref, slo_ref, shi_ref,
    dq_ref, dk_ref, dv_ref, bias_ref, kacc_ref, vacc_ref,
):
    def write(which, at, value):
        (dq_ref, dk_ref, dv_ref)[which][at, :] = value

    sums = attend_back_pair(
        q_ref[...], k_ref[...], v_ref[...], g_ref[...], o_ref[...],
        lambda e, at: p_ref[e, at, :], (cos_ref, slo_ref, shi_ref), kacc_ref, vacc_ref, write)
    sums = jnp.concatenate(list(sums) + [jnp.zeros((5, 128), f32)], 0)

    @pl.when(pl.program_id(1) == 0)
    def _():
        bias_ref[...] = sums

    @pl.when(pl.program_id(1) > 0)
    def _():
        bias_ref[...] += sums


def attend_back(q, k, v, g, o, probs, tables, rows):
    tokens, local = q.shape
    length = tokens // rows
    pairs = local // 128
    stored = probs.shape[2]
    block = pl.BlockSpec((length, 128), lambda h, r: (r, h))
    table = pl.BlockSpec((length, 128), lambda h, r: (r, 0))
    shape = jax.ShapeDtypeStruct((tokens, local), bf16)
    return pl.pallas_call(
        attend_back_kernel,
        grid=(pairs, rows),
        out_shape=(shape,) * 3 + (jax.ShapeDtypeStruct((8, local), f32),),
        in_specs=[block] * 5
        + [pl.BlockSpec((pl.Squeezed(), 128 // HD, stored, BLOCK), lambda h, r: (r, h, 0, 0))]
        + [table] * 3,
        out_specs=(block,) * 3 + (pl.BlockSpec((8, 128), lambda h, r: (0, h)),),
        scratch_shapes=[pltpu.VMEM((length, 128), f32)] * 2,
        compiler_params=pltpu.CompilerParams(vmem_limit_bytes=VMEM_LIMIT),
        cost_estimate=pl.CostEstimate(
            flops=32 * tokens * 768 * local, bytes_accessed=24 << 20, transcendentals=0
        ),
        name="attend_back",
    )(q, k, v, g, o, probs, *tables)


def attend_pair(query, key, value, mask_ref, keep, write):
    length = query.shape[0]
    spans, _ = spans_of(length)
    for i, (low, high, at) in enumerate(spans):
        mine = slice(i * BLOCK, (i + 1) * BLOCK)
        total = jnp.zeros((BLOCK, 128), f32)
        for e in range(128 // HD):
            scores = dot_nt(only(key[low:high], e), query[mine]) + mask_ref[at : at + high - low, :]
            exponent = jnp.exp(scores - jnp.max(scores, 0, keepdims=True))
            inverse = 1.0 / jnp.sum(exponent, 0, keepdims=True)
            probs = (exponent * inverse).astype(bf16)
            keep(e, slice(at, at + high - low), probs)
            total = total + dot_tn(probs, only(value[low:high], e))
        write(mine, total.astype(bf16))


def fill_mask(mask_ref, segc_ref, segr_ref, length):
    for i, (low, high, at) in enumerate(spans_of(length)[0]):
        keys = lax.broadcasted_iota(jnp.int32, (high - low, BLOCK), 0) + low
        queries = lax.broadcasted_iota(jnp.int32, (high - low, BLOCK), 1) + i * BLOCK
        own = segr_ref[:, i * BLOCK : (i + 1) * BLOCK].astype(f32)
        same = segc_ref[low:high, 0:1].astype(f32) == own
        mask_ref[at : at + high - low, :] = jnp.where((keys <= queries) & same, 0.0, -1e30)


def fill_tables(seg_ref, column_ref, cos_ref, slo_ref, shi_ref):
    length = seg_ref.shape[1]
    row = seg_ref[...].astype(f32)
    column_ref[...] = jnp.broadcast_to(row, (128, length)).T
    starts = [jnp.sum(jnp.where(row < number, 1.0, 0.0), 1, keepdims=True) for number in range(1, 4)]
    lane = lax.broadcasted_iota(jnp.int32, (1, 128), 1) % HD
    exponent = (2 * (lane % (ROT // 2))).astype(f32) / ROT
    frequency = 1.0 / jnp.exp(exponent * f32(9.210340371976184))

    @pl.loop(0, length, step=128)
    def _(r):
        at = pl.ds(pl.multiple_of(r, 128), 128)
        column = column_ref[at, :]
        start = jnp.zeros_like(column)
        for number in range(1, 4):
            start = jnp.where(column == number, starts[number - 1], start)
        index = (lax.broadcasted_iota(jnp.int32, (128, 128), 0) + r).astype(f32)
        angle = (index - start) * frequency
        cosine, sine = jnp.cos(angle), jnp.sin(angle)
        cos_ref[at, :] = jnp.where(lane < ROT, cosine, 1.0)
        slo_ref[at, :] = jnp.where(lane < ROT // 2, -sine, 0.0)
        shi_ref[at, :] = jnp.where((lane >= ROT // 2) & (lane < ROT), sine, 0.0)


def attend_back_pair(query, key, value, grad, result, probs_of, tables, kacc_ref, vacc_ref, write):
    length = query.shape[0]
    spans, _ = spans_of(length)
    heads = 128 // HD
    inner = grad.astype(f32) * result.astype(f32)
    lane = lax.broadcasted_iota(jnp.int32, (8, 128), 1)
    row = lax.broadcasted_iota(jnp.int32, (8, 128), 0)
    pick = jnp.where(lax.div(lane, HD) == row, 1.0, 0.0)
    delta = lax.dot_general(
        pick, inner, (((1,), (1,)), ((), ())),
        precision=lax.Precision.HIGHEST, preferred_element_type=f32)
    kacc_ref[...] = jnp.zeros_like(kacc_ref)
    vacc_ref[...] = jnp.zeros_like(vacc_ref)
    cos_ref, slo_ref, shi_ref = tables
    first = jnp.zeros((1, 128), f32)
    for i, (low, high, at) in enumerate(spans):
        mine = slice(i * BLOCK, (i + 1) * BLOCK)
        g_i, q_i = grad[mine], query[mine]
        dq = jnp.zeros((BLOCK, 128), f32)
        ps, dss = [], []
        for e in range(heads):
            probs = probs_of(e, slice(at, at + high - low))
            dprobs = dot_nt(only(value[low:high], e), g_i)
            ds = (probs.astype(f32) * (dprobs - delta[e : e + 1, mine])).astype(bf16)
            dq = dq + dot_tn(ds, only(key[low:high], e))
            ps.append(probs)
            dss.append(ds)
        g_cat = jnp.concatenate([only(g_i, e) for e in range(heads)], 0)
        q_cat = jnp.concatenate([only(q_i, e) for e in range(heads)], 0)
        vacc_ref[low:high, :] += dot_nn(jnp.concatenate(ps, 1), g_cat)
        kacc_ref[low:high, :] += dot_nn(jnp.concatenate(dss, 1), q_cat)
        dq = dq * f32(HD**-0.5)
        dq = turn(dq, cos_ref[mine, :], -slo_ref[mine, :], -shi_ref[mine, :]).astype(bf16)
        write(0, mine, dq)
        first = first + jnp.sum(dq.astype(f32), 0, keepdims=True)
    everything = slice(0, length)
    dk = turn(kacc_ref[...], cos_ref[...], -slo_ref[...], -shi_ref[...]).astype(bf16)
    dv = vacc_ref[...].astype(bf16)
    write(1, everything, dk)
    write(2, everything, dv)
    return first, jnp.sum(dk.astype(f32), 0, keepdims=True), jnp.sum(dv.astype(f32), 0, keepdims=True)


def forward_call(dp, tensor, arrays):
    hidden, cotangent, w_qkv, w_dense, w_fc1, w_fc2, vectors = arrays[:7]
    rows, width = hidden.shape
    local = w_qkv.shape[2]
    units = w_fc1.shape[1]
    part = width // dp
    chips = dp // 2
    tokens = rows * tensor
    pairs = local // 128
    stored = spans_of(tokens)[1]
    sems = Sems()
    orders = orders_of(dp)
    vec_ids = [sems.take() for _ in range(dp - 1)]
    plan_qkv, plan_dense, plan_fc1, plan_fc2 = (CubeGather(sems, orders) for _ in range(4))
    plan_n, plan_c = LineGather(sems, tensor, 2), LineGather(sems, tensor, 2)
    line_out = LineReduce(sems, tensor)
    reduce_fc2, reduce_dense = ChipReduce(sems), ChipReduce(sems)
    swaps = [sems.take() for _ in range(2 * chips + 4)]

    def kernel(
        x_ref, c_ref, wq_ref, wd_ref, w1_ref, w2_ref, vec_ref,
        qb_ref, fb_ref, seg_ref,
        out_ref, gq_ref, g1_ref, g2_ref, n_out, nx_out, c_out, cx_out, ax_out, d_out,
        tx_out, dq_out, dqx_out, gp_out, gpx_out, s2_out, sd_out, gvec_ref, qsum_ref, sum_ref,
        x_buf, vec_buf, nv, wa, wb, wd, act, slope, qkv3, attn, pb, mask, g_buf, kacc, vacc,
        cos_ref, slo_ref, shi_ref, rz, r2, rd,
        send_sem, recv_sem, local_sem,
    ):
        me, line = lax.axis_index("dp"), lax.axis_index("tensor")
        twin = flip(me, 0)
        half = part // 2
        local_count = [0]

        def cols(a):
            return pl.ds(pl.multiple_of(a * part, part), part)

        def half_rows(a, h):
            return pl.ds(pl.multiple_of(a * part + h * half, half), half)

        def tok(b, u):
            return pl.ds(pl.multiple_of(b * rows + u * (rows // 2), rows // 2), rows // 2)

        def block(b):
            return pl.ds(pl.multiple_of(b * rows, rows), rows)

        def piece(n, h):
            return pl.ds(h * (n // 2), n // 2)

        def copy_of(a, b):
            local_count[0] += 1
            return pltpu.make_async_copy(a, b, local_sem.at[local_count[0] - 1])

        def to_twin(k, source, target):
            return pltpu.make_async_remote_copy(
                src_ref=source, dst_ref=target,
                send_sem=send_sem.at[swaps[k]], recv_sem=recv_sem.at[swaps[k]],
                device_id=(twin, line), device_id_type=MESH)

        pair = (send_sem, recv_sem)
        vec = [
            pltpu.make_async_remote_copy(
                src_ref=vec_ref, dst_ref=vec_buf.at[:, cols(me)],
                send_sem=send_sem.at[k], recv_sem=recv_sem.at[k],
                device_id=(relative(me, r), line), device_id_type=MESH)
            for r, k in enumerate(vec_ids, 1)
        ]
        qkv = plan_qkv.bind(
            me, line,
            lambda h: wq_ref.at[:, pl.ds(h * half, half), :],
            lambda a, h: gq_ref.at[:, half_rows(a, h), :], *pair)
        fc1 = plan_fc1.bind(
            me, line,
            lambda h: w1_ref.at[pl.ds(h * half, half), :],
            lambda a, h: g1_ref.at[half_rows(a, h), :], *pair)
        dense = plan_dense.bind(
            me, line,
            lambda h: wd_ref.at[piece(local, h), :],
            lambda a, h: wd.at[piece(local, h), cols(a)], *pair)
        fc2 = plan_fc2.bind(
            me, line,
            lambda h: w2_ref.at[piece(units, h), :],
            lambda a, h: g2_ref.at[piece(units, h), cols(a)], *pair)
        norm = plan_n.bind(
            line, me, lambda u: nv.at[tok(line, u)], lambda b, u: nv.at[tok(b, u)], *pair)
        cot = plan_c.bind(
            line, me, lambda u: c_ref.at[piece(rows, u)], lambda b, u: c_out.at[tok(b, u)], *pair)
        outs = line_out.bind(line, me, lambda d: nv.at[pl.ds(d * rows, rows), :], rz, *pair)
        stages = dp.bit_length() - 1

        takes = [
            copy_of(x_ref, x_buf),
            copy_of(vec_ref, vec_buf.at[:, cols(me)]),
            copy_of(wd_ref, wd.at[:, cols(me)]),
            copy_of(wq_ref, qkv3.at[:, pl.ds(0, part), :]),
            copy_of(w1_ref, act.at[pl.ds(0, part), :]),
            copy_of(c_ref, act.at[pl.ds(part, rows), :]),
            copy_of(w2_ref, wb.at[:, pl.ds(0, part)]),
        ]
        keeps = [
            copy_of(qkv3.at[:, pl.ds(0, part), :], gq_ref.at[:, cols(me), :]),
            copy_of(act.at[pl.ds(0, part), :], g1_ref.at[cols(me), :]),
            copy_of(act.at[pl.ds(part, rows), :], c_out.at[block(line), :]),
            copy_of(wb.at[:, pl.ds(0, part)], g2_ref.at[:, cols(me)]),
        ]
        for copy in takes[:2]:
            copy.start()
        greet(dp, me, tensor, line, False)
        for copy in vec:
            copy.start()
        qkv.start()
        cot.start(0)
        for copy in takes[2:]:
            copy.start()
        fill_tables(seg_ref, kacc, cos_ref, slo_ref, shi_ref)
        for copy in takes[:2]:
            copy.wait()
        for copy in vec:
            copy.wait_recv()

        @pl.loop(0, rows, step=32)
        def _(r):
            x = x_buf[pl.ds(r, 32), :].astype(f32)
            centred = x - jnp.mean(x, -1, keepdims=True)
            spread = jnp.mean(centred * centred, -1, keepdims=True)
            unit = centred * lax.rsqrt(spread + layer_eps)
            at = pl.ds(pl.multiple_of(line * rows + r, 32), 32)
            nv[at, :] = (unit * vec_buf[0:1, :] + vec_buf[1:2, :]).astype(bf16)

        norm.start(0)
        norm.start(1)
        gvec_ref[...] = vec_buf[...]
        qkv.advance(0)
        fc1.start()
        for take, copy in zip(takes[3:], keeps):
            take.wait()
            copy.start()
        fill_mask(mask, kacc, seg_ref, tokens)

        def project(b):
            at = block(b)
            cosine, slo, shi = cos_ref[at, :], slo_ref[at, :], shi_ref[at, :]
            for i in range(3):
                value = dot_nn(nv[at, :], wa[:, i * local : (i + 1) * local]) + qb_ref[i : i + 1, :].astype(f32)
                if i == 2:
                    qkv3[2, at, :] = value.astype(bf16)
                    continue
                for h in range(pairs):
                    lanes = slice(h * 128, (h + 1) * 128)
                    turned = turn(value[:, lanes], cosine, slo, shi).astype(bf16)
                    if i == 0:
                        turned = turned * bf16(HD**-0.5)
                    qkv3[i, at, lanes] = turned

        def hidden_layer(b):
            at = block(b)

            @pl.loop(0, units, step=512)
            def _(n):
                to = pl.ds(pl.multiple_of(n, 512), 512)
                pre = dot_nn(nv[at, :], wb[:, to]) + fb_ref[0:1, to].astype(f32)
                square = pre * pre
                bend = jnp.tanh(0.7978845608028654 * pre * (1.0 + 0.044715 * square))
                act[at, to] = (0.5 * pre * (1.0 + bend)).astype(bf16)
                rise = 0.7978845608028654 * (1.0 + 3 * 0.044715 * square)
                slope[at, to] = (
                    0.5 * (1.0 + bend) + 0.5 * pre * (1.0 - bend * bend) * rise
                ).astype(bf16)

        def blocks_of(s, task):
            @pl.loop(0, 2)
            def _(way):
                b = line + (2 * way - 1) * (1 + s)

                @pl.when((b >= 0) & (b < tensor) & ((s >= 0) | (way == 0)))
                def _():
                    task(b)

        norm.advance(0, 0)
        for j in range(1, stages - 1):
            qkv.advance(j)
        norm.advance(0, 1)
        qkv.advance(stages - 1)
        keeps[0].wait()
        load_q = [
            copy_of(gq_ref.at[i], wa.at[:, pl.ds(i * local, local)]) for i in range(3)
        ]
        for copy in load_q:
            copy.start()
        fc1.advance(0)
        dense.start()
        fc2.start()
        for copy in load_q:
            copy.wait()

        @pl.loop(-1, tensor - 2)
        def _(s):
            @pl.when(s == tensor - 3)
            def _():
                norm.advance(tensor - 3, 0)
                norm.advance(tensor - 3, 1)
                cot.start(1)
                cot.advance(0, 0)

            blocks_of(s, project)

        for j in range(1, stages):
            fc1.advance(j)
        dense.advance(0)
        for copy in keeps[1:]:
            copy.wait()
        load_1 = copy_of(g1_ref, wb)
        load_1.start()
        load_1.wait()

        @pl.loop(-1, tensor - 1)
        def _(s):
            @pl.when(s == tensor - 2)
            def _():
                norm.advance(tensor - 2, 0)
                norm.advance(tensor - 2, 1)
                fc2.advance(0)
                blocks_of(tensor - 2, project)

            blocks_of(s, hidden_layer)

        n_store = copy_of(nv, n_out)
        n_store.start()
        cross_n = [
            to_twin(r, nv.at[:, cols(relative(twin, r << 1))], nx_out.at[r]) for r in range(chips)
        ]
        store_d = copy_of(slope, d_out)
        cross_a = to_twin(chips, act, ax_out)
        for copy in cross_n + [store_d, cross_a]:
            copy.start()

        @pl.loop(0, pairs)
        def _(h):
            lanes = pl.ds(pl.multiple_of(h * 128, 128), 128)

            def keep(e, at, value):
                pb[2 * h + e, at, :] = value

            def write(at, value):
                attn[at, lanes] = value

            attend_pair(
                qkv3[0, :, lanes], qkv3[1, :, lanes], qkv3[2, :, lanes], mask, keep, write)

            @pl.when(h == 0)
            def _():
                for j in range(1, stages - 1):
                    dense.advance(j)

            @pl.when(h == 1)
            def _():
                cot.advance(0, 1)

        cross_t = to_twin(chips + 1, attn, tx_out)
        cross_t.start()
        for j in range(1, stages - 1):
            fc2.advance(j)
        dense.advance(stages - 1)
        fc2.advance(stages - 1)
        takes[2].wait()
        load_2 = copy_of(g2_ref, wa)
        load_2.start()
        cot.advance(1, 0)
        norm.finish()
        n_store.wait()
        for copy in cross_n:
            copy.wait_send()
        load_2.wait()
        upper = lax.div(line, tensor // 2)

        @pl.loop(0, tensor)
        def _(i):
            d = (1 - upper) * (tensor - 1 - i) + upper * i
            at = block(d)

            @pl.loop(0, width, step=1024)
            def _(n):
                to = pl.ds(pl.multiple_of(n, 1024), 1024)
                value = dot_nn(act[at, :], wa[:, to]) + dot_nn(attn[at, :], wd[:, to])
                nv[at, to] = value.astype(bf16)

            for k in range(tensor - 1):

                @pl.when(i == k)
                def _():
                    outs.start(0, k)
                    outs.start(1, k)

            @pl.when(i == tensor - 2)
            def _():
                cot.advance(1, 1)

        store_d.wait()
        cross_a.wait_recv()
        cross_t.wait_recv()
        load_ax = copy_of(ax_out, slope)
        load_tx = copy_of(tx_out, wb.at[pl.ds(tokens, tokens), pl.ds(width // 2, local)])
        load_ax.start()
        load_tx.start()
        cot.advance(2, 0)
        outs.advance(1, add_into)
        cot.advance(2, 1)
        grad = wa.at[pl.ds(0, tokens), :]
        load_c = copy_of(c_out, grad)
        cross_c = [
            to_twin(chips + 2 + r, c_out.at[:, cols(relative(twin, r << 1))], cx_out.at[r])
            for r in range(chips)
        ]
        for copy in cross_c:
            copy.start()
        load_c.start()
        load_c.wait()
        g_buf[...] = dot_nt(grad[...], wd[...]).astype(bf16)
        load_cx = [
            copy_of(cx_out.at[r], wb.at[pl.ds(tokens, tokens), pl.ds(r * part, part)])
            for r in range(chips)
        ]
        for crossed, copy in zip(cross_c, load_cx):
            crossed.wait_recv()
            copy.start()
        for copy in load_cx + [load_ax, load_tx]:
            copy.wait()

        def weight_grad(left, spot, plan, own, crossed, size, step):
            @pl.loop(0, chips)
            def _(i):
                r = chips - 1 - i
                slot = chip_slot(me, r)

                @pl.loop(0, size, step=step)
                def _(n):
                    at = pl.multiple_of(n, step)
                    value = dot_tn(left[:, cols(slot)], own(at))
                    crossed_left = wb[pl.ds(tokens, tokens), pl.ds(pl.multiple_of(r * part, part), part)]
                    value = value + dot_tn(crossed_left, crossed(at))
                    spot(r, at, value.astype(bf16))

                for k in range(1, chips):

                    @pl.when(r == k)
                    def _():
                        plan.start(k)

        def spot_2(r, at, value):
            wa[pl.ds(pl.multiple_of(tokens + r * part, part), part), pl.ds(at, 1024)] = value

        def spot_d(r, at, value):
            wb[pl.ds(pl.multiple_of(r * part, part), part), pl.ds(3 * local, local)] = value

        sum_2 = reduce_fc2.bind(
            me, line,
            lambda r, h: wa.at[pl.ds(tokens + r * part, part), pl.ds(h * (units // 2), units // 2)],
            r2, *pair)
        sum_d = reduce_dense.bind(
            me, line,
            lambda r, h: wb.at[pl.ds(r * part, part), pl.ds(3 * local + h * (local // 2), local // 2)],
            rd, *pair)
        weight_grad(
            grad, spot_2, sum_2, lambda at: act[:, pl.ds(at, 1024)],
            lambda at: slope[:, pl.ds(at, 1024)], units, 1024)
        weight_grad(
            grad, spot_d, sum_d, lambda at: attn[...],
            lambda at: wb[pl.ds(tokens, tokens), pl.ds(width // 2, local)], local, local)
        sum_2.middle()
        cross_a.wait_send()
        load_d = copy_of(d_out, act)
        load_d.start()
        qsum_ref[...] = jnp.zeros_like(qsum_ref)

        @pl.loop(0, pairs)
        def _(h):
            lanes = pl.ds(pl.multiple_of(h * 128, 128), 128)

            def write(which, at, value):
                wb[at, pl.ds(pl.multiple_of(which * local + h * 128, 128), 128)] = value

            sums = attend_back_pair(
                qkv3[0, :, lanes], qkv3[1, :, lanes], qkv3[2, :, lanes],
                g_buf[:, lanes], attn[:, lanes], lambda e, at: pb[2 * h + e, at, :],
                (cos_ref, slo_ref, shi_ref), kacc, vacc, write)
            for k in range(3):
                qsum_ref[k : k + 1, lanes] = sums[k]

            @pl.when(h == 0)
            def _():
                outs.advance(2, add_into)

            @pl.when(h == 2)
            def _():
                sum_d.middle()

        slabs = width // BLOCK
        load_w = [
            copy_of(g2_ref.at[:, pl.ds(e * BLOCK, BLOCK)], pb.at[e, pl.ds(0, units), :])
            for e in range(slabs)
        ]
        for copy in load_w:
            copy.start()
        back = wb.at[pl.ds(0, tokens), pl.ds(0, 3 * local)]
        store_q = copy_of(back, dq_out)
        store_q.start()
        cross_d = to_twin(2 * chips + 2, back, dqx_out)
        cross_d.start()
        for copy in load_w:
            copy.wait()
        load_d.wait()

        @pl.loop(0, units, step=512)
        def _(n):
            at = pl.ds(pl.multiple_of(n, 512), 512)
            weight = jnp.concatenate([pb[e, at, :] for e in range(slabs)], 1)
            value = dot_nt(grad[...], weight) * act[:, at].astype(f32)
            value = value.astype(bf16)
            act[:, at] = value
            sum_ref[0:1, at] = jnp.sum(value.astype(f32), 0, keepdims=True)

        store_p = copy_of(act, gp_out)
        store_p.start()
        cross_p = to_twin(2 * chips + 3, act, gpx_out)
        cross_p.start()
        outs.arrive()

        @pl.loop(0, rows, step=32)
        def _(r):
            at = pl.ds(r, 32)
            own = pl.ds(pl.multiple_of(line * rows + r, 32), 32)
            total = x_buf[at, :].astype(f32) + outs.total(nv[own, :], at) + vec_buf[2:3, :]
            x_buf[at, :] = total.astype(bf16)

        store_o = copy_of(x_buf, out_ref)
        store_o.start()
        sum_2.final()
        sum_d.final()
        store_2 = copy_of(wa.at[pl.ds(tokens, part), :], s2_out)
        store_dense = copy_of(wb.at[pl.ds(0, part), pl.ds(3 * local, local)], sd_out)
        store_2.start()
        store_dense.start()
        for copy in cross_n + [cross_d, cross_p]:
            copy.wait_recv()
        for copy in vec + [cross_t] + cross_c + [cross_d, cross_p]:
            copy.wait_send()
        for plan in (qkv, fc1, dense, fc2, cot, outs, sum_2, sum_d):
            plan.finish()
        for copy in (store_q, store_p, store_o, store_2, store_dense):
            copy.wait()

    def shape(*dims):
        return jax.ShapeDtypeStruct(dims, bf16)

    return pl.pallas_call(
        kernel,
        out_shape=(
            shape(rows, width),
            shape(3, width, local),
            shape(width, units),
            shape(units, width),
            shape(tokens, width),
            shape(chips, tokens, part),
            shape(tokens, width),
            shape(chips, tokens, part),
            shape(tokens, units),
            shape(tokens, units),
            shape(tokens, local),
            shape(tokens, 3 * local),
            shape(tokens, 3 * local),
            shape(tokens, units),
            shape(tokens, units),
            shape(part, units),
            shape(part, local),
            jax.ShapeDtypeStruct((8, width), f32),
            jax.ShapeDtypeStruct((8, local), f32),
            jax.ShapeDtypeStruct((8, units), f32),
        ),
        in_specs=[ANY] * 7 + [VMEM] * 3,
        out_specs=(ANY,) * 17 + (VMEM,) * 3,
        scratch_shapes=[
            pltpu.VMEM((rows, width), bf16),
            pltpu.VMEM((8, width), f32),
            pltpu.VMEM((tokens, width), bf16),
            pltpu.VMEM((width, width), bf16),
            pltpu.VMEM((width, units), bf16),
            pltpu.VMEM((local, width), bf16),
            pltpu.VMEM((tokens, units), bf16),
            pltpu.VMEM((tokens, units), bf16),
            pltpu.VMEM((3, tokens, local), bf16),
            pltpu.VMEM((tokens, local), bf16),
            pltpu.VMEM((local // HD, stored, BLOCK), bf16),
            pltpu.VMEM((stored, BLOCK), f32),
            pltpu.VMEM((tokens, local), bf16),
        ]
        + [pltpu.VMEM((tokens, 128), f32)] * 5
        + [
            pltpu.VMEM((2 * tensor - 3, rows, width), bf16),
            pltpu.VMEM((6, part, units // 2), bf16),
            pltpu.VMEM((6, part, local // 2), bf16),
            pltpu.SemaphoreType.DMA((sems.count,)),
            pltpu.SemaphoreType.DMA((sems.count,)),
            pltpu.SemaphoreType.DMA((48,)),
        ],
        compiler_params=pltpu.CompilerParams(
            collective_id=0, has_side_effects=True, vmem_limit_bytes=VMEM_LIMIT
        ),
        name="forward",
    )(*arrays)


def finish_kernel(s2_ref, sd_ref, s1_ref, sq_ref, o_ref, h_ref, w2_ref, wd_ref, w1_ref, wq_ref, out_ref, hid_ref):
    w2_ref[...] = s2_ref[...].T.astype(f32)
    wd_ref[...] = sd_ref[...].T.astype(f32)
    w1_ref[...] = s1_ref[...].astype(f32)
    local = wq_ref.shape[2]
    for i in range(3):
        wq_ref[i] = sq_ref[:, i * local : (i + 1) * local].astype(f32)
    out_ref[...] = o_ref[...]
    hid_ref[...] = h_ref[...]


def finish(sent_fc2, sent_dense, sent_fc1, sent_qkv, out, hidden_grad):
    part, units = sent_fc2.shape
    local = sent_dense.shape[1]
    rows, width = out.shape
    steps = 4

    def down(n, m):
        return pl.BlockSpec((n // steps, m), lambda i: (i, 0))

    def across(n, m):
        return pl.BlockSpec((n, m // steps), lambda i: (0, i))

    return pl.pallas_call(
        finish_kernel,
        grid=(steps,),
        out_shape=(
            jax.ShapeDtypeStruct((units, part), f32),
            jax.ShapeDtypeStruct((local, part), f32),
            jax.ShapeDtypeStruct((part, units), f32),
            jax.ShapeDtypeStruct((3, part, local), f32),
            jax.ShapeDtypeStruct((rows, width), bf16),
            jax.ShapeDtypeStruct((rows, width), bf16),
        ),
        in_specs=[
            across(part, units), across(part, local), down(part, units), down(part, 3 * local),
            down(rows, width), down(rows, width),
        ],
        out_specs=(
            down(units, part), down(local, part), down(part, units),
            pl.BlockSpec((3, part // steps, local), lambda i: (0, i, 0)),
            down(rows, width), down(rows, width),
        ),
        compiler_params=pltpu.CompilerParams(vmem_limit_bytes=VMEM_LIMIT),
        name="finish",
    )(sent_fc2, sent_dense, sent_fc1, sent_qkv, out, hidden_grad)


def rotary_tables(segments):
    rows, length = segments.shape
    index = jnp.arange(length, dtype=jnp.int32)[None]
    start = jnp.zeros_like(segments)
    for number in range(1, 4):
        start = jnp.where(segments == number, jnp.sum(segments < number, -1, keepdims=True), start)
    position = (index - start).astype(f32).reshape(rows * length, 1)
    lane = jnp.arange(128, dtype=jnp.int32) % HD
    exponent = (2 * (lane % (ROT // 2))).astype(f32) / ROT
    angle = position * (1.0 / 10000.0**exponent)[None]
    cosine, sine = jnp.cos(angle), jnp.sin(angle)
    low, high = lane < ROT // 2, (lane >= ROT // 2) & (lane < ROT)
    return (
        jnp.where(lane < ROT, cosine, 1.0),
        jnp.where(low, -sine, 0.0),
        jnp.where(high, sine, 0.0),
    )


def matmul(a, b):
    return jnp.dot(a, b, preferred_element_type=f32)


def on_device(
    dp, tensor, fast,
    hidden_in, segments, ln_gain, ln_bias, qkv_weight, qkv_bias, dense_weight, dense_bias,
    fc1_weight, fc1_bias, fc2_weight, fc2_bias, cotangent,
):
    seqs = segments.shape[0]
    local = qkv_weight.shape[2]
    number = lax.broadcasted_iota(jnp.int32, (8, ln_gain.shape[0]), 0)
    vectors = jnp.where(number == 1, ln_bias.astype(f32)[None], ln_gain.astype(f32)[None])
    vectors = jnp.where(
        number == 2, dense_bias.astype(f32)[None] + fc2_bias.astype(f32)[None], vectors)
    mine = (
        hidden_in, cotangent, qkv_weight.transpose(1, 0, 2),
        dense_weight, fc1_weight, fc2_weight, vectors,
    )
    if fast:
        (
            out, w_qkv, w_fc1, _, normed, crossed_normed, _, _, _, _, _,
            grad_qkv, crossed_qkv, grad_pre, crossed_pre, sent_fc2, sent_dense,
            vec, qkv_sums, fc1_sums,
        ) = forward_call(dp, tensor, (*mine, qkv_bias, fc1_bias[None], segments))
        sums = jnp.concatenate([fc1_sums[0].reshape(4, local), qkv_sums[:3], jnp.zeros((1, local), f32)], 0)
        hidden_grad, sent_fc1, sent_qkv, vec_sums, all_sums = second_call(
            dp, tensor,
            (hidden_in, cotangent, vec, sums, normed, grad_pre, grad_qkv,
             crossed_normed, crossed_pre, crossed_qkv, w_qkv, w_fc1))
        quarter = vec_sums.shape[1] // tensor
        at = lax.axis_index("tensor") * quarter
        small = lax.dynamic_slice(vec_sums, (0, at), (3, quarter))
        grad_w2, grad_wd, grad_w1, grad_wq, out, hidden_grad = finish(
            sent_fc2, sent_dense, sent_fc1, sent_qkv, out, hidden_grad)
        return (
            out,
            hidden_grad,
            small[0],
            small[1],
            grad_wq.transpose(1, 0, 2),
            all_sums[4:7],
            grad_wd,
            small[2],
            grad_w1,
            all_sums[:4].reshape(-1),
            grad_w2,
            small[2],
        )

    tables = rotary_tables(segments)
    bias = jnp.pad(qkv_bias.astype(f32), ((0, 5), (0, 0)))
    w_qkv, w_dense, w_fc1, w_fc2, normed, grad_out, vec = gather_plain(*mine)
    gain, out_bias = vec[0:1], vec[2:3]
    query, key, value, attn_vec, probs = attend(
        *(matmul(normed, w_qkv[i]) for i in range(3)), bias, tables, segments, seqs
    )
    pre_act = matmul(normed, w_fc1) + fc1_bias.astype(f32)
    act_vals, gelu_pull = jax.vjp(lambda pre: jax.nn.gelu(pre, approximate=True), pre_act)
    act_vals = act_vals.astype(bf16)
    slope = gelu_pull(jnp.ones_like(pre_act))[0].astype(bf16)
    branches = matmul(attn_vec, w_dense) + matmul(act_vals, w_fc2)
    grad_attn = matmul(grad_out, w_dense.T).astype(bf16)
    *grads, qkv_sums = attend_back(query, key, value, grad_attn, attn_vec, probs, tables, seqs)
    resid_in = hidden_in.astype(f32)
    cot_float = cotangent.astype(f32)
    centred = resid_in - jnp.mean(resid_in, -1, keepdims=True)
    spread = jnp.mean(centred * centred, -1, keepdims=True)
    inv_std = lax.rsqrt(spread + layer_eps)
    unit_rows = centred * inv_std
    summed = lax.psum_scatter(branches.astype(bf16), "tensor", scatter_dimension=0, tiled=True)
    out = (resid_in + summed.astype(f32) + out_bias).astype(bf16)
    out_bias_part = jnp.sum(cot_float, 0)
    grad_fc2 = matmul(act_vals.T, grad_out)
    grad_dense = matmul(attn_vec.T, grad_out)
    grad_pre = (matmul(grad_out, w_fc2.T) * slope.astype(f32)).astype(bf16)
    fc1_bias_part = jnp.sum(grad_pre.astype(f32), 0)
    grad_fc1 = matmul(normed.T, grad_pre)
    grad_wqkv = jnp.stack([matmul(normed.T, g) for g in grads])
    grad_normed = matmul(grad_pre, w_fc1.T) + sum(matmul(g, w.T) for g, w in zip(grads, w_qkv))
    sent_qkv, sent_dense, sent_fc1, sent_fc2 = (
        lax.psum_scatter(grad_wqkv.astype(bf16), "dp", scatter_dimension=1, tiled=True),
        lax.psum_scatter(grad_dense.astype(bf16), "dp", scatter_dimension=1, tiled=True),
        lax.psum_scatter(grad_fc1.astype(bf16), "dp", scatter_dimension=0, tiled=True),
        lax.psum_scatter(grad_fc2.astype(bf16), "dp", scatter_dimension=1, tiled=True),
    )
    grad_local = lax.psum_scatter(
        grad_normed.astype(bf16), "tensor", scatter_dimension=0, tiled=True
    ).astype(f32)
    gain_part = jnp.sum(grad_local * unit_rows, 0)
    beta_part = jnp.sum(grad_local, 0)
    scaled_grad = grad_local * gain
    first_mean = jnp.mean(scaled_grad, -1, keepdims=True)
    second_mean = jnp.mean(scaled_grad * unit_rows, -1, keepdims=True)
    hidden_grad = (
        cot_float + inv_std * (scaled_grad - first_mean - unit_rows * second_mean)
    ).astype(bf16)
    gain_grad, beta_grad, out_bias_grad = (
        lax.psum_scatter(gain_part, ("dp", "tensor"), scatter_dimension=0, tiled=True),
        lax.psum_scatter(beta_part, ("dp", "tensor"), scatter_dimension=0, tiled=True),
        lax.psum_scatter(out_bias_part, ("dp", "tensor"), scatter_dimension=0, tiled=True),
    )
    qkv_bias_grad, fc1_bias_grad = lax.psum((qkv_sums[:3], fc1_bias_part), "dp")
    return (
        out,
        hidden_grad,
        gain_grad,
        beta_grad,
        sent_qkv.transpose(1, 0, 2).astype(f32),
        qkv_bias_grad,
        sent_dense.astype(f32),
        out_bias_grad,
        sent_fc1.astype(f32),
        fc1_bias_grad,
        sent_fc2.astype(f32),
        out_bias_grad,
    )


def solution(mesh):
    dp, tensor = mesh.shape["dp"], mesh.shape["tensor"]
    fast = dp == 8 and tensor == 4
    placed = (
        P(("dp", "tensor"), None),
        P("dp", None),
        P("dp"),
        P("dp"),
        P("dp", None, "tensor"),
        P(None, "tensor"),
        P("tensor", "dp"),
        P("dp"),
        P("dp", "tensor"),
        P("tensor"),
        P("tensor", "dp"),
        P("dp"),
        P(("dp", "tensor"), None),
    )
    return jax.shard_map(
        functools.partial(on_device, dp, tensor, fast),
        mesh=mesh,
        in_specs=placed,
        out_specs=(
            P(("dp", "tensor"), None),
            P(("dp", "tensor"), None),
            P(("dp", "tensor")),
            P(("dp", "tensor")),
            P("dp", None, "tensor"),
            P(None, "tensor"),
            P("tensor", "dp"),
            P(("dp", "tensor")),
            P("dp", "tensor"),
            P("tensor"),
            P("tensor", "dp"),
            P(("dp", "tensor")),
        ),
        check_vma=False,
    )
```

```python
import functools

import jax
import jax.numpy as jnp
from jax import lax
from jax.experimental import pallas as pl
from jax.experimental.pallas import tpu as pltpu
from jax.sharding import PartitionSpec as P

HD = 64
ROT = 32
BLOCK = 256
MAX_DOC = 512
VMEM_LIMIT = 66_000_000
MESH = pl.DeviceIdType.MESH
ANY = pl.BlockSpec(memory_space=pl.ANY)
VMEM = pl.BlockSpec(memory_space=pltpu.VMEM)

layer_eps = 1e-05
f32 = jnp.float32
bf16 = jnp.bfloat16


def dot_nn(a, b):
    return lax.dot_general(a, b, (((1,), (0,)), ((), ())), preferred_element_type=f32)


def dot_nt(a, b):
    return lax.dot_general(a, b, (((1,), (1,)), ((), ())), preferred_element_type=f32)


def dot_tn(a, b):
    return lax.dot_general(a, b, (((0,), (0,)), ((), ())), preferred_element_type=f32)


def flip(index, bit):
    step = 1 << bit
    return index + step * (1 - 2 * (lax.div(index, step) % 2))


def relative(index, offset):
    bit = 0
    while offset >> bit:
        if (offset >> bit) & 1:
            index = flip(index, bit)
        bit += 1
    return index


def stages_of(order):
    held, stages = [0], []
    for bit in order:
        got = [r ^ (1 << bit) for r in held]
        stages.append((bit, list(held), got))
        held = held + got
    return stages


class Sems:
    def __init__(self):
        self.count = 0

    def take(self):
        self.count += 1
        return self.count - 1


class CubeGather:
    def __init__(self, sems, orders):
        self.plans = [stages_of(order) for order in orders]
        self.ids = {
            (h, j, i): sems.take()
            for h, stages in enumerate(self.plans)
            for j, (_, held, _) in enumerate(stages)
            for i in range(len(held))
        }

    def bind(self, me, other, own, window, send_sem, recv_sem):
        self.me, self.other, self.own, self.window = me, other, own, window
        self.send_sem, self.recv_sem = send_sem, recv_sem
        return self

    def copy(self, h, j, i):
        bit, held, _ = self.plans[h][j]
        slot = relative(self.me, held[i])
        target = self.window(slot, h)
        source = self.own(h) if held[i] == 0 else target
        k = self.ids[h, j, i]
        return pltpu.make_async_remote_copy(
            src_ref=source,
            dst_ref=target,
            send_sem=self.send_sem.at[k],
            recv_sem=self.recv_sem.at[k],
            device_id=(flip(self.me, bit), self.other),
            device_id_type=MESH,
        )

    def start(self):
        depth = len(self.plans[0])
        for j in range(depth):
            for h in range(len(self.plans)):
                self.copy(h, j, 0).start()

    def advance(self, j):
        for i in range(len(self.plans[0][j][1])):
            for h, stages in enumerate(self.plans):
                self.copy(h, j, i).wait_recv()
                slot = stages[j][2][i]
                for later in range(j + 1, len(stages)):
                    self.copy(h, later, stages[later][1].index(slot)).start()

    def finish(self):
        for h, j, i in self.ids:
            self.copy(h, j, i).wait_send()


class LineGather:
    def __init__(self, sems, size, subs):
        self.size, self.subs = size, subs
        self.ids = {
            (way, s, u): sems.take()
            for way in (0, 1)
            for s in range(size - 1)
            for u in range(subs)
        }

    def bind(self, me, other, own, window, send_sem, recv_sem):
        self.me, self.other, self.own, self.window = me, other, own, window
        self.send_sem, self.recv_sem = send_sem, recv_sem
        return self

    def copy(self, way, s, u):
        block = self.me - s if way == 0 else self.me + s
        target = self.window(block, u)
        k = self.ids[way, s, u]
        return pltpu.make_async_remote_copy(
            src_ref=self.own(u) if s == 0 else target,
            dst_ref=target,
            send_sem=self.send_sem.at[k],
            recv_sem=self.recv_sem.at[k],
            device_id=(self.other, self.me + 1 if way == 0 else self.me - 1),
            device_id_type=MESH,
        )

    def sends(self, way, s):
        if way == 0:
            return (self.me >= s) & (self.me < self.size - 1)
        return (self.me + s < self.size) & (self.me > 0)

    def gets(self, way, s):
        if way == 0:
            return self.me - 1 - s >= 0
        return self.me + 1 + s < self.size

    def start(self, u):
        for way in (0, 1):

            @pl.when(self.sends(way, 0))
            def _():
                self.copy(way, 0, u).start()

    def advance(self, s, u):
        for way in (0, 1):

            @pl.when(self.gets(way, s))
            def _():
                self.copy(way, s, u).wait_recv()

            if s + 1 < self.size - 1:

                @pl.when(self.sends(way, s + 1))
                def _():
                    self.copy(way, s + 1, u).start()

    def finish(self):
        for way, s, u in self.ids:

            @pl.when(self.sends(way, s))
            def _():
                self.copy(way, s, u).wait_send()


def greet(dp, me, tensor, line, meanwhile):
    barrier = pltpu.get_barrier_semaphore()
    for r in range(1, dp):
        pl.semaphore_signal(barrier, inc=1, device_id=(relative(me, r), line), device_id_type=MESH)
    for k in range(1, tensor):
        to = (me, lax.rem(line + k, tensor))
        pl.semaphore_signal(barrier, inc=1, device_id=to, device_id_type=MESH)
    meanwhile()
    pl.semaphore_wait(barrier, dp + tensor - 2)


def orders_of(dp):
    bits = list(range(1, dp.bit_length() - 1))
    return [bits + [0], bits[::-1] + [0]]


def normalize(x, gain, bias):
    centred = x - jnp.mean(x, -1, keepdims=True)
    spread = jnp.mean(centred * centred, -1, keepdims=True)
    unit = centred * lax.rsqrt(spread + layer_eps)
    return (unit * gain + bias).astype(bf16)


def gather_plain(hidden, cotangent, w_qkv, w_dense, w_fc1, w_fc2, vectors):
    vec = lax.all_gather(vectors, "dp", axis=1, tiled=True)
    normed = normalize(hidden.astype(f32), vec[0:1], vec[1:2])
    return (
        lax.all_gather(w_qkv, "dp", axis=1, tiled=True),
        lax.all_gather(w_dense, "dp", axis=1, tiled=True),
        lax.all_gather(w_fc1, "dp", axis=0, tiled=True),
        lax.all_gather(w_fc2, "dp", axis=1, tiled=True),
        lax.all_gather(normed, "tensor", axis=0, tiled=True),
        lax.all_gather(cotangent, "tensor", axis=0, tiled=True),
        vec,
    )


class ChipReduce:
    COUNT = 6

    def __init__(self, sems):
        self.ids = [sems.take() for _ in range(self.COUNT)]

    def bind(self, me, other, view, landing, stage, stage_sem, send_sem, recv_sem):
        self.me, self.other, self.view, self.landing = me, other, view, landing
        self.stage, self.stage_sem = stage, stage_sem
        self.send_sem, self.recv_sem = send_sem, recv_sem
        return self

    def copy(self, slot):
        r, h, bit = [(2, 0, 2), (3, 0, 2), (1, 0, 1), (1, 1, 1), (3, 1, 1), (2, 1, 2)][slot]
        k = self.ids[slot]
        return pltpu.make_async_remote_copy(
            src_ref=self.view(r, h),
            dst_ref=self.landing.at[slot],
            send_sem=self.send_sem.at[k],
            recv_sem=self.recv_sem.at[k],
            device_id=(flip(self.me, bit), self.other),
            device_id_type=MESH,
        )

    def start(self, r):
        for slot in {3: (1, 4), 2: (0,), 1: (3,), 0: ()}[r]:
            self.copy(slot).start()

    def fetch(self, slots):
        half = self.landing.shape[-1]
        held = [self.stage.at[k, :, pl.ds(0, half)] for k in range(len(slots))]
        copies = []
        for k, slot in enumerate(slots):
            self.copy(slot).wait_recv()
            copies.append(
                pltpu.make_async_copy(self.landing.at[slot], held[k], self.stage_sem.at[k]))
            copies[k].start()
        for copy in copies:
            copy.wait()
        return held

    def middle(self):
        held = self.fetch((1, 4))
        for k, (r, h, last) in enumerate(((1, 0, 2), (2, 1, 5))):
            view = self.view(r, h)
            view[...] = (view[...].astype(f32) + held[k][...].astype(f32)).astype(bf16)
            self.copy(last).start()

    def final(self):
        for h, slots in ((0, (0, 2)), (1, (3, 5))):
            a, b = self.fetch(slots)
            view = self.view(0, h)
            total = view[...].astype(f32) + a[...].astype(f32) + b[...].astype(f32)
            view[...] = total.astype(bf16)

    def finish(self):
        for slot in range(self.COUNT):
            self.copy(slot).wait_send()


class LineReduce:
    def __init__(self, sems, size):
        self.size = size
        self.ids = {(way, i): sems.take() for way in (0, 1) for i in range(size - 1)}

    def bind(self, me, other, own, landing, stage, last, stage_sem, send_sem, recv_sem):
        self.me, self.other, self.own, self.landing = me, other, own, landing
        self.stage, self.last, self.stage_sem = stage, last, stage_sem
        self.send_sem, self.recv_sem = send_sem, recv_sem
        return self

    def target(self, way, i):
        return self.size - 1 - i if way == 0 else i

    def place(self, way, i):
        return i if way == 0 else 2 * self.size - 4 - i

    def buffer(self, way, i):
        return self.stage.at[i if way == 0 else self.size - 2 - i]

    def copy(self, way, i, edge):
        k = self.ids[way, i]
        return pltpu.make_async_remote_copy(
            src_ref=self.own(self.target(way, i)) if edge else self.buffer(way, i),
            dst_ref=self.landing.at[self.place(way, i)],
            send_sem=self.send_sem.at[k],
            recv_sem=self.recv_sem.at[k],
            device_id=(self.other, self.me + 1 if way == 0 else self.me - 1),
            device_id_type=MESH,
        )

    def edge(self, way):
        return self.me == (0 if way == 0 else self.size - 1)

    def passes(self, way, i):
        d = self.target(way, i)
        return (self.me > 0) & (self.me < d) if way == 0 else (self.me < self.size - 1) & (self.me > d)

    def start(self, way, i):
        @pl.when(self.edge(way))
        def _():
            self.copy(way, i, True).start()

    def advance(self, step):
        for way in (0, 1):
            steps_from_edge = self.me if way == 0 else self.size - 1 - self.me
            for i in range(step):

                @pl.when(self.passes(way, i) & (steps_from_edge == step - i))
                def _():
                    self.copy(way, i, False).wait_recv()
                    held = self.buffer(way, i)
                    fetch = pltpu.make_async_copy(
                        self.landing.at[self.place(way, i)], held, self.stage_sem.at[0])
                    fetch.start()
                    fetch.wait()
                    add_into(held, self.own(self.target(way, i)))
                    self.copy(way, i, False).start()

    def arrive(self):
        for way, i in self.ids:

            @pl.when(self.edge(way))
            def _():
                self.copy(way, i, True).wait_send()

            @pl.when(self.passes(way, i))
            def _():
                self.copy(way, i, False).wait_send()

        def fetch(way, i):
            return pltpu.make_async_copy(
                self.landing.at[self.place(way, i)], self.last(way), self.stage_sem.at[way])

        for way, i in self.ids:

            @pl.when(self.me == self.target(way, i))
            def _():
                self.copy(way, i, False).wait_recv()
                fetch(way, i).start()

        for way, i in self.ids:

            @pl.when(self.me == self.target(way, i))
            def _():
                fetch(way, i).wait()

    def total(self, own, rows):
        value = own.astype(f32)
        for way, there in ((0, self.me > 0), (1, self.me < self.size - 1)):
            value = value + jnp.where(there, self.last(way)[rows, :].astype(f32), 0.0)
        return value


def add_into(landing, own):
    rows = landing.shape[0]

    @pl.loop(0, rows, step=64)
    def _(r):
        at = pl.ds(r, 64)
        landing[at, :] = (landing[at, :].astype(f32) + own[at, :].astype(f32)).astype(bf16)


def chip_slot(me, r):
    return (
        me
        + 2 * ((r % 2) * (1 - 2 * (lax.div(me, 2) % 2)))
        + 4 * (lax.div(r, 2) * (1 - 2 * (lax.div(me, 4) % 2)))
    )


def spans_of(length):
    back = -(-(MAX_DOC - 1) // BLOCK)
    spans, at = [], 0
    for i in range(length // BLOCK):
        low = max(0, i - back) * BLOCK
        spans.append((low, (i + 1) * BLOCK, at))
        at += (i + 1) * BLOCK - low
    return spans, at


def turn(x, cosine, sine_lo, sine_hi):
    return x * cosine + pltpu.roll(x, 128 - ROT // 2, 1) * sine_lo + pltpu.roll(x, ROT // 2, 1) * sine_hi


def head_lanes(shape, e):
    lane = lax.broadcasted_iota(jnp.int32, shape, 1)
    return (lane >= e * HD) & (lane < (e + 1) * HD)


def only(x, e):
    return jnp.where(head_lanes(x.shape, e), x, jnp.zeros_like(x))


def attend_kernel(
    q_ref, k_ref, v_ref, bias_ref, cos_ref, slo_ref, shi_ref, segc_ref, segr_ref,
    qs_ref, ks_ref, vs_ref, o_ref, p_ref, mask_ref,
):
    @pl.when(pl.program_id(1) == 0)
    def _():
        fill_mask(mask_ref, segc_ref, segr_ref, q_ref.shape[0])

    cosine, slo, shi = cos_ref[...], slo_ref[...], shi_ref[...]
    query = turn(q_ref[...] + bias_ref[0:1, :], cosine, slo, shi).astype(bf16) * bf16(HD**-0.5)
    key = turn(k_ref[...] + bias_ref[1:2, :], cosine, slo, shi).astype(bf16)
    value = (v_ref[...] + bias_ref[2:3, :]).astype(bf16)
    qs_ref[...] = query
    ks_ref[...] = key
    vs_ref[...] = value

    def keep(e, at, probs):
        p_ref[e, at, :] = probs

    def write(at, result):
        o_ref[at, :] = result

    attend_pair(query, key, value, mask_ref, keep, write)


def attend(q, k, v, qkv_bias, tables, segments, rows):
    tokens, local = q.shape
    length = tokens // rows
    pairs = local // 128
    _, stored = spans_of(length)
    block = pl.BlockSpec((length, 128), lambda r, h: (r, h))
    table = pl.BlockSpec((length, 128), lambda r, h: (r, 0))
    shape = jax.ShapeDtypeStruct((tokens, local), bf16)
    return pl.pallas_call(
        attend_kernel,
        grid=(rows, pairs),
        out_shape=(shape,) * 4 + (jax.ShapeDtypeStruct((rows, local // HD, stored, BLOCK), bf16),),
        in_specs=[block] * 3
        + [pl.BlockSpec((8, 128), lambda r, h: (0, h))]
        + [table] * 3
        + [
            pl.BlockSpec((length, 1), lambda r, h: (r, 0)),
            pl.BlockSpec((pl.Squeezed(), 1, length), lambda r, h: (r, 0, 0)),
        ],
        out_specs=(block,) * 4
        + (pl.BlockSpec((pl.Squeezed(), 128 // HD, stored, BLOCK), lambda r, h: (r, h, 0, 0)),),
        scratch_shapes=[pltpu.VMEM((stored, BLOCK), f32)],
        compiler_params=pltpu.CompilerParams(vmem_limit_bytes=VMEM_LIMIT),
        cost_estimate=pl.CostEstimate(
            flops=16 * tokens * 768 * local, bytes_accessed=24 << 20, transcendentals=0
        ),
        name="attend",
    )(q, k, v, qkv_bias, *tables, segments.reshape(tokens, 1), segments.reshape(rows, 1, length))


def attend_back_kernel(
    q_ref, k_ref, v_ref, g_ref, o_ref, p_ref, cos_ref, slo_ref, shi_ref,
    dq_ref, dk_ref, dv_ref, bias_ref, kacc_ref, vacc_ref,
):
    def write(which, at, value):
        (dq_ref, dk_ref, dv_ref)[which][at, :] = value

    sums = attend_back_pair(
        q_ref[...], k_ref[...], v_ref[...], g_ref[...], o_ref[...],
        lambda e, at: p_ref[e, at, :], (cos_ref, slo_ref, shi_ref), kacc_ref, vacc_ref, write)
    sums = jnp.concatenate(list(sums) + [jnp.zeros((5, 128), f32)], 0)

    @pl.when(pl.program_id(1) == 0)
    def _():
        bias_ref[...] = sums

    @pl.when(pl.program_id(1) > 0)
    def _():
        bias_ref[...] += sums


def attend_back(q, k, v, g, o, probs, tables, rows):
    tokens, local = q.shape
    length = tokens // rows
    pairs = local // 128
    stored = probs.shape[2]
    block = pl.BlockSpec((length, 128), lambda h, r: (r, h))
    table = pl.BlockSpec((length, 128), lambda h, r: (r, 0))
    shape = jax.ShapeDtypeStruct((tokens, local), bf16)
    return pl.pallas_call(
        attend_back_kernel,
        grid=(pairs, rows),
        out_shape=(shape,) * 3 + (jax.ShapeDtypeStruct((8, local), f32),),
        in_specs=[block] * 5
        + [pl.BlockSpec((pl.Squeezed(), 128 // HD, stored, BLOCK), lambda h, r: (r, h, 0, 0))]
        + [table] * 3,
        out_specs=(block,) * 3 + (pl.BlockSpec((8, 128), lambda h, r: (0, h)),),
        scratch_shapes=[pltpu.VMEM((length, 128), f32)] * 2,
        compiler_params=pltpu.CompilerParams(vmem_limit_bytes=VMEM_LIMIT),
        cost_estimate=pl.CostEstimate(
            flops=32 * tokens * 768 * local, bytes_accessed=24 << 20, transcendentals=0
        ),
        name="attend_back",
    )(q, k, v, g, o, probs, *tables)


def attend_pair(query, key, value, mask_ref, keep, write):
    length = query.shape[0]
    spans, _ = spans_of(length)
    for i, (low, high, at) in enumerate(spans):
        mine = slice(i * BLOCK, (i + 1) * BLOCK)
        total = jnp.zeros((BLOCK, 128), f32)
        for e in range(128 // HD):
            scores = dot_nt(only(key[low:high], e), query[mine]) + mask_ref[at : at + high - low, :].astype(f32)
            exponent = jnp.exp(scores - jnp.max(scores, 0, keepdims=True))
            inverse = 1.0 / jnp.sum(exponent, 0, keepdims=True)
            probs = (exponent * inverse).astype(bf16)
            keep(e, slice(at, at + high - low), probs)
            total = total + dot_tn(probs, only(value[low:high], e))
        write(mine, total.astype(bf16))


def fill_mask(mask_ref, segc_ref, segr_ref, length):
    for i, (low, high, at) in enumerate(spans_of(length)[0]):
        keys = lax.broadcasted_iota(jnp.int32, (high - low, BLOCK), 0) + low
        queries = lax.broadcasted_iota(jnp.int32, (high - low, BLOCK), 1) + i * BLOCK
        own = segr_ref[:, i * BLOCK : (i + 1) * BLOCK].astype(f32)
        same = segc_ref[low:high, 0:1].astype(f32) == own
        allowed = jnp.where((keys <= queries) & same, 0.0, -1e30)
        mask_ref[at : at + high - low, :] = allowed.astype(mask_ref.dtype)


def fill_tables(seg_ref, column_ref, cos_ref, slo_ref, shi_ref):
    length = seg_ref.shape[1]
    row = seg_ref[...].astype(f32)
    column_ref[...] = jnp.broadcast_to(row, (128, length)).T
    starts = [jnp.sum(jnp.where(row < number, 1.0, 0.0), 1, keepdims=True) for number in range(1, 4)]
    lane = lax.broadcasted_iota(jnp.int32, (1, 128), 1) % HD
    exponent = (2 * (lane % (ROT // 2))).astype(f32) / ROT
    frequency = 1.0 / jnp.exp(exponent * f32(9.210340371976184))

    @pl.loop(0, length, step=128)
    def _(r):
        at = pl.ds(pl.multiple_of(r, 128), 128)
        column = column_ref[at, :]
        start = jnp.zeros_like(column)
        for number in range(1, 4):
            start = jnp.where(column == number, starts[number - 1], start)
        index = (lax.broadcasted_iota(jnp.int32, (128, 128), 0) + r).astype(f32)
        angle = (index - start) * frequency
        cosine, sine = jnp.cos(angle), jnp.sin(angle)
        cos_ref[at, :] = jnp.where(lane < ROT, cosine, 1.0)
        slo_ref[at, :] = jnp.where(lane < ROT // 2, -sine, 0.0)
        shi_ref[at, :] = jnp.where((lane >= ROT // 2) & (lane < ROT), sine, 0.0)


def attend_back_pair(query, key, value, grad, result, probs_of, tables, kacc_ref, vacc_ref, write):
    length = query.shape[0]
    spans, _ = spans_of(length)
    heads = 128 // HD
    inner = grad.astype(f32) * result.astype(f32)
    lane = lax.broadcasted_iota(jnp.int32, (8, 128), 1)
    row = lax.broadcasted_iota(jnp.int32, (8, 128), 0)
    pick = jnp.where(lax.div(lane, HD) == row, 1.0, 0.0)
    delta = lax.dot_general(
        pick, inner, (((1,), (1,)), ((), ())),
        precision=lax.Precision.HIGHEST, preferred_element_type=f32)
    kacc_ref[...] = jnp.zeros_like(kacc_ref)
    vacc_ref[...] = jnp.zeros_like(vacc_ref)
    cos_ref, slo_ref, shi_ref = tables
    first = jnp.zeros((1, 128), f32)
    for i, (low, high, at) in enumerate(spans):
        mine = slice(i * BLOCK, (i + 1) * BLOCK)
        g_i, q_i = grad[mine], query[mine]
        dq = jnp.zeros((BLOCK, 128), f32)
        ps, dss = [], []
        for e in range(heads):
            probs = probs_of(e, slice(at, at + high - low))
            dprobs = dot_nt(only(value[low:high], e), g_i)
            ds = (probs.astype(f32) * (dprobs - delta[e : e + 1, mine])).astype(bf16)
            dq = dq + dot_tn(ds, only(key[low:high], e))
            ps.append(probs)
            dss.append(ds)
        g_cat = jnp.concatenate([only(g_i, e) for e in range(heads)], 0)
        q_cat = jnp.concatenate([only(q_i, e) for e in range(heads)], 0)
        vacc_ref[low:high, :] += dot_nn(jnp.concatenate(ps, 1), g_cat)
        kacc_ref[low:high, :] += dot_nn(jnp.concatenate(dss, 1), q_cat)
        dq = dq * f32(HD**-0.5)
        dq = turn(dq, cos_ref[mine, :], -slo_ref[mine, :], -shi_ref[mine, :]).astype(bf16)
        write(0, mine, dq)
        first = first + jnp.sum(dq.astype(f32), 0, keepdims=True)
    everything = slice(0, length)
    dk = turn(kacc_ref[...], cos_ref[...], -slo_ref[...], -shi_ref[...]).astype(bf16)
    dv = vacc_ref[...].astype(bf16)
    write(1, everything, dk)
    write(2, everything, dv)
    return first, jnp.sum(dk.astype(f32), 0, keepdims=True), jnp.sum(dv.astype(f32), 0, keepdims=True)


def block_call(dp, tensor, arrays):
    hidden, cotangent, w_qkv, w_dense, w_fc1, w_fc2, vectors = arrays[:7]
    rows, width = hidden.shape
    local = w_qkv.shape[2]
    wide = 3 * local
    units = w_fc1.shape[1]
    part = width // dp
    chips = dp // 2
    tokens = rows * tensor
    pairs = local // 128
    stored = spans_of(tokens)[1]
    sems = Sems()
    orders = orders_of(dp)
    vec_ids = [sems.take() for _ in range(dp - 1)]
    plan_qkv, plan_dense, plan_fc1, plan_fc2 = (CubeGather(sems, orders) for _ in range(4))
    plan_n, plan_c = LineGather(sems, tensor, 2), LineGather(sems, tensor, 2)
    line_out, line_in = LineReduce(sems, tensor), LineReduce(sems, tensor)
    reduce_fc2, reduce_dense, reduce_fc1, reduce_qkv = (ChipReduce(sems) for _ in range(4))
    swaps = [sems.take() for _ in range(2 * chips + 4)]
    tells = [sems.take() for _ in range(2 * (dp - 1) + tensor - 1)]

    def kernel(
        x_ref, c_ref, wq_ref, wd_ref, w1_ref, w2_ref, vec_ref, qb_ref, fb_ref, seg_ref,
        out_ref, hid_ref, s2_out, sd_out, s1_out, sq_out,
        gq_ref, g1_ref, g2_ref, n_out, nx_out, ax_out, gqx_out, gpx_out,
        land_out, land_in, land_2, land_d, land_1, land_q, vout_ref, bout_ref,
        x_buf, vec_buf, nv, wa, wb, wd, act, slope, qkv3, abuf, pb, mask, cbuf, xbuf,
        kacc, vacc, cos_ref, slo_ref, shi_ref, line_stage, chip_stage,
        fsum, bsum, parts, tell_v, tell_b, tell_z,
        send_sem, recv_sem, local_sem, stage_sem,
    ):
        me, line = lax.axis_index("dp"), lax.axis_index("tensor")
        twin = flip(me, 0)
        half = part // 2
        local_count = [0]
        attn = abuf.at[:, pl.ds(0, local)]

        def cols(a):
            return pl.ds(pl.multiple_of(a * part, part), part)

        def half_rows(a, h):
            return pl.ds(pl.multiple_of(a * part + h * half, half), half)

        def tok(b, u):
            return pl.ds(pl.multiple_of(b * rows + u * (rows // 2), rows // 2), rows // 2)

        def block(b):
            return pl.ds(pl.multiple_of(b * rows, rows), rows)

        def piece(n, h):
            return pl.ds(h * (n // 2), n // 2)

        def copy_of(a, b):
            local_count[0] += 1
            return pltpu.make_async_copy(a, b, local_sem.at[local_count[0] - 1])

        def remote(k, source, target, device):
            return pltpu.make_async_remote_copy(
                src_ref=source, dst_ref=target,
                send_sem=send_sem.at[k], recv_sem=recv_sem.at[k],
                device_id=device, device_id_type=MESH)

        def to_twin(k, source, target):
            return remote(swaps[k], source, target, (twin, line))

        pair = (send_sem, recv_sem)
        vec = [
            remote(k, vec_ref, vec_buf.at[:, cols(me)], (relative(me, r), line))
            for r, k in enumerate(vec_ids, 1)
        ]
        qkv = plan_qkv.bind(
            me, line,
            lambda h: wq_ref.at[:, pl.ds(h * half, half), :],
            lambda a, h: gq_ref.at[:, half_rows(a, h), :], *pair)
        fc1 = plan_fc1.bind(
            me, line,
            lambda h: w1_ref.at[pl.ds(h * half, half), :],
            lambda a, h: g1_ref.at[half_rows(a, h), :], *pair)
        dense = plan_dense.bind(
            me, line,
            lambda h: wd_ref.at[piece(local, h), :],
            lambda a, h: wd.at[piece(local, h), cols(a)], *pair)
        fc2 = plan_fc2.bind(
            me, line,
            lambda h: w2_ref.at[piece(units, h), :],
            lambda a, h: g2_ref.at[piece(units, h), cols(a)], *pair)
        norm = plan_n.bind(
            line, me, lambda u: nv.at[tok(line, u)], lambda b, u: nv.at[tok(b, u)], *pair)
        cot = plan_c.bind(
            line, me, lambda u: c_ref.at[piece(rows, u)], lambda b, u: cbuf.at[tok(b, u)], *pair)
        staged = (stage_sem, *pair)

        def lasts(way):
            return wd.at[pl.ds(way * rows, rows), :]

        outs = line_out.bind(
            line, me, lambda d: nv.at[pl.ds(d * rows, rows), :], land_out, line_stage, lasts, *staged)
        ins = line_in.bind(
            line, me, lambda d: act.at[pl.ds(d * rows, rows), :], land_in, line_stage, lasts, *staged)
        low, high = pl.ds(0, tokens), pl.ds(tokens, tokens)
        sum_2 = reduce_fc2.bind(
            me, line,
            lambda r, h: wa.at[pl.ds(tokens + r * part, part), piece(units, h)],
            land_2, chip_stage, *staged)
        sum_d = reduce_dense.bind(
            me, line,
            lambda r, h: mask.at[pl.ds((2 * r + h) * part, part), :],
            land_d, chip_stage, *staged)
        sum_1 = reduce_fc1.bind(
            me, line,
            lambda r, h: wb.at[pl.ds(r * part, part), piece(units, h)],
            land_1, chip_stage, *staged)
        sum_q = reduce_qkv.bind(
            me, line,
            lambda r, h: abuf.at[pl.ds(r * part, part), piece(wide, h)],
            land_q, chip_stage, *staged)
        stages = dp.bit_length() - 1

        takes = [
            copy_of(x_ref, x_buf),
            copy_of(vec_ref, vec_buf.at[:, cols(me)]),
            copy_of(wd_ref, wd.at[:, cols(me)]),
            copy_of(c_ref, cbuf.at[block(line), :]),
            copy_of(wq_ref, qkv3.at[:, pl.ds(0, part), :]),
            copy_of(w1_ref, act.at[pl.ds(0, part), :]),
            copy_of(w2_ref, wb.at[:, pl.ds(0, part)]),
        ]
        keeps = [
            copy_of(qkv3.at[:, pl.ds(0, part), :], gq_ref.at[:, cols(me), :]),
            copy_of(act.at[pl.ds(0, part), :], g1_ref.at[cols(me), :]),
            copy_of(wb.at[:, pl.ds(0, part)], g2_ref.at[:, cols(me)]),
        ]
        for copy in takes[:2]:
            copy.start()
        greet(
            dp, me, tensor, line,
            lambda: fill_tables(seg_ref, kacc, cos_ref, slo_ref, shi_ref))
        for copy in vec:
            copy.start()
        qkv.start()
        cot.start(0)
        for copy in takes[2:]:
            copy.start()
        for copy in takes[:2]:
            copy.wait()
        for copy in vec:
            copy.wait_recv()

        @pl.loop(0, rows, step=32)
        def _(r):
            x = x_buf[pl.ds(r, 32), :].astype(f32)
            centred = x - jnp.mean(x, -1, keepdims=True)
            spread = jnp.mean(centred * centred, -1, keepdims=True)
            unit = centred * lax.rsqrt(spread + layer_eps)
            at = pl.ds(pl.multiple_of(line * rows + r, 32), 32)
            nv[at, :] = (unit * vec_buf[0:1, :] + vec_buf[1:2, :]).astype(bf16)

        norm.start(0)
        norm.start(1)
        qkv.advance(0)
        fc1.start()
        for take, copy in zip(takes[4:], keeps):
            take.wait()
            copy.start()
        fill_mask(mask, kacc, seg_ref, tokens)

        def project(b):
            at = block(b)
            cosine, slo, shi = cos_ref[at, :], slo_ref[at, :], shi_ref[at, :]
            for i in range(3):
                value = dot_nn(nv[at, :], wa[:, i * local : (i + 1) * local])
                value = value + qb_ref[i : i + 1, :].astype(f32)
                if i == 2:
                    qkv3[2, at, :] = value.astype(bf16)
                    continue
                for h in range(pairs):
                    lanes = slice(h * 128, (h + 1) * 128)
                    turned = turn(value[:, lanes], cosine, slo, shi).astype(bf16)
                    if i == 0:
                        turned = turned * bf16(HD**-0.5)
                    qkv3[i, at, lanes] = turned

        def hidden_layer(b, first):
            at = block(b)

            @pl.loop(0, units, step=512)
            def _(n):
                @pl.when(first & (n == units // 2))
                def _():
                    load_1[1].wait()

                to = pl.ds(pl.multiple_of(n, 512), 512)
                pre = dot_nn(nv[at, :], wb[:, to]) + fb_ref[0:1, to].astype(f32)
                square = pre * pre
                bend = jnp.tanh(0.7978845608028654 * pre * (1.0 + 0.044715 * square))
                act[at, to] = (0.5 * pre * (1.0 + bend)).astype(bf16)
                rise = 0.7978845608028654 * (1.0 + 3 * 0.044715 * square)
                slope[at, to] = (
                    0.5 * (1.0 + bend) + 0.5 * pre * (1.0 - bend * bend) * rise
                ).astype(bf16)

        def slope_layer(b):
            at = block(b)
            abuf[at, pl.ds(local, local)] = dot_nt(cbuf[at, :], wd[...]).astype(bf16)

            @pl.loop(0, units, step=1024)
            def _(n):
                to = pl.ds(pl.multiple_of(n, 1024), 1024)
                value = dot_nt(cbuf[at, :], wa[to, :]) * slope[at, to].astype(f32)
                value = value.astype(bf16)
                slope[at, to] = value
                fsum[0:1, to] += jnp.sum(value.astype(f32), 0, keepdims=True)

        def blocks_of(s, task):
            @pl.loop(0, 2)
            def _(way):
                b = line + (2 * way - 1) * (1 + s)

                @pl.when((b >= 0) & (b < tensor) & ((s >= 0) | (way == 0)))
                def _():
                    task(b)

        norm.advance(0, 0)
        for j in range(1, stages - 1):
            qkv.advance(j)
        norm.advance(0, 1)
        qkv.advance(stages - 1)
        keeps[0].wait()
        load_q = [
            copy_of(gq_ref.at[i], wa.at[:, pl.ds(i * local, local)]) for i in range(3)
        ]
        for copy in load_q:
            copy.start()
        fc1.advance(0)
        dense.start()
        fc2.start()
        for copy in load_q:
            copy.wait()

        @pl.loop(-1, tensor - 2)
        def _(s):
            @pl.when(s == tensor - 3)
            def _():
                norm.advance(tensor - 3, 0)
                norm.advance(tensor - 3, 1)
                cot.start(1)
                cot.advance(0, 0)

            blocks_of(s, project)

        for j in range(1, stages):
            fc1.advance(j)
        for copy in keeps[1:]:
            copy.wait()
        load_1 = [copy_of(g1_ref.at[:, piece(units, h)], wb.at[:, piece(units, h)]) for h in (0, 1)]
        load_1[0].start()
        load_1[0].wait()
        load_1[1].start()

        @pl.loop(-1, tensor - 1)
        def _(s):
            @pl.when(s == tensor - 2)
            def _():
                norm.advance(tensor - 2, 0)
                norm.advance(tensor - 2, 1)
                fc2.advance(0)
                blocks_of(tensor - 2, project)

            @pl.when(s == 0)
            def _():
                dense.advance(0)

            blocks_of(s, lambda b: hidden_layer(b, s == -1))

        n_store = copy_of(nv, n_out)
        n_store.start()
        cross_n = [
            to_twin(r, nv.at[:, cols(relative(twin, r << 1))], nx_out.at[r]) for r in range(chips)
        ]
        cross_a = to_twin(chips, act, ax_out)
        for copy in cross_n + [cross_a]:
            copy.start()

        def prob_lanes(h, e):
            return pl.ds(pl.multiple_of((2 * h + e) * BLOCK, BLOCK), BLOCK)

        @pl.loop(0, pairs)
        def _(h):
            lanes = pl.ds(pl.multiple_of(h * 128, 128), 128)

            def keep(e, at, value):
                pb[at, prob_lanes(h, e)] = value

            def write(at, value):
                abuf[at, lanes] = value

            attend_pair(
                qkv3[0, :, lanes], qkv3[1, :, lanes], qkv3[2, :, lanes], mask, keep, write)

            @pl.when(h == 1)
            def _():
                cot.advance(0, 1)
                for j in range(1, stages - 1):
                    dense.advance(j)

            @pl.when(h == 2)
            def _():
                for j in range(1, stages - 1):
                    fc2.advance(j)

        cross_t = to_twin(chips + 1, attn, xbuf.at[:, pl.ds(chips * part, local)])
        cross_t.start()
        cross_a.wait_recv()
        load_ax = copy_of(ax_out, wb.at[low, :])
        load_ax.start()
        dense.advance(stages - 1)
        fc2.advance(stages - 1)
        takes[2].wait()
        takes[3].wait()
        load_2 = [copy_of(g2_ref.at[:, piece(width, h)], wa.at[:, piece(width, h)]) for h in (0, 1)]
        load_2[0].start()
        cot.advance(1, 0)
        norm.finish()
        n_store.wait()
        for copy in cross_n:
            copy.wait_send()
        load_2[0].wait()
        load_2[1].start()
        upper = lax.div(line, tensor // 2)

        def outward(i):
            return (1 - upper) * (tensor - 1 - i) + upper * i

        @pl.loop(0, tensor)
        def _(i):
            at = block(outward(i))

            @pl.loop(0, width, step=1024)
            def _(n):
                @pl.when((i == 0) & (n > 0))
                def _():
                    load_2[1].wait()

                to = pl.ds(pl.multiple_of(n, 1024), 1024)
                value = dot_nn(act[at, :], wa[:, to]) + dot_nn(attn[at, :], wd[:, to])
                nv[at, to] = value.astype(bf16)

            for k in range(tensor - 1):

                @pl.when(i == k)
                def _():
                    outs.start(0, k)
                    outs.start(1, k)

            @pl.when(i == tensor - 2)
            def _():
                cot.advance(1, 1)

        fsum[...] = jnp.zeros_like(fsum)
        cross_c = [
            to_twin(chips + 2 + r, cbuf.at[:, cols(relative(twin, r << 1))],
                    xbuf.at[:, pl.ds(r * part, part)])
            for r in range(chips)
        ]

        @pl.loop(-1, tensor - 1)
        def _(s):
            @pl.when(s == tensor - 2)
            def _():
                cot.advance(tensor - 2, 0)
                outs.advance(1)
                cot.advance(tensor - 2, 1)
                for copy in cross_c:
                    copy.start()

            blocks_of(s, slope_layer)

        cross_p = to_twin(2 * chips + 3, slope, gpx_out)
        cross_p.start()
        for copy in cross_c + [cross_t]:
            copy.wait_recv()
        load_ax.wait()
        dense.finish()

        def weight_grad(left, plan, own, crossed, spot, size, step, hook=None):
            @pl.loop(0, chips)
            def _(i):
                r = chips - 1 - i
                slot = chip_slot(me, r)
                across = pl.ds(pl.multiple_of(r * part, part), part)

                @pl.loop(0, size, step=step)
                def _(n):
                    at = pl.multiple_of(n, step)
                    value = dot_tn(left(cols(slot)), own(at)) + dot_tn(xbuf[:, across], crossed(at))
                    spot(r, at, value.astype(bf16))

                for k in range(1, chips):

                    @pl.when(r == k)
                    def _():
                        plan.start(k)

                if hook is not None:
                    hook(i)

        def spot_a(r, at, value):
            wa[pl.ds(pl.multiple_of(tokens + r * part, part), part), pl.ds(at, 1024)] = value

        def spot_d(r, at, value):
            for h in (0, 1):
                to = pl.ds(pl.multiple_of((2 * r + h) * part, part), part)
                mask[to, :] = value[:, h * (local // 2) : (h + 1) * (local // 2)]

        def spot_1(r, at, value):
            wb[pl.ds(pl.multiple_of(r * part, part), part), pl.ds(at, 1024)] = value

        def spot_q(r, at, value):
            abuf[pl.ds(pl.multiple_of(r * part, part), part), pl.ds(at, local)] = value

        weight_grad(
            lambda a: cbuf[:, a], sum_2, lambda at: act[:, pl.ds(at, 1024)],
            lambda at: wb[low, pl.ds(at, 1024)], spot_a, units, 1024)
        weight_grad(
            lambda a: cbuf[:, a], sum_d, lambda at: attn[...],
            lambda at: xbuf[:, pl.ds(chips * part, local)], spot_d, local, local)
        load_n = copy_of(n_out, wa.at[low, :])
        load_n.start()
        load_g1 = copy_of(g1_ref.at[low, :], wb.at[low, :])
        load_g1.start()
        for copy in cross_n:
            copy.wait_recv()
        load_nx = [copy_of(nx_out.at[r], xbuf.at[:, pl.ds(r * part, part)]) for r in range(chips)]
        for copy in load_nx:
            copy.start()
        cot.finish()
        for copy in cross_c + [cross_a]:
            copy.wait_send()
        bsum[...] = jnp.zeros_like(bsum)
        for k in range(units // local):
            bsum[k : k + 1, :] = fsum[0:1, k * local : (k + 1) * local]
        load_w = [copy_of(gq_ref.at[i], pb.at[pl.ds(0, width), pl.ds(i * local, local)]) for i in range(3)]

        @pl.loop(0, pairs)
        def _(h):
            lanes = pl.ds(pl.multiple_of(h * 128, 128), 128)

            def write(which, at, value):
                cbuf[at, pl.ds(pl.multiple_of(which * local + h * 128, 128), 128)] = value

            sums = attend_back_pair(
                qkv3[0, :, lanes], qkv3[1, :, lanes], qkv3[2, :, lanes],
                abuf[:, pl.ds(pl.multiple_of(local + h * 128, 128), 128)], abuf[:, lanes],
                lambda e, at: pb[at, prob_lanes(h, e)],
                (cos_ref, slo_ref, shi_ref), kacc, vacc, write)
            for k in range(3):
                bsum[units // local + k : units // local + k + 1, lanes] = sums[k]

            for k in range(3):

                @pl.when(h == k)
                def _():
                    load_w[k].start()

            @pl.when(h == 0)
            def _():
                sum_2.middle()

            @pl.when(h == 1)
            def _():
                outs.advance(2)

        back = cbuf.at[:, pl.ds(0, wide)]
        cross_d = to_twin(2 * chips + 2, back, gqx_out)
        cross_d.start()
        bias_tells = [
            remote(tells[r - 1], bsum, tell_b.at[r], (relative(me, r), line)) for r in range(1, dp)
        ]
        for copy in bias_tells:
            copy.start()
        for copy in load_w + [load_g1]:
            copy.wait()
        load_gx = [copy_of(gqx_out.at[:, pl.ds(i * local, local)], qkv3.at[i]) for i in range(3)]
        store_o = copy_of(x_buf, out_ref)
        load_px = copy_of(gpx_out, nv)
        spare = pb.at[pl.ds(width, rows), :]
        load_c = copy_of(c_ref, spare)

        @pl.loop(0, tensor)
        def _(i):
            at = block(outward(i))

            @pl.loop(0, width, step=1024)
            def _(n):
                to = pl.ds(pl.multiple_of(n, 1024), 1024)
                value = dot_nt(slope[at, :], wb[to, :])
                value = value + dot_nt(cbuf[at, pl.ds(0, wide)], pb[to, pl.ds(0, wide)])
                act[at, to] = value.astype(bf16)

            for k in range(tensor - 1):

                @pl.when(i == k)
                def _():
                    ins.start(0, k)
                    ins.start(1, k)

            @pl.when(i == 0)
            def _():
                load_c.start()
                sum_d.middle()

            @pl.when(i == 1)
            def _():
                cross_d.wait_recv()
                for copy in load_gx:
                    copy.start()
                load_n.wait()
                for copy in load_nx + load_gx:
                    copy.wait()
                cross_t.wait_send()
                weight_grad(
                    lambda a: wa[low, a], sum_q, lambda at: cbuf[:, pl.ds(at, local)],
                    lambda at: qkv3[lax.div(at, local)], spot_q, wide, local)

            @pl.when(i == tensor - 2)
            def _():
                cross_p.wait_recv()
                outs.arrive()

                @pl.loop(0, rows, step=32)
                def _(r):
                    at = pl.ds(r, 32)
                    own = pl.ds(pl.multiple_of(line * rows + r, 32), 32)
                    total = x_buf[at, :].astype(f32) + outs.total(nv[own, :], at) + vec_buf[2:3, :]
                    x_buf[at, :] = total.astype(bf16)

                store_o.start()
                load_px.start()

        ins.advance(1)
        load_px.wait()

        def late_steps(i):
            @pl.when(i == 0)
            def _():
                sum_q.middle()

        weight_grad(
            lambda a: wa[low, a], sum_1, lambda at: slope[:, pl.ds(at, 1024)],
            lambda at: nv[:, pl.ds(at, 1024)], spot_1, units, 1024, late_steps)
        sum_2.final()
        sum_d.final()
        store_2 = copy_of(wa.at[pl.ds(tokens, part), :], s2_out)
        store_dense = [
            copy_of(mask.at[pl.ds(h * part, part), :], sd_out.at[:, piece(local, h)]) for h in (0, 1)
        ]
        for copy in [store_2] + store_dense:
            copy.start()
        store_o.wait()
        load_x = copy_of(x_ref, x_buf)
        load_x.start()
        for copy in bias_tells:
            copy.wait_recv()
        total_b = bsum[...]
        for r in range(1, dp):
            total_b = total_b + tell_b[r]
        bout_ref[...] = total_b
        ins.advance(2)
        sum_1.middle()
        sum_q.final()
        store_q = copy_of(abuf.at[pl.ds(0, part), :], sq_out)
        store_q.start()
        load_c.wait()
        load_x.wait()
        parts[...] = jnp.zeros_like(parts)
        ins.arrive()

        @pl.loop(0, rows, step=32)
        def _(r):
            at = pl.ds(r, 32)
            x = x_buf[at, :].astype(f32)
            centred = x - jnp.mean(x, -1, keepdims=True)
            inv_std = lax.rsqrt(jnp.mean(centred * centred, -1, keepdims=True) + layer_eps)
            unit = centred * inv_std
            own = pl.ds(pl.multiple_of(line * rows + r, 32), 32)
            grad = ins.total(act[own, :], at)
            cot_rows = pl.ds(pl.multiple_of(width + r, 32), 32)
            cotan = pb[cot_rows, :].astype(f32)
            scaled = grad * vec_buf[0:1, :]
            first = jnp.mean(scaled, -1, keepdims=True)
            second = jnp.mean(scaled * unit, -1, keepdims=True)
            x_buf[at, :] = (cotan + inv_std * (scaled - first - unit * second)).astype(bf16)
            parts[0:1, :] += jnp.sum(grad * unit, 0, keepdims=True)
            parts[1:2, :] += jnp.sum(grad, 0, keepdims=True)
            parts[2:3, :] += jnp.sum(cotan, 0, keepdims=True)

        vec_tells = [
            remote(tells[dp - 2 + r], parts.at[:, cols(relative(me, r))], tell_v.at[r],
                   (relative(me, r), line))
            for r in range(1, dp)
        ]
        for copy in vec_tells:
            copy.start()
        store_h = copy_of(x_buf, hid_ref)
        store_h.start()
        for copy in vec_tells:
            copy.wait_recv()
        total_v = parts[:, cols(me)]
        for r in range(1, dp):
            total_v = total_v + tell_v[r]
        tell_z[0] = total_v
        line_tells = [
            remote(tells[2 * dp - 3 + k], tell_z.at[0], tell_z.at[k], (me, lax.rem(line + k, tensor)))
            for k in range(1, tensor)
        ]
        for copy in line_tells:
            copy.start()
        sum_1.final()
        store_1 = copy_of(wb.at[pl.ds(0, part), :], s1_out)
        store_1.start()
        for copy in line_tells:
            copy.wait_recv()
        total_z = tell_z[0]
        for k in range(1, tensor):
            total_z = total_z + tell_z[k]
        vout_ref[...] = total_z
        for copy in vec + [cross_p] + bias_tells + vec_tells + line_tells:
            copy.wait_send()
        for plan in (qkv, fc1, fc2, sum_2, sum_d, sum_1, sum_q):
            plan.finish()
        for copy in [cross_d]:
            copy.wait_send()
        for copy in store_dense + [store_2, store_q, store_h, store_1]:
            copy.wait()

    def shape(*dims):
        return jax.ShapeDtypeStruct(dims, bf16)

    def vmem(*dims):
        return pltpu.VMEM(dims, bf16)

    landings = [
        shape(2 * tensor - 3, rows, width),
        shape(2 * tensor - 3, rows, width),
        shape(6, part, units // 2),
        shape(6, part, local // 2),
        shape(6, part, units // 2),
        shape(6, part, wide // 2),
    ]
    return pl.pallas_call(
        kernel,
        out_shape=(
            shape(rows, width),
            shape(rows, width),
            shape(part, units),
            shape(part, local),
            shape(part, units),
            shape(part, wide),
            shape(3, width, local),
            shape(width, units),
            shape(units, width),
            shape(tokens, width),
            shape(chips, tokens, part),
            shape(tokens, units),
            shape(tokens, wide),
            shape(tokens, units),
            *landings,
            jax.ShapeDtypeStruct((8, part), f32),
            jax.ShapeDtypeStruct((8, local), f32),
        ),
        in_specs=[ANY] * 7 + [VMEM] * 3,
        out_specs=(ANY,) * 20 + (VMEM,) * 2,
        scratch_shapes=[
            vmem(rows, width),
            pltpu.VMEM((8, width), f32),
            vmem(tokens, width),
            vmem(width, width),
            vmem(width, units),
            vmem(local, width),
            vmem(tokens, units),
            vmem(tokens, units),
            vmem(3, tokens, local),
            vmem(tokens, wide),
            vmem(stored, local // HD * BLOCK),
            vmem(stored, BLOCK),
            vmem(tokens, width),
            vmem(tokens, chips * part + local),
        ]
        + [pltpu.VMEM((tokens, 128), f32)] * 5
        + [
            vmem(tensor - 1, rows, width),
            vmem(2, part, units // 2),
            pltpu.VMEM((8, units), f32),
            pltpu.VMEM((8, local), f32),
            pltpu.VMEM((8, width), f32),
            pltpu.VMEM((dp, 8, part), f32),
            pltpu.VMEM((dp, 8, local), f32),
            pltpu.VMEM((tensor, 8, part), f32),
            pltpu.SemaphoreType.DMA((sems.count,)),
            pltpu.SemaphoreType.DMA((sems.count,)),
            pltpu.SemaphoreType.DMA((48,)),
            pltpu.SemaphoreType.DMA((2,)),
        ],
        compiler_params=pltpu.CompilerParams(
            collective_id=0, has_side_effects=True, vmem_limit_bytes=67_043_328
        ),
        name="block",
    )(*arrays)


def finish_kernel(s2_ref, sd_ref, s1_ref, sq_ref, o_ref, h_ref, w2_ref, wd_ref, w1_ref, wq_ref, out_ref, hid_ref):
    w2_ref[...] = s2_ref[...].T.astype(f32)
    wd_ref[...] = sd_ref[...].T.astype(f32)
    w1_ref[...] = s1_ref[...].astype(f32)
    local = wq_ref.shape[2]
    for i in range(3):
        wq_ref[i] = sq_ref[:, i * local : (i + 1) * local].astype(f32)
    out_ref[...] = o_ref[...]
    hid_ref[...] = h_ref[...]


def finish(sent_fc2, sent_dense, sent_fc1, sent_qkv, out, hidden_grad):
    part, units = sent_fc2.shape
    local = sent_dense.shape[1]
    rows, width = out.shape
    steps = 4

    def down(n, m):
        return pl.BlockSpec((n // steps, m), lambda i: (i, 0))

    def across(n, m):
        return pl.BlockSpec((n, m // steps), lambda i: (0, i))

    return pl.pallas_call(
        finish_kernel,
        grid=(steps,),
        out_shape=(
            jax.ShapeDtypeStruct((units, part), f32),
            jax.ShapeDtypeStruct((local, part), f32),
            jax.ShapeDtypeStruct((part, units), f32),
            jax.ShapeDtypeStruct((3, part, local), f32),
            jax.ShapeDtypeStruct((rows, width), bf16),
            jax.ShapeDtypeStruct((rows, width), bf16),
        ),
        in_specs=[
            across(part, units), across(part, local), down(part, units), down(part, 3 * local),
            down(rows, width), down(rows, width),
        ],
        out_specs=(
            down(units, part), down(local, part), down(part, units),
            pl.BlockSpec((3, part // steps, local), lambda i: (0, i, 0)),
            down(rows, width), down(rows, width),
        ),
        compiler_params=pltpu.CompilerParams(vmem_limit_bytes=VMEM_LIMIT),
        name="finish",
    )(sent_fc2, sent_dense, sent_fc1, sent_qkv, out, hidden_grad)


def rotary_tables(segments):
    rows, length = segments.shape
    index = jnp.arange(length, dtype=jnp.int32)[None]
    start = jnp.zeros_like(segments)
    for number in range(1, 4):
        start = jnp.where(segments == number, jnp.sum(segments < number, -1, keepdims=True), start)
    position = (index - start).astype(f32).reshape(rows * length, 1)
    lane = jnp.arange(128, dtype=jnp.int32) % HD
    exponent = (2 * (lane % (ROT // 2))).astype(f32) / ROT
    angle = position * (1.0 / 10000.0**exponent)[None]
    cosine, sine = jnp.cos(angle), jnp.sin(angle)
    low, high = lane < ROT // 2, (lane >= ROT // 2) & (lane < ROT)
    return (
        jnp.where(lane < ROT, cosine, 1.0),
        jnp.where(low, -sine, 0.0),
        jnp.where(high, sine, 0.0),
    )


def matmul(a, b):
    return jnp.dot(a, b, preferred_element_type=f32)


def on_device(
    dp, tensor, fast,
    hidden_in, segments, ln_gain, ln_bias, qkv_weight, qkv_bias, dense_weight, dense_bias,
    fc1_weight, fc1_bias, fc2_weight, fc2_bias, cotangent,
):
    seqs = segments.shape[0]
    local = qkv_weight.shape[2]
    number = lax.broadcasted_iota(jnp.int32, (8, ln_gain.shape[0]), 0)
    vectors = jnp.where(number == 1, ln_bias.astype(f32)[None], ln_gain.astype(f32)[None])
    vectors = jnp.where(
        number == 2, dense_bias.astype(f32)[None] + fc2_bias.astype(f32)[None], vectors)
    mine = (
        hidden_in, cotangent, qkv_weight.transpose(1, 0, 2),
        dense_weight, fc1_weight, fc2_weight, vectors,
    )
    if fast:
        (out, hidden_grad, sent_fc2, sent_dense, sent_fc1, sent_qkv, *_, vec_sums, all_sums) = block_call(
            dp, tensor, (*mine, qkv_bias, fc1_bias[None], segments))
        quarter = vec_sums.shape[1] // tensor
        at = lax.axis_index("tensor") * quarter
        small = lax.dynamic_slice(vec_sums, (0, at), (3, quarter))
        grad_w2, grad_wd, grad_w1, grad_wq, out, hidden_grad = finish(
            sent_fc2, sent_dense, sent_fc1, sent_qkv, out, hidden_grad)
        return (
            out,
            hidden_grad,
            small[0],
            small[1],
            grad_wq.transpose(1, 0, 2),
            all_sums[4:7],
            grad_wd,
            small[2],
            grad_w1,
            all_sums[:4].reshape(-1),
            grad_w2,
            small[2],
        )

    tables = rotary_tables(segments)
    bias = jnp.pad(qkv_bias.astype(f32), ((0, 5), (0, 0)))
    w_qkv, w_dense, w_fc1, w_fc2, normed, grad_out, vec = gather_plain(*mine)
    gain, out_bias = vec[0:1], vec[2:3]
    query, key, value, attn_vec, probs = attend(
        *(matmul(normed, w_qkv[i]) for i in range(3)), bias, tables, segments, seqs
    )
    pre_act = matmul(normed, w_fc1) + fc1_bias.astype(f32)
    act_vals, gelu_pull = jax.vjp(lambda pre: jax.nn.gelu(pre, approximate=True), pre_act)
    act_vals = act_vals.astype(bf16)
    slope = gelu_pull(jnp.ones_like(pre_act))[0].astype(bf16)
    branches = matmul(attn_vec, w_dense) + matmul(act_vals, w_fc2)
    grad_attn = matmul(grad_out, w_dense.T).astype(bf16)
    *grads, qkv_sums = attend_back(query, key, value, grad_attn, attn_vec, probs, tables, seqs)
    resid_in = hidden_in.astype(f32)
    cot_float = cotangent.astype(f32)
    centred = resid_in - jnp.mean(resid_in, -1, keepdims=True)
    spread = jnp.mean(centred * centred, -1, keepdims=True)
    inv_std = lax.rsqrt(spread + layer_eps)
    unit_rows = centred * inv_std
    summed = lax.psum_scatter(branches.astype(bf16), "tensor", scatter_dimension=0, tiled=True)
    out = (resid_in + summed.astype(f32) + out_bias).astype(bf16)
    out_bias_part = jnp.sum(cot_float, 0)
    grad_fc2 = matmul(act_vals.T, grad_out)
    grad_dense = matmul(attn_vec.T, grad_out)
    grad_pre = (matmul(grad_out, w_fc2.T) * slope.astype(f32)).astype(bf16)
    fc1_bias_part = jnp.sum(grad_pre.astype(f32), 0)
    grad_fc1 = matmul(normed.T, grad_pre)
    grad_wqkv = jnp.stack([matmul(normed.T, g) for g in grads])
    grad_normed = matmul(grad_pre, w_fc1.T) + sum(matmul(g, w.T) for g, w in zip(grads, w_qkv))
    sent_qkv, sent_dense, sent_fc1, sent_fc2 = (
        lax.psum_scatter(grad_wqkv.astype(bf16), "dp", scatter_dimension=1, tiled=True),
        lax.psum_scatter(grad_dense.astype(bf16), "dp", scatter_dimension=1, tiled=True),
        lax.psum_scatter(grad_fc1.astype(bf16), "dp", scatter_dimension=0, tiled=True),
        lax.psum_scatter(grad_fc2.astype(bf16), "dp", scatter_dimension=1, tiled=True),
    )
    grad_local = lax.psum_scatter(
        grad_normed.astype(bf16), "tensor", scatter_dimension=0, tiled=True
    ).astype(f32)
    gain_part = jnp.sum(grad_local * unit_rows, 0)
    beta_part = jnp.sum(grad_local, 0)
    scaled_grad = grad_local * gain
    first_mean = jnp.mean(scaled_grad, -1, keepdims=True)
    second_mean = jnp.mean(scaled_grad * unit_rows, -1, keepdims=True)
    hidden_grad = (
        cot_float + inv_std * (scaled_grad - first_mean - unit_rows * second_mean)
    ).astype(bf16)
    gain_grad, beta_grad, out_bias_grad = (
        lax.psum_scatter(gain_part, ("dp", "tensor"), scatter_dimension=0, tiled=True),
        lax.psum_scatter(beta_part, ("dp", "tensor"), scatter_dimension=0, tiled=True),
        lax.psum_scatter(out_bias_part, ("dp", "tensor"), scatter_dimension=0, tiled=True),
    )
    qkv_bias_grad, fc1_bias_grad = lax.psum((qkv_sums[:3], fc1_bias_part), "dp")
    return (
        out,
        hidden_grad,
        gain_grad,
        beta_grad,
        sent_qkv.transpose(1, 0, 2).astype(f32),
        qkv_bias_grad,
        sent_dense.astype(f32),
        out_bias_grad,
        sent_fc1.astype(f32),
        fc1_bias_grad,
        sent_fc2.astype(f32),
        out_bias_grad,
    )


def solution(mesh):
    dp, tensor = mesh.shape["dp"], mesh.shape["tensor"]
    fast = dp == 8 and tensor == 4
    placed = (
        P(("dp", "tensor"), None),
        P("dp", None),
        P("dp"),
        P("dp"),
        P("dp", None, "tensor"),
        P(None, "tensor"),
        P("tensor", "dp"),
        P("dp"),
        P("dp", "tensor"),
        P("tensor"),
        P("tensor", "dp"),
        P("dp"),
        P(("dp", "tensor"), None),
    )
    return jax.shard_map(
        functools.partial(on_device, dp, tensor, fast),
        mesh=mesh,
        in_specs=placed,
        out_specs=(
            P(("dp", "tensor"), None),
            P(("dp", "tensor"), None),
            P(("dp", "tensor")),
            P(("dp", "tensor")),
            P("dp", None, "tensor"),
            P(None, "tensor"),
            P("tensor", "dp"),
            P(("dp", "tensor")),
            P("dp", "tensor"),
            P("tensor"),
            P("tensor", "dp"),
            P(("dp", "tensor")),
        ),
        check_vma=False,
    )
```

```python
import functools

import jax
import jax.numpy as jnp
from jax import lax
from jax.experimental import pallas as pl
from jax.experimental.pallas import tpu as pltpu
from jax.sharding import PartitionSpec as P

HD = 64
ROT = 32
BLOCK = 256
MAX_DOC = 512
VMEM_LIMIT = 66_000_000
MESH = pl.DeviceIdType.MESH
ANY = pl.BlockSpec(memory_space=pl.ANY)
VMEM = pl.BlockSpec(memory_space=pltpu.VMEM)

layer_eps = 1e-05
f32 = jnp.float32
bf16 = jnp.bfloat16


def dot_nn(a, b):
    return lax.dot_general(a, b, (((1,), (0,)), ((), ())), preferred_element_type=f32)


def dot_nt(a, b):
    return lax.dot_general(a, b, (((1,), (1,)), ((), ())), preferred_element_type=f32)


def dot_tn(a, b):
    return lax.dot_general(a, b, (((0,), (0,)), ((), ())), preferred_element_type=f32)


def flip(index, bit):
    step = 1 << bit
    return index + step * (1 - 2 * (lax.div(index, step) % 2))


def relative(index, offset):
    bit = 0
    while offset >> bit:
        if (offset >> bit) & 1:
            index = flip(index, bit)
        bit += 1
    return index


def stages_of(order):
    held, stages = [0], []
    for bit in order:
        got = [r ^ (1 << bit) for r in held]
        stages.append((bit, list(held), got))
        held = held + got
    return stages


class Sems:
    def __init__(self):
        self.count = 0

    def take(self):
        self.count += 1
        return self.count - 1


class CubeGather:
    def __init__(self, sems, orders):
        self.plans = [stages_of(order) for order in orders]
        self.ids = {
            (h, j, i): sems.take()
            for h, stages in enumerate(self.plans)
            for j, (_, held, _) in enumerate(stages)
            for i in range(len(held))
        }

    def bind(self, me, other, own, window, send_sem, recv_sem):
        self.me, self.other, self.own, self.window = me, other, own, window
        self.send_sem, self.recv_sem = send_sem, recv_sem
        return self

    def copy(self, h, j, i):
        bit, held, _ = self.plans[h][j]
        slot = relative(self.me, held[i])
        target = self.window(slot, h)
        source = self.own(h) if held[i] == 0 else target
        k = self.ids[h, j, i]
        return pltpu.make_async_remote_copy(
            src_ref=source,
            dst_ref=target,
            send_sem=self.send_sem.at[k],
            recv_sem=self.recv_sem.at[k],
            device_id=(flip(self.me, bit), self.other),
            device_id_type=MESH,
        )

    def start(self):
        depth = len(self.plans[0])
        for j in range(depth):
            for h in range(len(self.plans)):
                self.copy(h, j, 0).start()

    def advance(self, j):
        for i in range(len(self.plans[0][j][1])):
            for h, stages in enumerate(self.plans):
                self.copy(h, j, i).wait_recv()
                slot = stages[j][2][i]
                for later in range(j + 1, len(stages)):
                    self.copy(h, later, stages[later][1].index(slot)).start()

    def finish(self):
        for h, j, i in self.ids:
            self.copy(h, j, i).wait_send()


class LineGather:
    def __init__(self, sems, size, subs):
        self.size, self.subs = size, subs
        self.ids = {
            (way, s, u): sems.take()
            for way in (0, 1)
            for s in range(size - 1)
            for u in range(subs)
        }

    def bind(self, me, other, own, window, send_sem, recv_sem):
        self.me, self.other, self.own, self.window = me, other, own, window
        self.send_sem, self.recv_sem = send_sem, recv_sem
        return self

    def copy(self, way, s, u):
        block = self.me - s if way == 0 else self.me + s
        target = self.window(block, u)
        k = self.ids[way, s, u]
        return pltpu.make_async_remote_copy(
            src_ref=self.own(u) if s == 0 else target,
            dst_ref=target,
            send_sem=self.send_sem.at[k],
            recv_sem=self.recv_sem.at[k],
            device_id=(self.other, self.me + 1 if way == 0 else self.me - 1),
            device_id_type=MESH,
        )

    def sends(self, way, s):
        if way == 0:
            return (self.me >= s) & (self.me < self.size - 1)
        return (self.me + s < self.size) & (self.me > 0)

    def gets(self, way, s):
        if way == 0:
            return self.me - 1 - s >= 0
        return self.me + 1 + s < self.size

    def start(self, u):
        for way in (0, 1):

            @pl.when(self.sends(way, 0))
            def _():
                self.copy(way, 0, u).start()

    def advance(self, s, u):
        for way in (0, 1):

            @pl.when(self.gets(way, s))
            def _():
                self.copy(way, s, u).wait_recv()

            if s + 1 < self.size - 1:

                @pl.when(self.sends(way, s + 1))
                def _():
                    self.copy(way, s + 1, u).start()

    def finish(self):
        for way, s, u in self.ids:

            @pl.when(self.sends(way, s))
            def _():
                self.copy(way, s, u).wait_send()


def greet(dp, me, tensor, line, meanwhile):
    barrier = pltpu.get_barrier_semaphore()
    for r in range(1, dp):
        pl.semaphore_signal(barrier, inc=1, device_id=(relative(me, r), line), device_id_type=MESH)
    for k in range(1, tensor):
        to = (me, lax.rem(line + k, tensor))
        pl.semaphore_signal(barrier, inc=1, device_id=to, device_id_type=MESH)
    meanwhile()
    pl.semaphore_wait(barrier, dp + tensor - 2)


def orders_of(dp):
    bits = list(range(1, dp.bit_length() - 1))
    return [bits + [0], bits[::-1] + [0]]


def normalize(x, gain, bias):
    centred = x - jnp.mean(x, -1, keepdims=True)
    spread = jnp.mean(centred * centred, -1, keepdims=True)
    unit = centred * lax.rsqrt(spread + layer_eps)
    return (unit * gain + bias).astype(bf16)


def gather_plain(hidden, cotangent, w_qkv, w_dense, w_fc1, w_fc2, vectors):
    vec = lax.all_gather(vectors, "dp", axis=1, tiled=True)
    normed = normalize(hidden.astype(f32), vec[0:1], vec[1:2])
    return (
        lax.all_gather(w_qkv, "dp", axis=1, tiled=True),
        lax.all_gather(w_dense, "dp", axis=1, tiled=True),
        lax.all_gather(w_fc1, "dp", axis=0, tiled=True),
        lax.all_gather(w_fc2, "dp", axis=1, tiled=True),
        lax.all_gather(normed, "tensor", axis=0, tiled=True),
        lax.all_gather(cotangent, "tensor", axis=0, tiled=True),
        vec,
    )


class ChipReduce:
    COUNT = 6

    def __init__(self, sems):
        self.ids = [sems.take() for _ in range(self.COUNT)]

    def bind(self, me, other, view, landing, stage, stage_sem, send_sem, recv_sem):
        self.me, self.other, self.view, self.landing = me, other, view, landing
        self.stage, self.stage_sem = stage, stage_sem
        self.send_sem, self.recv_sem = send_sem, recv_sem
        return self

    def copy(self, slot):
        r, h, bit = [(2, 0, 2), (3, 0, 2), (1, 0, 1), (1, 1, 1), (3, 1, 1), (2, 1, 2)][slot]
        k = self.ids[slot]
        return pltpu.make_async_remote_copy(
            src_ref=self.view(r, h),
            dst_ref=self.landing.at[slot],
            send_sem=self.send_sem.at[k],
            recv_sem=self.recv_sem.at[k],
            device_id=(flip(self.me, bit), self.other),
            device_id_type=MESH,
        )

    def start(self, r):
        for slot in {3: (1, 4), 2: (0,), 1: (3,), 0: ()}[r]:
            self.copy(slot).start()

    def fetch(self, slots):
        half = self.landing.shape[-1]
        held = [self.stage.at[k, :, pl.ds(0, half)] for k in range(len(slots))]
        copies = []
        for k, slot in enumerate(slots):
            self.copy(slot).wait_recv()
            copies.append(
                pltpu.make_async_copy(self.landing.at[slot], held[k], self.stage_sem.at[k]))
            copies[k].start()
        for copy in copies:
            copy.wait()
        return held

    def middle(self):
        held = self.fetch((1, 4))
        for k, (r, h, last) in enumerate(((1, 0, 2), (2, 1, 5))):
            view = self.view(r, h)
            view[...] = (view[...].astype(f32) + held[k][...].astype(f32)).astype(bf16)
            self.copy(last).start()

    def final(self):
        for h, slots in ((0, (0, 2)), (1, (3, 5))):
            a, b = self.fetch(slots)
            view = self.view(0, h)
            total = view[...].astype(f32) + a[...].astype(f32) + b[...].astype(f32)
            view[...] = total.astype(bf16)

    def finish(self):
        for slot in range(self.COUNT):
            self.copy(slot).wait_send()


class LineReduce:
    def __init__(self, sems, size):
        self.size = size
        self.ids = {(way, i): sems.take() for way in (0, 1) for i in range(size - 1)}

    def bind(self, me, other, own, landing, stage, last, stage_sem, send_sem, recv_sem):
        self.me, self.other, self.own, self.landing = me, other, own, landing
        self.stage, self.last, self.stage_sem = stage, last, stage_sem
        self.send_sem, self.recv_sem = send_sem, recv_sem
        return self

    def target(self, way, i):
        return self.size - 1 - i if way == 0 else i

    def place(self, way, i):
        return i if way == 0 else 2 * self.size - 4 - i

    def buffer(self, way, i):
        return self.stage.at[i if way == 0 else self.size - 2 - i]

    def copy(self, way, i, edge):
        k = self.ids[way, i]
        return pltpu.make_async_remote_copy(
            src_ref=self.own(self.target(way, i)) if edge else self.buffer(way, i),
            dst_ref=self.landing.at[self.place(way, i)],
            send_sem=self.send_sem.at[k],
            recv_sem=self.recv_sem.at[k],
            device_id=(self.other, self.me + 1 if way == 0 else self.me - 1),
            device_id_type=MESH,
        )

    def edge(self, way):
        return self.me == (0 if way == 0 else self.size - 1)

    def passes(self, way, i):
        d = self.target(way, i)
        return (self.me > 0) & (self.me < d) if way == 0 else (self.me < self.size - 1) & (self.me > d)

    def start(self, way, i):
        @pl.when(self.edge(way))
        def _():
            self.copy(way, i, True).start()

    def advance(self, step):
        for way in (0, 1):
            steps_from_edge = self.me if way == 0 else self.size - 1 - self.me
            for i in range(step):

                @pl.when(self.passes(way, i) & (steps_from_edge == step - i))
                def _():
                    self.copy(way, i, False).wait_recv()
                    held = self.buffer(way, i)
                    fetch = pltpu.make_async_copy(
                        self.landing.at[self.place(way, i)], held, self.stage_sem.at[0])
                    fetch.start()
                    fetch.wait()
                    add_into(held, self.own(self.target(way, i)))
                    self.copy(way, i, False).start()

    def settle(self):
        for way, i in self.ids:

            @pl.when(self.edge(way))
            def _():
                self.copy(way, i, True).wait_send()

            @pl.when(self.passes(way, i))
            def _():
                self.copy(way, i, False).wait_send()

    def arrive(self):
        def fetch(way, i):
            return pltpu.make_async_copy(
                self.landing.at[self.place(way, i)], self.last(way), self.stage_sem.at[way])

        for way, i in self.ids:

            @pl.when(self.me == self.target(way, i))
            def _():
                self.copy(way, i, False).wait_recv()
                fetch(way, i).start()

        for way, i in self.ids:

            @pl.when(self.me == self.target(way, i))
            def _():
                fetch(way, i).wait()

    def total(self, own, rows):
        value = own.astype(f32)
        for way, there in ((0, self.me > 0), (1, self.me < self.size - 1)):
            value = value + jnp.where(there, self.last(way)[rows, :].astype(f32), 0.0)
        return value


def add_into(landing, own):
    rows = landing.shape[0]

    @pl.loop(0, rows, step=64)
    def _(r):
        at = pl.ds(r, 64)
        landing[at, :] = (landing[at, :].astype(f32) + own[at, :].astype(f32)).astype(bf16)


def chip_slot(me, r):
    return (
        me
        + 2 * ((r % 2) * (1 - 2 * (lax.div(me, 2) % 2)))
        + 4 * (lax.div(r, 2) * (1 - 2 * (lax.div(me, 4) % 2)))
    )


def spans_of(length):
    back = -(-(MAX_DOC - 1) // BLOCK)
    spans, at = [], 0
    for i in range(length // BLOCK):
        low = max(0, i - back) * BLOCK
        spans.append((low, (i + 1) * BLOCK, at))
        at += (i + 1) * BLOCK - low
    return spans, at


def turn(x, cosine, sine_lo, sine_hi):
    return x * cosine + pltpu.roll(x, 128 - ROT // 2, 1) * sine_lo + pltpu.roll(x, ROT // 2, 1) * sine_hi


def head_lanes(shape, e):
    lane = lax.broadcasted_iota(jnp.int32, shape, 1)
    return (lane >= e * HD) & (lane < (e + 1) * HD)


def only(x, e):
    return jnp.where(head_lanes(x.shape, e), x, jnp.zeros_like(x))


def attend_kernel(
    q_ref, k_ref, v_ref, bias_ref, cos_ref, slo_ref, shi_ref, segc_ref, segr_ref,
    qs_ref, ks_ref, vs_ref, o_ref, p_ref, mask_ref,
):
    @pl.when(pl.program_id(1) == 0)
    def _():
        fill_mask(mask_ref, segc_ref, segr_ref, q_ref.shape[0])

    cosine, slo, shi = cos_ref[...], slo_ref[...], shi_ref[...]
    query = turn(q_ref[...] + bias_ref[0:1, :], cosine, slo, shi).astype(bf16) * bf16(HD**-0.5)
    key = turn(k_ref[...] + bias_ref[1:2, :], cosine, slo, shi).astype(bf16)
    value = (v_ref[...] + bias_ref[2:3, :]).astype(bf16)
    qs_ref[...] = query
    ks_ref[...] = key
    vs_ref[...] = value

    def keep(e, at, probs):
        p_ref[e, at, :] = probs

    def write(at, result):
        o_ref[at, :] = result

    attend_pair(query, key, value, mask_ref, keep, write)


def attend(q, k, v, qkv_bias, tables, segments, rows):
    tokens, local = q.shape
    length = tokens // rows
    pairs = local // 128
    _, stored = spans_of(length)
    block = pl.BlockSpec((length, 128), lambda r, h: (r, h))
    table = pl.BlockSpec((length, 128), lambda r, h: (r, 0))
    shape = jax.ShapeDtypeStruct((tokens, local), bf16)
    return pl.pallas_call(
        attend_kernel,
        grid=(rows, pairs),
        out_shape=(shape,) * 4 + (jax.ShapeDtypeStruct((rows, local // HD, stored, BLOCK), bf16),),
        in_specs=[block] * 3
        + [pl.BlockSpec((8, 128), lambda r, h: (0, h))]
        + [table] * 3
        + [
            pl.BlockSpec((length, 1), lambda r, h: (r, 0)),
            pl.BlockSpec((pl.Squeezed(), 1, length), lambda r, h: (r, 0, 0)),
        ],
        out_specs=(block,) * 4
        + (pl.BlockSpec((pl.Squeezed(), 128 // HD, stored, BLOCK), lambda r, h: (r, h, 0, 0)),),
        scratch_shapes=[pltpu.VMEM((stored, BLOCK), f32)],
        compiler_params=pltpu.CompilerParams(vmem_limit_bytes=VMEM_LIMIT),
        cost_estimate=pl.CostEstimate(
            flops=16 * tokens * 768 * local, bytes_accessed=24 << 20, transcendentals=0
        ),
        name="attend",
    )(q, k, v, qkv_bias, *tables, segments.reshape(tokens, 1), segments.reshape(rows, 1, length))


def attend_back_kernel(
    q_ref, k_ref, v_ref, g_ref, o_ref, p_ref, cos_ref, slo_ref, shi_ref,
    dq_ref, dk_ref, dv_ref, bias_ref, kacc_ref, vacc_ref,
):
    def write(which, at, value):
        (dq_ref, dk_ref, dv_ref)[which][at, :] = value

    sums = attend_back_pair(
        q_ref[...], k_ref[...], v_ref[...], g_ref[...], o_ref[...],
        lambda e, at: p_ref[e, at, :], (cos_ref, slo_ref, shi_ref), kacc_ref, vacc_ref, write)
    sums = jnp.concatenate(list(sums) + [jnp.zeros((5, 128), f32)], 0)

    @pl.when(pl.program_id(1) == 0)
    def _():
        bias_ref[...] = sums

    @pl.when(pl.program_id(1) > 0)
    def _():
        bias_ref[...] += sums


def attend_back(q, k, v, g, o, probs, tables, rows):
    tokens, local = q.shape
    length = tokens // rows
    pairs = local // 128
    stored = probs.shape[2]
    block = pl.BlockSpec((length, 128), lambda h, r: (r, h))
    table = pl.BlockSpec((length, 128), lambda h, r: (r, 0))
    shape = jax.ShapeDtypeStruct((tokens, local), bf16)
    return pl.pallas_call(
        attend_back_kernel,
        grid=(pairs, rows),
        out_shape=(shape,) * 3 + (jax.ShapeDtypeStruct((8, local), f32),),
        in_specs=[block] * 5
        + [pl.BlockSpec((pl.Squeezed(), 128 // HD, stored, BLOCK), lambda h, r: (r, h, 0, 0))]
        + [table] * 3,
        out_specs=(block,) * 3 + (pl.BlockSpec((8, 128), lambda h, r: (0, h)),),
        scratch_shapes=[pltpu.VMEM((length, 128), f32)] * 2,
        compiler_params=pltpu.CompilerParams(vmem_limit_bytes=VMEM_LIMIT),
        cost_estimate=pl.CostEstimate(
            flops=32 * tokens * 768 * local, bytes_accessed=24 << 20, transcendentals=0
        ),
        name="attend_back",
    )(q, k, v, g, o, probs, *tables)


def attend_pair(query, key, value, mask_ref, keep, write):
    length = query.shape[0]
    spans, _ = spans_of(length)
    for i, (low, high, at) in enumerate(spans):
        mine = slice(i * BLOCK, (i + 1) * BLOCK)
        total = jnp.zeros((BLOCK, 128), f32)
        for e in range(128 // HD):
            scores = dot_nt(only(key[low:high], e), query[mine]) + mask_ref[at : at + high - low, :].astype(f32)
            exponent = jnp.exp(scores - jnp.max(scores, 0, keepdims=True))
            inverse = 1.0 / jnp.sum(exponent, 0, keepdims=True)
            probs = (exponent * inverse).astype(bf16)
            keep(e, slice(at, at + high - low), probs)
            total = total + dot_tn(probs, only(value[low:high], e))
        write(mine, total.astype(bf16))


def fill_mask(mask_ref, segc_ref, segr_ref, length):
    for i, (low, high, at) in enumerate(spans_of(length)[0]):
        keys = lax.broadcasted_iota(jnp.int32, (high - low, BLOCK), 0) + low
        queries = lax.broadcasted_iota(jnp.int32, (high - low, BLOCK), 1) + i * BLOCK
        own = segr_ref[:, i * BLOCK : (i + 1) * BLOCK].astype(f32)
        same = segc_ref[low:high, 0:1].astype(f32) == own
        allowed = jnp.where((keys <= queries) & same, 0.0, -1e30)
        mask_ref[at : at + high - low, :] = allowed.astype(mask_ref.dtype)


def fill_tables(seg_ref, column_ref, cos_ref, slo_ref, shi_ref):
    length = seg_ref.shape[1]
    row = seg_ref[...].astype(f32)
    column_ref[...] = jnp.broadcast_to(row, (128, length)).T
    starts = [jnp.sum(jnp.where(row < number, 1.0, 0.0), 1, keepdims=True) for number in range(1, 4)]
    lane = lax.broadcasted_iota(jnp.int32, (1, 128), 1) % HD
    exponent = (2 * (lane % (ROT // 2))).astype(f32) / ROT
    frequency = 1.0 / jnp.exp(exponent * f32(9.210340371976184))

    @pl.loop(0, length, step=128)
    def _(r):
        at = pl.ds(pl.multiple_of(r, 128), 128)
        column = column_ref[at, :]
        start = jnp.zeros_like(column)
        for number in range(1, 4):
            start = jnp.where(column == number, starts[number - 1], start)
        index = (lax.broadcasted_iota(jnp.int32, (128, 128), 0) + r).astype(f32)
        angle = (index - start) * frequency
        cosine, sine = jnp.cos(angle), jnp.sin(angle)
        cos_ref[at, :] = jnp.where(lane < ROT, cosine, 1.0)
        slo_ref[at, :] = jnp.where(lane < ROT // 2, -sine, 0.0)
        shi_ref[at, :] = jnp.where((lane >= ROT // 2) & (lane < ROT), sine, 0.0)


def attend_back_pair(query, key, value, grad, result, probs_of, tables, kacc_ref, vacc_ref, write):
    length = query.shape[0]
    spans, _ = spans_of(length)
    heads = 128 // HD
    inner = grad.astype(f32) * result.astype(f32)
    lane = lax.broadcasted_iota(jnp.int32, (8, 128), 1)
    row = lax.broadcasted_iota(jnp.int32, (8, 128), 0)
    pick = jnp.where(lax.div(lane, HD) == row, 1.0, 0.0)
    delta = lax.dot_general(
        pick, inner, (((1,), (1,)), ((), ())),
        precision=lax.Precision.HIGHEST, preferred_element_type=f32)
    kacc_ref[...] = jnp.zeros_like(kacc_ref)
    vacc_ref[...] = jnp.zeros_like(vacc_ref)
    cos_ref, slo_ref, shi_ref = tables
    first = jnp.zeros((1, 128), f32)
    for i, (low, high, at) in enumerate(spans):
        mine = slice(i * BLOCK, (i + 1) * BLOCK)
        g_i, q_i = grad[mine], query[mine]
        dq = jnp.zeros((BLOCK, 128), f32)
        ps, dss = [], []
        for e in range(heads):
            probs = probs_of(e, slice(at, at + high - low))
            dprobs = dot_nt(only(value[low:high], e), g_i)
            ds = (probs.astype(f32) * (dprobs - delta[e : e + 1, mine])).astype(bf16)
            dq = dq + dot_tn(ds, only(key[low:high], e))
            ps.append(probs)
            dss.append(ds)
        g_cat = jnp.concatenate([only(g_i, e) for e in range(heads)], 0)
        q_cat = jnp.concatenate([only(q_i, e) for e in range(heads)], 0)
        vacc_ref[low:high, :] += dot_nn(jnp.concatenate(ps, 1), g_cat)
        kacc_ref[low:high, :] += dot_nn(jnp.concatenate(dss, 1), q_cat)
        dq = dq * f32(HD**-0.5)
        dq = turn(dq, cos_ref[mine, :], -slo_ref[mine, :], -shi_ref[mine, :]).astype(bf16)
        write(0, mine, dq)
        first = first + jnp.sum(dq.astype(f32), 0, keepdims=True)
    everything = slice(0, length)
    dk = turn(kacc_ref[...], cos_ref[...], -slo_ref[...], -shi_ref[...]).astype(bf16)
    dv = vacc_ref[...].astype(bf16)
    write(1, everything, dk)
    write(2, everything, dv)
    return first, jnp.sum(dk.astype(f32), 0, keepdims=True), jnp.sum(dv.astype(f32), 0, keepdims=True)


def block_call(dp, tensor, arrays):
    hidden, cotangent, w_qkv, w_dense, w_fc1, w_fc2 = arrays[:6]
    rows, width = hidden.shape
    local = w_qkv.shape[2]
    wide = 3 * local
    units = w_fc1.shape[1]
    part = width // dp
    chips = dp // 2
    tokens = rows * tensor
    pairs = local // 128
    stored = spans_of(tokens)[1]
    sems = Sems()
    orders = orders_of(dp)
    vec_ids = [sems.take() for _ in range(dp - 1)]
    plan_qkv, plan_dense, plan_fc1, plan_fc2 = (CubeGather(sems, orders) for _ in range(4))
    plan_n, plan_c = LineGather(sems, tensor, 2), LineGather(sems, tensor, 2)
    line_out, line_in = LineReduce(sems, tensor), LineReduce(sems, tensor)
    reduce_fc2, reduce_dense, reduce_fc1, reduce_qkv = (ChipReduce(sems) for _ in range(4))
    swaps = [sems.take() for _ in range(2 * chips + 4)]
    tells = [sems.take() for _ in range(2 * (dp - 1) + tensor - 1)]

    def kernel(
        x_ref, c_ref, wq_ref, wd_ref, w1_ref, w2_ref, gain_ref, beta_ref, bd_ref, b2_ref,
        qb_ref, fb_ref, seg_ref,
        out_ref, hid_ref, s2_out, sd_out, s1_out, sq_out,
        gq_ref, g1_ref, g2_ref, x_out, n_out, nx_out, ax_out, gqx_out, gpx_out,
        land_out, land_in, land_2, land_d, land_1, land_q, vout_ref, bout_ref,
        x_buf, vec_buf, nv, wa, wb, wd, act, slope, qkv3, abuf, pb, mask, cbuf, xbuf,
        kacc, vacc, cos_ref, slo_ref, shi_ref, line_stage, chip_stage,
        fsum, bsum, parts, tell_v, tell_b, tell_z, vec_ref,
        send_sem, recv_sem, local_sem, stage_sem,
    ):
        me, line = lax.axis_index("dp"), lax.axis_index("tensor")
        twin = flip(me, 0)
        half = part // 2
        local_count = [0]
        attn = abuf.at[:, pl.ds(0, local)]

        def cols(a):
            return pl.ds(pl.multiple_of(a * part, part), part)

        def half_rows(a, h):
            return pl.ds(pl.multiple_of(a * part + h * half, half), half)

        def tok(b, u):
            return pl.ds(pl.multiple_of(b * rows + u * (rows // 2), rows // 2), rows // 2)

        def block(b):
            return pl.ds(pl.multiple_of(b * rows, rows), rows)

        def piece(n, h):
            return pl.ds(h * (n // 2), n // 2)

        def copy_of(a, b):
            local_count[0] += 1
            return pltpu.make_async_copy(a, b, local_sem.at[local_count[0] - 1])

        def remote(k, source, target, device):
            return pltpu.make_async_remote_copy(
                src_ref=source, dst_ref=target,
                send_sem=send_sem.at[k], recv_sem=recv_sem.at[k],
                device_id=device, device_id_type=MESH)

        def to_twin(k, source, target):
            return remote(swaps[k], source, target, (twin, line))

        pair = (send_sem, recv_sem)
        vec = [
            remote(k, vec_ref, vec_buf.at[:, cols(me)], (relative(me, r), line))
            for r, k in enumerate(vec_ids, 1)
        ]
        qkv = plan_qkv.bind(
            me, line,
            lambda h: wq_ref.at[:, pl.ds(h * half, half), :],
            lambda a, h: gq_ref.at[:, half_rows(a, h), :], *pair)
        fc1 = plan_fc1.bind(
            me, line,
            lambda h: w1_ref.at[pl.ds(h * half, half), :],
            lambda a, h: g1_ref.at[half_rows(a, h), :], *pair)
        dense = plan_dense.bind(
            me, line,
            lambda h: wd_ref.at[piece(local, h), :],
            lambda a, h: wd.at[piece(local, h), cols(a)], *pair)
        fc2 = plan_fc2.bind(
            me, line,
            lambda h: w2_ref.at[piece(units, h), :],
            lambda a, h: g2_ref.at[piece(units, h), cols(a)], *pair)
        norm = plan_n.bind(
            line, me, lambda u: x_ref.at[piece(rows, u)], lambda b, u: pb.at[tok(b, u)], *pair)
        cot = plan_c.bind(
            line, me, lambda u: c_ref.at[piece(rows, u)], lambda b, u: cbuf.at[tok(b, u)], *pair)
        staged = (stage_sem, *pair)

        def lasts(way):
            return wd.at[pl.ds(way * rows, rows), :]

        outs = line_out.bind(
            line, me, lambda d: nv.at[pl.ds(d * rows, rows), :], land_out, line_stage, lasts, *staged)
        ins = line_in.bind(
            line, me, lambda d: act.at[pl.ds(d * rows, rows), :], land_in, line_stage, lasts, *staged)
        low, high = pl.ds(0, tokens), pl.ds(tokens, tokens)
        sum_2 = reduce_fc2.bind(
            me, line,
            lambda r, h: wa.at[pl.ds(tokens + r * part, part), piece(units, h)],
            land_2, chip_stage, *staged)
        sum_d = reduce_dense.bind(
            me, line,
            lambda r, h: mask.at[pl.ds((2 * r + h) * part, part), :],
            land_d, chip_stage, *staged)
        sum_1 = reduce_fc1.bind(
            me, line,
            lambda r, h: wb.at[pl.ds(r * part, part), piece(units, h)],
            land_1, chip_stage, *staged)
        sum_q = reduce_qkv.bind(
            me, line,
            lambda r, h: abuf.at[pl.ds(r * part, part), piece(wide, h)],
            land_q, chip_stage, *staged)
        stages = dp.bit_length() - 1

        takes = [
            copy_of(x_ref, x_buf),
            copy_of(wd_ref, wd.at[:, cols(me)]),
            copy_of(c_ref, cbuf.at[block(line), :]),
            copy_of(wq_ref, qkv3.at[:, pl.ds(0, part), :]),
            copy_of(w1_ref, act.at[pl.ds(0, part), :]),
            copy_of(w2_ref, wb.at[:, pl.ds(0, part)]),
            copy_of(x_ref, pb.at[block(line), :]),
        ]
        keeps = [
            copy_of(qkv3.at[:, pl.ds(0, part), :], gq_ref.at[:, cols(me), :]),
            copy_of(act.at[pl.ds(0, part), :], g1_ref.at[cols(me), :]),
            copy_of(wb.at[:, pl.ds(0, part)], g2_ref.at[:, cols(me)]),
        ]
        takes[0].start()
        for k, ref in enumerate((gain_ref, beta_ref, bd_ref)):
            vec_ref[k : k + 1, :] = ref[...].astype(f32).reshape(1, part)
        vec_ref[2:3, :] += b2_ref[...].astype(f32).reshape(1, part)
        vec_buf[:, cols(me)] = vec_ref[...]
        parts[0:1, :] = fb_ref[...].astype(f32).reshape(1, units)
        greet(
            dp, me, tensor, line,
            lambda: fill_tables(seg_ref, kacc, cos_ref, slo_ref, shi_ref))
        for copy in vec:
            copy.start()
        norm.start(0)
        norm.start(1)
        qkv.start()
        for copy in takes[1:]:
            copy.start()
        takes[0].wait()
        for copy in vec:
            copy.wait_recv()
        qkv.advance(0)
        fc1.start()
        for take, copy in zip(takes[3:6], keeps):
            take.wait()
            copy.start()
        fill_mask(mask, kacc, seg_ref, tokens)

        def project(b):
            at = block(b)

            @pl.loop(0, rows, step=32)
            def _(r):
                some = pl.ds(pl.multiple_of(b * rows + r, 32), 32)
                x = pb[some, :].astype(f32)
                centred = x - jnp.mean(x, -1, keepdims=True)
                spread = jnp.mean(centred * centred, -1, keepdims=True)
                unit = centred * lax.rsqrt(spread + layer_eps)
                nv[some, :] = (unit * vec_buf[0:1, :] + vec_buf[1:2, :]).astype(bf16)

            cosine, slo, shi = cos_ref[at, :], slo_ref[at, :], shi_ref[at, :]
            for i in range(3):
                value = dot_nn(nv[at, :], wa[:, i * local : (i + 1) * local])
                value = value + qb_ref[i : i + 1, :].astype(f32)
                if i == 2:
                    qkv3[2, at, :] = value.astype(bf16)
                    continue
                for h in range(pairs):
                    lanes = slice(h * 128, (h + 1) * 128)
                    turned = turn(value[:, lanes], cosine, slo, shi).astype(bf16)
                    if i == 0:
                        turned = turned * bf16(HD**-0.5)
                    qkv3[i, at, lanes] = turned

        def hidden_layer(b, first):
            at = block(b)

            @pl.loop(0, units, step=512)
            def _(n):
                @pl.when(first & (n == units // 2))
                def _():
                    load_1[1].wait()

                to = pl.ds(pl.multiple_of(n, 512), 512)
                pre = dot_nn(nv[at, :], wb[:, to]) + parts[0:1, to]
                square = pre * pre
                bend = jnp.tanh(0.7978845608028654 * pre * (1.0 + 0.044715 * square))
                act[at, to] = (0.5 * pre * (1.0 + bend)).astype(bf16)
                rise = 0.7978845608028654 * (1.0 + 3 * 0.044715 * square)
                slope[at, to] = (
                    0.5 * (1.0 + bend) + 0.5 * pre * (1.0 - bend * bend) * rise
                ).astype(bf16)

        def slope_layer(b):
            at = block(b)
            abuf[at, pl.ds(local, local)] = dot_nt(cbuf[at, :], wd[...]).astype(bf16)

            @pl.loop(0, units, step=1024)
            def _(n):
                to = pl.ds(pl.multiple_of(n, 1024), 1024)
                value = dot_nt(cbuf[at, :], wa[to, :]) * slope[at, to].astype(f32)
                value = value.astype(bf16)
                slope[at, to] = value
                fsum[0:1, to] += jnp.sum(value.astype(f32), 0, keepdims=True)

        def blocks_of(s, task):
            @pl.loop(0, 2)
            def _(way):
                b = line + (2 * way - 1) * (1 + s)

                @pl.when((b >= 0) & (b < tensor) & ((s >= 0) | (way == 0)))
                def _():
                    task(b)

        norm.advance(0, 0)
        norm.advance(0, 1)
        for j in range(1, stages):
            qkv.advance(j)
        keeps[0].wait()
        load_q = [
            copy_of(gq_ref.at[i], wa.at[:, pl.ds(i * local, local)]) for i in range(3)
        ]
        for copy in load_q:
            copy.start()
        fc1.advance(0)
        dense.start()
        fc2.start()
        for copy in load_q + [takes[6]]:
            copy.wait()
        for s in range(1, tensor - 2):
            norm.advance(s, 0)
            norm.advance(s, 1)
        cot.start(0)
        cot.start(1)

        @pl.loop(-1, tensor - 2)
        def _(s):
            blocks_of(s, project)

        for j in range(1, stages):
            fc1.advance(j)
        for copy in keeps[1:]:
            copy.wait()
        load_1 = [copy_of(g1_ref.at[:, piece(units, h)], wb.at[:, piece(units, h)]) for h in (0, 1)]
        load_1[0].start()
        load_1[0].wait()
        load_1[1].start()

        x_store = copy_of(pb.at[low, :], x_out)

        @pl.loop(-1, tensor - 1)
        def _(s):
            @pl.when(s == tensor - 2)
            def _():
                norm.advance(tensor - 2, 0)
                norm.advance(tensor - 2, 1)
                x_store.start()
                fc2.advance(0)
                blocks_of(tensor - 2, project)

            @pl.when(s == 0)
            def _():
                dense.advance(0)

            blocks_of(s, lambda b: hidden_layer(b, s == -1))

        n_store = copy_of(nv, n_out)
        n_store.start()
        cross_n = [
            to_twin(r, nv.at[:, cols(relative(twin, r << 1))], nx_out.at[r]) for r in range(chips)
        ]
        cross_a = to_twin(chips, act, ax_out)
        for copy in cross_n + [cross_a]:
            copy.start()
        norm.finish()
        x_store.wait()

        def prob_lanes(h, e):
            return pl.ds(pl.multiple_of((2 * h + e) * BLOCK, BLOCK), BLOCK)

        @pl.loop(0, pairs)
        def _(h):
            lanes = pl.ds(pl.multiple_of(h * 128, 128), 128)

            def keep(e, at, value):
                pb[at, prob_lanes(h, e)] = value

            def write(at, value):
                abuf[at, lanes] = value

            attend_pair(
                qkv3[0, :, lanes], qkv3[1, :, lanes], qkv3[2, :, lanes], mask, keep, write)

            @pl.when(h == 0)
            def _():
                cot.advance(0, 0)
                cot.advance(0, 1)

            @pl.when(h == 1)
            def _():
                for j in range(1, stages - 1):
                    dense.advance(j)

            @pl.when(h == 2)
            def _():
                for j in range(1, stages - 1):
                    fc2.advance(j)

        cross_t = to_twin(chips + 1, attn, xbuf.at[:, pl.ds(chips * part, local)])
        cross_t.start()
        dense.advance(stages - 1)
        fc2.advance(stages - 1)
        takes[1].wait()
        takes[2].wait()
        load_2 = [copy_of(g2_ref.at[:, piece(width, h)], wa.at[:, piece(width, h)]) for h in (0, 1)]
        load_2[0].start()
        cot.advance(1, 0)
        n_store.wait()
        for copy in cross_n:
            copy.wait_send()
        load_2[0].wait()
        load_2[1].start()
        upper = lax.div(line, tensor // 2)

        def outward(i):
            return (1 - upper) * (tensor - 1 - i) + upper * i

        @pl.loop(0, tensor)
        def _(i):
            at = block(outward(i))

            @pl.loop(0, width, step=1024)
            def _(n):
                @pl.when((i == 0) & (n > 0))
                def _():
                    load_2[1].wait()

                to = pl.ds(pl.multiple_of(n, 1024), 1024)
                value = dot_nn(act[at, :], wa[:, to]) + dot_nn(attn[at, :], wd[:, to])
                nv[at, to] = value.astype(bf16)

            for k in range(tensor - 1):

                @pl.when(i == k)
                def _():
                    outs.start(0, k)
                    outs.start(1, k)

            @pl.when(i == tensor - 2)
            def _():
                cot.advance(1, 1)

        cross_a.wait_recv()
        load_ax = copy_of(ax_out, wb.at[low, :])
        load_ax.start()
        fsum[...] = jnp.zeros_like(fsum)
        cross_c = [
            to_twin(chips + 2 + r, cbuf.at[:, cols(relative(twin, r << 1))],
                    xbuf.at[:, pl.ds(r * part, part)])
            for r in range(chips)
        ]

        @pl.loop(-1, tensor - 1)
        def _(s):
            @pl.when(s == tensor - 2)
            def _():
                cot.advance(tensor - 2, 0)
                outs.advance(1)
                cot.advance(tensor - 2, 1)
                for copy in cross_c:
                    copy.start()

            blocks_of(s, slope_layer)

        cross_p = to_twin(2 * chips + 3, slope, gpx_out)
        cross_p.start()
        for copy in cross_c + [cross_t]:
            copy.wait_recv()
        load_ax.wait()
        dense.finish()

        def weight_grad(left, plan, own, crossed, spot, size, step, hook=None, second=None):
            @pl.loop(0, chips)
            def _(i):
                r = chips - 1 - i
                slot = chip_slot(me, r)
                across = pl.ds(pl.multiple_of(r * part, part), part)

                @pl.loop(0, size, step=step)
                def _(n):
                    if second is not None:

                        @pl.when((i == 0) & (n == step))
                        def _():
                            second.wait()

                    at = pl.multiple_of(n, step)
                    value = dot_tn(left(cols(slot)), own(at)) + dot_tn(xbuf[:, across], crossed(at))
                    spot(r, at, value.astype(bf16))

                for k in range(1, chips):

                    @pl.when(r == k)
                    def _():
                        plan.start(k)

                if hook is not None:
                    hook(i)

        def spot_a(r, at, value):
            wa[pl.ds(pl.multiple_of(tokens + r * part, part), part), pl.ds(at, 1024)] = value

        def spot_d(r, at, value):
            for h in (0, 1):
                to = pl.ds(pl.multiple_of((2 * r + h) * part, part), part)
                mask[to, :] = value[:, h * (local // 2) : (h + 1) * (local // 2)]

        def spot_1(r, at, value):
            wb[pl.ds(pl.multiple_of(r * part, part), part), pl.ds(at, 1024)] = value

        def spot_q(r, at, value):
            abuf[pl.ds(pl.multiple_of(r * part, part), part), pl.ds(at, local)] = value

        weight_grad(
            lambda a: cbuf[:, a], sum_2, lambda at: act[:, pl.ds(at, 1024)],
            lambda at: wb[low, pl.ds(at, 1024)], spot_a, units, 1024)
        weight_grad(
            lambda a: cbuf[:, a], sum_d, lambda at: attn[...],
            lambda at: xbuf[:, pl.ds(chips * part, local)], spot_d, local, local)
        load_n = copy_of(n_out, wa.at[low, :])
        load_n.start()
        load_g1 = copy_of(g1_ref.at[low, :], wb.at[low, :])
        load_g1.start()
        for copy in cross_n:
            copy.wait_recv()
        load_nx = [copy_of(nx_out.at[r], xbuf.at[:, pl.ds(r * part, part)]) for r in range(chips)]
        for copy in load_nx:
            copy.start()
        cot.finish()
        for copy in cross_c + [cross_a]:
            copy.wait_send()
        bsum[...] = jnp.zeros_like(bsum)
        for k in range(units // local):
            bsum[k : k + 1, :] = fsum[0:1, k * local : (k + 1) * local]
        load_w = [copy_of(gq_ref.at[i], pb.at[pl.ds(0, width), pl.ds(i * local, local)]) for i in range(3)]

        @pl.loop(0, pairs)
        def _(h):
            lanes = pl.ds(pl.multiple_of(h * 128, 128), 128)

            def write(which, at, value):
                cbuf[at, pl.ds(pl.multiple_of(which * local + h * 128, 128), 128)] = value

            sums = attend_back_pair(
                qkv3[0, :, lanes], qkv3[1, :, lanes], qkv3[2, :, lanes],
                abuf[:, pl.ds(pl.multiple_of(local + h * 128, 128), 128)], abuf[:, lanes],
                lambda e, at: pb[at, prob_lanes(h, e)],
                (cos_ref, slo_ref, shi_ref), kacc, vacc, write)
            for k in range(3):
                bsum[units // local + k : units // local + k + 1, lanes] = sums[k]

            for k in range(3):

                @pl.when(h == k)
                def _():
                    load_w[k].start()

            @pl.when(h == 0)
            def _():
                sum_2.middle()

            @pl.when(h == 1)
            def _():
                outs.advance(2)

        back = cbuf.at[:, pl.ds(0, wide)]
        cross_d = to_twin(2 * chips + 2, back, gqx_out)
        cross_d.start()
        bias_tells = [
            remote(tells[r - 1], bsum, tell_b.at[r], (relative(me, r), line)) for r in range(1, dp)
        ]
        for copy in bias_tells:
            copy.start()
        for copy in load_w + [load_g1]:
            copy.wait()
        load_gx = [copy_of(gqx_out.at[:, pl.ds(i * local, local)], qkv3.at[i]) for i in range(3)]
        store_o = copy_of(x_buf, out_ref)
        load_px = [copy_of(gpx_out.at[:, piece(units, h)], cbuf.at[:, piece(units, h)]) for h in (0, 1)]
        spare = pb.at[pl.ds(width, rows), :]
        load_c = copy_of(c_ref, spare)

        def dense_step(i):
            @pl.when(i == chips - 2)
            def _():
                sum_d.middle()

        @pl.loop(0, tensor)
        def _(i):
            at = block(outward(i))

            @pl.loop(0, width, step=1024)
            def _(n):
                to = pl.ds(pl.multiple_of(n, 1024), 1024)
                value = dot_nt(slope[at, :], wb[to, :])
                value = value + dot_nt(cbuf[at, pl.ds(0, wide)], pb[to, pl.ds(0, wide)])
                act[at, to] = value.astype(bf16)

            for k in range(tensor - 1):

                @pl.when(i == k)
                def _():
                    ins.start(0, k)
                    ins.start(1, k)

            @pl.when(i == 0)
            def _():
                load_c.start()

            @pl.when(i == 1)
            def _():
                cross_d.wait_recv()
                for copy in load_gx:
                    copy.start()
                load_n.wait()
                for copy in load_nx + load_gx:
                    copy.wait()
                cross_t.wait_send()
                weight_grad(
                    lambda a: wa[low, a], sum_q, lambda at: cbuf[:, pl.ds(at, local)],
                    lambda at: qkv3[lax.div(at, local)], spot_q, wide, local, dense_step)

        cross_d.wait_send()
        cross_p.wait_recv()
        load_px[0].start()
        outs.settle()
        ins.advance(1)
        load_xa = copy_of(x_out, wb.at[high, :])
        load_px[0].wait()
        load_px[1].start()
        load_xa.start()

        def late_steps(i):
            @pl.when(i == 0)
            def _():
                sum_q.middle()

        weight_grad(
            lambda a: wa[low, a], sum_1, lambda at: slope[:, pl.ds(at, 1024)],
            lambda at: cbuf[:, pl.ds(at, 1024)], spot_1, units, 1024, late_steps, load_px[1])
        def finish_out():
            outs.arrive()

            @pl.loop(0, rows, step=32)
            def _(r):
                at = pl.ds(r, 32)
                own = pl.ds(pl.multiple_of(line * rows + r, 32), 32)
                total = x_buf[at, :].astype(f32) + outs.total(nv[own, :], at) + vec_buf[2:3, :]
                x_buf[at, :] = total.astype(bf16)

            store_o.start()

        parts[...] = jnp.zeros_like(parts)
        load_xa.wait()
        load_c.wait()

        def norm_sums(b):
            @pl.loop(0, rows, step=32)
            def _(r):
                some = pl.ds(pl.multiple_of(b * rows + r, 32), 32)
                x = wb[pl.ds(pl.multiple_of(tokens + b * rows + r, 32), 32), :].astype(f32)
                grad = act[some, :].astype(f32)
                centred = x - jnp.mean(x, -1, keepdims=True)
                inv_std = lax.rsqrt(jnp.mean(centred * centred, -1, keepdims=True) + layer_eps)
                parts[0:1, :] += jnp.sum(grad * (centred * inv_std), 0, keepdims=True)
                parts[1:2, :] += jnp.sum(grad, 0, keepdims=True)

        @pl.loop(0, tensor)
        def _(b):
            @pl.when(b == tensor - 1)
            def _():
                finish_out()
                ins.advance(2)

            norm_sums(b)

        @pl.loop(0, rows, step=32)
        def _(r):
            cotan = pb[pl.ds(pl.multiple_of(width + r, 32), 32), :].astype(f32)
            parts[2:3, :] += jnp.sum(cotan, 0, keepdims=True)

        vec_tells = [
            remote(tells[dp - 2 + r], parts.at[:, cols(relative(me, r))], tell_v.at[r],
                   (relative(me, r), line))
            for r in range(1, dp)
        ]
        for copy in vec_tells:
            copy.start()
        sum_1.middle()
        sum_2.final()
        sum_d.final()
        store_2 = copy_of(wa.at[pl.ds(tokens, part), :], s2_out)
        store_dense = [
            copy_of(mask.at[pl.ds(h * part, part), :], sd_out.at[:, piece(local, h)]) for h in (0, 1)
        ]
        for copy in [store_2] + store_dense:
            copy.start()
        store_o.wait()
        load_x = copy_of(x_ref, x_buf)
        load_x.start()
        for copy in bias_tells:
            copy.wait_recv()
        total_b = bsum[...]
        for r in range(1, dp):
            total_b = total_b + tell_b[r]
        bout_ref[...] = total_b
        for copy in vec_tells:
            copy.wait_recv()
        total_v = parts[:, cols(me)]
        for r in range(1, dp):
            total_v = total_v + tell_v[r]
        tell_z[0] = total_v
        line_tells = [
            remote(tells[2 * dp - 3 + k], tell_z.at[0], tell_z.at[k], (me, lax.rem(line + k, tensor)))
            for k in range(1, tensor)
        ]
        for copy in line_tells:
            copy.start()
        sum_q.final()
        store_q = copy_of(abuf.at[pl.ds(0, part), :], sq_out)
        store_q.start()
        load_x.wait()
        sum_1.final()
        store_1 = copy_of(wb.at[pl.ds(0, part), :], s1_out)
        store_1.start()
        for copy in line_tells:
            copy.wait_recv()
        total_z = tell_z[0]
        for k in range(1, tensor):
            total_z = total_z + tell_z[k]
        vout_ref[...] = total_z
        ins.settle()
        ins.arrive()

        @pl.loop(0, rows, step=32)
        def _(r):
            at = pl.ds(r, 32)
            x = x_buf[at, :].astype(f32)
            centred = x - jnp.mean(x, -1, keepdims=True)
            inv_std = lax.rsqrt(jnp.mean(centred * centred, -1, keepdims=True) + layer_eps)
            unit = centred * inv_std
            own = pl.ds(pl.multiple_of(line * rows + r, 32), 32)
            scaled = ins.total(act[own, :], at) * vec_buf[0:1, :]
            cotan = pb[pl.ds(pl.multiple_of(width + r, 32), 32), :].astype(f32)
            first = jnp.mean(scaled, -1, keepdims=True)
            second = jnp.mean(scaled * unit, -1, keepdims=True)
            x_buf[at, :] = (cotan + inv_std * (scaled - first - unit * second)).astype(bf16)

        store_h = copy_of(x_buf, hid_ref)
        store_h.start()
        for copy in vec + [cross_p] + bias_tells + vec_tells + line_tells:
            copy.wait_send()
        for plan in (qkv, fc1, fc2, sum_2, sum_d, sum_1, sum_q):
            plan.finish()
        for copy in store_dense + [store_2, store_q, store_h, store_1]:
            copy.wait()

    def shape(*dims):
        return jax.ShapeDtypeStruct(dims, bf16)

    def vmem(*dims):
        return pltpu.VMEM(dims, bf16)

    landings = [
        shape(2 * tensor - 3, rows, width),
        shape(2 * tensor - 3, rows, width),
        shape(6, part, units // 2),
        shape(6, part, local // 2),
        shape(6, part, units // 2),
        shape(6, part, wide // 2),
    ]
    return pl.pallas_call(
        kernel,
        out_shape=(
            shape(rows, width),
            shape(rows, width),
            shape(part, units),
            shape(part, local),
            shape(part, units),
            shape(part, wide),
            shape(3, width, local),
            shape(width, units),
            shape(units, width),
            shape(tokens, width),
            shape(tokens, width),
            shape(chips, tokens, part),
            shape(tokens, units),
            shape(tokens, wide),
            shape(tokens, units),
            *landings,
            jax.ShapeDtypeStruct((8, part), f32),
            jax.ShapeDtypeStruct((8, local), f32),
        ),
        in_specs=[ANY] * 6 + [VMEM] * 7,
        out_specs=(ANY,) * 21 + (VMEM,) * 2,
        scratch_shapes=[
            vmem(rows, width),
            pltpu.VMEM((8, width), f32),
            vmem(tokens, width),
            vmem(width, width),
            vmem(width, units),
            vmem(local, width),
            vmem(tokens, units),
            vmem(tokens, units),
            vmem(3, tokens, local),
            vmem(tokens, wide),
            vmem(stored, local // HD * BLOCK),
            vmem(stored, BLOCK),
            vmem(tokens, width),
            vmem(tokens, chips * part + local),
        ]
        + [pltpu.VMEM((tokens, 128), f32)] * 5
        + [
            vmem(tensor - 1, rows, width),
            vmem(2, part, units // 2),
            pltpu.VMEM((8, units), f32),
            pltpu.VMEM((8, local), f32),
            pltpu.VMEM((8, width), f32),
            pltpu.VMEM((dp, 8, part), f32),
            pltpu.VMEM((dp, 8, local), f32),
            pltpu.VMEM((tensor, 8, part), f32),
            pltpu.VMEM((8, part), f32),
            pltpu.SemaphoreType.DMA((sems.count,)),
            pltpu.SemaphoreType.DMA((sems.count,)),
            pltpu.SemaphoreType.DMA((48,)),
            pltpu.SemaphoreType.DMA((2,)),
        ],
        compiler_params=pltpu.CompilerParams(
            collective_id=0, has_side_effects=True, vmem_limit_bytes=67_043_328
        ),
        name="block",
    )(*arrays)


def finish_kernel(
    s2_ref, sd_ref, s1_ref, sq_ref, o_ref, h_ref, v_ref, b_ref,
    w2_ref, wd_ref, w1_ref, wq_ref, out_ref, hid_ref, gain_ref, beta_ref, both_ref, same_ref, bq_ref, b1_ref,
):
    w2_ref[...] = s2_ref[...].T.astype(f32)
    wd_ref[...] = sd_ref[...].T.astype(f32)
    w1_ref[...] = s1_ref[...].astype(f32)
    local = wq_ref.shape[2]
    for i in range(3):
        wq_ref[i] = sq_ref[:, i * local : (i + 1) * local].astype(f32)
    out_ref[...] = o_ref[...]
    hid_ref[...] = h_ref[...]

    @pl.when(pl.program_id(0) == 0)
    def _():
        line = lax.axis_index("tensor")
        count = gain_ref.shape[0]
        mine = v_ref[:, :count]
        for k in range(1, v_ref.shape[1] // count):
            mine = jnp.where(line == k, v_ref[:, k * count : (k + 1) * count], mine)
        gain_ref[...] = mine[0]
        beta_ref[...] = mine[1]
        both_ref[...] = mine[2]
        same_ref[...] = mine[2]
        lines = b1_ref.shape[0] // b_ref.shape[1]
        bq_ref[...] = b_ref[lines : lines + 3, :]
        for k in range(lines):
            b1_ref[pl.ds(k * b_ref.shape[1], b_ref.shape[1])] = b_ref[k]


def finish(tensor, sent_fc2, sent_dense, sent_fc1, sent_qkv, out, hidden_grad, vec_sums, all_sums):
    part, units = sent_fc2.shape
    local = sent_dense.shape[1]
    rows, width = out.shape
    steps = 4
    quarter = vec_sums.shape[1] // tensor
    fixed = VMEM

    def down(n, m):
        return pl.BlockSpec((n // steps, m), lambda i: (i, 0))

    def across(n, m):
        return pl.BlockSpec((n, m // steps), lambda i: (0, i))

    return pl.pallas_call(
        finish_kernel,
        grid=(steps,),
        out_shape=(
            jax.ShapeDtypeStruct((units, part), f32),
            jax.ShapeDtypeStruct((local, part), f32),
            jax.ShapeDtypeStruct((part, units), f32),
            jax.ShapeDtypeStruct((3, part, local), f32),
            jax.ShapeDtypeStruct((rows, width), bf16),
            jax.ShapeDtypeStruct((rows, width), bf16),
            *[jax.ShapeDtypeStruct((quarter,), f32)] * 4,
            jax.ShapeDtypeStruct((3, local), f32),
            jax.ShapeDtypeStruct((units,), f32),
        ),
        in_specs=[
            across(part, units), across(part, local), down(part, units), down(part, 3 * local),
            down(rows, width), down(rows, width), fixed, fixed,
        ],
        out_specs=(
            down(units, part), down(local, part), down(part, units),
            pl.BlockSpec((3, part // steps, local), lambda i: (0, i, 0)),
            down(rows, width), down(rows, width), *[fixed] * 6,
        ),
        compiler_params=pltpu.CompilerParams(vmem_limit_bytes=VMEM_LIMIT),
        name="finish",
    )(sent_fc2, sent_dense, sent_fc1, sent_qkv, out, hidden_grad, vec_sums, all_sums)


def rotary_tables(segments):
    rows, length = segments.shape
    index = jnp.arange(length, dtype=jnp.int32)[None]
    start = jnp.zeros_like(segments)
    for number in range(1, 4):
        start = jnp.where(segments == number, jnp.sum(segments < number, -1, keepdims=True), start)
    position = (index - start).astype(f32).reshape(rows * length, 1)
    lane = jnp.arange(128, dtype=jnp.int32) % HD
    exponent = (2 * (lane % (ROT // 2))).astype(f32) / ROT
    angle = position * (1.0 / 10000.0**exponent)[None]
    cosine, sine = jnp.cos(angle), jnp.sin(angle)
    low, high = lane < ROT // 2, (lane >= ROT // 2) & (lane < ROT)
    return (
        jnp.where(lane < ROT, cosine, 1.0),
        jnp.where(low, -sine, 0.0),
        jnp.where(high, sine, 0.0),
    )


def matmul(a, b):
    return jnp.dot(a, b, preferred_element_type=f32)


def on_device(
    dp, tensor, fast,
    hidden_in, segments, ln_gain, ln_bias, qkv_weight, qkv_bias, dense_weight, dense_bias,
    fc1_weight, fc1_bias, fc2_weight, fc2_bias, cotangent,
):
    seqs = segments.shape[0]
    local = qkv_weight.shape[2]
    mine = (
        hidden_in, cotangent, qkv_weight.transpose(1, 0, 2), dense_weight, fc1_weight, fc2_weight,
    )
    if fast:
        (out, hidden_grad, sent_fc2, sent_dense, sent_fc1, sent_qkv, *_, vec_sums, all_sums) = block_call(
            dp, tensor, (*mine, ln_gain, ln_bias, dense_bias, fc2_bias, qkv_bias, fc1_bias, segments))
        (
            grad_w2, grad_wd, grad_w1, grad_wq, out, hidden_grad,
            gain_grad, beta_grad, bias_grad, same_grad, qkv_grad, fc1_grad,
        ) = finish(
            tensor, sent_fc2, sent_dense, sent_fc1, sent_qkv, out, hidden_grad, vec_sums, all_sums)
        return (
            out,
            hidden_grad,
            gain_grad,
            beta_grad,
            grad_wq.transpose(1, 0, 2),
            qkv_grad,
            grad_wd,
            bias_grad,
            grad_w1,
            fc1_grad,
            grad_w2,
            same_grad,
        )

    number = lax.broadcasted_iota(jnp.int32, (8, ln_gain.shape[0]), 0)
    vectors = jnp.where(number == 1, ln_bias.astype(f32)[None], ln_gain.astype(f32)[None])
    vectors = jnp.where(
        number == 2, dense_bias.astype(f32)[None] + fc2_bias.astype(f32)[None], vectors)
    tables = rotary_tables(segments)
    bias = jnp.pad(qkv_bias.astype(f32), ((0, 5), (0, 0)))
    w_qkv, w_dense, w_fc1, w_fc2, normed, grad_out, vec = gather_plain(*mine, vectors)
    gain, out_bias = vec[0:1], vec[2:3]
    query, key, value, attn_vec, probs = attend(
        *(matmul(normed, w_qkv[i]) for i in range(3)), bias, tables, segments, seqs
    )
    pre_act = matmul(normed, w_fc1) + fc1_bias.astype(f32)
    act_vals, gelu_pull = jax.vjp(lambda pre: jax.nn.gelu(pre, approximate=True), pre_act)
    act_vals = act_vals.astype(bf16)
    slope = gelu_pull(jnp.ones_like(pre_act))[0].astype(bf16)
    branches = matmul(attn_vec, w_dense) + matmul(act_vals, w_fc2)
    grad_attn = matmul(grad_out, w_dense.T).astype(bf16)
    *grads, qkv_sums = attend_back(query, key, value, grad_attn, attn_vec, probs, tables, seqs)
    resid_in = hidden_in.astype(f32)
    cot_float = cotangent.astype(f32)
    centred = resid_in - jnp.mean(resid_in, -1, keepdims=True)
    spread = jnp.mean(centred * centred, -1, keepdims=True)
    inv_std = lax.rsqrt(spread + layer_eps)
    unit_rows = centred * inv_std
    summed = lax.psum_scatter(branches.astype(bf16), "tensor", scatter_dimension=0, tiled=True)
    out = (resid_in + summed.astype(f32) + out_bias).astype(bf16)
    out_bias_part = jnp.sum(cot_float, 0)
    grad_fc2 = matmul(act_vals.T, grad_out)
    grad_dense = matmul(attn_vec.T, grad_out)
    grad_pre = (matmul(grad_out, w_fc2.T) * slope.astype(f32)).astype(bf16)
    fc1_bias_part = jnp.sum(grad_pre.astype(f32), 0)
    grad_fc1 = matmul(normed.T, grad_pre)
    grad_wqkv = jnp.stack([matmul(normed.T, g) for g in grads])
    grad_normed = matmul(grad_pre, w_fc1.T) + sum(matmul(g, w.T) for g, w in zip(grads, w_qkv))
    sent_qkv, sent_dense, sent_fc1, sent_fc2 = (
        lax.psum_scatter(grad_wqkv.astype(bf16), "dp", scatter_dimension=1, tiled=True),
        lax.psum_scatter(grad_dense.astype(bf16), "dp", scatter_dimension=1, tiled=True),
        lax.psum_scatter(grad_fc1.astype(bf16), "dp", scatter_dimension=0, tiled=True),
        lax.psum_scatter(grad_fc2.astype(bf16), "dp", scatter_dimension=1, tiled=True),
    )
    grad_local = lax.psum_scatter(
        grad_normed.astype(bf16), "tensor", scatter_dimension=0, tiled=True
    ).astype(f32)
    gain_part = jnp.sum(grad_local * unit_rows, 0)
    beta_part = jnp.sum(grad_local, 0)
    scaled_grad = grad_local * gain
    first_mean = jnp.mean(scaled_grad, -1, keepdims=True)
    second_mean = jnp.mean(scaled_grad * unit_rows, -1, keepdims=True)
    hidden_grad = (
        cot_float + inv_std * (scaled_grad - first_mean - unit_rows * second_mean)
    ).astype(bf16)
    gain_grad, beta_grad, out_bias_grad = (
        lax.psum_scatter(gain_part, ("dp", "tensor"), scatter_dimension=0, tiled=True),
        lax.psum_scatter(beta_part, ("dp", "tensor"), scatter_dimension=0, tiled=True),
        lax.psum_scatter(out_bias_part, ("dp", "tensor"), scatter_dimension=0, tiled=True),
    )
    qkv_bias_grad, fc1_bias_grad = lax.psum((qkv_sums[:3], fc1_bias_part), "dp")
    return (
        out,
        hidden_grad,
        gain_grad,
        beta_grad,
        sent_qkv.transpose(1, 0, 2).astype(f32),
        qkv_bias_grad,
        sent_dense.astype(f32),
        out_bias_grad,
        sent_fc1.astype(f32),
        fc1_bias_grad,
        sent_fc2.astype(f32),
        out_bias_grad,
    )


def solution(mesh):
    dp, tensor = mesh.shape["dp"], mesh.shape["tensor"]
    fast = dp == 8 and tensor == 4
    placed = (
        P(("dp", "tensor"), None),
        P("dp", None),
        P("dp"),
        P("dp"),
        P("dp", None, "tensor"),
        P(None, "tensor"),
        P("tensor", "dp"),
        P("dp"),
        P("dp", "tensor"),
        P("tensor"),
        P("tensor", "dp"),
        P("dp"),
        P(("dp", "tensor"), None),
    )
    return jax.shard_map(
        functools.partial(on_device, dp, tensor, fast),
        mesh=mesh,
        in_specs=placed,
        out_specs=(
            P(("dp", "tensor"), None),
            P(("dp", "tensor"), None),
            P(("dp", "tensor")),
            P(("dp", "tensor")),
            P("dp", None, "tensor"),
            P(None, "tensor"),
            P("tensor", "dp"),
            P(("dp", "tensor")),
            P("dp", "tensor"),
            P("tensor"),
            P("tensor", "dp"),
            P(("dp", "tensor")),
        ),
        check_vma=False,
    )
```

```python
import functools

import jax
import jax.numpy as jnp
from jax import lax
from jax.experimental import pallas as pl
from jax.experimental.pallas import tpu as pltpu
from jax.sharding import PartitionSpec as P

HD = 64
ROT = 32
BLOCK = 256
MAX_DOC = 512
VMEM_LIMIT = 66_000_000
MESH = pl.DeviceIdType.MESH
ANY = pl.BlockSpec(memory_space=pl.ANY)
VMEM = pl.BlockSpec(memory_space=pltpu.VMEM)

layer_eps = 1e-05
f32 = jnp.float32
bf16 = jnp.bfloat16


def dot_nn(a, b):
    return lax.dot_general(a, b, (((1,), (0,)), ((), ())), preferred_element_type=f32)


def dot_nt(a, b):
    return lax.dot_general(a, b, (((1,), (1,)), ((), ())), preferred_element_type=f32)


def dot_tn(a, b):
    return lax.dot_general(a, b, (((0,), (0,)), ((), ())), preferred_element_type=f32)


def flip(index, bit):
    step = 1 << bit
    return index + step * (1 - 2 * (lax.div(index, step) % 2))


def relative(index, offset):
    bit = 0
    while offset >> bit:
        if (offset >> bit) & 1:
            index = flip(index, bit)
        bit += 1
    return index


def stages_of(order):
    held, stages = [0], []
    for bit in order:
        got = [r ^ (1 << bit) for r in held]
        stages.append((bit, list(held), got))
        held = held + got
    return stages


class Sems:
    def __init__(self):
        self.count = 0

    def take(self):
        self.count += 1
        return self.count - 1


class CubeGather:
    def __init__(self, sems, orders):
        self.plans = [stages_of(order) for order in orders]
        self.ids = {
            (h, j, i): sems.take()
            for h, stages in enumerate(self.plans)
            for j, (_, held, _) in enumerate(stages)
            for i in range(len(held))
        }

    def bind(self, me, other, own, window, send_sem, recv_sem):
        self.me, self.other, self.own, self.window = me, other, own, window
        self.send_sem, self.recv_sem = send_sem, recv_sem
        return self

    def copy(self, h, j, i):
        bit, held, _ = self.plans[h][j]
        slot = relative(self.me, held[i])
        target = self.window(slot, h)
        source = self.own(h) if held[i] == 0 else target
        k = self.ids[h, j, i]
        return pltpu.make_async_remote_copy(
            src_ref=source,
            dst_ref=target,
            send_sem=self.send_sem.at[k],
            recv_sem=self.recv_sem.at[k],
            device_id=(flip(self.me, bit), self.other),
            device_id_type=MESH,
        )

    def start(self):
        depth = len(self.plans[0])
        for j in range(depth):
            for h in range(len(self.plans)):
                self.copy(h, j, 0).start()

    def advance(self, j):
        for i in range(len(self.plans[0][j][1])):
            for h, stages in enumerate(self.plans):
                self.copy(h, j, i).wait_recv()
                slot = stages[j][2][i]
                for later in range(j + 1, len(stages)):
                    self.copy(h, later, stages[later][1].index(slot)).start()

    def finish(self):
        for h, j, i in self.ids:
            self.copy(h, j, i).wait_send()


class LineGather:
    def __init__(self, sems, size, subs):
        self.size, self.subs = size, subs
        self.ids = {
            (way, s, u): sems.take()
            for way in (0, 1)
            for s in range(size - 1)
            for u in range(subs)
        }

    def bind(self, me, other, own, window, send_sem, recv_sem):
        self.me, self.other, self.own, self.window = me, other, own, window
        self.send_sem, self.recv_sem = send_sem, recv_sem
        return self

    def copy(self, way, s, u):
        block = self.me - s if way == 0 else self.me + s
        target = self.window(block, u)
        k = self.ids[way, s, u]
        return pltpu.make_async_remote_copy(
            src_ref=self.own(u) if s == 0 else target,
            dst_ref=target,
            send_sem=self.send_sem.at[k],
            recv_sem=self.recv_sem.at[k],
            device_id=(self.other, self.me + 1 if way == 0 else self.me - 1),
            device_id_type=MESH,
        )

    def sends(self, way, s):
        if way == 0:
            return (self.me >= s) & (self.me < self.size - 1)
        return (self.me + s < self.size) & (self.me > 0)

    def gets(self, way, s):
        if way == 0:
            return self.me - 1 - s >= 0
        return self.me + 1 + s < self.size

    def start(self, u):
        for way in (0, 1):

            @pl.when(self.sends(way, 0))
            def _():
                self.copy(way, 0, u).start()

    def advance(self, s, u):
        for way in (0, 1):

            @pl.when(self.gets(way, s))
            def _():
                self.copy(way, s, u).wait_recv()

            if s + 1 < self.size - 1:

                @pl.when(self.sends(way, s + 1))
                def _():
                    self.copy(way, s + 1, u).start()

    def finish(self):
        for way, s, u in self.ids:

            @pl.when(self.sends(way, s))
            def _():
                self.copy(way, s, u).wait_send()


def greet(dp, me, tensor, line, meanwhile):
    barrier = pltpu.get_barrier_semaphore()
    for r in range(1, dp):
        pl.semaphore_signal(barrier, inc=1, device_id=(relative(me, r), line), device_id_type=MESH)
    for k in range(1, tensor):
        to = (me, lax.rem(line + k, tensor))
        pl.semaphore_signal(barrier, inc=1, device_id=to, device_id_type=MESH)
    meanwhile()
    pl.semaphore_wait(barrier, dp + tensor - 2)


def orders_of(dp):
    bits = list(range(1, dp.bit_length() - 1))
    return [bits + [0], bits[::-1] + [0]]


def normalize(x, gain, bias):
    centred = x - jnp.mean(x, -1, keepdims=True)
    spread = jnp.mean(centred * centred, -1, keepdims=True)
    unit = centred * lax.rsqrt(spread + layer_eps)
    return (unit * gain + bias).astype(bf16)


def gather_plain(hidden, cotangent, w_qkv, w_dense, w_fc1, w_fc2, vectors):
    vec = lax.all_gather(vectors, "dp", axis=1, tiled=True)
    normed = normalize(hidden.astype(f32), vec[0:1], vec[1:2])
    return (
        lax.all_gather(w_qkv, "dp", axis=1, tiled=True),
        lax.all_gather(w_dense, "dp", axis=1, tiled=True),
        lax.all_gather(w_fc1, "dp", axis=0, tiled=True),
        lax.all_gather(w_fc2, "dp", axis=1, tiled=True),
        lax.all_gather(normed, "tensor", axis=0, tiled=True),
        lax.all_gather(cotangent, "tensor", axis=0, tiled=True),
        vec,
    )


class ChipReduce:
    COUNT = 6

    def __init__(self, sems):
        self.ids = [sems.take() for _ in range(self.COUNT)]

    def bind(self, me, other, view, landing, stage, stage_sem, send_sem, recv_sem):
        self.me, self.other, self.view, self.landing = me, other, view, landing
        self.stage, self.stage_sem = stage, stage_sem
        self.send_sem, self.recv_sem = send_sem, recv_sem
        return self

    def copy(self, slot):
        r, h, bit = [(2, 0, 2), (3, 0, 2), (1, 0, 1), (1, 1, 1), (3, 1, 1), (2, 1, 2)][slot]
        k = self.ids[slot]
        return pltpu.make_async_remote_copy(
            src_ref=self.view(r, h),
            dst_ref=self.landing.at[slot],
            send_sem=self.send_sem.at[k],
            recv_sem=self.recv_sem.at[k],
            device_id=(flip(self.me, bit), self.other),
            device_id_type=MESH,
        )

    def start(self, r):
        for slot in {3: (1, 4), 2: (0,), 1: (3,), 0: ()}[r]:
            self.copy(slot).start()

    def fetch(self, slots):
        half = self.landing.shape[-1]
        held = [self.stage.at[k, :, pl.ds(0, half)] for k in range(len(slots))]
        copies = []
        for k, slot in enumerate(slots):
            self.copy(slot).wait_recv()
            copies.append(
                pltpu.make_async_copy(self.landing.at[slot], held[k], self.stage_sem.at[k]))
            copies[k].start()
        for copy in copies:
            copy.wait()
        return held

    def middle(self):
        held = self.fetch((1, 4))
        for k, (r, h, last) in enumerate(((1, 0, 2), (2, 1, 5))):
            view = self.view(r, h)
            view[...] = (view[...].astype(f32) + held[k][...].astype(f32)).astype(bf16)
            self.copy(last).start()

    def final(self):
        for h, slots in ((0, (0, 2)), (1, (3, 5))):
            a, b = self.fetch(slots)
            view = self.view(0, h)
            total = view[...].astype(f32) + a[...].astype(f32) + b[...].astype(f32)
            view[...] = total.astype(bf16)

    def finish(self):
        for slot in range(self.COUNT):
            self.copy(slot).wait_send()


class LineReduce:
    def __init__(self, sems, size):
        self.size = size
        self.ids = {(way, i): sems.take() for way in (0, 1) for i in range(size - 1)}

    def bind(self, me, other, own, landing, stage, last, stage_sem, send_sem, recv_sem):
        self.me, self.other, self.own, self.landing = me, other, own, landing
        self.stage, self.last, self.stage_sem = stage, last, stage_sem
        self.send_sem, self.recv_sem = send_sem, recv_sem
        return self

    def target(self, way, i):
        return self.size - 1 - i if way == 0 else i

    def place(self, way, i):
        return i if way == 0 else 2 * self.size - 4 - i

    def buffer(self, way, i):
        return self.stage.at[i if way == 0 else self.size - 2 - i]

    def copy(self, way, i, edge):
        k = self.ids[way, i]
        return pltpu.make_async_remote_copy(
            src_ref=self.own(self.target(way, i)) if edge else self.buffer(way, i),
            dst_ref=self.landing.at[self.place(way, i)],
            send_sem=self.send_sem.at[k],
            recv_sem=self.recv_sem.at[k],
            device_id=(self.other, self.me + 1 if way == 0 else self.me - 1),
            device_id_type=MESH,
        )

    def edge(self, way):
        return self.me == (0 if way == 0 else self.size - 1)

    def passes(self, way, i):
        d = self.target(way, i)
        return (self.me > 0) & (self.me < d) if way == 0 else (self.me < self.size - 1) & (self.me > d)

    def start(self, way, i):
        @pl.when(self.edge(way))
        def _():
            self.copy(way, i, True).start()

    def advance(self, step):
        for way in (0, 1):
            steps_from_edge = self.me if way == 0 else self.size - 1 - self.me
            for i in range(step):

                @pl.when(self.passes(way, i) & (steps_from_edge == step - i))
                def _():
                    self.copy(way, i, False).wait_recv()
                    held = self.buffer(way, i)
                    fetch = pltpu.make_async_copy(
                        self.landing.at[self.place(way, i)], held, self.stage_sem.at[0])
                    fetch.start()
                    fetch.wait()
                    add_into(held, self.own(self.target(way, i)))
                    self.copy(way, i, False).start()

    def settle(self):
        for way, i in self.ids:

            @pl.when(self.edge(way))
            def _():
                self.copy(way, i, True).wait_send()

            @pl.when(self.passes(way, i))
            def _():
                self.copy(way, i, False).wait_send()

    def arrive(self):
        def fetch(way, i):
            return pltpu.make_async_copy(
                self.landing.at[self.place(way, i)], self.last(way), self.stage_sem.at[way])

        for way, i in self.ids:

            @pl.when(self.me == self.target(way, i))
            def _():
                self.copy(way, i, False).wait_recv()
                fetch(way, i).start()

        for way, i in self.ids:

            @pl.when(self.me == self.target(way, i))
            def _():
                fetch(way, i).wait()

    def total(self, own, rows):
        value = own.astype(f32)
        for way, there in ((0, self.me > 0), (1, self.me < self.size - 1)):
            value = value + jnp.where(there, self.last(way)[rows, :].astype(f32), 0.0)
        return value


def add_into(landing, own):
    rows = landing.shape[0]

    @pl.loop(0, rows, step=64)
    def _(r):
        at = pl.ds(r, 64)
        landing[at, :] = (landing[at, :].astype(f32) + own[at, :].astype(f32)).astype(bf16)


def chip_slot(me, r):
    return (
        me
        + 2 * ((r % 2) * (1 - 2 * (lax.div(me, 2) % 2)))
        + 4 * (lax.div(r, 2) * (1 - 2 * (lax.div(me, 4) % 2)))
    )


def spans_of(length):
    back = -(-(MAX_DOC - 1) // BLOCK)
    spans, at = [], 0
    for i in range(length // BLOCK):
        low = max(0, i - back) * BLOCK
        spans.append((low, (i + 1) * BLOCK, at))
        at += (i + 1) * BLOCK - low
    return spans, at


def turn(x, cosine, sine_lo, sine_hi):
    return x * cosine + pltpu.roll(x, 128 - ROT // 2, 1) * sine_lo + pltpu.roll(x, ROT // 2, 1) * sine_hi


def head_lanes(shape, e):
    lane = lax.broadcasted_iota(jnp.int32, shape, 1)
    return (lane >= e * HD) & (lane < (e + 1) * HD)


def only(x, e):
    return jnp.where(head_lanes(x.shape, e), x, jnp.zeros_like(x))


def attend_kernel(
    q_ref, k_ref, v_ref, bias_ref, cos_ref, slo_ref, shi_ref, segc_ref, segr_ref,
    qs_ref, ks_ref, vs_ref, o_ref, p_ref, mask_ref,
):
    @pl.when(pl.program_id(1) == 0)
    def _():
        fill_mask(mask_ref, segc_ref, segr_ref, q_ref.shape[0])

    cosine, slo, shi = cos_ref[...], slo_ref[...], shi_ref[...]
    query = turn(q_ref[...] + bias_ref[0:1, :], cosine, slo, shi).astype(bf16) * bf16(HD**-0.5)
    key = turn(k_ref[...] + bias_ref[1:2, :], cosine, slo, shi).astype(bf16)
    value = (v_ref[...] + bias_ref[2:3, :]).astype(bf16)
    qs_ref[...] = query
    ks_ref[...] = key
    vs_ref[...] = value

    def keep(e, at, probs):
        p_ref[e, at, :] = probs

    def write(at, result):
        o_ref[at, :] = result

    attend_pair(query, key, value, mask_ref, keep, write)


def attend(q, k, v, qkv_bias, tables, segments, rows):
    tokens, local = q.shape
    length = tokens // rows
    pairs = local // 128
    _, stored = spans_of(length)
    block = pl.BlockSpec((length, 128), lambda r, h: (r, h))
    table = pl.BlockSpec((length, 128), lambda r, h: (r, 0))
    shape = jax.ShapeDtypeStruct((tokens, local), bf16)
    return pl.pallas_call(
        attend_kernel,
        grid=(rows, pairs),
        out_shape=(shape,) * 4 + (jax.ShapeDtypeStruct((rows, local // HD, stored, BLOCK), bf16),),
        in_specs=[block] * 3
        + [pl.BlockSpec((8, 128), lambda r, h: (0, h))]
        + [table] * 3
        + [
            pl.BlockSpec((length, 1), lambda r, h: (r, 0)),
            pl.BlockSpec((pl.Squeezed(), 1, length), lambda r, h: (r, 0, 0)),
        ],
        out_specs=(block,) * 4
        + (pl.BlockSpec((pl.Squeezed(), 128 // HD, stored, BLOCK), lambda r, h: (r, h, 0, 0)),),
        scratch_shapes=[pltpu.VMEM((stored, BLOCK), f32)],
        compiler_params=pltpu.CompilerParams(vmem_limit_bytes=VMEM_LIMIT),
        cost_estimate=pl.CostEstimate(
            flops=16 * tokens * 768 * local, bytes_accessed=24 << 20, transcendentals=0
        ),
        name="attend",
    )(q, k, v, qkv_bias, *tables, segments.reshape(tokens, 1), segments.reshape(rows, 1, length))


def attend_back_kernel(
    q_ref, k_ref, v_ref, g_ref, o_ref, p_ref, cos_ref, slo_ref, shi_ref,
    dq_ref, dk_ref, dv_ref, bias_ref, kacc_ref, vacc_ref,
):
    def write(which, at, value):
        (dq_ref, dk_ref, dv_ref)[which][at, :] = value

    sums = attend_back_pair(
        q_ref[...], k_ref[...], v_ref[...], g_ref[...], o_ref[...],
        lambda e, at: p_ref[e, at, :], (cos_ref, slo_ref, shi_ref), kacc_ref, vacc_ref, write)
    sums = jnp.concatenate(list(sums) + [jnp.zeros((5, 128), f32)], 0)

    @pl.when(pl.program_id(1) == 0)
    def _():
        bias_ref[...] = sums

    @pl.when(pl.program_id(1) > 0)
    def _():
        bias_ref[...] += sums


def attend_back(q, k, v, g, o, probs, tables, rows):
    tokens, local = q.shape
    length = tokens // rows
    pairs = local // 128
    stored = probs.shape[2]
    block = pl.BlockSpec((length, 128), lambda h, r: (r, h))
    table = pl.BlockSpec((length, 128), lambda h, r: (r, 0))
    shape = jax.ShapeDtypeStruct((tokens, local), bf16)
    return pl.pallas_call(
        attend_back_kernel,
        grid=(pairs, rows),
        out_shape=(shape,) * 3 + (jax.ShapeDtypeStruct((8, local), f32),),
        in_specs=[block] * 5
        + [pl.BlockSpec((pl.Squeezed(), 128 // HD, stored, BLOCK), lambda h, r: (r, h, 0, 0))]
        + [table] * 3,
        out_specs=(block,) * 3 + (pl.BlockSpec((8, 128), lambda h, r: (0, h)),),
        scratch_shapes=[pltpu.VMEM((length, 128), f32)] * 2,
        compiler_params=pltpu.CompilerParams(vmem_limit_bytes=VMEM_LIMIT),
        cost_estimate=pl.CostEstimate(
            flops=32 * tokens * 768 * local, bytes_accessed=24 << 20, transcendentals=0
        ),
        name="attend_back",
    )(q, k, v, g, o, probs, *tables)


def attend_pair(query, key, value, mask_ref, keep, write):
    length = query.shape[0]
    spans, _ = spans_of(length)
    for i, (low, high, at) in enumerate(spans):
        mine = slice(i * BLOCK, (i + 1) * BLOCK)
        total = jnp.zeros((BLOCK, 128), f32)
        for e in range(128 // HD):
            scores = dot_nt(only(key[low:high], e), query[mine]) + mask_ref[at : at + high - low, :].astype(f32)
            exponent = jnp.exp(scores - jnp.max(scores, 0, keepdims=True))
            inverse = 1.0 / jnp.sum(exponent, 0, keepdims=True)
            probs = (exponent * inverse).astype(bf16)
            keep(e, slice(at, at + high - low), probs)
            total = total + dot_tn(probs, only(value[low:high], e))
        write(mine, total.astype(bf16))


def fill_mask(mask_ref, segc_ref, segr_ref, length):
    for i, (low, high, at) in enumerate(spans_of(length)[0]):
        keys = lax.broadcasted_iota(jnp.int32, (high - low, BLOCK), 0) + low
        queries = lax.broadcasted_iota(jnp.int32, (high - low, BLOCK), 1) + i * BLOCK
        own = segr_ref[:, i * BLOCK : (i + 1) * BLOCK].astype(f32)
        same = segc_ref[low:high, 0:1].astype(f32) == own
        allowed = jnp.where((keys <= queries) & same, 0.0, -1e30)
        mask_ref[at : at + high - low, :] = allowed.astype(mask_ref.dtype)


def fill_tables(seg_ref, column_ref, cos_ref, slo_ref, shi_ref):
    length = seg_ref.shape[1]
    row = seg_ref[...].astype(f32)
    column_ref[...] = jnp.broadcast_to(row, (128, length)).T
    starts = [jnp.sum(jnp.where(row < number, 1.0, 0.0), 1, keepdims=True) for number in range(1, 4)]
    lane = lax.broadcasted_iota(jnp.int32, (1, 128), 1) % HD
    exponent = (2 * (lane % (ROT // 2))).astype(f32) / ROT
    frequency = 1.0 / jnp.exp(exponent * f32(9.210340371976184))

    @pl.loop(0, length, step=128)
    def _(r):
        at = pl.ds(pl.multiple_of(r, 128), 128)
        column = column_ref[at, :]
        start = jnp.zeros_like(column)
        for number in range(1, 4):
            start = jnp.where(column == number, starts[number - 1], start)
        index = (lax.broadcasted_iota(jnp.int32, (128, 128), 0) + r).astype(f32)
        angle = (index - start) * frequency
        cosine, sine = jnp.cos(angle), jnp.sin(angle)
        cos_ref[at, :] = jnp.where(lane < ROT, cosine, 1.0)
        slo_ref[at, :] = jnp.where(lane < ROT // 2, -sine, 0.0)
        shi_ref[at, :] = jnp.where((lane >= ROT // 2) & (lane < ROT), sine, 0.0)


def attend_back_pair(query, key, value, grad, result, probs_of, tables, kacc_ref, vacc_ref, write):
    length = query.shape[0]
    spans, _ = spans_of(length)
    heads = 128 // HD
    inner = grad.astype(f32) * result.astype(f32)
    lane = lax.broadcasted_iota(jnp.int32, (8, 128), 1)
    row = lax.broadcasted_iota(jnp.int32, (8, 128), 0)
    pick = jnp.where(lax.div(lane, HD) == row, 1.0, 0.0)
    delta = lax.dot_general(
        pick, inner, (((1,), (1,)), ((), ())),
        precision=lax.Precision.HIGHEST, preferred_element_type=f32)
    kacc_ref[...] = jnp.zeros_like(kacc_ref)
    vacc_ref[...] = jnp.zeros_like(vacc_ref)
    cos_ref, slo_ref, shi_ref = tables
    first = jnp.zeros((1, 128), f32)
    for i, (low, high, at) in enumerate(spans):
        mine = slice(i * BLOCK, (i + 1) * BLOCK)
        g_i, q_i = grad[mine], query[mine]
        dq = jnp.zeros((BLOCK, 128), f32)
        ps, dss = [], []
        for e in range(heads):
            probs = probs_of(e, slice(at, at + high - low))
            dprobs = dot_nt(only(value[low:high], e), g_i)
            ds = (probs.astype(f32) * (dprobs - delta[e : e + 1, mine])).astype(bf16)
            dq = dq + dot_tn(ds, only(key[low:high], e))
            ps.append(probs)
            dss.append(ds)
        g_cat = jnp.concatenate([only(g_i, e) for e in range(heads)], 0)
        q_cat = jnp.concatenate([only(q_i, e) for e in range(heads)], 0)
        vacc_ref[low:high, :] += dot_nn(jnp.concatenate(ps, 1), g_cat)
        kacc_ref[low:high, :] += dot_nn(jnp.concatenate(dss, 1), q_cat)
        dq = dq * f32(HD**-0.5)
        dq = turn(dq, cos_ref[mine, :], -slo_ref[mine, :], -shi_ref[mine, :]).astype(bf16)
        write(0, mine, dq)
        first = first + jnp.sum(dq.astype(f32), 0, keepdims=True)
    everything = slice(0, length)
    dk = turn(kacc_ref[...], cos_ref[...], -slo_ref[...], -shi_ref[...]).astype(bf16)
    dv = vacc_ref[...].astype(bf16)
    write(1, everything, dk)
    write(2, everything, dv)
    return first, jnp.sum(dk.astype(f32), 0, keepdims=True), jnp.sum(dv.astype(f32), 0, keepdims=True)


def block_call(dp, tensor, arrays):
    hidden, cotangent, w_qkv, w_dense, w_fc1, w_fc2 = arrays[:6]
    rows, width = hidden.shape
    local = w_qkv.shape[2]
    wide = 3 * local
    units = w_fc1.shape[1]
    part = width // dp
    chips = dp // 2
    tokens = rows * tensor
    pairs = local // 128
    stored = spans_of(tokens)[1]
    sems = Sems()
    orders = orders_of(dp)
    vec_ids = [sems.take() for _ in range(dp - 1)]
    plan_qkv, plan_dense, plan_fc1, plan_fc2 = (CubeGather(sems, orders) for _ in range(4))
    plan_n, plan_c = LineGather(sems, tensor, 2), LineGather(sems, tensor, 2)
    line_out, line_in = LineReduce(sems, tensor), LineReduce(sems, tensor)
    reduce_fc2, reduce_dense, reduce_fc1, reduce_qkv = (ChipReduce(sems) for _ in range(4))
    swaps = [sems.take() for _ in range(2 * chips + 4)]
    tells = [sems.take() for _ in range(2 * (dp - 1) + tensor - 1)]

    def kernel(
        x_ref, c_ref, wq_ref, wd_ref, w1_ref, w2_ref, gain_ref, beta_ref, bd_ref, b2_ref,
        qb_ref, fb_ref, seg_ref,
        out_ref, hid_ref, s2_out, sd_out, s1_out, sq_out,
        gq_ref, g1_ref, g2_ref, x_out, n_out, nx_out, ax_out, gqx_out, gpx_out,
        land_out, land_in, land_2, land_d, land_1, land_q, vout_ref, bout_ref,
        x_buf, vec_buf, nv, wa, wb, wd, act, slope, qkv3, abuf, pb, mask, cbuf, xbuf,
        kacc, vacc, cos_ref, slo_ref, shi_ref, line_stage, chip_stage,
        fsum, bsum, parts, tell_v, tell_b, tell_z, vec_ref,
        send_sem, recv_sem, local_sem, stage_sem,
    ):
        me, line = lax.axis_index("dp"), lax.axis_index("tensor")
        twin = flip(me, 0)
        half = part // 2
        local_count = [0]
        attn = abuf.at[:, pl.ds(0, local)]

        def cols(a):
            return pl.ds(pl.multiple_of(a * part, part), part)

        def half_rows(a, h):
            return pl.ds(pl.multiple_of(a * part + h * half, half), half)

        def tok(b, u):
            return pl.ds(pl.multiple_of(b * rows + u * (rows // 2), rows // 2), rows // 2)

        def block(b):
            return pl.ds(pl.multiple_of(b * rows, rows), rows)

        def piece(n, h):
            return pl.ds(h * (n // 2), n // 2)

        def copy_of(a, b):
            local_count[0] += 1
            return pltpu.make_async_copy(a, b, local_sem.at[local_count[0] - 1])

        def remote(k, source, target, device):
            return pltpu.make_async_remote_copy(
                src_ref=source, dst_ref=target,
                send_sem=send_sem.at[k], recv_sem=recv_sem.at[k],
                device_id=device, device_id_type=MESH)

        def to_twin(k, source, target):
            return remote(swaps[k], source, target, (twin, line))

        pair = (send_sem, recv_sem)
        vec = [
            remote(k, vec_ref, vec_buf.at[:, cols(me)], (relative(me, r), line))
            for r, k in enumerate(vec_ids, 1)
        ]
        qkv = plan_qkv.bind(
            me, line,
            lambda h: wq_ref.at[:, pl.ds(h * half, half), :],
            lambda a, h: gq_ref.at[:, half_rows(a, h), :], *pair)
        fc1 = plan_fc1.bind(
            me, line,
            lambda h: w1_ref.at[pl.ds(h * half, half), :],
            lambda a, h: g1_ref.at[half_rows(a, h), :], *pair)
        dense = plan_dense.bind(
            me, line,
            lambda h: wd_ref.at[piece(local, h), :],
            lambda a, h: wd.at[piece(local, h), cols(a)], *pair)
        fc2 = plan_fc2.bind(
            me, line,
            lambda h: w2_ref.at[piece(units, h), :],
            lambda a, h: g2_ref.at[piece(units, h), cols(a)], *pair)
        norm = plan_n.bind(
            line, me, lambda u: x_ref.at[piece(rows, u)], lambda b, u: pb.at[tok(b, u)], *pair)
        cot = plan_c.bind(
            line, me, lambda u: c_ref.at[piece(rows, u)], lambda b, u: cbuf.at[tok(b, u)], *pair)
        staged = (stage_sem, *pair)

        def lasts(way):
            return wd.at[pl.ds(way * rows, rows), :]

        outs = line_out.bind(
            line, me, lambda d: nv.at[pl.ds(d * rows, rows), :], land_out, line_stage, lasts, *staged)
        ins = line_in.bind(
            line, me, lambda d: act.at[pl.ds(d * rows, rows), :], land_in, line_stage, lasts, *staged)
        low, high = pl.ds(0, tokens), pl.ds(tokens, tokens)
        sum_2 = reduce_fc2.bind(
            me, line,
            lambda r, h: wa.at[pl.ds(tokens + r * part, part), piece(units, h)],
            land_2, chip_stage, *staged)
        sum_d = reduce_dense.bind(
            me, line,
            lambda r, h: mask.at[pl.ds((2 * r + h) * part, part), :],
            land_d, chip_stage, *staged)
        sum_1 = reduce_fc1.bind(
            me, line,
            lambda r, h: wb.at[pl.ds(r * part, part), piece(units, h)],
            land_1, chip_stage, *staged)
        sum_q = reduce_qkv.bind(
            me, line,
            lambda r, h: abuf.at[pl.ds(r * part, part), piece(wide, h)],
            land_q, chip_stage, *staged)
        stages = dp.bit_length() - 1

        takes = [
            copy_of(x_ref, x_buf),
            copy_of(wd_ref, wd.at[:, cols(me)]),
            copy_of(c_ref, cbuf.at[block(line), :]),
            copy_of(wq_ref, qkv3.at[:, pl.ds(0, part), :]),
            copy_of(w1_ref, act.at[pl.ds(0, part), :]),
            copy_of(w2_ref, wb.at[:, pl.ds(0, part)]),
            copy_of(x_ref, pb.at[block(line), :]),
        ]
        keeps = [
            copy_of(qkv3.at[:, pl.ds(0, part), :], gq_ref.at[:, cols(me), :]),
            copy_of(act.at[pl.ds(0, part), :], g1_ref.at[cols(me), :]),
            copy_of(wb.at[:, pl.ds(0, part)], g2_ref.at[:, cols(me)]),
        ]
        takes[0].start()
        for k, ref in enumerate((gain_ref, beta_ref, bd_ref)):
            vec_ref[k : k + 1, :] = ref[...].astype(f32).reshape(1, part)
        vec_ref[2:3, :] += b2_ref[...].astype(f32).reshape(1, part)
        vec_buf[:, cols(me)] = vec_ref[...]
        parts[0:1, :] = fb_ref[...].astype(f32).reshape(1, units)
        greet(
            dp, me, tensor, line,
            lambda: fill_tables(seg_ref, kacc, cos_ref, slo_ref, shi_ref))
        for copy in vec:
            copy.start()
        norm.start(0)
        norm.start(1)
        qkv.start()
        for copy in takes[1:]:
            copy.start()
        takes[0].wait()
        for copy in vec:
            copy.wait_recv()
        qkv.advance(0)
        fc1.start()
        for take, copy in zip(takes[3:6], keeps):
            take.wait()
            copy.start()
        fill_mask(mask, kacc, seg_ref, tokens)

        def project(b):
            at = block(b)

            @pl.loop(0, rows, step=32)
            def _(r):
                some = pl.ds(pl.multiple_of(b * rows + r, 32), 32)
                x = pb[some, :].astype(f32)
                centred = x - jnp.mean(x, -1, keepdims=True)
                spread = jnp.mean(centred * centred, -1, keepdims=True)
                unit = centred * lax.rsqrt(spread + layer_eps)
                nv[some, :] = (unit * vec_buf[0:1, :] + vec_buf[1:2, :]).astype(bf16)

            cosine, slo, shi = cos_ref[at, :], slo_ref[at, :], shi_ref[at, :]
            for i in range(3):
                value = dot_nn(nv[at, :], wa[:, i * local : (i + 1) * local])
                value = value + qb_ref[i : i + 1, :].astype(f32)
                if i == 2:
                    qkv3[2, at, :] = value.astype(bf16)
                    continue
                for h in range(pairs):
                    lanes = slice(h * 128, (h + 1) * 128)
                    turned = turn(value[:, lanes], cosine, slo, shi).astype(bf16)
                    if i == 0:
                        turned = turned * bf16(HD**-0.5)
                    qkv3[i, at, lanes] = turned

        def hidden_layer(b, first):
            at = block(b)

            @pl.loop(0, units, step=512)
            def _(n):
                @pl.when(first & (n == units // 2))
                def _():
                    load_1[1].wait()

                to = pl.ds(pl.multiple_of(n, 512), 512)
                pre = dot_nn(nv[at, :], wb[:, to]) + parts[0:1, to]
                square = pre * pre
                bend = jnp.tanh(0.7978845608028654 * pre * (1.0 + 0.044715 * square))
                act[at, to] = (0.5 * pre * (1.0 + bend)).astype(bf16)
                rise = 0.7978845608028654 * (1.0 + 3 * 0.044715 * square)
                slope[at, to] = (
                    0.5 * (1.0 + bend) + 0.5 * pre * (1.0 - bend * bend) * rise
                ).astype(bf16)

        def slope_layer(b):
            at = block(b)
            abuf[at, pl.ds(local, local)] = dot_nt(cbuf[at, :], wd[...]).astype(bf16)

            @pl.loop(0, units, step=1024)
            def _(n):
                to = pl.ds(pl.multiple_of(n, 1024), 1024)
                value = dot_nt(cbuf[at, :], wa[to, :]) * slope[at, to].astype(f32)
                value = value.astype(bf16)
                slope[at, to] = value
                fsum[0:1, to] += jnp.sum(value.astype(f32), 0, keepdims=True)

        def blocks_of(s, task):
            @pl.loop(0, 2)
            def _(way):
                b = line + (2 * way - 1) * (1 + s)

                @pl.when((b >= 0) & (b < tensor) & ((s >= 0) | (way == 0)))
                def _():
                    task(b)

        norm.advance(0, 0)
        norm.advance(0, 1)
        for j in range(1, stages):
            qkv.advance(j)
        keeps[0].wait()
        load_q = [
            copy_of(gq_ref.at[i], wa.at[:, pl.ds(i * local, local)]) for i in range(3)
        ]
        for copy in load_q:
            copy.start()
        fc1.advance(0)
        dense.start()
        fc2.start()
        for copy in load_q + [takes[6]]:
            copy.wait()
        for s in range(1, tensor - 2):
            norm.advance(s, 0)
            norm.advance(s, 1)
        cot.start(0)
        cot.start(1)

        @pl.loop(-1, tensor - 2)
        def _(s):
            blocks_of(s, project)

        for j in range(1, stages):
            fc1.advance(j)
        for copy in keeps[1:]:
            copy.wait()
        load_1 = [copy_of(g1_ref.at[:, piece(units, h)], wb.at[:, piece(units, h)]) for h in (0, 1)]
        load_1[0].start()
        load_1[0].wait()
        load_1[1].start()

        x_store = copy_of(pb.at[low, :], x_out)

        @pl.loop(-1, tensor - 1)
        def _(s):
            @pl.when(s == tensor - 2)
            def _():
                norm.advance(tensor - 2, 0)
                norm.advance(tensor - 2, 1)
                x_store.start()
                fc2.advance(0)
                blocks_of(tensor - 2, project)

            @pl.when(s == 0)
            def _():
                dense.advance(0)

            blocks_of(s, lambda b: hidden_layer(b, s == -1))

        n_store = copy_of(nv, n_out)
        n_store.start()
        cross_n = [
            to_twin(r, nv.at[:, cols(relative(twin, r << 1))], nx_out.at[r]) for r in range(chips)
        ]
        cross_a = to_twin(chips, act, ax_out)
        for copy in cross_n + [cross_a]:
            copy.start()
        norm.finish()
        x_store.wait()

        def prob_lanes(h, e):
            return pl.ds(pl.multiple_of((2 * h + e) * BLOCK, BLOCK), BLOCK)

        @pl.loop(0, pairs)
        def _(h):
            lanes = pl.ds(pl.multiple_of(h * 128, 128), 128)

            def keep(e, at, value):
                pb[at, prob_lanes(h, e)] = value

            def write(at, value):
                abuf[at, lanes] = value

            attend_pair(
                qkv3[0, :, lanes], qkv3[1, :, lanes], qkv3[2, :, lanes], mask, keep, write)

            @pl.when(h == 0)
            def _():
                cot.advance(0, 0)
                cot.advance(0, 1)

            @pl.when(h == 1)
            def _():
                for j in range(1, stages - 1):
                    dense.advance(j)

            @pl.when(h == 2)
            def _():
                for j in range(1, stages - 1):
                    fc2.advance(j)

        cross_t = to_twin(chips + 1, attn, xbuf.at[:, pl.ds(chips * part, local)])
        cross_t.start()
        dense.advance(stages - 1)
        fc2.advance(stages - 1)
        takes[1].wait()
        takes[2].wait()
        load_2 = [copy_of(g2_ref.at[:, piece(width, h)], wa.at[:, piece(width, h)]) for h in (0, 1)]
        load_2[0].start()
        cot.advance(1, 0)
        n_store.wait()
        for copy in cross_n:
            copy.wait_send()
        load_2[0].wait()
        load_2[1].start()
        upper = lax.div(line, tensor // 2)

        def outward(i):
            return (1 - upper) * (tensor - 1 - i) + upper * i

        @pl.loop(0, tensor)
        def _(i):
            at = block(outward(i))

            @pl.loop(0, width, step=1024)
            def _(n):
                @pl.when((i == 0) & (n > 0))
                def _():
                    load_2[1].wait()

                to = pl.ds(pl.multiple_of(n, 1024), 1024)
                value = dot_nn(act[at, :], wa[:, to]) + dot_nn(attn[at, :], wd[:, to])
                nv[at, to] = value.astype(bf16)

            for k in range(tensor - 1):

                @pl.when(i == k)
                def _():
                    outs.start(0, k)
                    outs.start(1, k)

            @pl.when(i == tensor - 2)
            def _():
                cot.advance(1, 1)

        cross_a.wait_recv()
        load_ax = copy_of(ax_out, wb.at[low, :])
        load_ax.start()
        fsum[...] = jnp.zeros_like(fsum)
        cross_c = [
            to_twin(chips + 2 + r, cbuf.at[:, cols(relative(twin, r << 1))],
                    xbuf.at[:, pl.ds(r * part, part)])
            for r in range(chips)
        ]

        @pl.loop(-1, tensor - 1)
        def _(s):
            @pl.when(s == tensor - 2)
            def _():
                cot.advance(tensor - 2, 0)
                outs.advance(1)
                cot.advance(tensor - 2, 1)
                for copy in cross_c:
                    copy.start()

            blocks_of(s, slope_layer)

        cross_p = to_twin(2 * chips + 3, slope, gpx_out)
        cross_p.start()
        for copy in cross_c + [cross_t]:
            copy.wait_recv()
        load_ax.wait()
        dense.finish()

        def weight_grad(left, plan, own, crossed, spot, size, step, hook=None, second=None):
            @pl.loop(0, chips)
            def _(i):
                r = chips - 1 - i
                slot = chip_slot(me, r)
                across = pl.ds(pl.multiple_of(r * part, part), part)

                @pl.loop(0, size, step=step)
                def _(n):
                    if second is not None:

                        @pl.when((i == 0) & (n == step))
                        def _():
                            second.wait()

                    at = pl.multiple_of(n, step)
                    value = dot_tn(left(cols(slot)), own(at)) + dot_tn(xbuf[:, across], crossed(at))
                    spot(r, at, value.astype(bf16))

                for k in range(1, chips):

                    @pl.when(r == k)
                    def _():
                        plan.start(k)

                if hook is not None:
                    hook(i)

        def spot_a(r, at, value):
            wa[pl.ds(pl.multiple_of(tokens + r * part, part), part), pl.ds(at, 1024)] = value

        def spot_d(r, at, value):
            for h in (0, 1):
                to = pl.ds(pl.multiple_of((2 * r + h) * part, part), part)
                mask[to, :] = value[:, h * (local // 2) : (h + 1) * (local // 2)]

        def spot_1(r, at, value):
            wb[pl.ds(pl.multiple_of(r * part, part), part), pl.ds(at, 1024)] = value

        def spot_q(r, at, value):
            abuf[pl.ds(pl.multiple_of(r * part, part), part), pl.ds(at, local)] = value

        weight_grad(
            lambda a: cbuf[:, a], sum_2, lambda at: act[:, pl.ds(at, 1024)],
            lambda at: wb[low, pl.ds(at, 1024)], spot_a, units, 1024)
        weight_grad(
            lambda a: cbuf[:, a], sum_d, lambda at: attn[...],
            lambda at: xbuf[:, pl.ds(chips * part, local)], spot_d, local, local)
        load_n = copy_of(n_out, wa.at[low, :])
        load_n.start()
        load_g1 = copy_of(g1_ref.at[low, :], wb.at[low, :])
        load_g1.start()
        for copy in cross_n:
            copy.wait_recv()
        load_nx = [copy_of(nx_out.at[r], xbuf.at[:, pl.ds(r * part, part)]) for r in range(chips)]
        for copy in load_nx:
            copy.start()
        cot.finish()
        for copy in cross_c + [cross_a]:
            copy.wait_send()
        bsum[...] = jnp.zeros_like(bsum)
        for k in range(units // local):
            bsum[k : k + 1, :] = fsum[0:1, k * local : (k + 1) * local]
        load_w = [copy_of(gq_ref.at[i], pb.at[pl.ds(0, width), pl.ds(i * local, local)]) for i in range(3)]

        @pl.loop(0, pairs)
        def _(h):
            lanes = pl.ds(pl.multiple_of(h * 128, 128), 128)

            def write(which, at, value):
                cbuf[at, pl.ds(pl.multiple_of(which * local + h * 128, 128), 128)] = value

            sums = attend_back_pair(
                qkv3[0, :, lanes], qkv3[1, :, lanes], qkv3[2, :, lanes],
                abuf[:, pl.ds(pl.multiple_of(local + h * 128, 128), 128)], abuf[:, lanes],
                lambda e, at: pb[at, prob_lanes(h, e)],
                (cos_ref, slo_ref, shi_ref), kacc, vacc, write)
            for k in range(3):
                bsum[units // local + k : units // local + k + 1, lanes] = sums[k]

            for k in range(3):

                @pl.when(h == k)
                def _():
                    load_w[k].start()

            @pl.when(h == 0)
            def _():
                sum_2.middle()

            @pl.when(h == 1)
            def _():
                outs.advance(2)

        back = cbuf.at[:, pl.ds(0, wide)]
        cross_d = to_twin(2 * chips + 2, back, gqx_out)
        cross_d.start()
        bias_tells = [
            remote(tells[r - 1], bsum, tell_b.at[r], (relative(me, r), line)) for r in range(1, dp)
        ]
        for copy in bias_tells:
            copy.start()
        for copy in load_w + [load_g1]:
            copy.wait()
        load_gx = [copy_of(gqx_out.at[:, pl.ds(i * local, local)], qkv3.at[i]) for i in range(3)]
        store_o = copy_of(x_buf, out_ref)
        load_px = [copy_of(gpx_out.at[:, piece(units, h)], cbuf.at[:, piece(units, h)]) for h in (0, 1)]
        spare = pb.at[pl.ds(width, rows), :]
        load_c = copy_of(c_ref, spare)

        def dense_step(i):
            @pl.when(i == chips - 2)
            def _():
                sum_d.middle()

        @pl.loop(0, tensor)
        def _(i):
            at = block(outward(i))

            @pl.loop(0, width, step=1024)
            def _(n):
                to = pl.ds(pl.multiple_of(n, 1024), 1024)
                value = dot_nt(slope[at, :], wb[to, :])
                value = value + dot_nt(cbuf[at, pl.ds(0, wide)], pb[to, pl.ds(0, wide)])
                act[at, to] = value.astype(bf16)

            for k in range(tensor - 1):

                @pl.when(i == k)
                def _():
                    ins.start(0, k)
                    ins.start(1, k)

            @pl.when(i == 0)
            def _():
                load_c.start()

            @pl.when(i == 1)
            def _():
                cross_d.wait_recv()
                for copy in load_gx:
                    copy.start()
                load_n.wait()
                for copy in load_nx + load_gx:
                    copy.wait()
                cross_t.wait_send()
                weight_grad(
                    lambda a: wa[low, a], sum_q, lambda at: cbuf[:, pl.ds(at, local)],
                    lambda at: qkv3[lax.div(at, local)], spot_q, wide, local, dense_step)

        cross_d.wait_send()
        cross_p.wait_recv()
        load_px[0].start()
        outs.settle()
        ins.advance(1)
        load_xa = copy_of(x_out, wb.at[high, :])
        load_px[0].wait()
        load_px[1].start()
        load_xa.start()

        def late_steps(i):
            @pl.when(i == 0)
            def _():
                sum_q.middle()

        weight_grad(
            lambda a: wa[low, a], sum_1, lambda at: slope[:, pl.ds(at, 1024)],
            lambda at: cbuf[:, pl.ds(at, 1024)], spot_1, units, 1024, late_steps, load_px[1])
        def finish_out():
            outs.arrive()

            @pl.loop(0, rows, step=32)
            def _(r):
                at = pl.ds(r, 32)
                own = pl.ds(pl.multiple_of(line * rows + r, 32), 32)
                total = x_buf[at, :].astype(f32) + outs.total(nv[own, :], at) + vec_buf[2:3, :]
                x_buf[at, :] = total.astype(bf16)

            store_o.start()

        parts[...] = jnp.zeros_like(parts)
        load_xa.wait()
        load_c.wait()

        def norm_sums(b):
            @pl.loop(0, rows, step=32)
            def _(r):
                some = pl.ds(pl.multiple_of(b * rows + r, 32), 32)
                x = wb[pl.ds(pl.multiple_of(tokens + b * rows + r, 32), 32), :].astype(f32)
                grad = act[some, :].astype(f32)
                centred = x - jnp.mean(x, -1, keepdims=True)
                inv_std = lax.rsqrt(jnp.mean(centred * centred, -1, keepdims=True) + layer_eps)
                parts[0:1, :] += jnp.sum(grad * (centred * inv_std), 0, keepdims=True)
                parts[1:2, :] += jnp.sum(grad, 0, keepdims=True)

        @pl.loop(0, tensor)
        def _(b):
            @pl.when(b == tensor - 1)
            def _():
                finish_out()
                ins.advance(2)

            norm_sums(b)

        @pl.loop(0, rows, step=32)
        def _(r):
            cotan = pb[pl.ds(pl.multiple_of(width + r, 32), 32), :].astype(f32)
            parts[2:3, :] += jnp.sum(cotan, 0, keepdims=True)

        vec_tells = [
            remote(tells[dp - 2 + r], parts.at[:, cols(relative(me, r))], tell_v.at[r],
                   (relative(me, r), line))
            for r in range(1, dp)
        ]
        for copy in vec_tells:
            copy.start()
        sum_1.middle()
        sum_2.final()
        sum_d.final()
        store_2 = copy_of(wa.at[pl.ds(tokens, part), :], s2_out)
        store_dense = [
            copy_of(mask.at[pl.ds(h * part, part), :], sd_out.at[:, piece(local, h)]) for h in (0, 1)
        ]
        for copy in [store_2] + store_dense:
            copy.start()
        store_o.wait()
        load_x = copy_of(x_ref, x_buf)
        load_x.start()
        for copy in bias_tells:
            copy.wait_recv()
        total_b = bsum[...]
        for r in range(1, dp):
            total_b = total_b + tell_b[r]
        bout_ref[...] = total_b
        for copy in vec_tells:
            copy.wait_recv()
        total_v = parts[:, cols(me)]
        for r in range(1, dp):
            total_v = total_v + tell_v[r]
        tell_z[0] = total_v
        line_tells = [
            remote(tells[2 * dp - 3 + k], tell_z.at[0], tell_z.at[k], (me, lax.rem(line + k, tensor)))
            for k in range(1, tensor)
        ]
        for copy in line_tells:
            copy.start()
        sum_q.final()
        store_q = copy_of(abuf.at[pl.ds(0, part), :], sq_out)
        store_q.start()
        load_x.wait()
        sum_1.final()
        store_1 = copy_of(wb.at[pl.ds(0, part), :], s1_out)
        store_1.start()
        ins.settle()
        ins.arrive()

        @pl.loop(0, rows, step=32)
        def _(r):
            at = pl.ds(r, 32)
            x = x_buf[at, :].astype(f32)
            centred = x - jnp.mean(x, -1, keepdims=True)
            inv_std = lax.rsqrt(jnp.mean(centred * centred, -1, keepdims=True) + layer_eps)
            unit = centred * inv_std
            own = pl.ds(pl.multiple_of(line * rows + r, 32), 32)
            scaled = ins.total(act[own, :], at) * vec_buf[0:1, :]
            cotan = pb[pl.ds(pl.multiple_of(width + r, 32), 32), :].astype(f32)
            first = jnp.mean(scaled, -1, keepdims=True)
            second = jnp.mean(scaled * unit, -1, keepdims=True)
            x_buf[at, :] = (cotan + inv_std * (scaled - first - unit * second)).astype(bf16)

        store_h = copy_of(x_buf, hid_ref)
        store_h.start()
        for copy in line_tells:
            copy.wait_recv()
        total_z = tell_z[0]
        for k in range(1, tensor):
            total_z = total_z + tell_z[k]
        vout_ref[...] = total_z
        for copy in vec + [cross_p] + bias_tells + vec_tells + line_tells:
            copy.wait_send()
        for plan in (qkv, fc1, fc2, sum_2, sum_d, sum_1, sum_q):
            plan.finish()
        for copy in store_dense + [store_2, store_q, store_h, store_1]:
            copy.wait()

    def shape(*dims):
        return jax.ShapeDtypeStruct(dims, bf16)

    def vmem(*dims):
        return pltpu.VMEM(dims, bf16)

    landings = [
        shape(2 * tensor - 3, rows, width),
        shape(2 * tensor - 3, rows, width),
        shape(6, part, units // 2),
        shape(6, part, local // 2),
        shape(6, part, units // 2),
        shape(6, part, wide // 2),
    ]
    return pl.pallas_call(
        kernel,
        out_shape=(
            shape(rows, width),
            shape(rows, width),
            shape(part, units),
            shape(part, local),
            shape(part, units),
            shape(part, wide),
            shape(3, width, local),
            shape(width, units),
            shape(units, width),
            shape(tokens, width),
            shape(tokens, width),
            shape(chips, tokens, part),
            shape(tokens, units),
            shape(tokens, wide),
            shape(tokens, units),
            *landings,
            jax.ShapeDtypeStruct((8, part), f32),
            jax.ShapeDtypeStruct((8, local), f32),
        ),
        in_specs=[ANY] * 6 + [VMEM] * 7,
        out_specs=(ANY,) * 21 + (VMEM,) * 2,
        scratch_shapes=[
            vmem(rows, width),
            pltpu.VMEM((8, width), f32),
            vmem(tokens, width),
            vmem(width, width),
            vmem(width, units),
            vmem(local, width),
            vmem(tokens, units),
            vmem(tokens, units),
            vmem(3, tokens, local),
            vmem(tokens, wide),
            vmem(stored, local // HD * BLOCK),
            vmem(stored, BLOCK),
            vmem(tokens, width),
            vmem(tokens, chips * part + local),
        ]
        + [pltpu.VMEM((tokens, 128), f32)] * 5
        + [
            vmem(tensor - 1, rows, width),
            vmem(2, part, units // 2),
            pltpu.VMEM((8, units), f32),
            pltpu.VMEM((8, local), f32),
            pltpu.VMEM((8, width), f32),
            pltpu.VMEM((dp, 8, part), f32),
            pltpu.VMEM((dp, 8, local), f32),
            pltpu.VMEM((tensor, 8, part), f32),
            pltpu.VMEM((8, part), f32),
            pltpu.SemaphoreType.DMA((sems.count,)),
            pltpu.SemaphoreType.DMA((sems.count,)),
            pltpu.SemaphoreType.DMA((48,)),
            pltpu.SemaphoreType.DMA((2,)),
        ],
        compiler_params=pltpu.CompilerParams(
            collective_id=0, has_side_effects=True, vmem_limit_bytes=67_043_328
        ),
        name="block",
    )(*arrays)


def finish_kernel(
    s2_ref, sd_ref, s1_ref, sq_ref, o_ref, h_ref, v_ref, b_ref,
    w2_ref, wd_ref, w1_ref, wq_ref, out_ref, hid_ref, gain_ref, beta_ref, both_ref, same_ref, bq_ref, b1_ref,
):
    w2_ref[...] = s2_ref[...].T.astype(f32)
    wd_ref[...] = sd_ref[...].T.astype(f32)
    w1_ref[...] = s1_ref[...].astype(f32)
    local = wq_ref.shape[2]
    for i in range(3):
        wq_ref[i] = sq_ref[:, i * local : (i + 1) * local].astype(f32)
    out_ref[...] = o_ref[...]
    hid_ref[...] = h_ref[...]

    @pl.when(pl.program_id(0) == 0)
    def _():
        line = lax.axis_index("tensor")
        count = gain_ref.shape[0]
        mine = v_ref[:, :count]
        for k in range(1, v_ref.shape[1] // count):
            mine = jnp.where(line == k, v_ref[:, k * count : (k + 1) * count], mine)
        gain_ref[...] = mine[0]
        beta_ref[...] = mine[1]
        both_ref[...] = mine[2]
        same_ref[...] = mine[2]
        lines = b1_ref.shape[0] // b_ref.shape[1]
        bq_ref[...] = b_ref[lines : lines + 3, :]
        for k in range(lines):
            b1_ref[pl.ds(k * b_ref.shape[1], b_ref.shape[1])] = b_ref[k]


def finish(tensor, sent_fc2, sent_dense, sent_fc1, sent_qkv, out, hidden_grad, vec_sums, all_sums):
    part, units = sent_fc2.shape
    local = sent_dense.shape[1]
    rows, width = out.shape
    steps = 4
    quarter = vec_sums.shape[1] // tensor
    fixed = VMEM

    def down(n, m):
        return pl.BlockSpec((n // steps, m), lambda i: (i, 0))

    def across(n, m):
        return pl.BlockSpec((n, m // steps), lambda i: (0, i))

    return pl.pallas_call(
        finish_kernel,
        grid=(steps,),
        out_shape=(
            jax.ShapeDtypeStruct((units, part), f32),
            jax.ShapeDtypeStruct((local, part), f32),
            jax.ShapeDtypeStruct((part, units), f32),
            jax.ShapeDtypeStruct((3, part, local), f32),
            jax.ShapeDtypeStruct((rows, width), bf16),
            jax.ShapeDtypeStruct((rows, width), bf16),
            *[jax.ShapeDtypeStruct((quarter,), f32)] * 4,
            jax.ShapeDtypeStruct((3, local), f32),
            jax.ShapeDtypeStruct((units,), f32),
        ),
        in_specs=[
            across(part, units), across(part, local), down(part, units), down(part, 3 * local),
            down(rows, width), down(rows, width), fixed, fixed,
        ],
        out_specs=(
            down(units, part), down(local, part), down(part, units),
            pl.BlockSpec((3, part // steps, local), lambda i: (0, i, 0)),
            down(rows, width), down(rows, width), *[fixed] * 6,
        ),
        compiler_params=pltpu.CompilerParams(vmem_limit_bytes=VMEM_LIMIT),
        name="finish",
    )(sent_fc2, sent_dense, sent_fc1, sent_qkv, out, hidden_grad, vec_sums, all_sums)


def rotary_tables(segments):
    rows, length = segments.shape
    index = jnp.arange(length, dtype=jnp.int32)[None]
    start = jnp.zeros_like(segments)
    for number in range(1, 4):
        start = jnp.where(segments == number, jnp.sum(segments < number, -1, keepdims=True), start)
    position = (index - start).astype(f32).reshape(rows * length, 1)
    lane = jnp.arange(128, dtype=jnp.int32) % HD
    exponent = (2 * (lane % (ROT // 2))).astype(f32) / ROT
    angle = position * (1.0 / 10000.0**exponent)[None]
    cosine, sine = jnp.cos(angle), jnp.sin(angle)
    low, high = lane < ROT // 2, (lane >= ROT // 2) & (lane < ROT)
    return (
        jnp.where(lane < ROT, cosine, 1.0),
        jnp.where(low, -sine, 0.0),
        jnp.where(high, sine, 0.0),
    )


def matmul(a, b):
    return jnp.dot(a, b, preferred_element_type=f32)


def on_device(
    dp, tensor, fast,
    hidden_in, segments, ln_gain, ln_bias, qkv_weight, qkv_bias, dense_weight, dense_bias,
    fc1_weight, fc1_bias, fc2_weight, fc2_bias, cotangent,
):
    seqs = segments.shape[0]
    local = qkv_weight.shape[2]
    mine = (
        hidden_in, cotangent, qkv_weight.transpose(1, 0, 2), dense_weight, fc1_weight, fc2_weight,
    )
    if fast:
        (out, hidden_grad, sent_fc2, sent_dense, sent_fc1, sent_qkv, *_, vec_sums, all_sums) = block_call(
            dp, tensor, (*mine, ln_gain, ln_bias, dense_bias, fc2_bias, qkv_bias, fc1_bias, segments))
        (
            grad_w2, grad_wd, grad_w1, grad_wq, out, hidden_grad,
            gain_grad, beta_grad, bias_grad, same_grad, qkv_grad, fc1_grad,
        ) = finish(
            tensor, sent_fc2, sent_dense, sent_fc1, sent_qkv, out, hidden_grad, vec_sums, all_sums)
        return (
            out,
            hidden_grad,
            gain_grad,
            beta_grad,
            grad_wq.transpose(1, 0, 2),
            qkv_grad,
            grad_wd,
            bias_grad,
            grad_w1,
            fc1_grad,
            grad_w2,
            same_grad,
        )

    number = lax.broadcasted_iota(jnp.int32, (8, ln_gain.shape[0]), 0)
    vectors = jnp.where(number == 1, ln_bias.astype(f32)[None], ln_gain.astype(f32)[None])
    vectors = jnp.where(
        number == 2, dense_bias.astype(f32)[None] + fc2_bias.astype(f32)[None], vectors)
    tables = rotary_tables(segments)
    bias = jnp.pad(qkv_bias.astype(f32), ((0, 5), (0, 0)))
    w_qkv, w_dense, w_fc1, w_fc2, normed, grad_out, vec = gather_plain(*mine, vectors)
    gain, out_bias = vec[0:1], vec[2:3]
    query, key, value, attn_vec, probs = attend(
        *(matmul(normed, w_qkv[i]) for i in range(3)), bias, tables, segments, seqs
    )
    pre_act = matmul(normed, w_fc1) + fc1_bias.astype(f32)
    act_vals, gelu_pull = jax.vjp(lambda pre: jax.nn.gelu(pre, approximate=True), pre_act)
    act_vals = act_vals.astype(bf16)
    slope = gelu_pull(jnp.ones_like(pre_act))[0].astype(bf16)
    branches = matmul(attn_vec, w_dense) + matmul(act_vals, w_fc2)
    grad_attn = matmul(grad_out, w_dense.T).astype(bf16)
    *grads, qkv_sums = attend_back(query, key, value, grad_attn, attn_vec, probs, tables, seqs)
    resid_in = hidden_in.astype(f32)
    cot_float = cotangent.astype(f32)
    centred = resid_in - jnp.mean(resid_in, -1, keepdims=True)
    spread = jnp.mean(centred * centred, -1, keepdims=True)
    inv_std = lax.rsqrt(spread + layer_eps)
    unit_rows = centred * inv_std
    summed = lax.psum_scatter(branches.astype(bf16), "tensor", scatter_dimension=0, tiled=True)
    out = (resid_in + summed.astype(f32) + out_bias).astype(bf16)
    out_bias_part = jnp.sum(cot_float, 0)
    grad_fc2 = matmul(act_vals.T, grad_out)
    grad_dense = matmul(attn_vec.T, grad_out)
    grad_pre = (matmul(grad_out, w_fc2.T) * slope.astype(f32)).astype(bf16)
    fc1_bias_part = jnp.sum(grad_pre.astype(f32), 0)
    grad_fc1 = matmul(normed.T, grad_pre)
    grad_wqkv = jnp.stack([matmul(normed.T, g) for g in grads])
    grad_normed = matmul(grad_pre, w_fc1.T) + sum(matmul(g, w.T) for g, w in zip(grads, w_qkv))
    sent_qkv, sent_dense, sent_fc1, sent_fc2 = (
        lax.psum_scatter(grad_wqkv.astype(bf16), "dp", scatter_dimension=1, tiled=True),
        lax.psum_scatter(grad_dense.astype(bf16), "dp", scatter_dimension=1, tiled=True),
        lax.psum_scatter(grad_fc1.astype(bf16), "dp", scatter_dimension=0, tiled=True),
        lax.psum_scatter(grad_fc2.astype(bf16), "dp", scatter_dimension=1, tiled=True),
    )
    grad_local = lax.psum_scatter(
        grad_normed.astype(bf16), "tensor", scatter_dimension=0, tiled=True
    ).astype(f32)
    gain_part = jnp.sum(grad_local * unit_rows, 0)
    beta_part = jnp.sum(grad_local, 0)
    scaled_grad = grad_local * gain
    first_mean = jnp.mean(scaled_grad, -1, keepdims=True)
    second_mean = jnp.mean(scaled_grad * unit_rows, -1, keepdims=True)
    hidden_grad = (
        cot_float + inv_std * (scaled_grad - first_mean - unit_rows * second_mean)
    ).astype(bf16)
    gain_grad, beta_grad, out_bias_grad = (
        lax.psum_scatter(gain_part, ("dp", "tensor"), scatter_dimension=0, tiled=True),
        lax.psum_scatter(beta_part, ("dp", "tensor"), scatter_dimension=0, tiled=True),
        lax.psum_scatter(out_bias_part, ("dp", "tensor"), scatter_dimension=0, tiled=True),
    )
    qkv_bias_grad, fc1_bias_grad = lax.psum((qkv_sums[:3], fc1_bias_part), "dp")
    return (
        out,
        hidden_grad,
        gain_grad,
        beta_grad,
        sent_qkv.transpose(1, 0, 2).astype(f32),
        qkv_bias_grad,
        sent_dense.astype(f32),
        out_bias_grad,
        sent_fc1.astype(f32),
        fc1_bias_grad,
        sent_fc2.astype(f32),
        out_bias_grad,
    )


def solution(mesh):
    dp, tensor = mesh.shape["dp"], mesh.shape["tensor"]
    fast = dp == 8 and tensor == 4
    placed = (
        P(("dp", "tensor"), None),
        P("dp", None),
        P("dp"),
        P("dp"),
        P("dp", None, "tensor"),
        P(None, "tensor"),
        P("tensor", "dp"),
        P("dp"),
        P("dp", "tensor"),
        P("tensor"),
        P("tensor", "dp"),
        P("dp"),
        P(("dp", "tensor"), None),
    )
    return jax.shard_map(
        functools.partial(on_device, dp, tensor, fast),
        mesh=mesh,
        in_specs=placed,
        out_specs=(
            P(("dp", "tensor"), None),
            P(("dp", "tensor"), None),
            P(("dp", "tensor")),
            P(("dp", "tensor")),
            P("dp", None, "tensor"),
            P(None, "tensor"),
            P("tensor", "dp"),
            P(("dp", "tensor")),
            P("dp", "tensor"),
            P("tensor"),
            P("tensor", "dp"),
            P(("dp", "tensor")),
        ),
        check_vma=False,
    )
```

```python
import functools

import jax
import jax.numpy as jnp
from jax import lax
from jax.experimental import pallas as pl
from jax.experimental.pallas import tpu as pltpu
from jax.sharding import PartitionSpec as P

HD = 64
ROT = 32
BLOCK = 256
MAX_DOC = 512
VMEM_LIMIT = 66_000_000
MESH = pl.DeviceIdType.MESH
ANY = pl.BlockSpec(memory_space=pl.ANY)
VMEM = pl.BlockSpec(memory_space=pltpu.VMEM)

layer_eps = 1e-05
f32 = jnp.float32
bf16 = jnp.bfloat16


def dot_nn(a, b):
    return lax.dot_general(a, b, (((1,), (0,)), ((), ())), preferred_element_type=f32)


def dot_nt(a, b):
    return lax.dot_general(a, b, (((1,), (1,)), ((), ())), preferred_element_type=f32)


def dot_tn(a, b):
    return lax.dot_general(a, b, (((0,), (0,)), ((), ())), preferred_element_type=f32)


def flip(index, bit):
    step = 1 << bit
    return index + step * (1 - 2 * (lax.div(index, step) % 2))


def relative(index, offset):
    bit = 0
    while offset >> bit:
        if (offset >> bit) & 1:
            index = flip(index, bit)
        bit += 1
    return index


def stages_of(order):
    held, stages = [0], []
    for bit in order:
        got = [r ^ (1 << bit) for r in held]
        stages.append((bit, list(held), got))
        held = held + got
    return stages


class Sems:
    def __init__(self):
        self.count = 0

    def take(self):
        self.count += 1
        return self.count - 1


class CubeGather:
    def __init__(self, sems, orders):
        self.plans = [stages_of(order) for order in orders]
        self.ids = {
            (h, j, i): sems.take()
            for h, stages in enumerate(self.plans)
            for j, (_, held, _) in enumerate(stages)
            for i in range(len(held))
        }

    def bind(self, me, other, own, window, send_sem, recv_sem):
        self.me, self.other, self.own, self.window = me, other, own, window
        self.send_sem, self.recv_sem = send_sem, recv_sem
        return self

    def copy(self, h, j, i):
        bit, held, _ = self.plans[h][j]
        slot = relative(self.me, held[i])
        target = self.window(slot, h)
        source = self.own(h) if held[i] == 0 else target
        k = self.ids[h, j, i]
        return pltpu.make_async_remote_copy(
            src_ref=source,
            dst_ref=target,
            send_sem=self.send_sem.at[k],
            recv_sem=self.recv_sem.at[k],
            device_id=(flip(self.me, bit), self.other),
            device_id_type=MESH,
        )

    def start(self):
        depth = len(self.plans[0])
        for j in range(depth):
            for h in range(len(self.plans)):
                self.copy(h, j, 0).start()

    def advance(self, j, some=slice(None)):
        for i in range(len(self.plans[0][j][1]))[some]:
            for h, stages in enumerate(self.plans):
                self.copy(h, j, i).wait_recv()
                slot = stages[j][2][i]
                for later in range(j + 1, len(stages)):
                    self.copy(h, later, stages[later][1].index(slot)).start()

    def finish(self):
        for h, j, i in self.ids:
            self.copy(h, j, i).wait_send()


class LineGather:
    def __init__(self, sems, size, subs):
        self.size, self.subs = size, subs
        self.ids = {
            (way, s, u): sems.take()
            for way in (0, 1)
            for s in range(size - 1)
            for u in range(subs)
        }

    def bind(self, me, other, own, window, send_sem, recv_sem):
        self.me, self.other, self.own, self.window = me, other, own, window
        self.send_sem, self.recv_sem = send_sem, recv_sem
        return self

    def copy(self, way, s, u):
        block = self.me - s if way == 0 else self.me + s
        target = self.window(block, u)
        k = self.ids[way, s, u]
        return pltpu.make_async_remote_copy(
            src_ref=self.own(u) if s == 0 else target,
            dst_ref=target,
            send_sem=self.send_sem.at[k],
            recv_sem=self.recv_sem.at[k],
            device_id=(self.other, self.me + 1 if way == 0 else self.me - 1),
            device_id_type=MESH,
        )

    def sends(self, way, s):
        if way == 0:
            return (self.me >= s) & (self.me < self.size - 1)
        return (self.me + s < self.size) & (self.me > 0)

    def gets(self, way, s):
        if way == 0:
            return self.me - 1 - s >= 0
        return self.me + 1 + s < self.size

    def start(self, u):
        for way in (0, 1):

            @pl.when(self.sends(way, 0))
            def _():
                self.copy(way, 0, u).start()

    def advance(self, s, u):
        for way in (0, 1):

            @pl.when(self.gets(way, s))
            def _():
                self.copy(way, s, u).wait_recv()

            if s + 1 < self.size - 1:

                @pl.when(self.sends(way, s + 1))
                def _():
                    self.copy(way, s + 1, u).start()

    def finish(self):
        for way, s, u in self.ids:

            @pl.when(self.sends(way, s))
            def _():
                self.copy(way, s, u).wait_send()


def greet(dp, me, tensor, line, meanwhile):
    barrier = pltpu.get_barrier_semaphore()
    for r in range(1, dp):
        pl.semaphore_signal(barrier, inc=1, device_id=(relative(me, r), line), device_id_type=MESH)
    for k in range(1, tensor):
        to = (me, lax.rem(line + k, tensor))
        pl.semaphore_signal(barrier, inc=1, device_id=to, device_id_type=MESH)
    meanwhile()
    pl.semaphore_wait(barrier, dp + tensor - 2)


def orders_of(dp):
    bits = list(range(1, dp.bit_length() - 1))
    return [bits + [0], bits[::-1] + [0]]


def normalize(x, gain, bias):
    centred = x - jnp.mean(x, -1, keepdims=True)
    spread = jnp.mean(centred * centred, -1, keepdims=True)
    unit = centred * lax.rsqrt(spread + layer_eps)
    return (unit * gain + bias).astype(bf16)


def gather_plain(hidden, cotangent, w_qkv, w_dense, w_fc1, w_fc2, vectors):
    vec = lax.all_gather(vectors, "dp", axis=1, tiled=True)
    normed = normalize(hidden.astype(f32), vec[0:1], vec[1:2])
    return (
        lax.all_gather(w_qkv, "dp", axis=1, tiled=True),
        lax.all_gather(w_dense, "dp", axis=1, tiled=True),
        lax.all_gather(w_fc1, "dp", axis=0, tiled=True),
        lax.all_gather(w_fc2, "dp", axis=1, tiled=True),
        lax.all_gather(normed, "tensor", axis=0, tiled=True),
        lax.all_gather(cotangent, "tensor", axis=0, tiled=True),
        vec,
    )


class ChipReduce:
    COUNT = 6

    def __init__(self, sems):
        self.ids = [sems.take() for _ in range(self.COUNT)]

    def bind(self, me, other, view, landing, stage, stage_sem, send_sem, recv_sem):
        self.me, self.other, self.view, self.landing = me, other, view, landing
        self.stage, self.stage_sem = stage, stage_sem
        self.send_sem, self.recv_sem = send_sem, recv_sem
        return self

    def copy(self, slot):
        r, h, bit = [(2, 0, 2), (3, 0, 2), (1, 0, 1), (1, 1, 1), (3, 1, 1), (2, 1, 2)][slot]
        k = self.ids[slot]
        return pltpu.make_async_remote_copy(
            src_ref=self.view(r, h),
            dst_ref=self.landing.at[slot],
            send_sem=self.send_sem.at[k],
            recv_sem=self.recv_sem.at[k],
            device_id=(flip(self.me, bit), self.other),
            device_id_type=MESH,
        )

    def start(self, r):
        for slot in {3: (1, 4), 2: (0,), 1: (3,), 0: ()}[r]:
            self.copy(slot).start()

    def fetch(self, slots):
        half = self.landing.shape[-1]
        held = [self.stage.at[k, :, pl.ds(0, half)] for k in range(len(slots))]
        copies = []
        for k, slot in enumerate(slots):
            self.copy(slot).wait_recv()
            copies.append(
                pltpu.make_async_copy(self.landing.at[slot], held[k], self.stage_sem.at[k]))
            copies[k].start()
        for copy in copies:
            copy.wait()
        return held

    def middle(self):
        held = self.fetch((1, 4))
        for k, (r, h, last) in enumerate(((1, 0, 2), (2, 1, 5))):
            view = self.view(r, h)
            view[...] = (view[...].astype(f32) + held[k][...].astype(f32)).astype(bf16)
            self.copy(last).start()

    def final(self):
        for h, slots in ((0, (0, 2)), (1, (3, 5))):
            a, b = self.fetch(slots)
            view = self.view(0, h)
            total = view[...].astype(f32) + a[...].astype(f32) + b[...].astype(f32)
            view[...] = total.astype(bf16)

    def finish(self):
        for slot in range(self.COUNT):
            self.copy(slot).wait_send()


class LineReduce:
    def __init__(self, sems, size):
        self.size = size
        self.ids = {(way, i): sems.take() for way in (0, 1) for i in range(size - 1)}

    def bind(self, me, other, own, landing, stage, last, stage_sem, send_sem, recv_sem):
        self.me, self.other, self.own, self.landing = me, other, own, landing
        self.stage, self.last, self.stage_sem = stage, last, stage_sem
        self.send_sem, self.recv_sem = send_sem, recv_sem
        return self

    def target(self, way, i):
        return self.size - 1 - i if way == 0 else i

    def place(self, way, i):
        return i if way == 0 else 2 * self.size - 4 - i

    def buffer(self, way, i):
        return self.stage.at[i if way == 0 else self.size - 2 - i]

    def copy(self, way, i, edge):
        k = self.ids[way, i]
        return pltpu.make_async_remote_copy(
            src_ref=self.own(self.target(way, i)) if edge else self.buffer(way, i),
            dst_ref=self.landing.at[self.place(way, i)],
            send_sem=self.send_sem.at[k],
            recv_sem=self.recv_sem.at[k],
            device_id=(self.other, self.me + 1 if way == 0 else self.me - 1),
            device_id_type=MESH,
        )

    def edge(self, way):
        return self.me == (0 if way == 0 else self.size - 1)

    def passes(self, way, i):
        d = self.target(way, i)
        return (self.me > 0) & (self.me < d) if way == 0 else (self.me < self.size - 1) & (self.me > d)

    def start(self, way, i):
        @pl.when(self.edge(way))
        def _():
            self.copy(way, i, True).start()

    def advance(self, step):
        for way in (0, 1):
            steps_from_edge = self.me if way == 0 else self.size - 1 - self.me
            for i in range(step):

                @pl.when(self.passes(way, i) & (steps_from_edge == step - i))
                def _():
                    self.copy(way, i, False).wait_recv()
                    held = self.buffer(way, i)
                    fetch = pltpu.make_async_copy(
                        self.landing.at[self.place(way, i)], held, self.stage_sem.at[0])
                    fetch.start()
                    fetch.wait()
                    add_into(held, self.own(self.target(way, i)))
                    self.copy(way, i, False).start()

    def settle(self):
        for way, i in self.ids:

            @pl.when(self.edge(way))
            def _():
                self.copy(way, i, True).wait_send()

            @pl.when(self.passes(way, i))
            def _():
                self.copy(way, i, False).wait_send()

    def arrive(self):
        def fetch(way, i):
            return pltpu.make_async_copy(
                self.landing.at[self.place(way, i)], self.last(way), self.stage_sem.at[way])

        for way, i in self.ids:

            @pl.when(self.me == self.target(way, i))
            def _():
                self.copy(way, i, False).wait_recv()
                fetch(way, i).start()

        for way, i in self.ids:

            @pl.when(self.me == self.target(way, i))
            def _():
                fetch(way, i).wait()

    def total(self, own, rows):
        value = own.astype(f32)
        for way, there in ((0, self.me > 0), (1, self.me < self.size - 1)):
            value = value + jnp.where(there, self.last(way)[rows, :].astype(f32), 0.0)
        return value


def add_into(landing, own):
    rows = landing.shape[0]

    @pl.loop(0, rows, step=64)
    def _(r):
        at = pl.ds(r, 64)
        landing[at, :] = (landing[at, :].astype(f32) + own[at, :].astype(f32)).astype(bf16)


def chip_slot(me, r):
    return (
        me
        + 2 * ((r % 2) * (1 - 2 * (lax.div(me, 2) % 2)))
        + 4 * (lax.div(r, 2) * (1 - 2 * (lax.div(me, 4) % 2)))
    )


def spans_of(length):
    back = -(-(MAX_DOC - 1) // BLOCK)
    spans, at = [], 0
    for i in range(length // BLOCK):
        low = max(0, i - back) * BLOCK
        spans.append((low, (i + 1) * BLOCK, at))
        at += (i + 1) * BLOCK - low
    return spans, at


def turn(x, cosine, sine_lo, sine_hi):
    return x * cosine + pltpu.roll(x, 128 - ROT // 2, 1) * sine_lo + pltpu.roll(x, ROT // 2, 1) * sine_hi


def head_lanes(shape, e):
    lane = lax.broadcasted_iota(jnp.int32, shape, 1)
    return (lane >= e * HD) & (lane < (e + 1) * HD)


def only(x, e):
    return jnp.where(head_lanes(x.shape, e), x, jnp.zeros_like(x))


def attend_kernel(
    q_ref, k_ref, v_ref, bias_ref, cos_ref, slo_ref, shi_ref, segc_ref, segr_ref,
    qs_ref, ks_ref, vs_ref, o_ref, p_ref, mask_ref,
):
    @pl.when(pl.program_id(1) == 0)
    def _():
        fill_mask(mask_ref, segc_ref, segr_ref, q_ref.shape[0])

    cosine, slo, shi = cos_ref[...], slo_ref[...], shi_ref[...]
    query = turn(q_ref[...] + bias_ref[0:1, :], cosine, slo, shi).astype(bf16) * bf16(HD**-0.5)
    key = turn(k_ref[...] + bias_ref[1:2, :], cosine, slo, shi).astype(bf16)
    value = (v_ref[...] + bias_ref[2:3, :]).astype(bf16)
    qs_ref[...] = query
    ks_ref[...] = key
    vs_ref[...] = value

    def keep(e, at, probs):
        p_ref[e, at, :] = probs

    def write(at, result):
        o_ref[at, :] = result

    attend_pair(query, key, value, mask_ref, keep, write)


def attend(q, k, v, qkv_bias, tables, segments, rows):
    tokens, local = q.shape
    length = tokens // rows
    pairs = local // 128
    _, stored = spans_of(length)
    block = pl.BlockSpec((length, 128), lambda r, h: (r, h))
    table = pl.BlockSpec((length, 128), lambda r, h: (r, 0))
    shape = jax.ShapeDtypeStruct((tokens, local), bf16)
    return pl.pallas_call(
        attend_kernel,
        grid=(rows, pairs),
        out_shape=(shape,) * 4 + (jax.ShapeDtypeStruct((rows, local // HD, stored, BLOCK), bf16),),
        in_specs=[block] * 3
        + [pl.BlockSpec((8, 128), lambda r, h: (0, h))]
        + [table] * 3
        + [
            pl.BlockSpec((length, 1), lambda r, h: (r, 0)),
            pl.BlockSpec((pl.Squeezed(), 1, length), lambda r, h: (r, 0, 0)),
        ],
        out_specs=(block,) * 4
        + (pl.BlockSpec((pl.Squeezed(), 128 // HD, stored, BLOCK), lambda r, h: (r, h, 0, 0)),),
        scratch_shapes=[pltpu.VMEM((stored, BLOCK), f32)],
        compiler_params=pltpu.CompilerParams(vmem_limit_bytes=VMEM_LIMIT),
        cost_estimate=pl.CostEstimate(
            flops=16 * tokens * 768 * local, bytes_accessed=24 << 20, transcendentals=0
        ),
        name="attend",
    )(q, k, v, qkv_bias, *tables, segments.reshape(tokens, 1), segments.reshape(rows, 1, length))


def attend_back_kernel(
    q_ref, k_ref, v_ref, g_ref, o_ref, p_ref, cos_ref, slo_ref, shi_ref,
    dq_ref, dk_ref, dv_ref, bias_ref, kacc_ref, vacc_ref,
):
    def write(which, at, value):
        (dq_ref, dk_ref, dv_ref)[which][at, :] = value

    sums = attend_back_pair(
        q_ref[...], k_ref[...], v_ref[...], g_ref[...], o_ref[...],
        lambda e, at: p_ref[e, at, :], (cos_ref, slo_ref, shi_ref), kacc_ref, vacc_ref, write)
    sums = jnp.concatenate(list(sums) + [jnp.zeros((5, 128), f32)], 0)

    @pl.when(pl.program_id(1) == 0)
    def _():
        bias_ref[...] = sums

    @pl.when(pl.program_id(1) > 0)
    def _():
        bias_ref[...] += sums


def attend_back(q, k, v, g, o, probs, tables, rows):
    tokens, local = q.shape
    length = tokens // rows
    pairs = local // 128
    stored = probs.shape[2]
    block = pl.BlockSpec((length, 128), lambda h, r: (r, h))
    table = pl.BlockSpec((length, 128), lambda h, r: (r, 0))
    shape = jax.ShapeDtypeStruct((tokens, local), bf16)
    return pl.pallas_call(
        attend_back_kernel,
        grid=(pairs, rows),
        out_shape=(shape,) * 3 + (jax.ShapeDtypeStruct((8, local), f32),),
        in_specs=[block] * 5
        + [pl.BlockSpec((pl.Squeezed(), 128 // HD, stored, BLOCK), lambda h, r: (r, h, 0, 0))]
        + [table] * 3,
        out_specs=(block,) * 3 + (pl.BlockSpec((8, 128), lambda h, r: (0, h)),),
        scratch_shapes=[pltpu.VMEM((length, 128), f32)] * 2,
        compiler_params=pltpu.CompilerParams(vmem_limit_bytes=VMEM_LIMIT),
        cost_estimate=pl.CostEstimate(
            flops=32 * tokens * 768 * local, bytes_accessed=24 << 20, transcendentals=0
        ),
        name="attend_back",
    )(q, k, v, g, o, probs, *tables)


def attend_pair(query, key, value, mask_ref, keep, write):
    length = query.shape[0]
    spans, _ = spans_of(length)
    for i, (low, high, at) in enumerate(spans):
        mine = slice(i * BLOCK, (i + 1) * BLOCK)
        total = jnp.zeros((BLOCK, 128), f32)
        for e in range(128 // HD):
            scores = dot_nt(only(key[low:high], e), query[mine]) + mask_ref[at : at + high - low, :].astype(f32)
            exponent = jnp.exp(scores - jnp.max(scores, 0, keepdims=True))
            inverse = 1.0 / jnp.sum(exponent, 0, keepdims=True)
            probs = (exponent * inverse).astype(bf16)
            keep(e, slice(at, at + high - low), probs)
            total = total + dot_tn(probs, only(value[low:high], e))
        write(mine, total.astype(bf16))


def fill_mask(mask_ref, segc_ref, segr_ref, length):
    for i, (low, high, at) in enumerate(spans_of(length)[0]):
        keys = lax.broadcasted_iota(jnp.int32, (high - low, BLOCK), 0) + low
        queries = lax.broadcasted_iota(jnp.int32, (high - low, BLOCK), 1) + i * BLOCK
        own = segr_ref[:, i * BLOCK : (i + 1) * BLOCK].astype(f32)
        same = segc_ref[low:high, 0:1].astype(f32) == own
        allowed = jnp.where((keys <= queries) & same, 0.0, -1e30)
        mask_ref[at : at + high - low, :] = allowed.astype(mask_ref.dtype)


def fill_tables(seg_ref, column_ref, cos_ref, slo_ref, shi_ref):
    length = seg_ref.shape[1]
    row = seg_ref[...].astype(f32)
    column_ref[...] = jnp.broadcast_to(row, (128, length)).T
    starts = [jnp.sum(jnp.where(row < number, 1.0, 0.0), 1, keepdims=True) for number in range(1, 4)]
    lane = lax.broadcasted_iota(jnp.int32, (1, 128), 1) % HD
    exponent = (2 * (lane % (ROT // 2))).astype(f32) / ROT
    frequency = 1.0 / jnp.exp(exponent * f32(9.210340371976184))

    @pl.loop(0, length, step=128)
    def _(r):
        at = pl.ds(pl.multiple_of(r, 128), 128)
        column = column_ref[at, :]
        start = jnp.zeros_like(column)
        for number in range(1, 4):
            start = jnp.where(column == number, starts[number - 1], start)
        index = (lax.broadcasted_iota(jnp.int32, (128, 128), 0) + r).astype(f32)
        angle = (index - start) * frequency
        cosine, sine = jnp.cos(angle), jnp.sin(angle)
        cos_ref[at, :] = jnp.where(lane < ROT, cosine, 1.0)
        slo_ref[at, :] = jnp.where(lane < ROT // 2, -sine, 0.0)
        shi_ref[at, :] = jnp.where((lane >= ROT // 2) & (lane < ROT), sine, 0.0)


def attend_back_pair(query, key, value, grad, result, probs_of, tables, kacc_ref, vacc_ref, write):
    length = query.shape[0]
    spans, _ = spans_of(length)
    heads = 128 // HD
    inner = grad.astype(f32) * result.astype(f32)
    lane = lax.broadcasted_iota(jnp.int32, (8, 128), 1)
    row = lax.broadcasted_iota(jnp.int32, (8, 128), 0)
    pick = jnp.where(lax.div(lane, HD) == row, 1.0, 0.0)
    delta = lax.dot_general(
        pick, inner, (((1,), (1,)), ((), ())),
        precision=lax.Precision.HIGHEST, preferred_element_type=f32)
    kacc_ref[...] = jnp.zeros_like(kacc_ref)
    vacc_ref[...] = jnp.zeros_like(vacc_ref)
    cos_ref, slo_ref, shi_ref = tables
    first = jnp.zeros((1, 128), f32)
    for i, (low, high, at) in enumerate(spans):
        mine = slice(i * BLOCK, (i + 1) * BLOCK)
        g_i, q_i = grad[mine], query[mine]
        dq = jnp.zeros((BLOCK, 128), f32)
        ps, dss = [], []
        for e in range(heads):
            probs = probs_of(e, slice(at, at + high - low))
            dprobs = dot_nt(only(value[low:high], e), g_i)
            ds = (probs.astype(f32) * (dprobs - delta[e : e + 1, mine])).astype(bf16)
            dq = dq + dot_tn(ds, only(key[low:high], e))
            ps.append(probs)
            dss.append(ds)
        g_cat = jnp.concatenate([only(g_i, e) for e in range(heads)], 0)
        q_cat = jnp.concatenate([only(q_i, e) for e in range(heads)], 0)
        vacc_ref[low:high, :] += dot_nn(jnp.concatenate(ps, 1), g_cat)
        kacc_ref[low:high, :] += dot_nn(jnp.concatenate(dss, 1), q_cat)
        dq = dq * f32(HD**-0.5)
        dq = turn(dq, cos_ref[mine, :], -slo_ref[mine, :], -shi_ref[mine, :]).astype(bf16)
        write(0, mine, dq)
        first = first + jnp.sum(dq.astype(f32), 0, keepdims=True)
    everything = slice(0, length)
    dk = turn(kacc_ref[...], cos_ref[...], -slo_ref[...], -shi_ref[...]).astype(bf16)
    dv = vacc_ref[...].astype(bf16)
    write(1, everything, dk)
    write(2, everything, dv)
    return first, jnp.sum(dk.astype(f32), 0, keepdims=True), jnp.sum(dv.astype(f32), 0, keepdims=True)


def block_call(dp, tensor, arrays):
    hidden, cotangent, w_qkv, w_dense, w_fc1, w_fc2 = arrays[:6]
    rows, width = hidden.shape
    local = w_qkv.shape[2]
    wide = 3 * local
    units = w_fc1.shape[1]
    part = width // dp
    chips = dp // 2
    tokens = rows * tensor
    pairs = local // 128
    stored = spans_of(tokens)[1]
    sems = Sems()
    orders = orders_of(dp)
    vec_ids = [sems.take() for _ in range(dp - 1)]
    plan_qkv, plan_dense, plan_fc1, plan_fc2 = (CubeGather(sems, orders) for _ in range(4))
    plan_n, plan_c = LineGather(sems, tensor, 2), LineGather(sems, tensor, 2)
    line_out, line_in = LineReduce(sems, tensor), LineReduce(sems, tensor)
    reduce_fc2, reduce_dense, reduce_fc1, reduce_qkv = (ChipReduce(sems) for _ in range(4))
    swaps = [sems.take() for _ in range(2 * chips + 4)]
    tells = [sems.take() for _ in range(2 * (dp - 1) + tensor - 1)]

    def kernel(
        x_ref, c_ref, wq_ref, wd_ref, w1_ref, w2_ref, gain_ref, beta_ref, bd_ref, b2_ref,
        qb_ref, fb_ref, seg_ref,
        out_ref, hid_ref, s2_out, sd_out, s1_out, sq_out,
        gq_ref, g1_ref, g2_ref, x_out, n_out, nx_out, ax_out, gqx_out, gpx_out,
        land_out, land_in, land_2, land_d, land_1, land_q, vout_ref, bout_ref,
        x_buf, vec_buf, nv, wa, wb, wd, act, slope, qkv3, abuf, pb, mask, cbuf, xbuf,
        kacc, vacc, cos_ref, slo_ref, shi_ref, line_stage, chip_stage,
        fsum, bsum, parts, tell_v, tell_b, tell_z, vec_ref,
        send_sem, recv_sem, local_sem, stage_sem,
    ):
        me, line = lax.axis_index("dp"), lax.axis_index("tensor")
        twin = flip(me, 0)
        half = part // 2
        local_count = [0]
        attn = abuf.at[:, pl.ds(0, local)]

        def cols(a):
            return pl.ds(pl.multiple_of(a * part, part), part)

        def half_rows(a, h):
            return pl.ds(pl.multiple_of(a * part + h * half, half), half)

        def tok(b, u):
            return pl.ds(pl.multiple_of(b * rows + u * (rows // 2), rows // 2), rows // 2)

        def block(b):
            return pl.ds(pl.multiple_of(b * rows, rows), rows)

        def piece(n, h):
            return pl.ds(h * (n // 2), n // 2)

        def copy_of(a, b):
            local_count[0] += 1
            return pltpu.make_async_copy(a, b, local_sem.at[local_count[0] - 1])

        def remote(k, source, target, device):
            return pltpu.make_async_remote_copy(
                src_ref=source, dst_ref=target,
                send_sem=send_sem.at[k], recv_sem=recv_sem.at[k],
                device_id=device, device_id_type=MESH)

        def to_twin(k, source, target):
            return remote(swaps[k], source, target, (twin, line))

        pair = (send_sem, recv_sem)
        vec = [
            remote(k, vec_ref, vec_buf.at[:, cols(me)], (relative(me, r), line))
            for r, k in enumerate(vec_ids, 1)
        ]
        qkv = plan_qkv.bind(
            me, line,
            lambda h: wq_ref.at[:, pl.ds(h * half, half), :],
            lambda a, h: gq_ref.at[:, half_rows(a, h), :], *pair)
        fc1 = plan_fc1.bind(
            me, line,
            lambda h: w1_ref.at[pl.ds(h * half, half), :],
            lambda a, h: g1_ref.at[half_rows(a, h), :], *pair)
        dense = plan_dense.bind(
            me, line,
            lambda h: wd_ref.at[piece(local, h), :],
            lambda a, h: wd.at[piece(local, h), cols(a)], *pair)
        fc2 = plan_fc2.bind(
            me, line,
            lambda h: w2_ref.at[piece(units, h), :],
            lambda a, h: g2_ref.at[piece(units, h), cols(a)], *pair)
        norm = plan_n.bind(
            line, me, lambda u: x_ref.at[piece(rows, u)], lambda b, u: pb.at[tok(b, u)], *pair)
        cot = plan_c.bind(
            line, me, lambda u: c_ref.at[piece(rows, u)], lambda b, u: cbuf.at[tok(b, u)], *pair)
        staged = (stage_sem, *pair)

        def lasts(way):
            return wd.at[pl.ds(way * rows, rows), :]

        outs = line_out.bind(
            line, me, lambda d: nv.at[pl.ds(d * rows, rows), :], land_out, line_stage, lasts, *staged)
        ins = line_in.bind(
            line, me, lambda d: act.at[pl.ds(d * rows, rows), :], land_in, line_stage, lasts, *staged)
        low, high = pl.ds(0, tokens), pl.ds(tokens, tokens)
        sum_2 = reduce_fc2.bind(
            me, line,
            lambda r, h: wa.at[pl.ds(tokens + r * part, part), piece(units, h)],
            land_2, chip_stage, *staged)
        sum_d = reduce_dense.bind(
            me, line,
            lambda r, h: mask.at[pl.ds((2 * r + h) * part, part), :],
            land_d, chip_stage, *staged)
        sum_1 = reduce_fc1.bind(
            me, line,
            lambda r, h: wb.at[pl.ds(r * part, part), piece(units, h)],
            land_1, chip_stage, *staged)
        sum_q = reduce_qkv.bind(
            me, line,
            lambda r, h: abuf.at[pl.ds(r * part, part), piece(wide, h)],
            land_q, chip_stage, *staged)
        stages = dp.bit_length() - 1

        takes = [
            copy_of(x_ref, x_buf),
            copy_of(wd_ref, wd.at[:, cols(me)]),
            copy_of(c_ref, cbuf.at[block(line), :]),
            copy_of(wq_ref, qkv3.at[:, pl.ds(0, part), :]),
            copy_of(w1_ref, act.at[pl.ds(0, part), :]),
            copy_of(w2_ref, wb.at[:, pl.ds(0, part)]),
            copy_of(x_ref, pb.at[block(line), :]),
        ]
        keeps = [
            copy_of(qkv3.at[:, pl.ds(0, part), :], gq_ref.at[:, cols(me), :]),
            copy_of(act.at[pl.ds(0, part), :], g1_ref.at[cols(me), :]),
            copy_of(wb.at[:, pl.ds(0, part)], g2_ref.at[:, cols(me)]),
        ]
        takes[0].start()
        for k, ref in enumerate((gain_ref, beta_ref, bd_ref)):
            vec_ref[k : k + 1, :] = ref[...].astype(f32).reshape(1, part)
        vec_ref[2:3, :] += b2_ref[...].astype(f32).reshape(1, part)
        vec_buf[:, cols(me)] = vec_ref[...]
        parts[0:1, :] = fb_ref[...].astype(f32).reshape(1, units)
        greet(
            dp, me, tensor, line,
            lambda: fill_tables(seg_ref, kacc, cos_ref, slo_ref, shi_ref))
        for copy in vec:
            copy.start()
        norm.start(0)
        norm.start(1)
        qkv.start()
        for copy in takes[1:]:
            copy.start()
        takes[0].wait()
        for copy in vec:
            copy.wait_recv()
        qkv.advance(0)
        fc1.start()
        for take, copy in zip(takes[3:6], keeps):
            take.wait()
            copy.start()
        fill_mask(mask, kacc, seg_ref, tokens)

        def project(b):
            at = block(b)

            @pl.loop(0, rows, step=32)
            def _(r):
                some = pl.ds(pl.multiple_of(b * rows + r, 32), 32)
                x = pb[some, :].astype(f32)
                centred = x - jnp.mean(x, -1, keepdims=True)
                spread = jnp.mean(centred * centred, -1, keepdims=True)
                unit = centred * lax.rsqrt(spread + layer_eps)
                nv[some, :] = (unit * vec_buf[0:1, :] + vec_buf[1:2, :]).astype(bf16)

            cosine, slo, shi = cos_ref[at, :], slo_ref[at, :], shi_ref[at, :]
            for i in range(3):
                value = dot_nn(nv[at, :], wa[:, i * local : (i + 1) * local])
                value = value + qb_ref[i : i + 1, :].astype(f32)
                if i == 2:
                    qkv3[2, at, :] = value.astype(bf16)
                    continue
                for h in range(pairs):
                    lanes = slice(h * 128, (h + 1) * 128)
                    turned = turn(value[:, lanes], cosine, slo, shi).astype(bf16)
                    if i == 0:
                        turned = turned * bf16(HD**-0.5)
                    qkv3[i, at, lanes] = turned

        def hidden_layer(b, first):
            at = block(b)

            @pl.loop(0, units, step=512)
            def _(n):
                @pl.when(first & (n == units // 2))
                def _():
                    load_1[1].wait()

                to = pl.ds(pl.multiple_of(n, 512), 512)
                pre = dot_nn(nv[at, :], wb[:, to]) + parts[0:1, to]
                square = pre * pre
                bend = jnp.tanh(0.7978845608028654 * pre * (1.0 + 0.044715 * square))
                act[at, to] = (0.5 * pre * (1.0 + bend)).astype(bf16)
                rise = 0.7978845608028654 * (1.0 + 3 * 0.044715 * square)
                slope[at, to] = (
                    0.5 * (1.0 + bend) + 0.5 * pre * (1.0 - bend * bend) * rise
                ).astype(bf16)

        def slope_layer(b):
            at = block(b)
            abuf[at, pl.ds(local, local)] = dot_nt(cbuf[at, :], wd[...]).astype(bf16)

            @pl.loop(0, units, step=1024)
            def _(n):
                to = pl.ds(pl.multiple_of(n, 1024), 1024)
                value = dot_nt(cbuf[at, :], wa[to, :]) * slope[at, to].astype(f32)
                value = value.astype(bf16)
                slope[at, to] = value
                fsum[0:1, to] += jnp.sum(value.astype(f32), 0, keepdims=True)

        def blocks_of(s, task):
            @pl.loop(0, 2)
            def _(way):
                b = line + (2 * way - 1) * (1 + s)

                @pl.when((b >= 0) & (b < tensor) & ((s >= 0) | (way == 0)))
                def _():
                    task(b)

        norm.advance(0, 0)
        norm.advance(0, 1)
        for j in range(1, stages):
            qkv.advance(j)
        keeps[0].wait()
        load_q = [
            copy_of(gq_ref.at[i], wa.at[:, pl.ds(i * local, local)]) for i in range(3)
        ]
        for copy in load_q:
            copy.start()
        fc1.advance(0)
        dense.start()
        fc2.start()
        for copy in load_q + [takes[6]]:
            copy.wait()
        for s in range(1, tensor - 2):
            norm.advance(s, 0)
            norm.advance(s, 1)
        cot.start(0)
        cot.start(1)

        @pl.loop(-1, tensor - 2)
        def _(s):
            blocks_of(s, project)

        for j in range(1, stages):
            fc1.advance(j)
        for copy in keeps[1:]:
            copy.wait()
        load_1 = [copy_of(g1_ref.at[:, piece(units, h)], wb.at[:, piece(units, h)]) for h in (0, 1)]
        load_1[0].start()
        load_1[0].wait()
        load_1[1].start()

        x_store = copy_of(pb.at[low, :], x_out)

        @pl.loop(-1, tensor - 1)
        def _(s):
            @pl.when(s == tensor - 2)
            def _():
                norm.advance(tensor - 2, 0)
                norm.advance(tensor - 2, 1)
                x_store.start()
                fc2.advance(0)
                blocks_of(tensor - 2, project)

            @pl.when(s == 0)
            def _():
                dense.advance(0)

            blocks_of(s, lambda b: hidden_layer(b, s == -1))

        n_store = copy_of(nv, n_out)
        n_store.start()
        cross_n = [
            to_twin(r, nv.at[:, cols(relative(twin, r << 1))], nx_out.at[r]) for r in range(chips)
        ]
        cross_a = to_twin(chips, act, ax_out)
        for copy in cross_n + [cross_a]:
            copy.start()
        norm.finish()
        x_store.wait()

        def prob_lanes(h, e):
            return pl.ds(pl.multiple_of((2 * h + e) * BLOCK, BLOCK), BLOCK)

        @pl.loop(0, pairs)
        def _(h):
            lanes = pl.ds(pl.multiple_of(h * 128, 128), 128)

            def keep(e, at, value):
                pb[at, prob_lanes(h, e)] = value

            def write(at, value):
                abuf[at, lanes] = value

            attend_pair(
                qkv3[0, :, lanes], qkv3[1, :, lanes], qkv3[2, :, lanes], mask, keep, write)

            @pl.when(h == 0)
            def _():
                cot.advance(0, 0)
                cot.advance(0, 1)

            @pl.when(h == 1)
            def _():
                for j in range(1, stages - 1):
                    dense.advance(j)

            @pl.when(h == 2)
            def _():
                fc2.advance(1, slice(0, 1))

        cross_t = to_twin(chips + 1, attn, xbuf.at[:, pl.ds(chips * part, local)])
        cross_t.start()
        fc2.advance(1, slice(1, None))
        for j in range(2, stages - 1):
            fc2.advance(j)
        dense.advance(stages - 1)
        fc2.advance(stages - 1)
        takes[1].wait()
        takes[2].wait()
        load_2 = [copy_of(g2_ref.at[:, piece(width, h)], wa.at[:, piece(width, h)]) for h in (0, 1)]
        load_2[0].start()
        cot.advance(1, 0)
        n_store.wait()
        for copy in cross_n:
            copy.wait_send()
        load_2[0].wait()
        load_2[1].start()
        upper = lax.div(line, tensor // 2)

        def outward(i):
            return (1 - upper) * (tensor - 1 - i) + upper * i

        @pl.loop(0, tensor)
        def _(i):
            at = block(outward(i))

            @pl.loop(0, width, step=1024)
            def _(n):
                @pl.when((i == 0) & (n > 0))
                def _():
                    load_2[1].wait()

                to = pl.ds(pl.multiple_of(n, 1024), 1024)
                value = dot_nn(act[at, :], wa[:, to]) + dot_nn(attn[at, :], wd[:, to])
                nv[at, to] = value.astype(bf16)

            for k in range(tensor - 1):

                @pl.when(i == k)
                def _():
                    outs.start(0, k)
                    outs.start(1, k)

            @pl.when(i == tensor - 2)
            def _():
                cot.advance(1, 1)

        cross_a.wait_recv()
        load_ax = copy_of(ax_out, wb.at[low, :])
        load_ax.start()
        fsum[...] = jnp.zeros_like(fsum)
        cross_c = [
            to_twin(chips + 2 + r, cbuf.at[:, cols(relative(twin, r << 1))],
                    xbuf.at[:, pl.ds(r * part, part)])
            for r in range(chips)
        ]

        @pl.loop(-1, tensor - 1)
        def _(s):
            @pl.when(s == tensor - 2)
            def _():
                cot.advance(tensor - 2, 0)
                outs.advance(1)
                cot.advance(tensor - 2, 1)
                for copy in cross_c:
                    copy.start()

            blocks_of(s, slope_layer)

        cross_p = to_twin(2 * chips + 3, slope, gpx_out)
        cross_p.start()
        for copy in cross_c + [cross_t]:
            copy.wait_recv()
        load_ax.wait()
        dense.finish()

        def weight_grad(left, plan, own, crossed, spot, size, step, hook=None, second=None):
            @pl.loop(0, chips)
            def _(i):
                r = chips - 1 - i
                slot = chip_slot(me, r)
                across = pl.ds(pl.multiple_of(r * part, part), part)

                @pl.loop(0, size, step=step)
                def _(n):
                    if second is not None:

                        @pl.when((i == 0) & (n == step))
                        def _():
                            second.wait()

                    at = pl.multiple_of(n, step)
                    value = dot_tn(left(cols(slot)), own(at)) + dot_tn(xbuf[:, across], crossed(at))
                    spot(r, at, value.astype(bf16))

                for k in range(1, chips):

                    @pl.when(r == k)
                    def _():
                        plan.start(k)

                if hook is not None:
                    hook(i)

        def spot_a(r, at, value):
            wa[pl.ds(pl.multiple_of(tokens + r * part, part), part), pl.ds(at, 1024)] = value

        def spot_d(r, at, value):
            for h in (0, 1):
                to = pl.ds(pl.multiple_of((2 * r + h) * part, part), part)
                mask[to, :] = value[:, h * (local // 2) : (h + 1) * (local // 2)]

        def spot_1(r, at, value):
            wb[pl.ds(pl.multiple_of(r * part, part), part), pl.ds(at, 1024)] = value

        def spot_q(r, at, value):
            abuf[pl.ds(pl.multiple_of(r * part, part), part), pl.ds(at, local)] = value

        weight_grad(
            lambda a: cbuf[:, a], sum_2, lambda at: act[:, pl.ds(at, 1024)],
            lambda at: wb[low, pl.ds(at, 1024)], spot_a, units, 1024)
        weight_grad(
            lambda a: cbuf[:, a], sum_d, lambda at: attn[...],
            lambda at: xbuf[:, pl.ds(chips * part, local)], spot_d, local, local)
        load_n = copy_of(n_out, wa.at[low, :])
        load_n.start()
        load_g1 = copy_of(g1_ref.at[low, :], wb.at[low, :])
        load_g1.start()
        for copy in cross_n:
            copy.wait_recv()
        load_nx = [copy_of(nx_out.at[r], xbuf.at[:, pl.ds(r * part, part)]) for r in range(chips)]
        for copy in load_nx:
            copy.start()
        cot.finish()
        for copy in cross_c + [cross_a]:
            copy.wait_send()
        bsum[...] = jnp.zeros_like(bsum)
        for k in range(units // local):
            bsum[k : k + 1, :] = fsum[0:1, k * local : (k + 1) * local]
        load_w = [copy_of(gq_ref.at[i], pb.at[pl.ds(0, width), pl.ds(i * local, local)]) for i in range(3)]

        @pl.loop(0, pairs)
        def _(h):
            lanes = pl.ds(pl.multiple_of(h * 128, 128), 128)

            def write(which, at, value):
                cbuf[at, pl.ds(pl.multiple_of(which * local + h * 128, 128), 128)] = value

            sums = attend_back_pair(
                qkv3[0, :, lanes], qkv3[1, :, lanes], qkv3[2, :, lanes],
                abuf[:, pl.ds(pl.multiple_of(local + h * 128, 128), 128)], abuf[:, lanes],
                lambda e, at: pb[at, prob_lanes(h, e)],
                (cos_ref, slo_ref, shi_ref), kacc, vacc, write)
            for k in range(3):
                bsum[units // local + k : units // local + k + 1, lanes] = sums[k]

            for k in range(3):

                @pl.when(h == k)
                def _():
                    load_w[k].start()

            @pl.when(h == 0)
            def _():
                sum_2.middle()

            @pl.when(h == 1)
            def _():
                outs.advance(2)

        back = cbuf.at[:, pl.ds(0, wide)]
        cross_d = to_twin(2 * chips + 2, back, gqx_out)
        cross_d.start()
        bias_tells = [
            remote(tells[r - 1], bsum, tell_b.at[r], (relative(me, r), line)) for r in range(1, dp)
        ]
        for copy in bias_tells:
            copy.start()
        for copy in load_w + [load_g1]:
            copy.wait()
        load_gx = [copy_of(gqx_out.at[:, pl.ds(i * local, local)], qkv3.at[i]) for i in range(3)]
        store_o = copy_of(x_buf, out_ref)
        load_px = [copy_of(gpx_out.at[:, piece(units, h)], cbuf.at[:, piece(units, h)]) for h in (0, 1)]
        spare = pb.at[pl.ds(width, rows), :]
        load_c = copy_of(c_ref, spare)

        def dense_step(i):
            @pl.when(i == chips - 2)
            def _():
                sum_d.middle()

        @pl.loop(0, tensor)
        def _(i):
            at = block(outward(i))

            @pl.loop(0, width, step=1024)
            def _(n):
                to = pl.ds(pl.multiple_of(n, 1024), 1024)
                value = dot_nt(slope[at, :], wb[to, :])
                value = value + dot_nt(cbuf[at, pl.ds(0, wide)], pb[to, pl.ds(0, wide)])
                act[at, to] = value.astype(bf16)

            for k in range(tensor - 1):

                @pl.when(i == k)
                def _():
                    ins.start(0, k)
                    ins.start(1, k)

            @pl.when(i == 0)
            def _():
                load_c.start()

            @pl.when(i == 1)
            def _():
                cross_d.wait_recv()
                for copy in load_gx:
                    copy.start()
                load_n.wait()
                for copy in load_nx + load_gx:
                    copy.wait()
                cross_t.wait_send()
                weight_grad(
                    lambda a: wa[low, a], sum_q, lambda at: cbuf[:, pl.ds(at, local)],
                    lambda at: qkv3[lax.div(at, local)], spot_q, wide, local, dense_step)

        cross_d.wait_send()
        cross_p.wait_recv()
        load_px[0].start()
        outs.settle()
        ins.advance(1)
        load_xa = copy_of(x_out, wb.at[high, :])
        load_px[0].wait()
        load_px[1].start()
        load_xa.start()

        def late_steps(i):
            @pl.when(i == 0)
            def _():
                sum_q.middle()

        weight_grad(
            lambda a: wa[low, a], sum_1, lambda at: slope[:, pl.ds(at, 1024)],
            lambda at: cbuf[:, pl.ds(at, 1024)], spot_1, units, 1024, late_steps, load_px[1])
        def finish_out():
            outs.arrive()

            @pl.loop(0, rows, step=32)
            def _(r):
                at = pl.ds(r, 32)
                own = pl.ds(pl.multiple_of(line * rows + r, 32), 32)
                total = x_buf[at, :].astype(f32) + outs.total(nv[own, :], at) + vec_buf[2:3, :]
                x_buf[at, :] = total.astype(bf16)

            store_o.start()

        parts[...] = jnp.zeros_like(parts)
        load_xa.wait()
        load_c.wait()

        def norm_sums(b):
            @pl.loop(0, rows, step=32)
            def _(r):
                some = pl.ds(pl.multiple_of(b * rows + r, 32), 32)
                x = wb[pl.ds(pl.multiple_of(tokens + b * rows + r, 32), 32), :].astype(f32)
                grad = act[some, :].astype(f32)
                centred = x - jnp.mean(x, -1, keepdims=True)
                inv_std = lax.rsqrt(jnp.mean(centred * centred, -1, keepdims=True) + layer_eps)
                parts[0:1, :] += jnp.sum(grad * (centred * inv_std), 0, keepdims=True)
                parts[1:2, :] += jnp.sum(grad, 0, keepdims=True)

        @pl.loop(0, tensor)
        def _(b):
            @pl.when(b == tensor - 1)
            def _():
                finish_out()
                ins.advance(2)

            norm_sums(b)

        @pl.loop(0, rows, step=32)
        def _(r):
            cotan = pb[pl.ds(pl.multiple_of(width + r, 32), 32), :].astype(f32)
            parts[2:3, :] += jnp.sum(cotan, 0, keepdims=True)

        vec_tells = [
            remote(tells[dp - 2 + r], parts.at[:, cols(relative(me, r))], tell_v.at[r],
                   (relative(me, r), line))
            for r in range(1, dp)
        ]
        for copy in vec_tells:
            copy.start()
        sum_1.middle()
        sum_2.final()
        sum_d.final()
        store_2 = copy_of(wa.at[pl.ds(tokens, part), :], s2_out)
        store_dense = [
            copy_of(mask.at[pl.ds(h * part, part), :], sd_out.at[:, piece(local, h)]) for h in (0, 1)
        ]
        for copy in [store_2] + store_dense:
            copy.start()
        store_o.wait()
        load_x = copy_of(x_ref, x_buf)
        load_x.start()
        for copy in bias_tells:
            copy.wait_recv()
        total_b = bsum[...]
        for r in range(1, dp):
            total_b = total_b + tell_b[r]
        bout_ref[...] = total_b
        for copy in vec_tells:
            copy.wait_recv()
        total_v = parts[:, cols(me)]
        for r in range(1, dp):
            total_v = total_v + tell_v[r]
        tell_z[0] = total_v
        line_tells = [
            remote(tells[2 * dp - 3 + k], tell_z.at[0], tell_z.at[k], (me, lax.rem(line + k, tensor)))
            for k in range(1, tensor)
        ]
        for copy in line_tells:
            copy.start()
        sum_q.final()
        store_q = copy_of(abuf.at[pl.ds(0, part), :], sq_out)
        store_q.start()
        load_x.wait()
        sum_1.final()
        store_1 = copy_of(wb.at[pl.ds(0, part), :], s1_out)
        store_1.start()
        ins.settle()
        ins.arrive()

        @pl.loop(0, rows, step=32)
        def _(r):
            at = pl.ds(r, 32)
            x = x_buf[at, :].astype(f32)
            centred = x - jnp.mean(x, -1, keepdims=True)
            inv_std = lax.rsqrt(jnp.mean(centred * centred, -1, keepdims=True) + layer_eps)
            unit = centred * inv_std
            own = pl.ds(pl.multiple_of(line * rows + r, 32), 32)
            scaled = ins.total(act[own, :], at) * vec_buf[0:1, :]
            cotan = pb[pl.ds(pl.multiple_of(width + r, 32), 32), :].astype(f32)
            first = jnp.mean(scaled, -1, keepdims=True)
            second = jnp.mean(scaled * unit, -1, keepdims=True)
            x_buf[at, :] = (cotan + inv_std * (scaled - first - unit * second)).astype(bf16)

        store_h = copy_of(x_buf, hid_ref)
        store_h.start()
        for copy in line_tells:
            copy.wait_recv()
        total_z = tell_z[0]
        for k in range(1, tensor):
            total_z = total_z + tell_z[k]
        vout_ref[...] = total_z
        for copy in vec + [cross_p] + bias_tells + vec_tells + line_tells:
            copy.wait_send()
        for plan in (qkv, fc1, fc2, sum_2, sum_d, sum_1, sum_q):
            plan.finish()
        for copy in store_dense + [store_2, store_q, store_h, store_1]:
            copy.wait()

    def shape(*dims):
        return jax.ShapeDtypeStruct(dims, bf16)

    def vmem(*dims):
        return pltpu.VMEM(dims, bf16)

    landings = [
        shape(2 * tensor - 3, rows, width),
        shape(2 * tensor - 3, rows, width),
        shape(6, part, units // 2),
        shape(6, part, local // 2),
        shape(6, part, units // 2),
        shape(6, part, wide // 2),
    ]
    return pl.pallas_call(
        kernel,
        out_shape=(
            shape(rows, width),
            shape(rows, width),
            shape(part, units),
            shape(part, local),
            shape(part, units),
            shape(part, wide),
            shape(3, width, local),
            shape(width, units),
            shape(units, width),
            shape(tokens, width),
            shape(tokens, width),
            shape(chips, tokens, part),
            shape(tokens, units),
            shape(tokens, wide),
            shape(tokens, units),
            *landings,
            jax.ShapeDtypeStruct((8, part), f32),
            jax.ShapeDtypeStruct((8, local), f32),
        ),
        in_specs=[ANY] * 6 + [VMEM] * 7,
        out_specs=(ANY,) * 21 + (VMEM,) * 2,
        scratch_shapes=[
            vmem(rows, width),
            pltpu.VMEM((8, width), f32),
            vmem(tokens, width),
            vmem(width, width),
            vmem(width, units),
            vmem(local, width),
            vmem(tokens, units),
            vmem(tokens, units),
            vmem(3, tokens, local),
            vmem(tokens, wide),
            vmem(stored, local // HD * BLOCK),
            vmem(stored, BLOCK),
            vmem(tokens, width),
            vmem(tokens, chips * part + local),
        ]
        + [pltpu.VMEM((tokens, 128), f32)] * 5
        + [
            vmem(tensor - 1, rows, width),
            vmem(2, part, units // 2),
            pltpu.VMEM((8, units), f32),
            pltpu.VMEM((8, local), f32),
            pltpu.VMEM((8, width), f32),
            pltpu.VMEM((dp, 8, part), f32),
            pltpu.VMEM((dp, 8, local), f32),
            pltpu.VMEM((tensor, 8, part), f32),
            pltpu.VMEM((8, part), f32),
            pltpu.SemaphoreType.DMA((sems.count,)),
            pltpu.SemaphoreType.DMA((sems.count,)),
            pltpu.SemaphoreType.DMA((48,)),
            pltpu.SemaphoreType.DMA((2,)),
        ],
        compiler_params=pltpu.CompilerParams(
            collective_id=0, has_side_effects=True, vmem_limit_bytes=67_043_328
        ),
        name="block",
    )(*arrays)


def finish_kernel(
    s2_ref, sd_ref, s1_ref, sq_ref, o_ref, h_ref, v_ref, b_ref,
    w2_ref, wd_ref, w1_ref, wq_ref, out_ref, hid_ref, gain_ref, beta_ref, both_ref, same_ref, bq_ref, b1_ref,
):
    w2_ref[...] = s2_ref[...].T.astype(f32)
    wd_ref[...] = sd_ref[...].T.astype(f32)
    w1_ref[...] = s1_ref[...].astype(f32)
    local = wq_ref.shape[2]
    for i in range(3):
        wq_ref[i] = sq_ref[:, i * local : (i + 1) * local].astype(f32)
    out_ref[...] = o_ref[...]
    hid_ref[...] = h_ref[...]

    @pl.when(pl.program_id(0) == 0)
    def _():
        line = lax.axis_index("tensor")
        count = gain_ref.shape[0]
        mine = v_ref[:, :count]
        for k in range(1, v_ref.shape[1] // count):
            mine = jnp.where(line == k, v_ref[:, k * count : (k + 1) * count], mine)
        gain_ref[...] = mine[0]
        beta_ref[...] = mine[1]
        both_ref[...] = mine[2]
        same_ref[...] = mine[2]
        lines = b1_ref.shape[0] // b_ref.shape[1]
        bq_ref[...] = b_ref[lines : lines + 3, :]
        for k in range(lines):
            b1_ref[pl.ds(k * b_ref.shape[1], b_ref.shape[1])] = b_ref[k]


def finish(tensor, sent_fc2, sent_dense, sent_fc1, sent_qkv, out, hidden_grad, vec_sums, all_sums):
    part, units = sent_fc2.shape
    local = sent_dense.shape[1]
    rows, width = out.shape
    steps = 4
    quarter = vec_sums.shape[1] // tensor
    fixed = VMEM

    def down(n, m):
        return pl.BlockSpec((n // steps, m), lambda i: (i, 0))

    def across(n, m):
        return pl.BlockSpec((n, m // steps), lambda i: (0, i))

    return pl.pallas_call(
        finish_kernel,
        grid=(steps,),
        out_shape=(
            jax.ShapeDtypeStruct((units, part), f32),
            jax.ShapeDtypeStruct((local, part), f32),
            jax.ShapeDtypeStruct((part, units), f32),
            jax.ShapeDtypeStruct((3, part, local), f32),
            jax.ShapeDtypeStruct((rows, width), bf16),
            jax.ShapeDtypeStruct((rows, width), bf16),
            *[jax.ShapeDtypeStruct((quarter,), f32)] * 4,
            jax.ShapeDtypeStruct((3, local), f32),
            jax.ShapeDtypeStruct((units,), f32),
        ),
        in_specs=[
            across(part, units), across(part, local), down(part, units), down(part, 3 * local),
            down(rows, width), down(rows, width), fixed, fixed,
        ],
        out_specs=(
            down(units, part), down(local, part), down(part, units),
            pl.BlockSpec((3, part // steps, local), lambda i: (0, i, 0)),
            down(rows, width), down(rows, width), *[fixed] * 6,
        ),
        compiler_params=pltpu.CompilerParams(vmem_limit_bytes=VMEM_LIMIT),
        name="finish",
    )(sent_fc2, sent_dense, sent_fc1, sent_qkv, out, hidden_grad, vec_sums, all_sums)


def rotary_tables(segments):
    rows, length = segments.shape
    index = jnp.arange(length, dtype=jnp.int32)[None]
    start = jnp.zeros_like(segments)
    for number in range(1, 4):
        start = jnp.where(segments == number, jnp.sum(segments < number, -1, keepdims=True), start)
    position = (index - start).astype(f32).reshape(rows * length, 1)
    lane = jnp.arange(128, dtype=jnp.int32) % HD
    exponent = (2 * (lane % (ROT // 2))).astype(f32) / ROT
    angle = position * (1.0 / 10000.0**exponent)[None]
    cosine, sine = jnp.cos(angle), jnp.sin(angle)
    low, high = lane < ROT // 2, (lane >= ROT // 2) & (lane < ROT)
    return (
        jnp.where(lane < ROT, cosine, 1.0),
        jnp.where(low, -sine, 0.0),
        jnp.where(high, sine, 0.0),
    )


def matmul(a, b):
    return jnp.dot(a, b, preferred_element_type=f32)


def on_device(
    dp, tensor, fast,
    hidden_in, segments, ln_gain, ln_bias, qkv_weight, qkv_bias, dense_weight, dense_bias,
    fc1_weight, fc1_bias, fc2_weight, fc2_bias, cotangent,
):
    seqs = segments.shape[0]
    local = qkv_weight.shape[2]
    mine = (
        hidden_in, cotangent, qkv_weight.transpose(1, 0, 2), dense_weight, fc1_weight, fc2_weight,
    )
    if fast:
        (out, hidden_grad, sent_fc2, sent_dense, sent_fc1, sent_qkv, *_, vec_sums, all_sums) = block_call(
            dp, tensor, (*mine, ln_gain, ln_bias, dense_bias, fc2_bias, qkv_bias, fc1_bias, segments))
        (
            grad_w2, grad_wd, grad_w1, grad_wq, out, hidden_grad,
            gain_grad, beta_grad, bias_grad, same_grad, qkv_grad, fc1_grad,
        ) = finish(
            tensor, sent_fc2, sent_dense, sent_fc1, sent_qkv, out, hidden_grad, vec_sums, all_sums)
        return (
            out,
            hidden_grad,
            gain_grad,
            beta_grad,
            grad_wq.transpose(1, 0, 2),
            qkv_grad,
            grad_wd,
            bias_grad,
            grad_w1,
            fc1_grad,
            grad_w2,
            same_grad,
        )

    number = lax.broadcasted_iota(jnp.int32, (8, ln_gain.shape[0]), 0)
    vectors = jnp.where(number == 1, ln_bias.astype(f32)[None], ln_gain.astype(f32)[None])
    vectors = jnp.where(
        number == 2, dense_bias.astype(f32)[None] + fc2_bias.astype(f32)[None], vectors)
    tables = rotary_tables(segments)
    bias = jnp.pad(qkv_bias.astype(f32), ((0, 5), (0, 0)))
    w_qkv, w_dense, w_fc1, w_fc2, normed, grad_out, vec = gather_plain(*mine, vectors)
    gain, out_bias = vec[0:1], vec[2:3]
    query, key, value, attn_vec, probs = attend(
        *(matmul(normed, w_qkv[i]) for i in range(3)), bias, tables, segments, seqs
    )
    pre_act = matmul(normed, w_fc1) + fc1_bias.astype(f32)
    act_vals, gelu_pull = jax.vjp(lambda pre: jax.nn.gelu(pre, approximate=True), pre_act)
    act_vals = act_vals.astype(bf16)
    slope = gelu_pull(jnp.ones_like(pre_act))[0].astype(bf16)
    branches = matmul(attn_vec, w_dense) + matmul(act_vals, w_fc2)
    grad_attn = matmul(grad_out, w_dense.T).astype(bf16)
    *grads, qkv_sums = attend_back(query, key, value, grad_attn, attn_vec, probs, tables, seqs)
    resid_in = hidden_in.astype(f32)
    cot_float = cotangent.astype(f32)
    centred = resid_in - jnp.mean(resid_in, -1, keepdims=True)
    spread = jnp.mean(centred * centred, -1, keepdims=True)
    inv_std = lax.rsqrt(spread + layer_eps)
    unit_rows = centred * inv_std
    summed = lax.psum_scatter(branches.astype(bf16), "tensor", scatter_dimension=0, tiled=True)
    out = (resid_in + summed.astype(f32) + out_bias).astype(bf16)
    out_bias_part = jnp.sum(cot_float, 0)
    grad_fc2 = matmul(act_vals.T, grad_out)
    grad_dense = matmul(attn_vec.T, grad_out)
    grad_pre = (matmul(grad_out, w_fc2.T) * slope.astype(f32)).astype(bf16)
    fc1_bias_part = jnp.sum(grad_pre.astype(f32), 0)
    grad_fc1 = matmul(normed.T, grad_pre)
    grad_wqkv = jnp.stack([matmul(normed.T, g) for g in grads])
    grad_normed = matmul(grad_pre, w_fc1.T) + sum(matmul(g, w.T) for g, w in zip(grads, w_qkv))
    sent_qkv, sent_dense, sent_fc1, sent_fc2 = (
        lax.psum_scatter(grad_wqkv.astype(bf16), "dp", scatter_dimension=1, tiled=True),
        lax.psum_scatter(grad_dense.astype(bf16), "dp", scatter_dimension=1, tiled=True),
        lax.psum_scatter(grad_fc1.astype(bf16), "dp", scatter_dimension=0, tiled=True),
        lax.psum_scatter(grad_fc2.astype(bf16), "dp", scatter_dimension=1, tiled=True),
    )
    grad_local = lax.psum_scatter(
        grad_normed.astype(bf16), "tensor", scatter_dimension=0, tiled=True
    ).astype(f32)
    gain_part = jnp.sum(grad_local * unit_rows, 0)
    beta_part = jnp.sum(grad_local, 0)
    scaled_grad = grad_local * gain
    first_mean = jnp.mean(scaled_grad, -1, keepdims=True)
    second_mean = jnp.mean(scaled_grad * unit_rows, -1, keepdims=True)
    hidden_grad = (
        cot_float + inv_std * (scaled_grad - first_mean - unit_rows * second_mean)
    ).astype(bf16)
    gain_grad, beta_grad, out_bias_grad = (
        lax.psum_scatter(gain_part, ("dp", "tensor"), scatter_dimension=0, tiled=True),
        lax.psum_scatter(beta_part, ("dp", "tensor"), scatter_dimension=0, tiled=True),
        lax.psum_scatter(out_bias_part, ("dp", "tensor"), scatter_dimension=0, tiled=True),
    )
    qkv_bias_grad, fc1_bias_grad = lax.psum((qkv_sums[:3], fc1_bias_part), "dp")
    return (
        out,
        hidden_grad,
        gain_grad,
        beta_grad,
        sent_qkv.transpose(1, 0, 2).astype(f32),
        qkv_bias_grad,
        sent_dense.astype(f32),
        out_bias_grad,
        sent_fc1.astype(f32),
        fc1_bias_grad,
        sent_fc2.astype(f32),
        out_bias_grad,
    )


def solution(mesh):
    dp, tensor = mesh.shape["dp"], mesh.shape["tensor"]
    fast = dp == 8 and tensor == 4
    placed = (
        P(("dp", "tensor"), None),
        P("dp", None),
        P("dp"),
        P("dp"),
        P("dp", None, "tensor"),
        P(None, "tensor"),
        P("tensor", "dp"),
        P("dp"),
        P("dp", "tensor"),
        P("tensor"),
        P("tensor", "dp"),
        P("dp"),
        P(("dp", "tensor"), None),
    )
    return jax.shard_map(
        functools.partial(on_device, dp, tensor, fast),
        mesh=mesh,
        in_specs=placed,
        out_specs=(
            P(("dp", "tensor"), None),
            P(("dp", "tensor"), None),
            P(("dp", "tensor")),
            P(("dp", "tensor")),
            P("dp", None, "tensor"),
            P(None, "tensor"),
            P("tensor", "dp"),
            P(("dp", "tensor")),
            P("dp", "tensor"),
            P("tensor"),
            P("tensor", "dp"),
            P(("dp", "tensor")),
        ),
        check_vma=False,
    )
```
